32 devices in a mesh: fsdp: 8 (over z, y), context: 2 (over x), tensor: 2 (over core).
Axes of the slice: x: 2, y: 2, z: 4, core: 2. Of those that a mesh axis runs over, the one named last changes fastest.
Arguments:
- tokens: bfloat16 [4096, 2048], P(('fsdp', 'context')), may hold values from -6 to 6
- cont_lengths: int32 [8, 4], P('fsdp'), may hold values from 1 to 128, 256 in all within a row
- w_query: bfloat16 [2048, 2048], P('fsdp', 'tensor'), may hold values from -0.125 to 0.125
- w_key: bfloat16 [2048, 2048], P('fsdp', 'tensor'), may hold values from -0.125 to 0.125
- w_value: bfloat16 [2048, 2048], P('fsdp', 'tensor'), may hold values from -0.125 to 0.125
- w_output: bfloat16 [2048, 2048], P('tensor', 'fsdp'), may hold values from -0.125 to 0.125
- query_gain: bfloat16 [16, 128], P('tensor', 'fsdp'), may hold values from 0.099609375 to 1.8984375
- key_gain: bfloat16 [16, 128], P('tensor', 'fsdp'), may hold values from 0.099609375 to 1.8984375
- attn_gain: bfloat16 [2048], P('fsdp'), may hold values from 0.099609375 to 1.8984375
- w_gate: bfloat16 [2048, 8192], P('fsdp', 'tensor'), may hold values from -0.125 to 0.125
- w_up: bfloat16 [2048, 8192], P('fsdp', 'tensor'), may hold values from -0.125 to 0.125
- w_down: bfloat16 [8192, 2048], P('tensor', 'fsdp'), may hold values from -0.0625 to 0.0625
- mlp_gain: bfloat16 [2048], P('fsdp'), may hold values from 0.099609375 to 1.8984375
- cotangent: bfloat16 [4096, 2048], P(('fsdp', 'context')), may hold values from -6 to 6
Outputs:
- outputs: bfloat16 [4096, 2048], P(('fsdp', 'context'))
- input_grad: float32 [4096, 2048], P(('fsdp', 'context'))
- grad_query: float32 [2048, 2048], P('fsdp', 'tensor')
- grad_key: float32 [2048, 2048], P('fsdp', 'tensor')
- grad_value: float32 [2048, 2048], P('fsdp', 'tensor')
- grad_output: float32 [2048, 2048], P('tensor', 'fsdp')
- grad_query_gain: float32 [16, 128], P('tensor', 'fsdp')
- grad_key_gain: float32 [16, 128], P('tensor', 'fsdp')
- grad_attn_gain: float32 [2048], P('fsdp')
- grad_gate: float32 [2048, 8192], P('fsdp', 'tensor')
- grad_up: float32 [2048, 8192], P('fsdp', 'tensor')
- grad_down: float32 [8192, 2048], P('tensor', 'fsdp')
- grad_mlp_gain: float32 [2048], P('fsdp')
The draws below stay inside these ranges and needn't reach their ends.
Inputs may be any that keep to these rules, and one draw needn't show every extreme that they name: `cont_lengths`: a group's 4 lengths sum to 256; in every group the longest is exactly 128.
All inputs are finite; a program needn't handle non-finite values.
Results may differ from the reference program's by a relative error of at most 0.017.
Values may be sent and summed in bfloat16 or wider, within the bound.
A program may use at most 320 MiB of HBM per device.

```python
import math
import jax
import jax.numpy as jnp
import numpy as np
from jax import lax

D = 2048
HEADS = 16
HD = 128
FF = 8192
ROWS = 256
CONTS = 4
CONT_MOST = 128
GROUPS = 8
TOKENS = 4096


def levels(stream_key, dims, cuts, smallest, top_value):
    loudness = 1.0
    for position, shards_of in cuts:
        heights = jax.random.uniform(jax.random.fold_in(jax.random.fold_in(stream_key, 6), position), (shards_of,), jnp.float32, smallest / len(cuts), top_value / len(cuts))
        loudness = loudness * jnp.repeat(jnp.exp(heights), dims[position] // shards_of).reshape((-1,) + (1,) * (len(dims) - 1 - position))
    return loudness


def split_up(number_of, total, limit, lean):
    loads = [(1 << 20) // math.isqrt(grade ** lean) + 1 for grade in range(2, number_of + 1)]
    spare, holding = total - limit - (number_of - 1), [1] * (number_of - 1)
    while spare > 0:
        candidates = [i for i in range(number_of - 1) if holding[i] < limit]
        whole, remaining = sum([loads[i] for i in candidates]), spare
        for i in candidates:
            more = min(limit - holding[i], max(1, remaining * loads[i] // whole), spare)
            holding[i] = holding[i] + more
            spare = spare - more
    return np.array([limit] + holding)


def ragged(rng, count, total, reach, slope):
    if count == 2:
        one = jax.random.randint(rng, (), max(1, total - reach), min(reach, total - 1) + 1)
        return jnp.stack([one, total - one])
    sizes = jnp.asarray(split_up(count, total, reach, slope), jnp.int32)
    pairs = (count - 1) // 2
    source_of, receiver = sizes[1:1 + 2 * pairs:2], sizes[2:2 + 2 * pairs:2]
    room = jnp.minimum(source_of - 1, reach - receiver)
    shifted = jax.random.randint(jax.random.fold_in(rng, 1), (pairs,), 0, 1 << 20) % (room + 1)
    sizes = sizes.at[1:1 + 2 * pairs:2].set(source_of - shifted).at[2:2 + 2 * pairs:2].set(receiver + shifted)
    return sizes[jax.random.permutation(jax.random.fold_in(rng, 2), count)]


def centred(rng, extent, spread, limit, pieces=(), kind=jnp.bfloat16):
    array = jax.random.normal(rng, extent, jnp.float32) * spread
    if len(pieces) > 0:
        array = levels(rng, extent, pieces, -0.22, 0.18) * array
    return jnp.clip(array, min=-limit, max=limit).astype(kind)


def setup_inputs(seed: int = 0) -> dict:
    splits = jax.random.split(jax.random.key(seed), 15)
    tokens = centred(splits[0], (TOKENS, D), 1.0, 6.0, ((0, 16),))
    cont_lengths = jax.vmap(lambda own: ragged(own, CONTS, ROWS, CONT_MOST, 2))(jax.random.split(splits[1], GROUPS)).reshape((GROUPS, CONTS)).astype(jnp.int32)
    w_query = centred(splits[2], (D, D), D ** -0.5, 0.125, ((0, 8), (1, 2)))
    w_key = centred(splits[3], (D, D), D ** -0.5, 0.125, ((0, 8), (1, 2)))
    w_value = centred(splits[4], (D, D), D ** -0.5, 0.125, ((0, 8), (1, 2)))
    w_output = centred(splits[5], (D, D), D ** -0.5, 0.125, ((0, 2), (1, 8)))
    query_gain = jnp.clip(1.0 + 0.18 * jax.random.normal(splits[6], (HEADS, HD), jnp.float32), 0.099609375, 1.8984375).astype(jnp.bfloat16)
    key_gain = jnp.clip(1.0 + 0.18 * jax.random.normal(splits[7], (HEADS, HD), jnp.float32), 0.099609375, 1.8984375).astype(jnp.bfloat16)
    attn_gain = jnp.clip(1.0 + 0.18 * jax.random.normal(splits[8], (D,), jnp.float32), 0.099609375, 1.8984375).astype(jnp.bfloat16)
    w_gate = centred(splits[9], (D, FF), D ** -0.5, 0.125, ((0, 8), (1, 2)))
    w_up = centred(splits[10], (D, FF), D ** -0.5, 0.125, ((0, 8), (1, 2)))
    w_down = centred(splits[11], (FF, D), FF ** -0.5, 0.0625, ((0, 2), (1, 8)))
    mlp_gain = jnp.clip(1.0 + 0.18 * jax.random.normal(splits[12], (D,), jnp.float32), 0.099609375, 1.8984375).astype(jnp.bfloat16)
    cotangent = centred(splits[13], (TOKENS, D), 1.0, 6.0, ((0, 16),))
    return dict(tokens=tokens, cont_lengths=cont_lengths, w_query=w_query, w_key=w_key, w_value=w_value, w_output=w_output, query_gain=query_gain, key_gain=key_gain, attn_gain=attn_gain, w_gate=w_gate, w_up=w_up, w_down=w_down, mlp_gain=mlp_gain, cotangent=cotangent)


@jax.custom_vjp
def low(v):
    return lax.optimization_barrier(v.astype(jnp.bfloat16)).astype(jnp.float32)

@jax.custom_vjp
def low_back(v):
    return v

def low_keep(v):
    return (low(v), None)

def low_pass(kept, grad):
    return (grad,)

def back_keep(v):
    return (v, None)

def back_low(kept, grad):
    return (low(grad),)
low.defvjp(low_keep, low_pass)
low_back.defvjp(back_keep, back_low)
EPS = 1e-06
THETA = 500000.0

def matmul(left, right):
    return jnp.dot(left, right, precision=lax.Precision.HIGHEST)

def rms_norm(values, gain):
    return values * lax.rsqrt(lax.optimization_barrier(jnp.mean(values * values, axis=-1, keepdims=True)) + EPS) * gain

def rotary_tables(positions, head_size):
    half = head_size // 2
    inverse = jnp.exp(-(2.0 * jnp.arange(half, dtype=jnp.float32) / head_size) * math.log(THETA))
    angles = positions.astype(jnp.float32)[:, None] * inverse[None, :]
    angles = jnp.concatenate([angles, angles], axis=1)
    return (jnp.cos(angles), jnp.sin(angles))

def rotate(values, cosine, sine):
    half = values.shape[-1] // 2
    turned = jnp.concatenate([-values[..., half:], values[..., :half]], axis=-1)
    return values * cosine[:, None, :] + turned * sine[:, None, :]

def layout(lengths, rows):
    segment_ends = jnp.cumsum(lengths).astype(jnp.int32)
    segment_starts = (segment_ends - lengths).astype(jnp.int32)
    row_index = jnp.arange(rows, dtype=jnp.int32)
    segment = lax.optimization_barrier(jnp.sum((row_index[:, None] >= segment_ends[None, :]).astype(jnp.int32), axis=1)).astype(jnp.int32)
    chosen = segment[:, None] == jnp.arange(lengths.shape[0], dtype=jnp.int32)[None, :]
    offset = (row_index - lax.optimization_barrier(jnp.sum(jnp.where(chosen, segment_starts[None, :], 0), axis=1))).astype(jnp.int32)
    return (segment, offset)

def group_layout(lengths):
    segment, offset = layout(lengths, ROWS)
    positions = jnp.concatenate([jnp.arange(ROWS, dtype=jnp.int32), (ROWS + offset).astype(jnp.int32)])
    segments = jnp.concatenate([jnp.full((ROWS,), -1, jnp.int32), segment])
    return (segments, positions)

def group_forward(inputs, segments, positions, weights):
    w_query, w_key, w_value, w_output, query_gain, key_gain, attn_gain, w_gate, w_up, w_down, mlp_gain = weights
    length = inputs.shape[0]
    query_raw = low_back(matmul(inputs, w_query))
    key_raw = low_back(matmul(inputs, w_key))
    value_low = low(low_back(matmul(inputs, w_value)))
    query_norm = rms_norm(query_raw, query_gain.reshape(-1))
    key_norm = rms_norm(key_raw, key_gain.reshape(-1))
    cosine, sine = rotary_tables(positions, HD)
    query_rot = low(rotate(query_norm.reshape(length, HEADS, HD), cosine, sine))
    key_rot = low(rotate(key_norm.reshape(length, HEADS, HD), cosine, sine))
    values = value_low.reshape(length, HEADS, HD)
    scores = low_back(jnp.einsum('qhd,khd->hqk', query_rot, key_rot, precision=lax.Precision.HIGHEST) * (1.0 / math.sqrt(HD)))
    index = jnp.arange(length, dtype=jnp.int32)
    allowed = (index[None, :] <= index[:, None]) & ((index[None, :] < ROWS) | (segments[None, :] == segments[:, None]))
    scores = jnp.where(allowed[None], scores, -1e+30)
    probs = low(jax.nn.softmax(scores, axis=-1))
    attended = low(low_back(jnp.einsum('hqk,khd->qhd', probs, values, precision=lax.Precision.HIGHEST))).reshape(length, D)
    attn_branch = low_back(matmul(attended, w_output))
    hidden = inputs + rms_norm(attn_branch, attn_gain)
    hidden_low = low(hidden)
    gate = low_back(matmul(hidden_low, w_gate))
    upward = low_back(matmul(hidden_low, w_up))
    inner = low(jax.nn.silu(gate) * upward)
    mlp_branch = low_back(matmul(inner, w_down))
    return hidden + rms_norm(mlp_branch, mlp_gain)

def reference(tokens, cont_lengths, w_query, w_key, w_value, w_output, query_gain, key_gain, attn_gain, w_gate, w_up, w_down, mlp_gain, cotangent):
    floats = tuple((weight.astype(jnp.float32) for weight in (w_query, w_key, w_value, w_output, query_gain, key_gain, attn_gain, w_gate, w_up, w_down, mlp_gain)))
    inputs = tokens.astype(jnp.float32).reshape(GROUPS, 2 * ROWS, D)
    segments, positions = lax.map(group_layout, cont_lengths)

    def forward(inputs, weights):

        def one_group(packed):
            return group_forward(packed[0], packed[1], packed[2], weights)
        return lax.map(jax.checkpoint(one_group), (inputs, segments, positions))
    results, pullback = jax.vjp(forward, inputs, floats)
    grad_inputs, grad_weights = pullback(cotangent.astype(jnp.float32).reshape(GROUPS, 2 * ROWS, D))
    return (results.reshape(TOKENS, D).astype(jnp.bfloat16), grad_inputs.reshape(TOKENS, D), grad_weights[0], grad_weights[1], grad_weights[2], grad_weights[3], grad_weights[4], grad_weights[5], grad_weights[6], grad_weights[7], grad_weights[8], grad_weights[9], grad_weights[10])
```

```python
import functools
import math

import jax
import jax.numpy as jnp
from jax import lax
from jax.experimental import pallas as pl
from jax.experimental.pallas import tpu as pltpu
from jax.sharding import PartitionSpec as P

EPS = 1e-06
THETA = 500000.0
BF = jnp.bfloat16
F32 = jnp.float32


def product(left, right):
    return jnp.dot(left, right, preferred_element_type=F32)


def product_left(left, right):
    return jnp.einsum("rd,rf->df", left, right, preferred_element_type=F32)


def product_right(left, right):
    return jnp.einsum("rf,df->rd", left, right, preferred_element_type=F32)


def rotary_tables(positions, head_size):
    half = head_size // 2
    inverse = jnp.exp(-(2.0 * jnp.arange(half, dtype=F32) / head_size) * math.log(THETA))
    angles = positions.astype(F32)[..., None] * inverse
    angles = jnp.concatenate([angles, angles], axis=-1)
    return (jnp.cos(angles), jnp.sin(angles))


def rotate(values, cosine, sine):
    half = values.shape[-1] // 2
    turned = jnp.concatenate([-values[..., half:], values[..., :half]], axis=-1)
    return values * cosine + turned * sine


def rotate_back(grads, cosine, sine):
    half = grads.shape[-1] // 2
    scaled = grads * sine
    turned = jnp.concatenate([scaled[..., half:], -scaled[..., :half]], axis=-1)
    return grads * cosine + turned


def norm_back(values, scale, gain, grads, total, width):
    return scale * gain * grads - values * scale * scale * scale * (total / width)


def layout(lengths, rows):
    segment_ends = jnp.cumsum(lengths)
    segment_starts = segment_ends - lengths
    row_index = jnp.arange(rows, dtype=jnp.int32)
    segment = jnp.sum((row_index[:, None] >= segment_ends[None, :]).astype(jnp.int32), axis=1)
    chosen = segment[:, None] == jnp.arange(lengths.shape[0], dtype=jnp.int32)[None, :]
    offset = row_index - jnp.sum(jnp.where(chosen, segment_starts[None, :], 0), axis=1)
    return (segment, offset)


LINE = 4
CHUNK = 16
MESH_ID = pl.DeviceIdType.MESH
HBM = pl.BlockSpec(memory_space=pl.ANY)
VMEM = pl.BlockSpec(memory_space=pltpu.VMEM)
DMA = pltpu.SemaphoreType.DMA


class Place:
    def __init__(self):
        device = lax.axis_index("fsdp")
        member = lax.rem(device, 2 * LINE)
        self.base = device - member
        self.z = member // 2
        self.y = lax.rem(member, 2)
        self.core = lax.axis_index("tensor")

    def at(self, z, y, core):
        return {"fsdp": self.base + 2 * z + y, "tensor": core}

    def near(self):
        yield None, self.at(self.z, self.y, 1 - self.core)
        yield None, self.at(self.z, 1 - self.y, self.core)
        yield self.z > 0, self.at(self.z - 1, self.y, self.core)
        yield self.z < LINE - 1, self.at(self.z + 1, self.y, self.core)

    def rows(self, z, y, core, count):
        start = ((2 * z + y) * 2 + core) * count
        return pl.ds(pl.multiple_of(start, count), count)


def guarded(condition, action):
    if condition is None:
        action()
    else:
        pl.when(condition)(action)


def greet(place):
    barrier = pltpu.get_barrier_semaphore()
    for condition, device in place.near():

        def signal(device=device):
            pl.semaphore_signal(barrier, inc=1, device_id=device, device_id_type=MESH_ID)

        guarded(condition, signal)
    inside = (place.z > 0) & (place.z < LINE - 1)
    pl.semaphore_wait(barrier, jnp.where(inside, 4, 3))


class Sender:
    def __init__(self):
        self.sent = []

    def __call__(self, condition, make):
        def start():
            make().start()

        guarded(condition, start)
        self.sent.append((condition, make))

    def drain(self):
        for condition, make in self.sent:

            def wait(make=make):
                make().wait_send()

            guarded(condition, wait)


def remote(source, target, send, receive, device):
    return pltpu.make_async_remote_copy(
        src_ref=source,
        dst_ref=target,
        send_sem=send,
        recv_sem=receive,
        device_id=device,
        device_id_type=MESH_ID,
    )


def by_rows(rows, body):
    def step(index, carry):
        body(pl.ds(pl.multiple_of(index * CHUNK, CHUNK), CHUNK))
        return carry

    lax.fori_loop(0, rows // CHUNK, step, 0)


def reduce_scratch(rows, width):
    return [
        pltpu.VMEM((2 * LINE, rows, width), BF),
        pltpu.VMEM((2 * LINE, rows, width), BF),
        pltpu.VMEM((LINE, rows, width), BF),
        pltpu.VMEM((LINE + 1, rows, width), BF),
        pltpu.VMEM((rows, width), F32),
        DMA((2 * LINE,)),
        DMA((2, 2 * LINE)),
        DMA((2, LINE)),
        DMA((2, LINE + 1)),
    ]


def reduce_phase(place, sender, partial, scratch):
    mine, core_in, y_in, line_in, total, local_sem, core_sem, y_sem, line_sem = scratch
    rows = total.shape[0]
    z, y, core = place.z, place.y, place.core
    low = z < LINE // 2
    order = []
    for k in range(LINE - 1):
        down = LINE - 1 - k
        down = jnp.where(down <= z, down - 1, down)
        up = jnp.where(k >= z, k + 1, k)
        order.append(jnp.where(low, down, up))
    order.append(z)

    def fetch(slot):
        half = lax.rem(slot, 2)
        return pltpu.make_async_copy(
            partial.at[place.rows(slot // 2, half, core, rows)], mine.at[slot], local_sem.at[slot]
        )

    def to_core(slot):
        half = lax.rem(slot, 2)
        return remote(
            partial.at[place.rows(slot // 2, half, 1 - core, rows)],
            core_in.at[slot],
            core_sem.at[0, slot],
            core_sem.at[1, slot],
            place.at(z, y, 1 - core),
        )

    def to_y(block):
        return remote(
            mine.at[2 * block + 1 - y],
            y_in.at[block],
            y_sem.at[0, block],
            y_sem.at[1, block],
            place.at(z, 1 - y, core),
        )

    def to_line(block):
        step = jnp.where(block > z, 1, -1)
        slot = jnp.where((step < 0) & (block == z - 1), LINE, block)
        return remote(
            mine.at[2 * block + y],
            line_in.at[slot],
            line_sem.at[0, block],
            line_sem.at[1, slot],
            place.at(z + step, y, core),
        )

    def from_line(slot):
        return remote(
            mine.at[0],
            line_in.at[slot],
            line_sem.at[0, 0],
            line_sem.at[1, slot],
            place.at(z, y, 1 - core),
        )

    for half in (1 - y, y):
        for block in order:
            sender(None, functools.partial(to_core, 2 * block + half))
            fetch(2 * block + half).start()

    for block in order:
        slot = 2 * block + 1 - y
        fetch(slot).wait()
        to_core(slot).wait_recv()

        def add(at, slot=slot):
            value = mine[slot, at].astype(F32) + core_in[slot, at].astype(F32)
            mine[slot, at] = value.astype(BF)

        by_rows(rows, add)
        sender(None, functools.partial(to_y, block))

    for block in order[:-1]:
        slot = 2 * block + y
        fetch(slot).wait()
        to_core(slot).wait_recv()
        to_y(block).wait_recv()
        inner = jnp.where(block > z, z > 0, z < LINE - 1)

        @pl.when(inner)
        def _(block=block, slot=slot):
            from_line(block).wait_recv()

            def add(at):
                value = mine[slot, at].astype(F32) + core_in[slot, at].astype(F32)
                value = value + y_in[block, at].astype(F32)
                mine[slot, at] = (value + line_in[block, at].astype(F32)).astype(BF)

            by_rows(rows, add)

        @pl.when(jnp.logical_not(inner))
        def _(block=block, slot=slot):
            def add(at):
                value = mine[slot, at].astype(F32) + core_in[slot, at].astype(F32)
                mine[slot, at] = (value + y_in[block, at].astype(F32)).astype(BF)

            by_rows(rows, add)

        sender(None, functools.partial(to_line, block))

    slot = 2 * z + y
    fetch(slot).wait()
    to_core(slot).wait_recv()
    to_y(z).wait_recv()

    def start(at):
        value = mine[slot, at].astype(F32) + core_in[slot, at].astype(F32)
        total[at] = value + y_in[z, at].astype(F32)

    by_rows(rows, start)
    for condition, source in ((z > 0, z), (z < LINE - 1, LINE)):

        @pl.when(condition)
        def _(source=source):
            from_line(source).wait_recv()

            def add(at):
                total[at] += line_in[source, at].astype(F32)

            by_rows(rows, add)


def gather_scratch(rows, width):
    return [
        pltpu.VMEM((rows, width), BF),
        DMA((1,)),
        DMA((2, 2 * LINE)),
        DMA((2, LINE)),
        DMA((2, LINE + 2)),
    ]


def gather_phase(place, sender, gathered, scratch):
    own, local_sem, core_sem, y_sem, line_sem = scratch
    rows = own.shape[0]
    z, y, core = place.z, place.y, place.core

    def spot(block, half):
        return gathered.at[place.rows(block, half, core, rows)]

    def to_core(source, block, half):
        return remote(
            source,
            spot(block, half),
            core_sem.at[0, 2 * block + half],
            core_sem.at[1, 2 * block + half],
            place.at(z, y, 1 - core),
        )

    def to_y(source, block):
        return remote(
            source,
            spot(block, y),
            y_sem.at[0, block],
            y_sem.at[1, block],
            place.at(z, 1 - y, core),
        )

    def to_line(source, block, step, index):
        return remote(
            source,
            spot(block, y),
            line_sem.at[0, index],
            line_sem.at[1, block],
            place.at(z + step, y, core),
        )

    keep = pltpu.make_async_copy(own, spot(z, y), local_sem.at[0])
    keep.start()
    sender(z < LINE - 1, functools.partial(to_line, own, z, 1, LINE))
    sender(z > 0, functools.partial(to_line, own, z, -1, LINE + 1))
    sender(None, functools.partial(to_y, own, z))
    sender(None, functools.partial(to_core, own, z, y))

    def took_y(block):
        remote(
            own,
            spot(block, 1 - y),
            y_sem.at[0, block],
            y_sem.at[1, block],
            place.at(z, 1 - y, core),
        ).wait_recv()

    def across(condition, block):
        guarded(condition, functools.partial(took_y, block))
        sender(condition, lambda: to_core(spot(block, 1 - y), block, 1 - y))

    def along(condition, block, step):
        def took():
            to_line(own, block, step, block).wait_recv()

        guarded(condition, took)
        onward = condition & ((z < LINE - 1) if step > 0 else (z > 0))
        sender(onward, lambda: to_line(spot(block, y), block, step, block))
        sender(condition, lambda: to_y(spot(block, y), block))
        sender(condition, lambda: to_core(spot(block, y), block, y))

    for distance in range(1, LINE + 1):
        if distance < LINE:
            along(z >= distance, z - distance, 1)
            along(z + distance < LINE, z + distance, -1)
        if distance == 1:
            across(None, z)
        else:
            across(z >= distance - 1, z - distance + 1)
            across(z + distance - 1 < LINE, z + distance - 1)

    keep.wait()
    for block in range(LINE):
        for half in range(2):
            remote(
                own,
                gathered.at[place.rows(block, half, 1 - core, rows)],
                core_sem.at[0, 2 * block + half],
                core_sem.at[1, 2 * block + half],
                place.at(z, y, 1 - core),
            ).wait_recv()


def pair_scratch():
    return [DMA((3,))]


def pair_phase(place, sender, own, pair, scratch):
    (sem,) = scratch
    rows = own.shape[0]
    spot = pair.at[pl.ds(pl.multiple_of(place.core * rows, rows), rows)]
    keep = pltpu.make_async_copy(own, spot, sem.at[0])
    keep.start()

    def send():
        return remote(
            own, spot, sem.at[1], sem.at[2], place.at(place.z, place.y, 1 - place.core)
        )

    sender(None, send)

    def finish():
        keep.wait()
        other = pair.at[pl.ds(pl.multiple_of((1 - place.core) * rows, rows), rows)]
        remote(
            own, other, sem.at[1], sem.at[2], place.at(place.z, place.y, 1 - place.core)
        ).wait_recv()

    return finish


REDUCE = 9
GATHER = 5


def first_kernel(own_ref, gathered, *scratch):
    place = Place()
    sender = Sender()
    own = scratch[0]
    own[...] = own_ref[...]
    greet(place)
    gather_phase(place, sender, gathered, scratch)
    sender.drain()


def hidden_kernel(partial, tokens, gain, gathered, branch, hidden, *scratch):
    place = Place()
    sender = Sender()
    greet(place)
    reduce_phase(place, sender, partial, scratch[:REDUCE])
    total, own = scratch[4], scratch[REDUCE]
    rows, width = total.shape

    def body(at):
        value = total[at]
        scale = lax.rsqrt(jnp.sum(value * value, axis=1, keepdims=True) / width + EPS)
        result = tokens[at].astype(F32) + value * scale * gain[...]
        branch[at] = value
        hidden[at] = result
        own[at] = result.astype(BF)

    by_rows(rows, body)
    gather_phase(place, sender, gathered, scratch[REDUCE:])
    sender.drain()


def turn_kernel(partial, hidden, cotangent, gain, gathered, outputs, gain_grad, *scratch):
    place = Place()
    sender = Sender()
    greet(place)
    reduce_phase(place, sender, partial, scratch[:REDUCE])
    total, own = scratch[4], scratch[REDUCE]
    out_own = scratch[REDUCE + GATHER]
    rows, width = total.shape
    gain_grad[...] = jnp.zeros_like(gain_grad)

    def body(at):
        value = total[at]
        scale = lax.rsqrt(jnp.sum(value * value, axis=1, keepdims=True) / width + EPS)
        grads = cotangent[at].astype(F32)
        normed = value * scale
        out_own[at] = (hidden[at] + normed * gain[...]).astype(BF)
        gain_grad[...] += jnp.sum(grads * normed, axis=0, keepdims=True)
        gained = gain[...] * grads
        inner = jnp.sum(normed * gained, axis=1, keepdims=True)
        own[at] = (scale * (gained - normed * (inner / width))).astype(BF)

    by_rows(rows, body)
    finish = pair_phase(place, sender, out_own, outputs, scratch[REDUCE + GATHER + 1 :])
    gather_phase(place, sender, gathered, scratch[REDUCE : REDUCE + GATHER])
    finish()
    sender.drain()


def branch_kernel(partial, branch, cotangent, gain, gathered, grad_hidden, gain_grad, *scratch):
    place = Place()
    sender = Sender()
    greet(place)
    reduce_phase(place, sender, partial, scratch[:REDUCE])
    total, own = scratch[4], scratch[REDUCE]
    rows, width = total.shape
    gain_grad[...] = jnp.zeros_like(gain_grad)

    def body(at):
        value = branch[at]
        scale = lax.rsqrt(jnp.sum(value * value, axis=1, keepdims=True) / width + EPS)
        grads = cotangent[at].astype(F32) + total[at]
        grad_hidden[at] = grads
        normed = value * scale
        gain_grad[...] += jnp.sum(grads * normed, axis=0, keepdims=True)
        gained = gain[...] * grads
        inner = jnp.sum(normed * gained, axis=1, keepdims=True)
        own[at] = (scale * (gained - normed * (inner / width))).astype(BF)

    by_rows(rows, body)
    gather_phase(place, sender, gathered, scratch[REDUCE:])
    sender.drain()


def last_kernel(partial, grad_hidden, result, *scratch):
    place = Place()
    sender = Sender()
    greet(place)
    reduce_phase(place, sender, partial, scratch[:REDUCE])
    total = scratch[4]

    def body(at):
        total[at] += grad_hidden[at]

    by_rows(total.shape[0], body)
    finish = pair_phase(place, sender, total, result, scratch[REDUCE:])
    finish()
    sender.drain()


def sum_kernel(value, result, core_in, y_in, held, line_in, sem):
    place = Place()
    sender = Sender()
    z, y, core = place.z, place.y, place.core
    barrier = pltpu.get_barrier_semaphore()
    others = [place.at(z, y, 1 - core), place.at(z, 1 - y, core)]
    others += [place.at(lax.rem(z + k, LINE), y, core) for k in range(1, LINE)]
    for device in others:
        pl.semaphore_signal(barrier, inc=1, device_id=device, device_id_type=MESH_ID)
    pl.semaphore_wait(barrier, len(others))
    first = remote(value, core_in, sem.at[0, 0], sem.at[1, 0], others[0])
    first.start()
    first.wait_recv()
    held[0] = value[...] + core_in[...]
    second = remote(held.at[0], y_in, sem.at[0, 1], sem.at[1, 1], others[1])
    second.start()
    second.wait_recv()
    held[1] = held[0] + y_in[...]
    sends = [
        remote(held.at[1], line_in.at[k - 1], sem.at[0, 1 + k], sem.at[1, 1 + k], others[1 + k])
        for k in range(1, LINE)
    ]
    for send in sends:
        send.start()
    line_in[LINE - 1] = held[1]
    for send in sends:
        send.wait_recv()
    added = jnp.zeros_like(value)
    for source in range(LINE):
        slot = lax.rem(z - source + 2 * LINE - 1, LINE)
        added = added + line_in[slot]
    result[...] = added
    first.wait_send()
    second.wait_send()
    for send in sends:
        send.wait_send()


def talk(kernel, which, shapes, specs, scratch, microseconds):
    def call(*operands):
        return pl.pallas_call(
            kernel,
            out_shape=shapes,
            in_specs=specs[0],
            out_specs=specs[1],
            scratch_shapes=scratch,
            compiler_params=pltpu.CompilerParams(
                collective_id=which, has_side_effects=True, vmem_limit_bytes=48 << 20
            ),
            cost_estimate=pl.CostEstimate(
                flops=0, bytes_accessed=int(microseconds * 3.0e6), transcendentals=0
            ),
            name=kernel.__name__,
        )(*operands)

    return call


class Team:
    def __init__(self, local_heads, rows, width):
        self.fsdp = lax.axis_size("fsdp")
        self.tensor = lax.axis_size("tensor")
        self.size = 2 * LINE
        self.teams = self.fsdp // self.size
        assert self.fsdp % self.size == 0 and self.tensor == 2 and local_heads % self.size == 0
        self.member = lax.rem(lax.axis_index("fsdp"), self.size)
        self.core = lax.axis_index("tensor")
        self.context = lax.axis_index("context")
        self.groups = None
        if self.teams > 1:
            self.groups = [
                [team * self.size + one for one in range(self.size)] for team in range(self.teams)
            ]
        self.rows = rows
        self.width = width
        self.all_low = jax.ShapeDtypeStruct((2 * self.size * rows, width), BF)
        self.own_wide = jax.ShapeDtypeStruct((rows, width), F32)
        self.line_wide = jax.ShapeDtypeStruct((1, width), F32)
        self.reduces = reduce_scratch(rows, width)
        self.gathers = gather_scratch(rows, width)

    def first(self, own):
        return talk(first_kernel, 0, self.all_low, ([VMEM], HBM), self.gathers, 50)(own)

    def hidden(self, partial, tokens, gain):
        return talk(
            hidden_kernel,
            1,
            (self.all_low, self.own_wide, self.own_wide),
            ([HBM, VMEM, VMEM], (HBM, VMEM, VMEM)),
            self.reduces + self.gathers,
            100,
        )(partial, tokens, gain)

    def turn(self, partial, hidden, cotangent, gain):
        pair = jax.ShapeDtypeStruct((2 * self.rows, self.width), BF)
        return talk(
            turn_kernel,
            2,
            (self.all_low, pair, self.line_wide),
            ([HBM, VMEM, VMEM, VMEM], (HBM, HBM, VMEM)),
            self.reduces + self.gathers + [pltpu.VMEM((self.rows, self.width), BF)] + pair_scratch(),
            100,
        )(partial, hidden, cotangent, gain)

    def branch(self, partial, branch, cotangent, gain):
        return talk(
            branch_kernel,
            3,
            (self.all_low, self.own_wide, self.line_wide),
            ([HBM, VMEM, VMEM, VMEM], (HBM, VMEM, VMEM)),
            self.reduces + self.gathers,
            100,
        )(partial, branch, cotangent, gain)

    def last(self, partial, grad_hidden):
        pair = jax.ShapeDtypeStruct((2 * self.rows, self.width), F32)
        return talk(
            last_kernel,
            4,
            pair,
            ([HBM, VMEM], HBM),
            self.reduces + pair_scratch(),
            50,
        )(partial, grad_hidden)

    def total(self, values):
        flat = values.reshape(-1, 128)
        shape = jax.ShapeDtypeStruct(flat.shape, F32)
        scratch = [pltpu.VMEM(flat.shape, F32)] * 2
        scratch += [pltpu.VMEM((2,) + flat.shape, F32), pltpu.VMEM((LINE,) + flat.shape, F32)]
        scratch += [DMA((2, LINE + 1))]
        which = 5 + self.sums
        self.sums += 1
        return talk(sum_kernel, which, shape, ([VMEM], VMEM), scratch, 10)(flat).reshape(
            values.shape
        )

    sums = 0

    def half(self, array, axis):
        count = array.shape[axis] // 2
        return lax.dynamic_slice_in_dim(array, self.context * count, count, axis)

    def swap(self, pieces):
        if self.teams > 1:
            pieces = jnp.concatenate([pieces] * self.teams, axis=0)
        return lax.all_to_all(pieces, "fsdp", split_axis=0, concat_axis=0, tiled=True)

    def columns_in(self, weights):
        pieces = []
        for weight in weights:
            rows, columns = weight.shape
            part = self.half(weight, 0).reshape(rows // 2, self.size, columns // self.size)
            pieces.append(part.transpose(1, 0, 2))
        came = self.swap(jnp.concatenate(pieces, axis=2))
        whole = lax.all_gather(came, "context", axis=1, tiled=True)
        return whole.reshape(self.fsdp * rows, whole.shape[2])

    def rows_in(self, weight):
        rows, columns = weight.shape
        pieces = self.half(weight.reshape(self.size, rows // self.size, columns), 1)
        came = self.swap(pieces).transpose(1, 0, 2)
        came = came.reshape(came.shape[0], self.fsdp * columns)
        return lax.all_gather(came, "context", axis=0, tiled=True)

    def back(self, pieces):
        pieces = lax.psum_scatter(
            pieces.astype(BF), "context", scatter_dimension=1, tiled=True
        )
        came = lax.all_to_all(pieces, "fsdp", split_axis=0, concat_axis=0, tiled=True)
        if self.teams > 1:
            came = came.reshape((self.teams, self.size) + came.shape[1:]).astype(F32)
            came = jnp.sum(came, axis=0).astype(BF)
        return lax.all_gather(came, "context", axis=1, tiled=True)

    def columns_out(self, grad, count):
        rows, columns = grad.shape
        came = self.back(grad.reshape(self.fsdp, rows // self.fsdp, columns))
        return [
            part.transpose(1, 0, 2).reshape(rows // self.fsdp, -1).astype(F32)
            for part in jnp.split(came, count, axis=2)
        ]

    def rows_out(self, grad):
        rows, columns = grad.shape
        came = self.back(grad.reshape(rows, self.fsdp, columns // self.fsdp).transpose(1, 0, 2))
        return came.reshape(self.size * rows, columns // self.fsdp).astype(F32)


def local(
    tokens,
    cont_lengths,
    w_query,
    w_key,
    w_value,
    w_output,
    query_gain,
    key_gain,
    attn_gain,
    w_gate,
    w_up,
    w_down,
    mlp_gain,
    cotangent,
):
    rows = tokens.shape[0]
    width = tokens.shape[1]
    fsdp = lax.axis_size("fsdp")
    tensor = lax.axis_size("tensor")
    local_heads = query_gain.shape[0]
    head_size = w_query.shape[1] // local_heads
    own_rows = rows // tensor
    team = Team(local_heads, own_rows, width)
    groups = team.size
    team_rows = groups * rows
    heads = local_heads // team.size
    later = lax.axis_index("context") == 1

    tokens_own = lax.dynamic_slice_in_dim(tokens, team.core * own_rows, own_rows, 0)
    grad_out = lax.dynamic_slice_in_dim(cotangent, team.core * own_rows, own_rows, 0)
    tokens_all = team.first(tokens_own)

    qkv_w = team.columns_in([w_query, w_key, w_value])
    output_w = team.rows_in(w_output)

    fsdp_gains = jnp.concatenate(
        [query_gain.reshape(-1), key_gain.reshape(-1), attn_gain, mlp_gain]
    )
    all_gains = lax.all_gather(fsdp_gains, "fsdp", axis=0, tiled=False).astype(F32)
    cut = query_gain.size
    query_gains = all_gains[:, :cut].reshape(fsdp, local_heads, -1)
    key_gains = all_gains[:, cut : 2 * cut].reshape(fsdp, local_heads, -1)
    query_gains = query_gains.transpose(1, 0, 2).reshape(local_heads, head_size)
    key_gains = key_gains.transpose(1, 0, 2).reshape(local_heads, head_size)
    flat_query = lax.dynamic_slice_in_dim(query_gains, team.member * heads, heads, 0).reshape(-1)
    flat_key = lax.dynamic_slice_in_dim(key_gains, team.member * heads, heads, 0).reshape(-1)
    gain_attn = all_gains[:, 2 * cut : 2 * cut + attn_gain.size].reshape(1, -1)
    gain_mlp = all_gains[:, 2 * cut + attn_gain.size :].reshape(1, -1)

    lengths = lax.all_gather(
        cont_lengths, "fsdp", axis=0, tiled=True, axis_index_groups=team.groups
    )
    segment, offset = jax.vmap(lambda one: layout(one, rows))(lengths)
    row_index = jnp.arange(rows, dtype=jnp.int32)
    positions = jnp.where(later, rows + offset, row_index[None, :])
    own_segment = jnp.where(later, segment, -1)
    cosine, sine = rotary_tables(positions, head_size)
    cosine = cosine[:, :, None, :]
    sine = sine[:, :, None, :]

    pair_w = team.columns_in([w_gate, w_up])
    down_w = team.rows_in(w_down)

    by_head = (groups, rows, heads, head_size)
    raw = product(tokens_all, qkv_w)
    query_raw, key_raw, value_raw = jnp.split(raw, 3, axis=1)
    sums = team.total(
        jnp.stack([jnp.sum(query_raw * query_raw, axis=1), jnp.sum(key_raw * key_raw, axis=1)])
    )
    scale_query = lax.rsqrt(sums[0] / width + EPS)[:, None]
    scale_key = lax.rsqrt(sums[1] / width + EPS)[:, None]
    query_norm = query_raw * scale_query * flat_query
    key_norm = key_raw * scale_key * flat_key
    query_low = rotate(query_norm.reshape(by_head), cosine, sine).astype(BF)
    key_low = rotate(key_norm.reshape(by_head), cosine, sine).astype(BF)
    value_low = value_raw.reshape(by_head).astype(BF)
    sent = lax.ppermute(jnp.stack([key_low, value_low]), "context", [(0, 1)])
    keys_all = jnp.concatenate([sent[0], key_low], axis=1)
    values_all = jnp.concatenate([sent[1], value_low], axis=1)
    key_index = jnp.arange(2 * rows, dtype=jnp.int32)
    key_segment = jnp.concatenate([jnp.full((groups, rows), -2, jnp.int32), own_segment], axis=1)
    remote = (key_index < rows)[None, None, :] & later
    own_keys = (
        (key_index >= rows)[None, None, :]
        & (key_index[None, None, :] - rows <= row_index[None, :, None])
        & (key_segment[:, None, :] == own_segment[:, :, None])
    )
    allowed = (remote | own_keys)[:, None]
    scale = 1.0 / math.sqrt(head_size)
    scores = (
        jnp.einsum("gqhd,gkhd->ghqk", query_low, keys_all, preferred_element_type=F32) * scale
    )
    scores = jnp.where(allowed, scores, -1e30)
    highest = jnp.max(scores, axis=-1, keepdims=True)
    weights = jnp.exp(scores - highest)
    probs = weights / jnp.sum(weights, axis=-1, keepdims=True)
    probs_low = probs.astype(BF)
    mixed = jnp.einsum("ghqk,gkhd->gqhd", probs_low, values_all, preferred_element_type=F32)
    attended_low = mixed.reshape(team_rows, heads * head_size).astype(BF)
    hidden_all, attn_sum, hidden = team.hidden(
        product(attended_low, output_w).astype(BF), tokens_own, gain_attn
    )

    gate, upward = jnp.split(product(hidden_all, pair_w), 2, axis=1)
    sigma = jax.nn.sigmoid(gate)
    inner_low = (gate * sigma * upward).astype(BF)
    grad_mlp_all, outputs, grad_mlp_gain = team.turn(
        product(inner_low, down_w).astype(BF), hidden, grad_out, gain_mlp
    )
    grad_w_down = team.rows_out(product_left(inner_low, grad_mlp_all))
    grad_inner = product_right(grad_mlp_all, down_w)
    grad_gate_low = (grad_inner * upward * sigma * (1.0 + gate * (1.0 - sigma))).astype(BF)
    grad_up_low = (grad_inner * gate * sigma).astype(BF)
    grad_pair = jnp.concatenate([grad_gate_low, grad_up_low], axis=1)
    grad_w_gate, grad_w_up = team.columns_out(product_left(hidden_all, grad_pair), 2)
    grad_branch_all, grad_hidden, grad_attn_gain = team.branch(
        product_right(grad_pair, pair_w).astype(BF), attn_sum, grad_out, gain_attn
    )
    grad_w_output = team.rows_out(product_left(attended_low, grad_branch_all))
    grad_attended = product_right(grad_branch_all, output_w).astype(BF).reshape(by_head)

    grad_probs = jnp.einsum("gqhd,gkhd->ghqk", grad_attended, values_all, preferred_element_type=F32)
    centre = jnp.sum(probs * grad_probs, axis=-1, keepdims=True)
    grad_scores = (probs * (grad_probs - centre)).astype(BF)
    grad_query_rot = (
        jnp.einsum("ghqk,gkhd->gqhd", grad_scores, keys_all, preferred_element_type=F32) * scale
    )
    grad_keys = (
        jnp.einsum("ghqk,gqhd->gkhd", grad_scores, query_low, preferred_element_type=F32) * scale
    )
    grad_values = jnp.einsum("ghqk,gqhd->gkhd", probs_low, grad_attended, preferred_element_type=F32)
    returned = lax.ppermute(
        jnp.stack([grad_keys[:, :rows], grad_values[:, :rows]]).astype(BF), "context", [(1, 0)]
    ).astype(F32)
    grad_key_rot = grad_keys[:, rows:] + returned[0]
    grad_value_low = (grad_values[:, rows:] + returned[1]).reshape(team_rows, -1).astype(BF)
    grad_query_norm = rotate_back(grad_query_rot, cosine, sine).reshape(team_rows, -1)
    grad_key_norm = rotate_back(grad_key_rot, cosine, sine).reshape(team_rows, -1)
    grad_query_gain = jnp.sum(grad_query_norm * query_raw * scale_query, axis=0)
    grad_key_gain = jnp.sum(grad_key_norm * key_raw * scale_key, axis=0)
    totals = team.total(
        jnp.stack(
            [
                jnp.sum(query_raw * flat_query * grad_query_norm, axis=1),
                jnp.sum(key_raw * flat_key * grad_key_norm, axis=1),
            ]
        )
    )
    grad_query_low = norm_back(
        query_raw, scale_query, flat_query, grad_query_norm, totals[0][:, None], width
    ).astype(BF)
    grad_key_low = norm_back(
        key_raw, scale_key, flat_key, grad_key_norm, totals[1][:, None], width
    ).astype(BF)
    grad_qkv = jnp.concatenate([grad_query_low, grad_key_low, grad_value_low], axis=1)
    grad_w_query, grad_w_key, grad_w_value = team.columns_out(product_left(tokens_all, grad_qkv), 3)
    input_grad = team.last(product_right(grad_qkv, qkv_w).astype(BF), grad_hidden)

    all_width = heads * head_size
    place = (team.core * team.size + team.member) * all_width
    spread = jnp.zeros((2, tensor * local_heads * head_size), F32)
    spread = lax.dynamic_update_slice(
        spread, jnp.stack([grad_query_gain, grad_key_gain]), (0, place)
    )
    gains = lax.psum(
        jnp.concatenate([spread.reshape(-1), grad_attn_gain.reshape(-1), grad_mlp_gain.reshape(-1)]),
        ("fsdp", "context", "tensor"),
    )
    device = lax.axis_index("fsdp")
    head_gains = gains[: 2 * tensor * local_heads * head_size].reshape(
        2, tensor, local_heads, fsdp, head_size // fsdp
    )
    head_gains = lax.dynamic_slice(
        head_gains,
        (0, team.core, 0, device, 0),
        (2, 1, local_heads, 1, head_size // fsdp),
    ).reshape(2, local_heads, head_size // fsdp)
    row_gains = gains[2 * tensor * local_heads * head_size :].reshape(2, fsdp, width // fsdp)
    row_gains = lax.dynamic_slice_in_dim(row_gains, device, 1, 1).reshape(2, width // fsdp)
    return (
        outputs,
        input_grad,
        grad_w_query,
        grad_w_key,
        grad_w_value,
        grad_w_output,
        head_gains[0],
        head_gains[1],
        row_gains[0],
        grad_w_gate,
        grad_w_up,
        grad_w_down,
        row_gains[1],
    )


def solution(mesh):
    return jax.shard_map(
        local,
        mesh=mesh,
        in_specs=(
            P(("fsdp", "context"), None),
            P("fsdp", None),
            P("fsdp", "tensor"),
            P("fsdp", "tensor"),
            P("fsdp", "tensor"),
            P("tensor", "fsdp"),
            P("tensor", "fsdp"),
            P("tensor", "fsdp"),
            P("fsdp"),
            P("fsdp", "tensor"),
            P("fsdp", "tensor"),
            P("tensor", "fsdp"),
            P("fsdp"),
            P(("fsdp", "context"), None),
        ),
        out_specs=(
            P(("fsdp", "context"), None),
            P(("fsdp", "context"), None),
            P("fsdp", "tensor"),
            P("fsdp", "tensor"),
            P("fsdp", "tensor"),
            P("tensor", "fsdp"),
            P("tensor", "fsdp"),
            P("tensor", "fsdp"),
            P("fsdp"),
            P("fsdp", "tensor"),
            P("fsdp", "tensor"),
            P("tensor", "fsdp"),
            P("fsdp"),
        ),
        check_vma=False,
    )
```

```python
import functools
import math

import jax
import jax.numpy as jnp
from jax import lax
from jax.experimental import pallas as pl
from jax.experimental.pallas import tpu as pltpu
from jax.sharding import PartitionSpec as P

EPS = 1e-06
THETA = 500000.0
BF = jnp.bfloat16
F32 = jnp.float32


def product(left, right):
    return jnp.dot(left, right, preferred_element_type=F32)


def product_left(left, right):
    return jnp.einsum("rd,rf->df", left, right, preferred_element_type=F32)


def product_right(left, right):
    return jnp.einsum("rf,df->rd", left, right, preferred_element_type=F32)


def rotary_tables(positions, head_size):
    half = head_size // 2
    inverse = jnp.exp(-(2.0 * jnp.arange(half, dtype=F32) / head_size) * math.log(THETA))
    angles = positions.astype(F32)[..., None] * inverse
    angles = jnp.concatenate([angles, angles], axis=-1)
    return (jnp.cos(angles), jnp.sin(angles))


def rotate(values, cosine, sine):
    half = values.shape[-1] // 2
    turned = jnp.concatenate([-values[..., half:], values[..., :half]], axis=-1)
    return values * cosine + turned * sine


def rotate_back(grads, cosine, sine):
    half = grads.shape[-1] // 2
    scaled = grads * sine
    turned = jnp.concatenate([scaled[..., half:], -scaled[..., :half]], axis=-1)
    return grads * cosine + turned


def norm_back(values, scale, gain, grads, total, width):
    return scale * gain * grads - values * scale * scale * scale * (total / width)


def layout(lengths, rows):
    segment_ends = jnp.cumsum(lengths)
    segment_starts = segment_ends - lengths
    row_index = jnp.arange(rows, dtype=jnp.int32)
    segment = jnp.sum((row_index[:, None] >= segment_ends[None, :]).astype(jnp.int32), axis=1)
    chosen = segment[:, None] == jnp.arange(lengths.shape[0], dtype=jnp.int32)[None, :]
    offset = row_index - jnp.sum(jnp.where(chosen, segment_starts[None, :], 0), axis=1)
    return (segment, offset)


LINE = 4
CHUNK = 16
MESH_ID = pl.DeviceIdType.MESH
HBM = pl.BlockSpec(memory_space=pl.ANY)
VMEM = pl.BlockSpec(memory_space=pltpu.VMEM)
DMA = pltpu.SemaphoreType.DMA


class Place:
    def __init__(self):
        device = lax.axis_index("fsdp")
        member = lax.rem(device, 2 * LINE)
        self.base = device - member
        self.z = member // 2
        self.y = lax.rem(member, 2)
        self.core = lax.axis_index("tensor")
        self.side = lax.axis_index("context")
        self.device = device
        self.count = lax.axis_size("fsdp")

    def across(self):
        return {"context": 1 - self.side}

    def at(self, z, y, core):
        return {"fsdp": self.base + 2 * z + y, "tensor": core}

    def near(self):
        yield None, self.at(self.z, self.y, 1 - self.core)
        yield None, self.at(self.z, 1 - self.y, self.core)
        yield self.z > 0, self.at(self.z - 1, self.y, self.core)
        yield self.z < LINE - 1, self.at(self.z + 1, self.y, self.core)

    def rows(self, z, y, core, count):
        start = ((2 * z + y) * 2 + core) * count
        return pl.ds(pl.multiple_of(start, count), count)


def guarded(condition, action):
    if condition is None:
        action()
    else:
        pl.when(condition)(action)


def signal(barrier, device):
    pl.semaphore_signal(barrier, inc=1, device_id=device, device_id_type=MESH_ID)


def greet(place, across=False):
    barrier = pltpu.get_barrier_semaphore()
    for condition, device in place.near():
        guarded(condition, functools.partial(signal, barrier, device))
    if across:
        signal(barrier, place.across())
    inside = (place.z > 0) & (place.z < LINE - 1)
    pl.semaphore_wait(barrier, jnp.where(inside, 4, 3) + int(across))


def greet_all(place):
    barrier = pltpu.get_barrier_semaphore()

    def one(step, carry):
        signal(barrier, {"fsdp": lax.rem(place.device + step, place.count)})
        return carry

    lax.fori_loop(1, place.count, one, 0)
    signal(barrier, place.across())
    signal(barrier, place.at(place.z, place.y, 1 - place.core))
    pl.semaphore_wait(barrier, place.count + 1)


class Sender:
    def __init__(self):
        self.sent = []

    def __call__(self, condition, make):
        def start():
            make().start()

        guarded(condition, start)
        self.sent.append((condition, make))

    def drain(self):
        for condition, make in self.sent:

            def wait(make=make):
                make().wait_send()

            guarded(condition, wait)


def remote(source, target, send, receive, device):
    return pltpu.make_async_remote_copy(
        src_ref=source,
        dst_ref=target,
        send_sem=send,
        recv_sem=receive,
        device_id=device,
        device_id_type=MESH_ID,
    )


def by_rows(rows, body):
    def step(index, carry):
        body(pl.ds(pl.multiple_of(index * CHUNK, CHUNK), CHUNK))
        return carry

    lax.fori_loop(0, rows // CHUNK, step, 0)


def reduce_scratch(rows, width):
    return [
        pltpu.VMEM((2 * LINE, rows, width), BF),
        pltpu.VMEM((2 * LINE, rows, width), BF),
        pltpu.VMEM((LINE, rows, width), BF),
        pltpu.VMEM((LINE + 1, rows, width), BF),
        pltpu.VMEM((rows, width), F32),
        DMA((2 * LINE,)),
        DMA((2, 2 * LINE)),
        DMA((2, LINE)),
        DMA((2, LINE + 1)),
    ]


def reduce_phase(place, sender, partial, scratch, between=None):
    mine, core_in, y_in, line_in, total, local_sem, core_sem, y_sem, line_sem = scratch
    rows = total.shape[0]
    z, y, core = place.z, place.y, place.core
    low = z < LINE // 2
    order = []
    for k in range(LINE - 1):
        down = LINE - 1 - k
        down = jnp.where(down <= z, down - 1, down)
        up = jnp.where(k >= z, k + 1, k)
        order.append(jnp.where(low, down, up))
    order.append(z)

    def fetch(slot):
        half = lax.rem(slot, 2)
        return pltpu.make_async_copy(
            partial.at[place.rows(slot // 2, half, core, rows)], mine.at[slot], local_sem.at[slot]
        )

    def to_core(slot):
        half = lax.rem(slot, 2)
        return remote(
            partial.at[place.rows(slot // 2, half, 1 - core, rows)],
            core_in.at[slot],
            core_sem.at[0, slot],
            core_sem.at[1, slot],
            place.at(z, y, 1 - core),
        )

    def to_y(block):
        return remote(
            mine.at[2 * block + 1 - y],
            y_in.at[block],
            y_sem.at[0, block],
            y_sem.at[1, block],
            place.at(z, 1 - y, core),
        )

    def to_line(block):
        step = jnp.where(block > z, 1, -1)
        slot = jnp.where((step < 0) & (block == z - 1), LINE, block)
        return remote(
            mine.at[2 * block + y],
            line_in.at[slot],
            line_sem.at[0, block],
            line_sem.at[1, slot],
            place.at(z + step, y, core),
        )

    def from_line(slot):
        return remote(
            mine.at[0],
            line_in.at[slot],
            line_sem.at[0, 0],
            line_sem.at[1, slot],
            place.at(z, y, 1 - core),
        )

    for half in (1 - y, y):
        for block in order:
            sender(None, functools.partial(to_core, 2 * block + half))
            fetch(2 * block + half).start()

    for block in order:
        slot = 2 * block + 1 - y
        fetch(slot).wait()
        to_core(slot).wait_recv()

        def add(at, slot=slot):
            value = mine[slot, at].astype(F32) + core_in[slot, at].astype(F32)
            mine[slot, at] = value.astype(BF)

        by_rows(rows, add)
        sender(None, functools.partial(to_y, block))
    if between is not None:
        between()

    for block in order[:-1]:
        slot = 2 * block + y
        fetch(slot).wait()
        to_core(slot).wait_recv()
        to_y(block).wait_recv()
        inner = jnp.where(block > z, z > 0, z < LINE - 1)

        @pl.when(inner)
        def _(block=block, slot=slot):
            from_line(block).wait_recv()

            def add(at):
                value = mine[slot, at].astype(F32) + core_in[slot, at].astype(F32)
                value = value + y_in[block, at].astype(F32)
                mine[slot, at] = (value + line_in[block, at].astype(F32)).astype(BF)

            by_rows(rows, add)

        @pl.when(jnp.logical_not(inner))
        def _(block=block, slot=slot):
            def add(at):
                value = mine[slot, at].astype(F32) + core_in[slot, at].astype(F32)
                mine[slot, at] = (value + y_in[block, at].astype(F32)).astype(BF)

            by_rows(rows, add)

        sender(None, functools.partial(to_line, block))

    slot = 2 * z + y
    fetch(slot).wait()
    to_core(slot).wait_recv()
    to_y(z).wait_recv()

    def start(at):
        value = mine[slot, at].astype(F32) + core_in[slot, at].astype(F32)
        total[at] = value + y_in[z, at].astype(F32)

    by_rows(rows, start)
    for condition, source in ((z > 0, z), (z < LINE - 1, LINE)):

        @pl.when(condition)
        def _(source=source):
            from_line(source).wait_recv()

            def add(at):
                total[at] += line_in[source, at].astype(F32)

            by_rows(rows, add)


def gather_scratch(rows, width):
    return [
        pltpu.VMEM((rows, width), BF),
        DMA((1,)),
        DMA((2, 2 * LINE)),
        DMA((2, LINE)),
        DMA((2, LINE + 2)),
    ]


def gather_phase(place, sender, gathered, scratch, between=None):
    own, local_sem, core_sem, y_sem, line_sem = scratch
    rows = own.shape[0]
    z, y, core = place.z, place.y, place.core

    def spot(block, half):
        return gathered.at[place.rows(block, half, core, rows)]

    def to_core(source, block, half):
        return remote(
            source,
            spot(block, half),
            core_sem.at[0, 2 * block + half],
            core_sem.at[1, 2 * block + half],
            place.at(z, y, 1 - core),
        )

    def to_y(source, block):
        return remote(
            source,
            spot(block, y),
            y_sem.at[0, block],
            y_sem.at[1, block],
            place.at(z, 1 - y, core),
        )

    def to_line(source, block, step, index):
        return remote(
            source,
            spot(block, y),
            line_sem.at[0, index],
            line_sem.at[1, block],
            place.at(z + step, y, core),
        )

    keep = pltpu.make_async_copy(own, spot(z, y), local_sem.at[0])
    keep.start()
    sender(z < LINE - 1, functools.partial(to_line, own, z, 1, LINE))
    sender(z > 0, functools.partial(to_line, own, z, -1, LINE + 1))
    sender(None, functools.partial(to_y, own, z))
    sender(None, functools.partial(to_core, own, z, y))
    if between is not None:
        between()

    def took_y(block):
        remote(
            own,
            spot(block, 1 - y),
            y_sem.at[0, block],
            y_sem.at[1, block],
            place.at(z, 1 - y, core),
        ).wait_recv()

    def across(condition, block):
        guarded(condition, functools.partial(took_y, block))
        sender(condition, lambda: to_core(spot(block, 1 - y), block, 1 - y))

    def along(condition, block, step):
        def took():
            to_line(own, block, step, block).wait_recv()

        guarded(condition, took)
        onward = condition & ((z < LINE - 1) if step > 0 else (z > 0))
        sender(onward, lambda: to_line(spot(block, y), block, step, block))
        sender(condition, lambda: to_y(spot(block, y), block))
        sender(condition, lambda: to_core(spot(block, y), block, y))

    for distance in range(1, LINE + 1):
        if distance < LINE:
            along(z >= distance, z - distance, 1)
            along(z + distance < LINE, z + distance, -1)
        if distance == 1:
            across(None, z)
        else:
            across(z >= distance - 1, z - distance + 1)
            across(z + distance - 1 < LINE, z + distance - 1)

    keep.wait()
    for block in range(LINE):
        for half in range(2):
            remote(
                own,
                gathered.at[place.rows(block, half, 1 - core, rows)],
                core_sem.at[0, 2 * block + half],
                core_sem.at[1, 2 * block + half],
                place.at(z, y, 1 - core),
            ).wait_recv()


def pair_scratch():
    return [DMA((3,))]


def pair_phase(place, sender, own, pair, scratch):
    (sem,) = scratch
    rows = own.shape[0]
    spot = pair.at[pl.ds(pl.multiple_of(place.core * rows, rows), rows)]
    keep = pltpu.make_async_copy(own, spot, sem.at[0])
    keep.start()

    def send():
        return remote(
            own, spot, sem.at[1], sem.at[2], place.at(place.z, place.y, 1 - place.core)
        )

    sender(None, send)

    def finish():
        keep.wait()
        other = pair.at[pl.ds(pl.multiple_of((1 - place.core) * rows, rows), rows)]
        remote(
            own, other, sem.at[1], sem.at[2], place.at(place.z, place.y, 1 - place.core)
        ).wait_recv()

    return finish


def swap_scratch(count, arrays):
    return [DMA((arrays,)), DMA((2, arrays, count)), DMA((2, arrays, count))]


class Swap:
    def __init__(self, place, pieces, wholes, scratch):
        self.place = place
        self.pairs = list(zip(pieces, wholes))
        self.local_sem, self.out_sem, self.side_sem = scratch

    def send(self, index, step):
        place = self.place
        pieces, whole = self.pairs[index]
        target = lax.rem(place.device + step, place.count)
        return remote(
            pieces.at[target],
            whole.at[place.device, place.side],
            self.out_sem.at[0, index, step],
            self.out_sem.at[1, index, step],
            {"fsdp": target},
        )

    def taken(self, index, step, side):
        source = lax.rem(self.place.device + self.place.count - step, self.place.count)
        return self.pairs[index][1].at[source, side]

    def come(self, index, step):
        place = self.place
        return remote(
            self.pairs[index][0].at[0],
            self.taken(index, step, place.side),
            self.out_sem.at[0, index, step],
            self.out_sem.at[1, index, step],
            place.across(),
        )

    def share(self, index, step, source=None):
        spot = self.taken(index, step, self.place.side)
        return remote(
            spot if source is None else source,
            spot,
            self.side_sem.at[0, index, step],
            self.side_sem.at[1, index, step],
            self.place.across(),
        )

    def shared(self, index, step):
        spot = self.taken(index, step, 1 - self.place.side)
        return remote(
            spot,
            spot,
            self.side_sem.at[0, index, step],
            self.side_sem.at[1, index, step],
            self.place.across(),
        )

    def keep(self, index):
        place = self.place
        pieces, whole = self.pairs[index]
        return pltpu.make_async_copy(
            pieces.at[place.device], whole.at[place.device, place.side], self.local_sem.at[index]
        )

    def each(self, first, body):
        def step(number, carry):
            for index in range(len(self.pairs)):
                body(index, number)
            return carry

        lax.fori_loop(first, self.place.count, step, 0)

    def start(self):
        self.each(1, lambda index, step: self.send(index, step).start())
        for index, (pieces, whole) in enumerate(self.pairs):
            self.keep(index).start()
            self.share(index, 0, pieces.at[self.place.device]).start()

    def pass_on(self):
        def one(index, step):
            self.come(index, step).wait_recv()
            self.share(index, step).start()

        self.each(1, one)

    def finish(self):
        for index in range(len(self.pairs)):
            self.keep(index).wait()
        self.each(0, lambda index, step: self.shared(index, step).wait_recv())
        self.each(1, lambda index, step: self.send(index, step).wait_send())
        self.each(0, lambda index, step: self.share(index, step).wait_send())


def halves_scratch(arrays):
    return [DMA((3, arrays))]


class Halves:
    def __init__(self, place, halves, wholes, scratch):
        self.place = place
        self.pairs = list(zip(halves, wholes))
        (self.sem,) = scratch

    def keep(self, index):
        half, whole = self.pairs[index]
        return pltpu.make_async_copy(half, whole.at[:, self.place.side], self.sem.at[0, index])

    def copy(self, index, side):
        half, whole = self.pairs[index]
        return remote(
            half,
            whole.at[:, side],
            self.sem.at[1, index],
            self.sem.at[2, index],
            self.place.across(),
        )

    def start(self):
        for index in range(len(self.pairs)):
            self.copy(index, self.place.side).start()
            self.keep(index).start()

    def finish(self):
        for index in range(len(self.pairs)):
            self.keep(index).wait()
            self.copy(index, 1 - self.place.side).wait_recv()
            self.copy(index, self.place.side).wait_send()


REDUCE = 9
GATHER = 5


def first_kernel(own_ref, qkv, out, small, gathered, qkv_all, out_all, small_all, *scratch):
    place = Place()
    sender = Sender()
    own = scratch[0]
    own[...] = own_ref[...]
    greet_all(place)
    swap = Swap(place, (small, qkv, out), (small_all, qkv_all, out_all), scratch[GATHER:])
    gather_phase(place, sender, gathered, scratch[:GATHER], swap.start)
    swap.pass_on()
    swap.finish()
    sender.drain()


def hidden_kernel(
    partial, tokens, gain, pair, down, gathered, branch, hidden, pair_all, down_all, *scratch
):
    place = Place()
    sender = Sender()
    greet(place, True)
    halves = Halves(place, (pair, down), (pair_all, down_all), scratch[REDUCE + GATHER :])
    halves.start()
    reduce_phase(place, sender, partial, scratch[:REDUCE])
    total, own = scratch[4], scratch[REDUCE]
    rows, width = total.shape

    def body(at):
        value = total[at]
        scale = lax.rsqrt(jnp.sum(value * value, axis=1, keepdims=True) / width + EPS)
        result = tokens[at].astype(F32) + value * scale * gain[...]
        branch[at] = value
        hidden[at] = result
        own[at] = result.astype(BF)

    by_rows(rows, body)
    gather_phase(place, sender, gathered, scratch[REDUCE : REDUCE + GATHER])
    halves.finish()
    sender.drain()


def turn_kernel(partial, hidden, cotangent, gain, gathered, outputs, gain_grad, *scratch):
    place = Place()
    sender = Sender()
    greet(place)
    reduce_phase(place, sender, partial, scratch[:REDUCE])
    total, own = scratch[4], scratch[REDUCE]
    out_own = scratch[REDUCE + GATHER]
    rows, width = total.shape
    gain_grad[...] = jnp.zeros_like(gain_grad)

    def body(at):
        value = total[at]
        scale = lax.rsqrt(jnp.sum(value * value, axis=1, keepdims=True) / width + EPS)
        grads = cotangent[at].astype(F32)
        normed = value * scale
        out_own[at] = (hidden[at] + normed * gain[...]).astype(BF)
        gain_grad[...] += jnp.sum(grads * normed, axis=0, keepdims=True)
        gained = gain[...] * grads
        inner = jnp.sum(normed * gained, axis=1, keepdims=True)
        own[at] = (scale * (gained - normed * (inner / width))).astype(BF)

    by_rows(rows, body)
    finish = pair_phase(place, sender, out_own, outputs, scratch[REDUCE + GATHER + 1 :])
    gather_phase(place, sender, gathered, scratch[REDUCE : REDUCE + GATHER])
    finish()
    sender.drain()


def branch_kernel(
    partial,
    branch,
    cotangent,
    gain,
    pair_grad,
    down_grad,
    gathered,
    grad_hidden,
    gain_grad,
    pair_other,
    down_other,
    *scratch,
):
    place = Place()
    sender = Sender()
    greet(place, True)
    (side_sem,) = scratch[REDUCE + GATHER :]
    count = down_other.shape[0]
    rows_out = pl.ds(pl.multiple_of((1 - place.side) * count, count), count)
    sources = (pair_grad.at[:, 1 - place.side], down_grad.at[rows_out])
    crossings = [
        remote(source, target, side_sem.at[0, index], side_sem.at[1, index], place.across())
        for index, (source, target) in enumerate(zip(sources, (pair_other, down_other)))
    ]
    for crossing in crossings:
        crossing.start()
    reduce_phase(place, sender, partial, scratch[:REDUCE])
    total, own = scratch[4], scratch[REDUCE]
    rows, width = total.shape
    gain_grad[...] = jnp.zeros_like(gain_grad)

    def body(at):
        value = branch[at]
        scale = lax.rsqrt(jnp.sum(value * value, axis=1, keepdims=True) / width + EPS)
        grads = cotangent[at].astype(F32) + total[at]
        grad_hidden[at] = grads
        normed = value * scale
        gain_grad[...] += jnp.sum(grads * normed, axis=0, keepdims=True)
        gained = gain[...] * grads
        inner = jnp.sum(normed * gained, axis=1, keepdims=True)
        own[at] = (scale * (gained - normed * (inner / width))).astype(BF)

    by_rows(rows, body)
    gather_phase(place, sender, gathered, scratch[REDUCE : REDUCE + GATHER])
    for crossing in crossings:
        crossing.wait()
    sender.drain()


def last_kernel(
    partial,
    grad_hidden,
    qkv,
    out,
    small,
    pair,
    down,
    result,
    qkv_all,
    out_all,
    small_all,
    pair_all,
    down_all,
    *scratch,
):
    place = Place()
    sender = Sender()
    parts = scratch[REDUCE + 1 :]
    swap_sems, halves_sems, parts = parts[:3], parts[3:4], parts[4:]
    qkv_own, qkv_other, out_own, out_other, small_own, small_other, fetch_sem, side_sem = parts
    greet_all(place)
    fetches, crossings = [], []
    for index, (grad, own, other) in enumerate(
        ((qkv, qkv_own, qkv_other), (out, out_own, out_other))
    ):
        fetches.append(
            pltpu.make_async_copy(grad.at[:, place.side], own, fetch_sem.at[index])
        )
        crossings.append(
            remote(
                grad.at[:, 1 - place.side],
                other,
                side_sem.at[0, index],
                side_sem.at[1, index],
                place.across(),
            )
        )
    crossings.append(
        remote(
            small,
            small_other,
            side_sem.at[0, 2],
            side_sem.at[1, 2],
            place.at(place.z, place.y, 1 - place.core),
        )
    )
    for copy in fetches + crossings:
        copy.start()
    swap = Swap(
        place, (small_own, qkv_own, out_own), (small_all, qkv_all, out_all), swap_sems
    )
    halves = Halves(place, (pair, down), (pair_all, down_all), halves_sems)
    shared_rows = 2 * partial.shape[1] // place.count // 128

    def between():
        for fetch in fetches:
            fetch.wait()
        for crossing in crossings:
            crossing.wait()
        halves.start()
        small_own[...] = small[...]
        small_own[:, :shared_rows] += small_other[:, :shared_rows]

        def one(index, carry):
            qkv_own[index] = (
                qkv_own[index].astype(F32) + qkv_other[index].astype(F32)
            ).astype(BF)
            out_own[index] = (
                out_own[index].astype(F32) + out_other[index].astype(F32)
            ).astype(BF)
            return carry

        lax.fori_loop(0, place.count, one, 0)
        swap.start()

    reduce_phase(place, sender, partial, scratch[:REDUCE], between)
    total = scratch[4]

    def body(at):
        total[at] += grad_hidden[at]

    by_rows(total.shape[0], body)
    finish = pair_phase(place, sender, total, result, scratch[REDUCE : REDUCE + 1])
    swap.pass_on()
    finish()
    halves.finish()
    swap.finish()
    sender.drain()


def sum_kernel(value, result, core_in, y_in, held, line_in, sem):
    place = Place()
    sender = Sender()
    z, y, core = place.z, place.y, place.core
    barrier = pltpu.get_barrier_semaphore()
    others = [place.at(z, y, 1 - core), place.at(z, 1 - y, core)]
    others += [place.at(lax.rem(z + k, LINE), y, core) for k in range(1, LINE)]
    for device in others:
        pl.semaphore_signal(barrier, inc=1, device_id=device, device_id_type=MESH_ID)
    pl.semaphore_wait(barrier, len(others))
    first = remote(value, core_in, sem.at[0, 0], sem.at[1, 0], others[0])
    first.start()
    first.wait_recv()
    held[0] = value[...] + core_in[...]
    second = remote(held.at[0], y_in, sem.at[0, 1], sem.at[1, 1], others[1])
    second.start()
    second.wait_recv()
    held[1] = held[0] + y_in[...]
    sends = [
        remote(held.at[1], line_in.at[k - 1], sem.at[0, 1 + k], sem.at[1, 1 + k], others[1 + k])
        for k in range(1, LINE)
    ]
    for send in sends:
        send.start()
    line_in[LINE - 1] = held[1]
    for send in sends:
        send.wait_recv()
    added = jnp.zeros_like(value)
    for source in range(LINE):
        slot = lax.rem(z - source + 2 * LINE - 1, LINE)
        added = added + line_in[slot]
    result[...] = added
    first.wait_send()
    second.wait_send()
    for send in sends:
        send.wait_send()


def talk(kernel, which, shapes, specs, scratch, microseconds):
    def call(*operands):
        return pl.pallas_call(
            kernel,
            out_shape=shapes,
            in_specs=specs[0],
            out_specs=specs[1],
            scratch_shapes=scratch,
            compiler_params=pltpu.CompilerParams(
                collective_id=which, has_side_effects=True, vmem_limit_bytes=48 << 20
            ),
            cost_estimate=pl.CostEstimate(
                flops=0, bytes_accessed=int(microseconds * 3.0e6), transcendentals=0
            ),
            name=kernel.__name__,
        )(*operands)

    return call


class Team:
    def __init__(self, local_heads, rows, width):
        self.fsdp = lax.axis_size("fsdp")
        self.tensor = lax.axis_size("tensor")
        self.size = 2 * LINE
        self.teams = self.fsdp // self.size
        assert self.fsdp % self.size == 0 and self.tensor == 2 and local_heads % self.size == 0
        self.member = lax.rem(lax.axis_index("fsdp"), self.size)
        self.core = lax.axis_index("tensor")
        self.context = lax.axis_index("context")
        self.groups = None
        if self.teams > 1:
            self.groups = [
                [team * self.size + one for one in range(self.size)] for team in range(self.teams)
            ]
        self.rows = rows
        self.width = width
        self.all_low = jax.ShapeDtypeStruct((2 * self.size * rows, width), BF)
        self.own_wide = jax.ShapeDtypeStruct((rows, width), F32)
        self.line_wide = jax.ShapeDtypeStruct((1, width), F32)
        self.reduces = reduce_scratch(rows, width)
        self.gathers = gather_scratch(rows, width)

    def whole(self, pieces):
        shape = (pieces.shape[0], 2) + pieces.shape[1:]
        return jax.ShapeDtypeStruct(shape, pieces.dtype)

    def first(self, own, qkv, out, small):
        return talk(
            first_kernel,
            0,
            (self.all_low, self.whole(qkv), self.whole(out), self.whole(small)),
            ([VMEM] * 4, (HBM,) * 4),
            self.gathers + swap_scratch(self.fsdp, 3),
            80,
        )(own, qkv, out, small)

    def hidden(self, partial, tokens, gain, pair, down):
        return talk(
            hidden_kernel,
            1,
            (self.all_low, self.own_wide, self.own_wide, self.whole(pair), self.whole(down)),
            ([HBM, VMEM, VMEM, VMEM, VMEM], (HBM, VMEM, VMEM, HBM, HBM)),
            self.reduces + self.gathers + halves_scratch(2),
            100,
        )(partial, tokens, gain, pair, down)

    def turn(self, partial, hidden, cotangent, gain):
        pair = jax.ShapeDtypeStruct((2 * self.rows, self.width), BF)
        return talk(
            turn_kernel,
            2,
            (self.all_low, pair, self.line_wide),
            ([HBM, VMEM, VMEM, VMEM], (HBM, HBM, VMEM)),
            self.reduces + self.gathers + [pltpu.VMEM((self.rows, self.width), BF)] + pair_scratch(),
            100,
        )(partial, hidden, cotangent, gain)

    def branch(self, partial, branch, cotangent, gain, pair_grad, down_grad):
        shape = pair_grad.shape
        pair_other = jax.ShapeDtypeStruct((shape[0],) + shape[2:], BF)
        down_other = jax.ShapeDtypeStruct((down_grad.shape[0] // 2, down_grad.shape[1]), BF)
        return talk(
            branch_kernel,
            3,
            (self.all_low, self.own_wide, self.line_wide, pair_other, down_other),
            ([HBM, VMEM, VMEM, VMEM, HBM, HBM], (HBM, VMEM, VMEM, HBM, HBM)),
            self.reduces + self.gathers + [DMA((2, 2))],
            100,
        )(partial, branch, cotangent, gain, pair_grad, down_grad)

    def last(self, partial, grad_hidden, qkv, out, small, pair, down):
        both = jax.ShapeDtypeStruct((2 * self.rows, self.width), F32)

        def same(array):
            return jax.ShapeDtypeStruct(array.shape, array.dtype)

        def half(array):
            return pltpu.VMEM((array.shape[0],) + array.shape[2:], array.dtype)

        held = pltpu.VMEM(small.shape, small.dtype)
        return talk(
            last_kernel,
            4,
            (both, same(qkv), same(out), self.whole(small), self.whole(pair), self.whole(down)),
            ([HBM, VMEM, HBM, HBM, VMEM, VMEM, VMEM], (HBM,) * 6),
            self.reduces
            + pair_scratch()
            + swap_scratch(self.fsdp, 3)
            + halves_scratch(2)
            + [half(qkv), half(qkv), half(out), half(out), held, held, DMA((2,)), DMA((2, 3))],
            80,
        )(partial, grad_hidden, qkv, out, small, pair, down)

    def total(self, values):
        flat = values.reshape(-1, 128)
        shape = jax.ShapeDtypeStruct(flat.shape, F32)
        scratch = [pltpu.VMEM(flat.shape, F32)] * 2
        scratch += [pltpu.VMEM((2,) + flat.shape, F32), pltpu.VMEM((LINE,) + flat.shape, F32)]
        scratch += [DMA((2, LINE + 1))]
        which = 5 + self.sums
        self.sums += 1
        return talk(sum_kernel, which, shape, ([VMEM], VMEM), scratch, 10)(flat).reshape(
            values.shape
        )

    sums = 0

    def half(self, array, axis):
        count = array.shape[axis] // 2
        return lax.dynamic_slice_in_dim(array, self.context * count, count, axis)

    def swap(self, pieces):
        return lax.all_to_all(pieces, "fsdp", split_axis=0, concat_axis=0, tiled=True)

    def repeat(self, pieces):
        return jnp.concatenate([pieces] * self.teams, axis=0) if self.teams > 1 else pieces

    def column_pieces(self, weights):
        pieces = []
        for weight in weights:
            rows, columns = weight.shape
            part = self.half(weight, 0).reshape(rows // 2, self.size, columns // self.size)
            pieces.append(part.transpose(1, 0, 2))
        return self.repeat(jnp.concatenate(pieces, axis=2))

    def row_pieces(self, weight):
        rows, columns = weight.shape
        return self.repeat(self.half(weight.reshape(self.size, rows // self.size, columns), 1))

    def columns_whole(self, came):
        return came.reshape(-1, came.shape[-1])

    def rows_whole(self, came):
        fsdp, two, rows, columns = came.shape
        return came.transpose(1, 2, 0, 3).reshape(two * rows, fsdp * columns)

    def of_columns(self, grad):
        rows, columns = grad.shape
        return grad.astype(BF).reshape(self.fsdp, 2, rows // self.fsdp // 2, columns)

    def of_rows(self, grad):
        rows, columns = grad.shape
        cut = grad.astype(BF).reshape(2, rows // 2, self.fsdp, columns // self.fsdp)
        return cut.transpose(2, 0, 1, 3)

    def added(self, came):
        if self.teams == 1:
            return came.astype(F32)
        came = came.reshape((self.teams, self.size) + came.shape[1:])
        return jnp.sum(came.astype(F32), axis=0)

    def columns_out(self, came, count):
        size, two, rows, columns = came.shape
        return [
            self.added(part.reshape(size, two * rows, -1))
            .transpose(1, 0, 2)
            .reshape(two * rows, -1)
            for part in jnp.split(came, count, axis=3)
        ]

    def rows_out(self, came):
        return self.added(came).reshape(-1, came.shape[-1])


def local(
    tokens,
    cont_lengths,
    w_query,
    w_key,
    w_value,
    w_output,
    query_gain,
    key_gain,
    attn_gain,
    w_gate,
    w_up,
    w_down,
    mlp_gain,
    cotangent,
):
    rows = tokens.shape[0]
    width = tokens.shape[1]
    fsdp = lax.axis_size("fsdp")
    tensor = lax.axis_size("tensor")
    local_heads = query_gain.shape[0]
    head_size = w_query.shape[1] // local_heads
    own_rows = rows // tensor
    team = Team(local_heads, own_rows, width)
    groups = team.size
    team_rows = groups * rows
    heads = local_heads // team.size
    later = lax.axis_index("context") == 1

    tokens_own = lax.dynamic_slice_in_dim(tokens, team.core * own_rows, own_rows, 0)
    grad_out = lax.dynamic_slice_in_dim(cotangent, team.core * own_rows, own_rows, 0)
    cut = query_gain.size
    share = attn_gain.size
    small = [query_gain.reshape(-1), key_gain.reshape(-1), attn_gain, mlp_gain]
    small = jnp.concatenate([one.astype(F32) for one in small + [cont_lengths.reshape(-1)]])
    small = jnp.pad(small, (0, 8 * 128 - small.size)).reshape(1, 8, 128)
    tokens_all, qkv_came, output_came, small_came = team.first(
        tokens_own,
        team.column_pieces([w_query, w_key, w_value]),
        team.row_pieces(w_output),
        jnp.broadcast_to(small, (fsdp, 8, 128)),
    )
    qkv_w = team.columns_whole(qkv_came)
    output_w = team.rows_whole(output_came)
    all_small = small_came[:, 0].reshape(fsdp, -1)
    query_gains = all_small[:, :cut].reshape(fsdp, local_heads, -1)
    key_gains = all_small[:, cut : 2 * cut].reshape(fsdp, local_heads, -1)
    query_gains = query_gains.transpose(1, 0, 2).reshape(local_heads, head_size)
    key_gains = key_gains.transpose(1, 0, 2).reshape(local_heads, head_size)
    flat_query = lax.dynamic_slice_in_dim(query_gains, team.member * heads, heads, 0).reshape(-1)
    flat_key = lax.dynamic_slice_in_dim(key_gains, team.member * heads, heads, 0).reshape(-1)
    gain_attn = all_small[:, 2 * cut : 2 * cut + share].reshape(1, -1)
    gain_mlp = all_small[:, 2 * cut + share : 2 * cut + 2 * share].reshape(1, -1)

    conts = cont_lengths.shape[1]
    lengths = all_small[:, 2 * cut + 2 * share : 2 * cut + 2 * share + conts].astype(jnp.int32)
    first_group = lax.axis_index("fsdp") - team.member
    lengths = lax.dynamic_slice_in_dim(lengths, first_group, groups, 0)
    segment, offset = jax.vmap(lambda one: layout(one, rows))(lengths)
    row_index = jnp.arange(rows, dtype=jnp.int32)
    positions = jnp.where(later, rows + offset, row_index[None, :])
    own_segment = jnp.where(later, segment, -1)
    cosine, sine = rotary_tables(positions, head_size)
    cosine = cosine[:, :, None, :]
    sine = sine[:, :, None, :]

    pair_mine, down_mine, tokens_all = lax.optimization_barrier(
        (team.column_pieces([w_gate, w_up]), team.row_pieces(w_down), tokens_all)
    )
    pair_came = team.swap(pair_mine)
    down_came = team.swap(down_mine)

    by_head = (groups, rows, heads, head_size)
    raw = product(tokens_all, qkv_w)
    query_raw, key_raw, value_raw = jnp.split(raw, 3, axis=1)
    sums = team.total(
        jnp.stack([jnp.sum(query_raw * query_raw, axis=1), jnp.sum(key_raw * key_raw, axis=1)])
    )
    scale_query = lax.rsqrt(sums[0] / width + EPS)[:, None]
    scale_key = lax.rsqrt(sums[1] / width + EPS)[:, None]
    query_norm = query_raw * scale_query * flat_query
    key_norm = key_raw * scale_key * flat_key
    query_low = rotate(query_norm.reshape(by_head), cosine, sine).astype(BF)
    key_low = rotate(key_norm.reshape(by_head), cosine, sine).astype(BF)
    value_low = value_raw.reshape(by_head).astype(BF)
    sent_value = lax.ppermute(value_low, "context", [(0, 1)])
    sent_key = lax.ppermute(key_low, "context", [(0, 1)])
    keys_all = jnp.concatenate([sent_key, key_low], axis=1)
    values_all = jnp.concatenate([sent_value, value_low], axis=1)
    key_index = jnp.arange(2 * rows, dtype=jnp.int32)
    key_segment = jnp.concatenate([jnp.full((groups, rows), -2, jnp.int32), own_segment], axis=1)
    remote = (key_index < rows)[None, None, :] & later
    own_keys = (
        (key_index >= rows)[None, None, :]
        & (key_index[None, None, :] - rows <= row_index[None, :, None])
        & (key_segment[:, None, :] == own_segment[:, :, None])
    )
    allowed = (remote | own_keys)[:, None]
    scale = 1.0 / math.sqrt(head_size)
    scores = (
        jnp.einsum("gqhd,gkhd->ghqk", query_low, keys_all, preferred_element_type=F32) * scale
    )
    scores = jnp.where(allowed, scores, -1e30)
    highest = jnp.max(scores, axis=-1, keepdims=True)
    weights = jnp.exp(scores - highest)
    probs = weights / jnp.sum(weights, axis=-1, keepdims=True)
    probs_low = probs.astype(BF)
    mixed = jnp.einsum("ghqk,gkhd->gqhd", probs_low, values_all, preferred_element_type=F32)
    attended_low = mixed.reshape(team_rows, heads * head_size).astype(BF)
    hidden_all, attn_sum, hidden, pair_came, down_came = team.hidden(
        product(attended_low, output_w).astype(BF), tokens_own, gain_attn, pair_came, down_came
    )
    pair_w = team.columns_whole(pair_came)
    down_w = team.rows_whole(down_came)

    gate, upward = jnp.split(product(hidden_all, pair_w), 2, axis=1)
    sigma = jax.nn.sigmoid(gate)
    inner_low = (gate * sigma * upward).astype(BF)
    grad_mlp_all, outputs, grad_mlp_gain = team.turn(
        product(inner_low, down_w).astype(BF), hidden, grad_out, gain_mlp
    )
    down_grad = product_left(inner_low, grad_mlp_all).astype(BF)
    grad_inner = product_right(grad_mlp_all, down_w)
    grad_gate_low = (grad_inner * upward * sigma * (1.0 + gate * (1.0 - sigma))).astype(BF)
    grad_up_low = (grad_inner * gate * sigma).astype(BF)
    grad_pair = jnp.concatenate([grad_gate_low, grad_up_low], axis=1)
    pair_grad = team.of_columns(product_left(hidden_all, grad_pair))
    grad_branch_all, grad_hidden, grad_attn_gain, pair_other, down_other = team.branch(
        product_right(grad_pair, pair_w).astype(BF),
        attn_sum,
        grad_out,
        gain_attn,
        pair_grad,
        down_grad,
    )
    pair_mine = lax.dynamic_index_in_dim(pair_grad, team.context, 1, keepdims=False)
    pair_mine = (pair_mine.astype(F32) + pair_other.astype(F32)).astype(BF)
    down_mine = (team.half(down_grad, 0).astype(F32) + down_other.astype(F32)).astype(BF)
    down_mine = down_mine.reshape(down_mine.shape[0], fsdp, -1).transpose(1, 0, 2)
    pair_came = team.swap(pair_mine)
    down_came = team.swap(down_mine)
    output_grad = team.of_rows(product_left(attended_low, grad_branch_all))
    grad_attended = product_right(grad_branch_all, output_w).astype(BF).reshape(by_head)

    grad_probs = jnp.einsum("gqhd,gkhd->ghqk", grad_attended, values_all, preferred_element_type=F32)
    centre = jnp.sum(probs * grad_probs, axis=-1, keepdims=True)
    grad_scores = (probs * (grad_probs - centre)).astype(BF)
    grad_query_rot = (
        jnp.einsum("ghqk,gkhd->gqhd", grad_scores, keys_all, preferred_element_type=F32) * scale
    )
    grad_keys = (
        jnp.einsum("ghqk,gqhd->gkhd", grad_scores, query_low, preferred_element_type=F32) * scale
    )
    grad_values = jnp.einsum("ghqk,gqhd->gkhd", probs_low, grad_attended, preferred_element_type=F32)
    back_value = lax.ppermute(grad_values[:, :rows].astype(BF), "context", [(1, 0)])
    back_key = lax.ppermute(grad_keys[:, :rows].astype(BF), "context", [(1, 0)])
    grad_key_rot = grad_keys[:, rows:] + back_key.astype(F32)
    grad_value_low = (
        (grad_values[:, rows:] + back_value.astype(F32)).reshape(team_rows, -1).astype(BF)
    )
    grad_query_norm = rotate_back(grad_query_rot, cosine, sine).reshape(team_rows, -1)
    grad_key_norm = rotate_back(grad_key_rot, cosine, sine).reshape(team_rows, -1)
    grad_query_gain = jnp.sum(grad_query_norm * query_raw * scale_query, axis=0)
    grad_key_gain = jnp.sum(grad_key_norm * key_raw * scale_key, axis=0)
    totals = team.total(
        jnp.stack(
            [
                jnp.sum(query_raw * flat_query * grad_query_norm, axis=1),
                jnp.sum(key_raw * flat_key * grad_key_norm, axis=1),
            ]
        )
    )
    grad_query_low = norm_back(
        query_raw, scale_query, flat_query, grad_query_norm, totals[0][:, None], width
    ).astype(BF)
    grad_key_low = norm_back(
        key_raw, scale_key, flat_key, grad_key_norm, totals[1][:, None], width
    ).astype(BF)
    grad_qkv = jnp.concatenate([grad_query_low, grad_key_low, grad_value_low], axis=1)
    qkv_grad = team.of_columns(product_left(tokens_all, grad_qkv))
    head_share = head_size // fsdp
    small = [
        grad_attn_gain.reshape(fsdp, share),
        grad_mlp_gain.reshape(fsdp, share),
        grad_query_gain.reshape(heads, fsdp, head_share).transpose(1, 0, 2).reshape(fsdp, -1),
        grad_key_gain.reshape(heads, fsdp, head_share).transpose(1, 0, 2).reshape(fsdp, -1),
    ]
    used = 2 * share + 2 * heads * head_share
    small = jnp.concatenate(small + [jnp.zeros((fsdp, 8 * 128 - used), F32)], axis=1)
    input_grad, qkv_came, output_came, small_came, pair_came, down_came = team.last(
        product_right(grad_qkv, qkv_w).astype(BF),
        grad_hidden,
        qkv_grad,
        output_grad,
        small.reshape(fsdp, 8, 128),
        pair_came,
        down_came,
    )
    grad_w_query, grad_w_key, grad_w_value = team.columns_out(qkv_came, 3)
    grad_w_gate, grad_w_up = team.columns_out(pair_came, 2)
    grad_w_output = team.rows_out(output_came)
    grad_w_down = team.rows_out(down_came)
    came = jnp.sum(small_came, axis=1).reshape(fsdp, -1)
    row_gains = jnp.sum(came[:, : 2 * share], axis=0).reshape(2, share)
    head_gains = team.added(came[:, 2 * share : used]).reshape(team.size, 2, heads, head_share)
    head_gains = head_gains.transpose(1, 0, 2, 3).reshape(2, local_heads, head_share)
    return (
        outputs,
        input_grad,
        grad_w_query,
        grad_w_key,
        grad_w_value,
        grad_w_output,
        head_gains[0],
        head_gains[1],
        row_gains[0],
        grad_w_gate,
        grad_w_up,
        grad_w_down,
        row_gains[1],
    )


def solution(mesh):
    return jax.shard_map(
        local,
        mesh=mesh,
        in_specs=(
            P(("fsdp", "context"), None),
            P("fsdp", None),
            P("fsdp", "tensor"),
            P("fsdp", "tensor"),
            P("fsdp", "tensor"),
            P("tensor", "fsdp"),
            P("tensor", "fsdp"),
            P("tensor", "fsdp"),
            P("fsdp"),
            P("fsdp", "tensor"),
            P("fsdp", "tensor"),
            P("tensor", "fsdp"),
            P("fsdp"),
            P(("fsdp", "context"), None),
        ),
        out_specs=(
            P(("fsdp", "context"), None),
            P(("fsdp", "context"), None),
            P("fsdp", "tensor"),
            P("fsdp", "tensor"),
            P("fsdp", "tensor"),
            P("tensor", "fsdp"),
            P("tensor", "fsdp"),
            P("tensor", "fsdp"),
            P("fsdp"),
            P("fsdp", "tensor"),
            P("fsdp", "tensor"),
            P("tensor", "fsdp"),
            P("fsdp"),
        ),
        check_vma=False,
    )
```

```python
import functools
import math

import jax
import jax.numpy as jnp
from jax import lax
from jax.experimental import pallas as pl
from jax.experimental.pallas import tpu as pltpu
from jax.sharding import PartitionSpec as P

EPS = 1e-06
THETA = 500000.0
BF = jnp.bfloat16
F32 = jnp.float32


def product(left, right):
    return jnp.dot(left, right, preferred_element_type=F32)


def product_left(left, right):
    return jnp.einsum("rd,rf->df", left, right, preferred_element_type=F32)


def product_right(left, right):
    return jnp.einsum("rf,df->rd", left, right, preferred_element_type=F32)


def rotary_tables(positions, head_size):
    half = head_size // 2
    inverse = jnp.exp(-(2.0 * jnp.arange(half, dtype=F32) / head_size) * math.log(THETA))
    angles = positions.astype(F32)[..., None] * inverse
    angles = jnp.concatenate([angles, angles], axis=-1)
    return (jnp.cos(angles), jnp.sin(angles))


def rotate(values, cosine, sine):
    half = values.shape[-1] // 2
    turned = jnp.concatenate([-values[..., half:], values[..., :half]], axis=-1)
    return values * cosine + turned * sine


def rotate_back(grads, cosine, sine):
    half = grads.shape[-1] // 2
    scaled = grads * sine
    turned = jnp.concatenate([scaled[..., half:], -scaled[..., :half]], axis=-1)
    return grads * cosine + turned


def norm_back(values, scale, gain, grads, total, width):
    return scale * gain * grads - values * scale * scale * scale * (total / width)


def layout(lengths, rows):
    segment_ends = jnp.cumsum(lengths)
    segment_starts = segment_ends - lengths
    row_index = jnp.arange(rows, dtype=jnp.int32)
    segment = jnp.sum((row_index[:, None] >= segment_ends[None, :]).astype(jnp.int32), axis=1)
    chosen = segment[:, None] == jnp.arange(lengths.shape[0], dtype=jnp.int32)[None, :]
    offset = row_index - jnp.sum(jnp.where(chosen, segment_starts[None, :], 0), axis=1)
    return (segment, offset)


LINE = 4
CHUNK = 16
MESH_ID = pl.DeviceIdType.MESH
HBM = pl.BlockSpec(memory_space=pl.ANY)
VMEM = pl.BlockSpec(memory_space=pltpu.VMEM)
DMA = pltpu.SemaphoreType.DMA


class Place:
    def __init__(self):
        device = lax.axis_index("fsdp")
        member = lax.rem(device, 2 * LINE)
        self.base = device - member
        self.z = member // 2
        self.y = lax.rem(member, 2)
        self.core = lax.axis_index("tensor")
        self.side = lax.axis_index("context")
        self.device = device
        self.count = lax.axis_size("fsdp")

    def across(self):
        return {"context": 1 - self.side}

    def at(self, z, y, core):
        return {"fsdp": self.base + 2 * z + y, "tensor": core}

    def near(self):
        yield None, self.at(self.z, self.y, 1 - self.core)
        yield None, self.at(self.z, 1 - self.y, self.core)
        yield self.z > 0, self.at(self.z - 1, self.y, self.core)
        yield self.z < LINE - 1, self.at(self.z + 1, self.y, self.core)

    def rows(self, z, y, core, count):
        start = ((2 * z + y) * 2 + core) * count
        return pl.ds(pl.multiple_of(start, count), count)


def guarded(condition, action):
    if condition is None:
        action()
    else:
        pl.when(condition)(action)


def signal(barrier, device):
    pl.semaphore_signal(barrier, inc=1, device_id=device, device_id_type=MESH_ID)


def greet(place, across=False):
    barrier = pltpu.get_barrier_semaphore()
    for condition, device in place.near():
        guarded(condition, functools.partial(signal, barrier, device))
    if across:
        signal(barrier, place.across())
    inside = (place.z > 0) & (place.z < LINE - 1)
    pl.semaphore_wait(barrier, jnp.where(inside, 4, 3) + int(across))


def greet_all(place):
    barrier = pltpu.get_barrier_semaphore()

    def one(step, carry):
        signal(barrier, {"fsdp": lax.rem(place.device + step, place.count)})
        return carry

    lax.fori_loop(1, place.count, one, 0)
    signal(barrier, place.across())
    signal(barrier, place.at(place.z, place.y, 1 - place.core))
    pl.semaphore_wait(barrier, place.count + 1)


class Sender:
    def __init__(self):
        self.sent = []

    def __call__(self, condition, make):
        def start():
            make().start()

        guarded(condition, start)
        self.sent.append((condition, make))

    def drain(self):
        for condition, make in self.sent:

            def wait(make=make):
                make().wait_send()

            guarded(condition, wait)


def remote(source, target, send, receive, device):
    return pltpu.make_async_remote_copy(
        src_ref=source,
        dst_ref=target,
        send_sem=send,
        recv_sem=receive,
        device_id=device,
        device_id_type=MESH_ID,
    )


def by_rows(rows, body):
    def step(index, carry):
        body(pl.ds(pl.multiple_of(index * CHUNK, CHUNK), CHUNK))
        return carry

    lax.fori_loop(0, rows // CHUNK, step, 0)


def reduce_scratch(rows, width):
    return [
        pltpu.VMEM((2 * LINE, rows, width), BF),
        pltpu.VMEM((2 * LINE, rows, width), BF),
        pltpu.VMEM((LINE, rows, width), BF),
        pltpu.VMEM((LINE + 1, rows, width), BF),
        pltpu.VMEM((rows, width), F32),
        DMA((2 * LINE,)),
        DMA((2, 2 * LINE)),
        DMA((2, LINE)),
        DMA((2, LINE + 1)),
    ]


def reduce_phase(place, sender, partial, scratch, between=None):
    mine, core_in, y_in, line_in, total, local_sem, core_sem, y_sem, line_sem = scratch
    rows = total.shape[0]
    z, y, core = place.z, place.y, place.core
    low = z < LINE // 2
    order = []
    for k in range(LINE - 1):
        down = LINE - 1 - k
        down = jnp.where(down <= z, down - 1, down)
        up = jnp.where(k >= z, k + 1, k)
        order.append(jnp.where(low, down, up))
    order.append(z)

    def fetch(slot):
        half = lax.rem(slot, 2)
        return pltpu.make_async_copy(
            partial.at[place.rows(slot // 2, half, core, rows)], mine.at[slot], local_sem.at[slot]
        )

    def to_core(slot):
        half = lax.rem(slot, 2)
        return remote(
            partial.at[place.rows(slot // 2, half, 1 - core, rows)],
            core_in.at[slot],
            core_sem.at[0, slot],
            core_sem.at[1, slot],
            place.at(z, y, 1 - core),
        )

    def to_y(block):
        return remote(
            mine.at[2 * block + 1 - y],
            y_in.at[block],
            y_sem.at[0, block],
            y_sem.at[1, block],
            place.at(z, 1 - y, core),
        )

    def to_line(block):
        step = jnp.where(block > z, 1, -1)
        slot = jnp.where((step < 0) & (block == z - 1), LINE, block)
        return remote(
            mine.at[2 * block + y],
            line_in.at[slot],
            line_sem.at[0, block],
            line_sem.at[1, slot],
            place.at(z + step, y, core),
        )

    def from_line(slot):
        return remote(
            mine.at[0],
            line_in.at[slot],
            line_sem.at[0, 0],
            line_sem.at[1, slot],
            place.at(z, y, 1 - core),
        )

    for half in (1 - y, y):
        for block in order:
            sender(None, functools.partial(to_core, 2 * block + half))
            fetch(2 * block + half).start()

    for block in order:
        slot = 2 * block + 1 - y
        fetch(slot).wait()
        to_core(slot).wait_recv()

        def add(at, slot=slot):
            value = mine[slot, at].astype(F32) + core_in[slot, at].astype(F32)
            mine[slot, at] = value.astype(BF)

        by_rows(rows, add)
        sender(None, functools.partial(to_y, block))
    if between is not None:
        between()

    for block in order[:-1]:
        slot = 2 * block + y
        fetch(slot).wait()
        to_core(slot).wait_recv()
        to_y(block).wait_recv()
        inner = jnp.where(block > z, z > 0, z < LINE - 1)

        @pl.when(inner)
        def _(block=block, slot=slot):
            from_line(block).wait_recv()

            def add(at):
                value = mine[slot, at].astype(F32) + core_in[slot, at].astype(F32)
                value = value + y_in[block, at].astype(F32)
                mine[slot, at] = (value + line_in[block, at].astype(F32)).astype(BF)

            by_rows(rows, add)

        @pl.when(jnp.logical_not(inner))
        def _(block=block, slot=slot):
            def add(at):
                value = mine[slot, at].astype(F32) + core_in[slot, at].astype(F32)
                mine[slot, at] = (value + y_in[block, at].astype(F32)).astype(BF)

            by_rows(rows, add)

        sender(None, functools.partial(to_line, block))

    slot = 2 * z + y
    fetch(slot).wait()
    to_core(slot).wait_recv()
    to_y(z).wait_recv()

    def start(at):
        value = mine[slot, at].astype(F32) + core_in[slot, at].astype(F32)
        total[at] = value + y_in[z, at].astype(F32)

    by_rows(rows, start)
    for condition, source in ((z > 0, z), (z < LINE - 1, LINE)):

        @pl.when(condition)
        def _(source=source):
            from_line(source).wait_recv()

            def add(at):
                total[at] += line_in[source, at].astype(F32)

            by_rows(rows, add)


def gather_scratch(rows, width):
    return [
        pltpu.VMEM((rows, width), BF),
        DMA((1,)),
        DMA((2, 2 * LINE)),
        DMA((2, LINE)),
        DMA((2, LINE + 2)),
    ]


def gather_phase(place, sender, gathered, scratch, between=None, later=None):
    own, local_sem, core_sem, y_sem, line_sem = scratch
    rows = own.shape[0]
    z, y, core = place.z, place.y, place.core

    def spot(block, half):
        return gathered.at[place.rows(block, half, core, rows)]

    def to_core(source, block, half):
        return remote(
            source,
            spot(block, half),
            core_sem.at[0, 2 * block + half],
            core_sem.at[1, 2 * block + half],
            place.at(z, y, 1 - core),
        )

    def to_y(source, block):
        return remote(
            source,
            spot(block, y),
            y_sem.at[0, block],
            y_sem.at[1, block],
            place.at(z, 1 - y, core),
        )

    def to_line(source, block, step, index):
        return remote(
            source,
            spot(block, y),
            line_sem.at[0, index],
            line_sem.at[1, block],
            place.at(z + step, y, core),
        )

    keep = pltpu.make_async_copy(own, spot(z, y), local_sem.at[0])
    keep.start()
    sender(z < LINE - 1, functools.partial(to_line, own, z, 1, LINE))
    sender(z > 0, functools.partial(to_line, own, z, -1, LINE + 1))
    sender(None, functools.partial(to_y, own, z))
    sender(None, functools.partial(to_core, own, z, y))
    if between is not None:
        between()

    def took_y(block):
        remote(
            own,
            spot(block, 1 - y),
            y_sem.at[0, block],
            y_sem.at[1, block],
            place.at(z, 1 - y, core),
        ).wait_recv()

    def across(condition, block):
        guarded(condition, functools.partial(took_y, block))
        sender(condition, lambda: to_core(spot(block, 1 - y), block, 1 - y))

    def along(condition, block, step):
        def took():
            to_line(own, block, step, block).wait_recv()

        guarded(condition, took)
        onward = condition & ((z < LINE - 1) if step > 0 else (z > 0))
        sender(onward, lambda: to_line(spot(block, y), block, step, block))
        sender(condition, lambda: to_y(spot(block, y), block))
        sender(condition, lambda: to_core(spot(block, y), block, y))

    for distance in range(1, LINE + 1):
        if distance < LINE:
            along(z >= distance, z - distance, 1)
            along(z + distance < LINE, z + distance, -1)
        if distance == 1:
            across(None, z)
        else:
            across(z >= distance - 1, z - distance + 1)
            across(z + distance - 1 < LINE, z + distance - 1)
        if distance == 1 and later is not None:
            later()

    keep.wait()
    for block in range(LINE):
        for half in range(2):
            remote(
                own,
                gathered.at[place.rows(block, half, 1 - core, rows)],
                core_sem.at[0, 2 * block + half],
                core_sem.at[1, 2 * block + half],
                place.at(z, y, 1 - core),
            ).wait_recv()


def pair_scratch():
    return [DMA((3,))]


def pair_phase(place, sender, own, pair, scratch):
    (sem,) = scratch
    rows = own.shape[0]
    spot = pair.at[pl.ds(pl.multiple_of(place.core * rows, rows), rows)]
    keep = pltpu.make_async_copy(own, spot, sem.at[0])
    keep.start()

    def send():
        return remote(
            own, spot, sem.at[1], sem.at[2], place.at(place.z, place.y, 1 - place.core)
        )

    sender(None, send)

    def finish():
        keep.wait()
        other = pair.at[pl.ds(pl.multiple_of((1 - place.core) * rows, rows), rows)]
        remote(
            own, other, sem.at[1], sem.at[2], place.at(place.z, place.y, 1 - place.core)
        ).wait_recv()

    return finish


def swap_scratch(count, arrays):
    return [DMA((arrays,)), DMA((2, arrays, count)), DMA((2, arrays, count))]


class Swap:
    def __init__(self, place, pairs, scratch):
        self.place = place
        self.pairs = pairs
        self.local_sem, self.out_sem, self.side_sem = scratch

    def send(self, index, step):
        place = self.place
        source, spot = self.pairs[index]
        target = lax.rem(place.device + step, place.count)
        return remote(
            source(target),
            spot(place.device, place.side),
            self.out_sem.at[0, index, step],
            self.out_sem.at[1, index, step],
            {"fsdp": target},
        )

    def taken(self, index, step, side):
        device = lax.rem(self.place.device + self.place.count - step, self.place.count)
        return self.pairs[index][1](device, side)

    def come(self, index, step):
        place = self.place
        return remote(
            self.pairs[index][0](place.device),
            self.taken(index, step, place.side),
            self.out_sem.at[0, index, step],
            self.out_sem.at[1, index, step],
            place.across(),
        )

    def share(self, index, step, source=None):
        spot = self.taken(index, step, self.place.side)
        return remote(
            spot if source is None else source,
            spot,
            self.side_sem.at[0, index, step],
            self.side_sem.at[1, index, step],
            self.place.across(),
        )

    def shared(self, index, step):
        spot = self.taken(index, step, 1 - self.place.side)
        return remote(
            spot,
            spot,
            self.side_sem.at[0, index, step],
            self.side_sem.at[1, index, step],
            self.place.across(),
        )

    def keep(self, index):
        place = self.place
        source, spot = self.pairs[index]
        return pltpu.make_async_copy(
            source(place.device), spot(place.device, place.side), self.local_sem.at[index]
        )

    def each(self, first, body):
        def step(number, carry):
            for index in range(len(self.pairs)):
                body(index, number)
            return carry

        lax.fori_loop(first, self.place.count, step, 0)

    def start(self):
        self.each(1, lambda index, step: self.send(index, step).start())
        for index, (source, _) in enumerate(self.pairs):
            self.keep(index).start()
            self.share(index, 0, source(self.place.device)).start()

    def pass_on(self):
        def one(index, step):
            self.come(index, step).wait_recv()
            self.share(index, step).start()

        self.each(1, one)

    def finish(self):
        for index in range(len(self.pairs)):
            self.keep(index).wait()
        self.each(0, lambda index, step: self.shared(index, step).wait_recv())
        self.each(1, lambda index, step: self.send(index, step).wait_send())
        self.each(0, lambda index, step: self.share(index, step).wait_send())


def whole_pair(pieces, whole):
    return (lambda target: pieces.at[target], lambda device, side: whole.at[device, side])


def halves_scratch(arrays):
    return [DMA((3, arrays))]


class Halves:
    def __init__(self, place, halves, wholes, scratch):
        self.place = place
        self.pairs = list(zip(halves, wholes))
        (self.sem,) = scratch

    def keep(self, index):
        half, whole = self.pairs[index]
        return pltpu.make_async_copy(half, whole.at[:, self.place.side], self.sem.at[0, index])

    def copy(self, index, side):
        half, whole = self.pairs[index]
        return remote(
            half,
            whole.at[:, side],
            self.sem.at[1, index],
            self.sem.at[2, index],
            self.place.across(),
        )

    def start(self):
        for index in range(len(self.pairs)):
            self.copy(index, self.place.side).start()
            self.keep(index).start()

    def finish(self):
        for index in range(len(self.pairs)):
            self.keep(index).wait()
            self.copy(index, 1 - self.place.side).wait_recv()
            self.copy(index, self.place.side).wait_send()


REDUCE = 9
GATHER = 5


def first_kernel(
    own_ref, query, key, value, out, small, gathered, qkv_all, out_all, small_all, *scratch
):
    place = Place()
    sender = Sender()
    own = scratch[0]
    own[...] = own_ref[...]
    greet_all(place)
    half, columns = qkv_all.shape[2], qkv_all.shape[3] // 3
    out_half = out_all.shape[2]
    rows = pl.ds(pl.multiple_of(place.side * half, half), half)

    def member(target):
        return lax.rem(target, 2 * LINE)

    def column_pair(weight, index):
        def source(target):
            start = pl.multiple_of(member(target) * columns, columns)
            return weight.at[rows, pl.ds(start, columns)]

        def spot(device, side):
            return qkv_all.at[device, side, :, pl.ds(index * columns, columns)]

        return (source, spot)

    def out_source(target):
        start = (2 * member(target) + place.side) * out_half
        return out.at[pl.ds(pl.multiple_of(start, out_half), out_half)]

    pairs = [
        (lambda target: small, lambda device, side: small_all.at[device, side]),
        column_pair(query, 0),
        column_pair(key, 1),
        column_pair(value, 2),
        (out_source, lambda device, side: out_all.at[device, side]),
    ]
    swap = Swap(place, pairs, scratch[GATHER:])
    gather_phase(place, sender, gathered, scratch[:GATHER], swap.start, swap.pass_on)
    swap.finish()
    sender.drain()


def hidden_kernel(
    partial, tokens, gain, pair, down, gathered, branch, hidden, pair_all, down_all, *scratch
):
    place = Place()
    sender = Sender()
    greet(place, True)
    halves = Halves(place, (pair, down), (pair_all, down_all), scratch[REDUCE + GATHER :])
    halves.start()
    reduce_phase(place, sender, partial, scratch[:REDUCE])
    total, own = scratch[4], scratch[REDUCE]
    rows, width = total.shape

    def body(at):
        value = total[at]
        scale = lax.rsqrt(jnp.sum(value * value, axis=1, keepdims=True) / width + EPS)
        result = tokens[at].astype(F32) + value * scale * gain[...]
        branch[at] = value
        hidden[at] = result
        own[at] = result.astype(BF)

    by_rows(rows, body)
    gather_phase(place, sender, gathered, scratch[REDUCE : REDUCE + GATHER])
    halves.finish()
    sender.drain()


def turn_kernel(partial, hidden, cotangent, gain, gathered, outputs, gain_grad, *scratch):
    place = Place()
    sender = Sender()
    greet(place)
    reduce_phase(place, sender, partial, scratch[:REDUCE])
    total, own = scratch[4], scratch[REDUCE]
    out_own = scratch[REDUCE + GATHER]
    rows, width = total.shape
    gain_grad[...] = jnp.zeros_like(gain_grad)

    def body(at):
        value = total[at]
        scale = lax.rsqrt(jnp.sum(value * value, axis=1, keepdims=True) / width + EPS)
        grads = cotangent[at].astype(F32)
        normed = value * scale
        out_own[at] = (hidden[at] + normed * gain[...]).astype(BF)
        gain_grad[...] += jnp.sum(grads * normed, axis=0, keepdims=True)
        gained = gain[...] * grads
        inner = jnp.sum(normed * gained, axis=1, keepdims=True)
        own[at] = (scale * (gained - normed * (inner / width))).astype(BF)

    by_rows(rows, body)
    finish = pair_phase(place, sender, out_own, outputs, scratch[REDUCE + GATHER + 1 :])
    gather_phase(place, sender, gathered, scratch[REDUCE : REDUCE + GATHER])
    finish()
    sender.drain()


def branch_kernel(
    partial,
    branch,
    cotangent,
    gain,
    pair_grad,
    down_grad,
    gathered,
    grad_hidden,
    gain_grad,
    pair_other,
    down_other,
    *scratch,
):
    place = Place()
    sender = Sender()
    greet(place, True)
    (side_sem,) = scratch[REDUCE + GATHER :]
    count = down_other.shape[0]
    rows_out = pl.ds(pl.multiple_of((1 - place.side) * count, count), count)
    sources = (pair_grad.at[:, 1 - place.side], down_grad.at[rows_out])
    crossings = [
        remote(source, target, side_sem.at[0, index], side_sem.at[1, index], place.across())
        for index, (source, target) in enumerate(zip(sources, (pair_other, down_other)))
    ]
    for crossing in crossings:
        crossing.start()
    reduce_phase(place, sender, partial, scratch[:REDUCE])
    total, own = scratch[4], scratch[REDUCE]
    rows, width = total.shape
    gain_grad[...] = jnp.zeros_like(gain_grad)

    def body(at):
        value = branch[at]
        scale = lax.rsqrt(jnp.sum(value * value, axis=1, keepdims=True) / width + EPS)
        grads = cotangent[at].astype(F32) + total[at]
        grad_hidden[at] = grads
        normed = value * scale
        gain_grad[...] += jnp.sum(grads * normed, axis=0, keepdims=True)
        gained = gain[...] * grads
        inner = jnp.sum(normed * gained, axis=1, keepdims=True)
        own[at] = (scale * (gained - normed * (inner / width))).astype(BF)

    by_rows(rows, body)
    gather_phase(place, sender, gathered, scratch[REDUCE : REDUCE + GATHER])
    for crossing in crossings:
        crossing.wait()
    sender.drain()


def last_kernel(
    partial,
    grad_hidden,
    qkv,
    out,
    small,
    result,
    qkv_all,
    out_all,
    small_all,
    *scratch,
):
    place = Place()
    sender = Sender()
    parts = scratch[REDUCE + 1 :]
    swap_sems, parts = parts[:3], parts[3:]
    qkv_own, qkv_other, out_own, out_other, small_own, small_other, fetch_sem, side_sem = parts
    greet_all(place)
    fetches, crossings = [], []
    for index, (grad, own, other) in enumerate(
        ((qkv, qkv_own, qkv_other), (out, out_own, out_other))
    ):
        fetches.append(
            pltpu.make_async_copy(grad.at[:, place.side], own, fetch_sem.at[index])
        )
        crossings.append(
            remote(
                grad.at[:, 1 - place.side],
                other,
                side_sem.at[0, index],
                side_sem.at[1, index],
                place.across(),
            )
        )
    crossings.append(
        remote(
            small,
            small_other,
            side_sem.at[0, 2],
            side_sem.at[1, 2],
            place.at(place.z, place.y, 1 - place.core),
        )
    )
    for copy in fetches + crossings:
        copy.start()
    pairs = ((small_own, small_all), (qkv_own, qkv_all), (out_own, out_all))
    swap = Swap(place, [whole_pair(*pair) for pair in pairs], swap_sems)
    shared_rows = 2 * partial.shape[1] // place.count // 128

    def between():
        for fetch in fetches:
            fetch.wait()
        for crossing in crossings:
            crossing.wait()
        small_own[...] = small[...]
        small_own[:, :shared_rows] += small_other[:, :shared_rows]

        def one(index, carry):
            qkv_own[index] = (
                qkv_own[index].astype(F32) + qkv_other[index].astype(F32)
            ).astype(BF)
            out_own[index] = (
                out_own[index].astype(F32) + out_other[index].astype(F32)
            ).astype(BF)
            return carry

        lax.fori_loop(0, place.count, one, 0)
        swap.start()

    reduce_phase(place, sender, partial, scratch[:REDUCE], between)
    total = scratch[4]

    def body(at):
        total[at] += grad_hidden[at]

    by_rows(total.shape[0], body)
    finish = pair_phase(place, sender, total, result, scratch[REDUCE : REDUCE + 1])
    swap.pass_on()
    finish()
    swap.finish()
    sender.drain()


def sum_kernel(carried, value, *rest):
    if carried:
        moved, result, arrived, core_in, y_in, held, line_in, sem, side_sem = rest
    else:
        result, core_in, y_in, held, line_in, sem = rest
    place = Place()
    z, y, core = place.z, place.y, place.core
    barrier = pltpu.get_barrier_semaphore()
    others = [place.at(z, y, 1 - core), place.at(z, 1 - y, core)]
    others += [place.at(lax.rem(z + k, LINE), y, core) for k in range(1, LINE)]
    for device in others + [place.across()] * carried:
        signal(barrier, device)
    pl.semaphore_wait(barrier, len(others) + carried)
    if carried:
        side = remote(moved, arrived, side_sem.at[0], side_sem.at[1], place.across())
        side.start()
    first = remote(value, core_in, sem.at[0, 0], sem.at[1, 0], others[0])
    first.start()
    first.wait_recv()
    held[0] = value[...] + core_in[...]
    second = remote(held.at[0], y_in, sem.at[0, 1], sem.at[1, 1], others[1])
    second.start()
    second.wait_recv()
    held[1] = held[0] + y_in[...]
    sends = [
        remote(held.at[1], line_in.at[k - 1], sem.at[0, 1 + k], sem.at[1, 1 + k], others[1 + k])
        for k in range(1, LINE)
    ]
    for send in sends:
        send.start()
    line_in[LINE - 1] = held[1]
    for send in sends:
        send.wait_recv()
    added = jnp.zeros_like(value)
    for source in range(LINE):
        slot = lax.rem(z - source + 2 * LINE - 1, LINE)
        added = added + line_in[slot]
    result[...] = added
    first.wait_send()
    second.wait_send()
    for send in sends:
        send.wait_send()
    if carried:
        side.wait()


def pack_kernel(side, gate, up, down, pair_out, down_out):
    columns = gate.shape[1]
    pair_out[0, :, :columns] = gate[...]
    pair_out[0, :, columns:] = up[...]
    down_out[0] = down[...]


def talk(kernel, which, shapes, specs, scratch, microseconds, name=None):
    def call(*operands):
        return pl.pallas_call(
            kernel,
            out_shape=shapes,
            in_specs=specs[0],
            out_specs=specs[1],
            scratch_shapes=scratch,
            compiler_params=pltpu.CompilerParams(
                collective_id=which, has_side_effects=True, vmem_limit_bytes=48 << 20
            ),
            cost_estimate=pl.CostEstimate(
                flops=0, bytes_accessed=int(microseconds * 3.0e6), transcendentals=0
            ),
            name=name or kernel.__name__,
        )(*operands)

    return call


class Team:
    def __init__(self, local_heads, rows, width):
        self.fsdp = lax.axis_size("fsdp")
        self.tensor = lax.axis_size("tensor")
        self.size = 2 * LINE
        self.teams = self.fsdp // self.size
        assert self.fsdp % self.size == 0 and self.tensor == 2 and local_heads % self.size == 0
        self.member = lax.rem(lax.axis_index("fsdp"), self.size)
        self.core = lax.axis_index("tensor")
        self.context = lax.axis_index("context")
        self.groups = None
        if self.teams > 1:
            self.groups = [
                [team * self.size + one for one in range(self.size)] for team in range(self.teams)
            ]
        self.rows = rows
        self.width = width
        self.all_low = jax.ShapeDtypeStruct((2 * self.size * rows, width), BF)
        self.own_wide = jax.ShapeDtypeStruct((rows, width), F32)
        self.line_wide = jax.ShapeDtypeStruct((1, width), F32)
        self.reduces = reduce_scratch(rows, width)
        self.gathers = gather_scratch(rows, width)

    def whole(self, pieces):
        shape = (pieces.shape[0], 2) + pieces.shape[1:]
        return jax.ShapeDtypeStruct(shape, pieces.dtype)

    def first(self, own, weights, out, small):
        rows, columns = weights[0].shape
        rows, columns = rows // 2, columns // self.size
        out_rows = out.shape[0] // self.size // 2
        return talk(
            first_kernel,
            0,
            (
                self.all_low,
                jax.ShapeDtypeStruct((self.fsdp, 2, rows, 3 * columns), BF),
                jax.ShapeDtypeStruct((self.fsdp, 2, out_rows, out.shape[1]), BF),
                jax.ShapeDtypeStruct((self.fsdp, 2) + small.shape, F32),
            ),
            ([VMEM] * 6, (HBM,) * 4),
            self.gathers + swap_scratch(self.fsdp, 5),
            80,
        )(own, *weights, out, small)

    def pack(self, gate, up, down):
        rows, columns = gate.shape
        rows, columns = rows // 2, columns // self.size
        down_rows, down_columns = down.shape
        down_rows = down_rows // self.size // 2

        def column_spec():
            return pl.BlockSpec((rows, columns), lambda d, side: (side[0], d))

        def piece_spec(*shape):
            return pl.BlockSpec((1,) + shape, lambda d, side: (d, 0, 0))

        pair, low = pl.pallas_call(
            pack_kernel,
            grid_spec=pltpu.PrefetchScalarGridSpec(
                num_scalar_prefetch=1,
                grid=(self.size,),
                in_specs=[
                    column_spec(),
                    column_spec(),
                    pl.BlockSpec((down_rows, down_columns), lambda d, side: (2 * d + side[0], 0)),
                ],
                out_specs=[piece_spec(rows, 2 * columns), piece_spec(down_rows, down_columns)],
            ),
            out_shape=[
                jax.ShapeDtypeStruct((self.size, rows, 2 * columns), BF),
                jax.ShapeDtypeStruct((self.size, down_rows, down_columns), BF),
            ],
            name="pack_kernel",
        )(self.context.reshape(1).astype(jnp.int32), gate, up, down)
        return self.repeat(pair), self.repeat(low)

    def hidden(self, partial, tokens, gain, pair, down):
        return talk(
            hidden_kernel,
            1,
            (self.all_low, self.own_wide, self.own_wide, self.whole(pair), self.whole(down)),
            ([HBM, VMEM, VMEM, VMEM, VMEM], (HBM, VMEM, VMEM, HBM, HBM)),
            self.reduces + self.gathers + halves_scratch(2),
            100,
        )(partial, tokens, gain, pair, down)

    def turn(self, partial, hidden, cotangent, gain):
        pair = jax.ShapeDtypeStruct((2 * self.rows, self.width), BF)
        return talk(
            turn_kernel,
            2,
            (self.all_low, pair, self.line_wide),
            ([HBM, VMEM, VMEM, VMEM], (HBM, HBM, VMEM)),
            self.reduces + self.gathers + [pltpu.VMEM((self.rows, self.width), BF)] + pair_scratch(),
            100,
        )(partial, hidden, cotangent, gain)

    def branch(self, partial, branch, cotangent, gain, pair_grad, down_grad):
        shape = pair_grad.shape
        pair_other = jax.ShapeDtypeStruct((shape[0],) + shape[2:], BF)
        down_other = jax.ShapeDtypeStruct((down_grad.shape[0] // 2, down_grad.shape[1]), BF)
        return talk(
            branch_kernel,
            3,
            (self.all_low, self.own_wide, self.line_wide, pair_other, down_other),
            ([HBM, VMEM, VMEM, VMEM, HBM, HBM], (HBM, VMEM, VMEM, HBM, HBM)),
            self.reduces + self.gathers + [DMA((2, 2))],
            100,
        )(partial, branch, cotangent, gain, pair_grad, down_grad)

    def last(self, partial, grad_hidden, qkv, out, small):
        both = jax.ShapeDtypeStruct((2 * self.rows, self.width), F32)

        def same(array):
            return jax.ShapeDtypeStruct(array.shape, array.dtype)

        def half(array):
            return pltpu.VMEM((array.shape[0],) + array.shape[2:], array.dtype)

        held = pltpu.VMEM(small.shape, small.dtype)
        return talk(
            last_kernel,
            4,
            (both, same(qkv), same(out), self.whole(small)),
            ([HBM, VMEM, HBM, HBM, VMEM], (HBM,) * 4),
            self.reduces
            + pair_scratch()
            + swap_scratch(self.fsdp, 3)
            + [half(qkv), half(qkv), half(out), half(out), held, held, DMA((2,)), DMA((2, 3))],
            80,
        )(partial, grad_hidden, qkv, out, small)

    def total(self, values, moved=None):
        flat = values.reshape(-1, 128)
        carried = int(moved is not None)
        shape = jax.ShapeDtypeStruct(flat.shape, F32)
        scratch = [pltpu.VMEM(flat.shape, F32)] * 2
        scratch += [pltpu.VMEM((2,) + flat.shape, F32), pltpu.VMEM((LINE,) + flat.shape, F32)]
        scratch += [DMA((2, LINE + 1))] + [DMA((2,))] * carried
        which = 5 + self.sums
        self.sums += 1
        kernel = functools.partial(sum_kernel, carried)
        if not carried:
            call = talk(kernel, which, shape, ([VMEM], VMEM), scratch, 10, "sum_kernel")
            return call(flat).reshape(values.shape)
        shapes = (shape, jax.ShapeDtypeStruct(moved.shape, moved.dtype))
        call = talk(kernel, which, shapes, ([VMEM] * 2, (VMEM,) * 2), scratch, 10, "sum_kernel")
        total, came = call(flat, moved)
        return total.reshape(values.shape), came

    sums = 0

    def half(self, array, axis):
        count = array.shape[axis] // 2
        return lax.dynamic_slice_in_dim(array, self.context * count, count, axis)

    def swap(self, pieces):
        return lax.all_to_all(pieces, "fsdp", split_axis=0, concat_axis=0, tiled=True)

    def repeat(self, pieces):
        return jnp.concatenate([pieces] * self.teams, axis=0) if self.teams > 1 else pieces

    def both_sides(self, half):
        other = lax.ppermute(half, "context", [(0, 1), (1, 0)])
        low = jnp.where(self.context == 0, half, other)
        high = jnp.where(self.context == 0, other, half)
        return jnp.stack([low, high], axis=1)

    def columns_whole(self, came):
        return came.reshape(-1, came.shape[-1])

    def rows_whole(self, came):
        fsdp, two, rows, columns = came.shape
        return came.transpose(1, 2, 0, 3).reshape(two * rows, fsdp * columns)

    def of_columns(self, grad):
        rows, columns = grad.shape
        return grad.astype(BF).reshape(self.fsdp, 2, rows // self.fsdp // 2, columns)

    def of_rows(self, grad):
        rows, columns = grad.shape
        cut = grad.astype(BF).reshape(2, rows // 2, self.fsdp, columns // self.fsdp)
        return cut.transpose(2, 0, 1, 3)

    def added(self, came):
        if self.teams == 1:
            return came.astype(F32)
        came = came.reshape((self.teams, self.size) + came.shape[1:])
        return jnp.sum(came.astype(F32), axis=0)

    def columns_out(self, came, count):
        size, two, rows, columns = came.shape
        return [
            self.added(part.reshape(size, two * rows, -1))
            .transpose(1, 0, 2)
            .reshape(two * rows, -1)
            for part in jnp.split(came, count, axis=3)
        ]

    def rows_out(self, came):
        return self.added(came).reshape(-1, came.shape[-1])


def local(
    tokens,
    cont_lengths,
    w_query,
    w_key,
    w_value,
    w_output,
    query_gain,
    key_gain,
    attn_gain,
    w_gate,
    w_up,
    w_down,
    mlp_gain,
    cotangent,
):
    rows = tokens.shape[0]
    width = tokens.shape[1]
    fsdp = lax.axis_size("fsdp")
    tensor = lax.axis_size("tensor")
    local_heads = query_gain.shape[0]
    head_size = w_query.shape[1] // local_heads
    own_rows = rows // tensor
    team = Team(local_heads, own_rows, width)
    groups = team.size
    team_rows = groups * rows
    heads = local_heads // team.size
    later = lax.axis_index("context") == 1

    tokens_own = lax.dynamic_slice_in_dim(tokens, team.core * own_rows, own_rows, 0)
    grad_out = lax.dynamic_slice_in_dim(cotangent, team.core * own_rows, own_rows, 0)
    cut = query_gain.size
    share = attn_gain.size
    small = [query_gain.reshape(-1), key_gain.reshape(-1), attn_gain, mlp_gain]
    small = jnp.concatenate([one.astype(F32) for one in small + [cont_lengths.reshape(-1)]])
    small = jnp.pad(small, (0, 8 * 128 - small.size)).reshape(8, 128)
    tokens_all, qkv_came, output_came, small_came = team.first(
        tokens_own, [w_query, w_key, w_value], w_output, small
    )
    qkv_w = team.columns_whole(qkv_came)
    output_w = team.rows_whole(output_came)
    all_small = small_came[:, 0].reshape(fsdp, -1)
    query_gains = all_small[:, :cut].reshape(fsdp, local_heads, -1)
    key_gains = all_small[:, cut : 2 * cut].reshape(fsdp, local_heads, -1)
    query_gains = query_gains.transpose(1, 0, 2).reshape(local_heads, head_size)
    key_gains = key_gains.transpose(1, 0, 2).reshape(local_heads, head_size)
    flat_query = lax.dynamic_slice_in_dim(query_gains, team.member * heads, heads, 0).reshape(-1)
    flat_key = lax.dynamic_slice_in_dim(key_gains, team.member * heads, heads, 0).reshape(-1)
    gain_attn = all_small[:, 2 * cut : 2 * cut + share].reshape(1, -1)
    gain_mlp = all_small[:, 2 * cut + share : 2 * cut + 2 * share].reshape(1, -1)

    conts = cont_lengths.shape[1]
    lengths = all_small[:, 2 * cut + 2 * share : 2 * cut + 2 * share + conts].astype(jnp.int32)
    first_group = lax.axis_index("fsdp") - team.member
    lengths = lax.dynamic_slice_in_dim(lengths, first_group, groups, 0)
    segment, offset = jax.vmap(lambda one: layout(one, rows))(lengths)
    row_index = jnp.arange(rows, dtype=jnp.int32)
    positions = jnp.where(later, rows + offset, row_index[None, :])
    own_segment = jnp.where(later, segment, -1)
    cosine, sine = rotary_tables(positions, head_size)
    cosine = cosine[:, :, None, :]
    sine = sine[:, :, None, :]

    pair_mine, down_mine, tokens_all = lax.optimization_barrier(
        team.pack(w_gate, w_up, w_down) + (tokens_all,)
    )
    pair_came = team.swap(pair_mine)
    down_came = team.swap(down_mine)

    by_head = (groups, rows, heads, head_size)
    raw = product(tokens_all, qkv_w)
    query_raw, key_raw, value_raw = jnp.split(raw, 3, axis=1)
    value_low = value_raw.astype(BF)
    sums, sent_value = team.total(
        jnp.stack([jnp.sum(query_raw * query_raw, axis=1), jnp.sum(key_raw * key_raw, axis=1)]),
        value_low,
    )
    value_low, sent_value = value_low.reshape(by_head), sent_value.reshape(by_head)
    scale_query = lax.rsqrt(sums[0] / width + EPS)[:, None]
    scale_key = lax.rsqrt(sums[1] / width + EPS)[:, None]
    query_norm = query_raw * scale_query * flat_query
    key_norm = key_raw * scale_key * flat_key
    query_low = rotate(query_norm.reshape(by_head), cosine, sine).astype(BF)
    key_low = rotate(key_norm.reshape(by_head), cosine, sine).astype(BF)
    sent_key = lax.ppermute(key_low, "context", [(0, 1)])
    keys_all = jnp.concatenate([sent_key, key_low], axis=1)
    values_all = jnp.concatenate([sent_value, value_low], axis=1)
    key_index = jnp.arange(2 * rows, dtype=jnp.int32)
    key_segment = jnp.concatenate([jnp.full((groups, rows), -2, jnp.int32), own_segment], axis=1)
    remote = (key_index < rows)[None, None, :] & later
    own_keys = (
        (key_index >= rows)[None, None, :]
        & (key_index[None, None, :] - rows <= row_index[None, :, None])
        & (key_segment[:, None, :] == own_segment[:, :, None])
    )
    allowed = (remote | own_keys)[:, None]
    scale = 1.0 / math.sqrt(head_size)
    scores = (
        jnp.einsum("gqhd,gkhd->ghqk", query_low, keys_all, preferred_element_type=F32) * scale
    )
    scores = jnp.where(allowed, scores, -1e30)
    highest = jnp.max(scores, axis=-1, keepdims=True)
    weights = jnp.exp(scores - highest)
    probs = weights / jnp.sum(weights, axis=-1, keepdims=True)
    probs_low = probs.astype(BF)
    mixed = jnp.einsum("ghqk,gkhd->gqhd", probs_low, values_all, preferred_element_type=F32)
    attended_low = mixed.reshape(team_rows, heads * head_size).astype(BF)
    hidden_all, attn_sum, hidden, pair_came, down_came = team.hidden(
        product(attended_low, output_w).astype(BF), tokens_own, gain_attn, pair_came, down_came
    )
    pair_w = team.columns_whole(pair_came)
    down_w = team.rows_whole(down_came)

    gate, upward = jnp.split(product(hidden_all, pair_w), 2, axis=1)
    sigma = jax.nn.sigmoid(gate)
    inner_low = (gate * sigma * upward).astype(BF)
    grad_mlp_all, outputs, grad_mlp_gain = team.turn(
        product(inner_low, down_w).astype(BF), hidden, grad_out, gain_mlp
    )
    down_grad = product_left(inner_low, grad_mlp_all).astype(BF)
    grad_inner = product_right(grad_mlp_all, down_w)
    grad_gate_low = (grad_inner * upward * sigma * (1.0 + gate * (1.0 - sigma))).astype(BF)
    grad_up_low = (grad_inner * gate * sigma).astype(BF)
    grad_pair = jnp.concatenate([grad_gate_low, grad_up_low], axis=1)
    pair_grad = team.of_columns(product_left(hidden_all, grad_pair))
    grad_branch_all, grad_hidden, grad_attn_gain, pair_other, down_other = team.branch(
        product_right(grad_pair, pair_w).astype(BF),
        attn_sum,
        grad_out,
        gain_attn,
        pair_grad,
        down_grad,
    )
    pair_mine = lax.dynamic_index_in_dim(pair_grad, team.context, 1, keepdims=False)
    pair_mine = (pair_mine.astype(F32) + pair_other.astype(F32)).astype(BF)
    down_mine = (team.half(down_grad, 0).astype(F32) + down_other.astype(F32)).astype(BF)
    down_mine = down_mine.reshape(down_mine.shape[0], fsdp, -1).transpose(1, 0, 2)
    pair_came = team.swap(pair_mine)
    down_came = team.swap(down_mine)
    output_grad = team.of_rows(product_left(attended_low, grad_branch_all))
    grad_attended = product_right(grad_branch_all, output_w).astype(BF).reshape(by_head)

    grad_probs = jnp.einsum("gqhd,gkhd->ghqk", grad_attended, values_all, preferred_element_type=F32)
    centre = jnp.sum(probs * grad_probs, axis=-1, keepdims=True)
    grad_scores = (probs * (grad_probs - centre)).astype(BF)
    grad_query_rot = (
        jnp.einsum("ghqk,gkhd->gqhd", grad_scores, keys_all, preferred_element_type=F32) * scale
    )
    grad_keys = (
        jnp.einsum("ghqk,gqhd->gkhd", grad_scores, query_low, preferred_element_type=F32) * scale
    )
    grad_values = jnp.einsum("ghqk,gqhd->gkhd", probs_low, grad_attended, preferred_element_type=F32)
    back_value = lax.ppermute(grad_values[:, :rows].astype(BF), "context", [(1, 0)])
    back_key = lax.ppermute(grad_keys[:, :rows].astype(BF), "context", [(1, 0)])
    grad_key_rot = grad_keys[:, rows:] + back_key.astype(F32)
    grad_value_low = (
        (grad_values[:, rows:] + back_value.astype(F32)).reshape(team_rows, -1).astype(BF)
    )
    grad_query_norm = rotate_back(grad_query_rot, cosine, sine).reshape(team_rows, -1)
    grad_key_norm = rotate_back(grad_key_rot, cosine, sine).reshape(team_rows, -1)
    grad_query_gain = jnp.sum(grad_query_norm * query_raw * scale_query, axis=0)
    grad_key_gain = jnp.sum(grad_key_norm * key_raw * scale_key, axis=0)
    totals = team.total(
        jnp.stack(
            [
                jnp.sum(query_raw * flat_query * grad_query_norm, axis=1),
                jnp.sum(key_raw * flat_key * grad_key_norm, axis=1),
            ]
        )
    )
    grad_query_low = norm_back(
        query_raw, scale_query, flat_query, grad_query_norm, totals[0][:, None], width
    ).astype(BF)
    grad_key_low = norm_back(
        key_raw, scale_key, flat_key, grad_key_norm, totals[1][:, None], width
    ).astype(BF)
    grad_qkv = jnp.concatenate([grad_query_low, grad_key_low, grad_value_low], axis=1)
    qkv_grad = team.of_columns(product_left(tokens_all, grad_qkv))
    head_share = head_size // fsdp
    small = [
        grad_attn_gain.reshape(fsdp, share),
        grad_mlp_gain.reshape(fsdp, share),
        grad_query_gain.reshape(heads, fsdp, head_share).transpose(1, 0, 2).reshape(fsdp, -1),
        grad_key_gain.reshape(heads, fsdp, head_share).transpose(1, 0, 2).reshape(fsdp, -1),
    ]
    used = 2 * share + 2 * heads * head_share
    small = jnp.concatenate(small + [jnp.zeros((fsdp, 8 * 128 - used), F32)], axis=1)
    pair_came = team.both_sides(pair_came)
    down_came = team.both_sides(down_came)
    input_grad, qkv_came, output_came, small_came = team.last(
        product_right(grad_qkv, qkv_w).astype(BF),
        grad_hidden,
        qkv_grad,
        output_grad,
        small.reshape(fsdp, 8, 128),
    )
    grad_w_query, grad_w_key, grad_w_value = team.columns_out(qkv_came, 3)
    grad_w_gate, grad_w_up = team.columns_out(pair_came, 2)
    grad_w_output = team.rows_out(output_came)
    grad_w_down = team.rows_out(down_came)
    came = jnp.sum(small_came, axis=1).reshape(fsdp, -1)
    row_gains = jnp.sum(came[:, : 2 * share], axis=0).reshape(2, share)
    head_gains = team.added(came[:, 2 * share : used]).reshape(team.size, 2, heads, head_share)
    head_gains = head_gains.transpose(1, 0, 2, 3).reshape(2, local_heads, head_share)
    return (
        outputs,
        input_grad,
        grad_w_query,
        grad_w_key,
        grad_w_value,
        grad_w_output,
        head_gains[0],
        head_gains[1],
        row_gains[0],
        grad_w_gate,
        grad_w_up,
        grad_w_down,
        row_gains[1],
    )


def solution(mesh):
    return jax.shard_map(
        local,
        mesh=mesh,
        in_specs=(
            P(("fsdp", "context"), None),
            P("fsdp", None),
            P("fsdp", "tensor"),
            P("fsdp", "tensor"),
            P("fsdp", "tensor"),
            P("tensor", "fsdp"),
            P("tensor", "fsdp"),
            P("tensor", "fsdp"),
            P("fsdp"),
            P("fsdp", "tensor"),
            P("fsdp", "tensor"),
            P("tensor", "fsdp"),
            P("fsdp"),
            P(("fsdp", "context"), None),
        ),
        out_specs=(
            P(("fsdp", "context"), None),
            P(("fsdp", "context"), None),
            P("fsdp", "tensor"),
            P("fsdp", "tensor"),
            P("fsdp", "tensor"),
            P("tensor", "fsdp"),
            P("tensor", "fsdp"),
            P("tensor", "fsdp"),
            P("fsdp"),
            P("fsdp", "tensor"),
            P("fsdp", "tensor"),
            P("tensor", "fsdp"),
            P("fsdp"),
        ),
        check_vma=False,
    )
```

```python
import functools
import math

import jax
import jax.numpy as jnp
from jax import lax
from jax.experimental import pallas as pl
from jax.experimental.pallas import tpu as pltpu
from jax.sharding import PartitionSpec as P

EPS = 1e-06
THETA = 500000.0
BF = jnp.bfloat16
F32 = jnp.float32


def product(left, right):
    return jnp.dot(left, right, preferred_element_type=F32)


def product_left(left, right):
    return jnp.einsum("rd,rf->df", left, right, preferred_element_type=F32)


def product_right(left, right):
    return jnp.einsum("rf,df->rd", left, right, preferred_element_type=F32)


def rotary_tables(positions, head_size):
    half = head_size // 2
    inverse = jnp.exp(-(2.0 * jnp.arange(half, dtype=F32) / head_size) * math.log(THETA))
    angles = positions.astype(F32)[..., None] * inverse
    angles = jnp.concatenate([angles, angles], axis=-1)
    return (jnp.cos(angles), jnp.sin(angles))


def rotate(values, cosine, sine):
    half = values.shape[-1] // 2
    turned = jnp.concatenate([-values[..., half:], values[..., :half]], axis=-1)
    return values * cosine + turned * sine


def rotate_back(grads, cosine, sine):
    half = grads.shape[-1] // 2
    scaled = grads * sine
    turned = jnp.concatenate([scaled[..., half:], -scaled[..., :half]], axis=-1)
    return grads * cosine + turned


def norm_back(values, scale, gain, grads, total, width):
    return scale * gain * grads - values * scale * scale * scale * (total / width)


def layout(lengths, rows):
    segment_ends = jnp.cumsum(lengths)
    segment_starts = segment_ends - lengths
    row_index = jnp.arange(rows, dtype=jnp.int32)
    segment = jnp.sum((row_index[:, None] >= segment_ends[None, :]).astype(jnp.int32), axis=1)
    chosen = segment[:, None] == jnp.arange(lengths.shape[0], dtype=jnp.int32)[None, :]
    offset = row_index - jnp.sum(jnp.where(chosen, segment_starts[None, :], 0), axis=1)
    return (segment, offset)


LINE = 4
CHUNK = 16
MESH_ID = pl.DeviceIdType.MESH
HBM = pl.BlockSpec(memory_space=pl.ANY)
VMEM = pl.BlockSpec(memory_space=pltpu.VMEM)
DMA = pltpu.SemaphoreType.DMA


class Place:
    def __init__(self):
        device = lax.axis_index("fsdp")
        member = lax.rem(device, 2 * LINE)
        self.base = device - member
        self.z = member // 2
        self.y = lax.rem(member, 2)
        self.core = lax.axis_index("tensor")
        self.side = lax.axis_index("context")
        self.device = device
        self.count = lax.axis_size("fsdp")

    def across(self):
        return {"context": 1 - self.side}

    def at(self, z, y, core):
        return {"fsdp": self.base + 2 * z + y, "tensor": core}

    def near(self):
        yield None, self.at(self.z, self.y, 1 - self.core)
        yield None, self.at(self.z, 1 - self.y, self.core)
        yield self.z > 0, self.at(self.z - 1, self.y, self.core)
        yield self.z < LINE - 1, self.at(self.z + 1, self.y, self.core)

    def rows(self, z, y, core, count):
        start = ((2 * z + y) * 2 + core) * count
        return pl.ds(pl.multiple_of(start, count), count)


def guarded(condition, action):
    if condition is None:
        action()
    else:
        pl.when(condition)(action)


def signal(barrier, device):
    pl.semaphore_signal(barrier, inc=1, device_id=device, device_id_type=MESH_ID)


def greet(place, across=False):
    barrier = pltpu.get_barrier_semaphore()
    for condition, device in place.near():
        guarded(condition, functools.partial(signal, barrier, device))
    if across:
        signal(barrier, place.across())
    inside = (place.z > 0) & (place.z < LINE - 1)
    pl.semaphore_wait(barrier, jnp.where(inside, 4, 3) + int(across))


def greet_all(place):
    barrier = pltpu.get_barrier_semaphore()

    def one(step, carry):
        signal(barrier, {"fsdp": lax.rem(place.device + step, place.count)})
        return carry

    lax.fori_loop(1, place.count, one, 0)
    signal(barrier, place.across())
    signal(barrier, place.at(place.z, place.y, 1 - place.core))
    pl.semaphore_wait(barrier, place.count + 1)


class Sender:
    def __init__(self):
        self.sent = []

    def __call__(self, condition, make):
        def start():
            make().start()

        guarded(condition, start)
        self.sent.append((condition, make))

    def drain(self):
        for condition, make in self.sent:

            def wait(make=make):
                make().wait_send()

            guarded(condition, wait)


def remote(source, target, send, receive, device):
    return pltpu.make_async_remote_copy(
        src_ref=source,
        dst_ref=target,
        send_sem=send,
        recv_sem=receive,
        device_id=device,
        device_id_type=MESH_ID,
    )


def by_rows(rows, body):
    def step(index, carry):
        body(pl.ds(pl.multiple_of(index * CHUNK, CHUNK), CHUNK))
        return carry

    lax.fori_loop(0, rows // CHUNK, step, 0)


def reduce_scratch(rows, width):
    return [
        pltpu.VMEM((2 * LINE, rows, width), BF),
        pltpu.VMEM((2 * LINE, rows, width), BF),
        pltpu.VMEM((LINE, rows, width), BF),
        pltpu.VMEM((LINE + 1, rows, width), BF),
        pltpu.VMEM((rows, width), F32),
        DMA((2 * LINE,)),
        DMA((2, 2 * LINE)),
        DMA((2, LINE)),
        DMA((2, LINE + 1)),
    ]


def reduce_phase(place, sender, partial, scratch, between=None):
    mine, core_in, y_in, line_in, total, local_sem, core_sem, y_sem, line_sem = scratch
    rows = total.shape[0]
    z, y, core = place.z, place.y, place.core
    low = z < LINE // 2
    order = []
    for k in range(LINE - 1):
        down = LINE - 1 - k
        down = jnp.where(down <= z, down - 1, down)
        up = jnp.where(k >= z, k + 1, k)
        order.append(jnp.where(low, down, up))
    order.append(z)

    def fetch(slot):
        half = lax.rem(slot, 2)
        return pltpu.make_async_copy(
            partial.at[place.rows(slot // 2, half, core, rows)], mine.at[slot], local_sem.at[slot]
        )

    def to_core(slot):
        half = lax.rem(slot, 2)
        return remote(
            partial.at[place.rows(slot // 2, half, 1 - core, rows)],
            core_in.at[slot],
            core_sem.at[0, slot],
            core_sem.at[1, slot],
            place.at(z, y, 1 - core),
        )

    def to_y(block):
        return remote(
            mine.at[2 * block + 1 - y],
            y_in.at[block],
            y_sem.at[0, block],
            y_sem.at[1, block],
            place.at(z, 1 - y, core),
        )

    def to_line(block):
        step = jnp.where(block > z, 1, -1)
        slot = jnp.where((step < 0) & (block == z - 1), LINE, block)
        return remote(
            mine.at[2 * block + y],
            line_in.at[slot],
            line_sem.at[0, block],
            line_sem.at[1, slot],
            place.at(z + step, y, core),
        )

    def from_line(slot):
        return remote(
            mine.at[0],
            line_in.at[slot],
            line_sem.at[0, 0],
            line_sem.at[1, slot],
            place.at(z, y, 1 - core),
        )

    for half in (1 - y, y):
        for block in order:
            sender(None, functools.partial(to_core, 2 * block + half))
            fetch(2 * block + half).start()

    for block in order:
        slot = 2 * block + 1 - y
        fetch(slot).wait()
        to_core(slot).wait_recv()

        def add(at, slot=slot):
            value = mine[slot, at].astype(F32) + core_in[slot, at].astype(F32)
            mine[slot, at] = value.astype(BF)

        by_rows(rows, add)
        sender(None, functools.partial(to_y, block))

    for number, block in enumerate(order[:-1]):
        if number == LINE - 2 and between is not None:
            between()
        slot = 2 * block + y
        fetch(slot).wait()
        to_core(slot).wait_recv()
        to_y(block).wait_recv()
        inner = jnp.where(block > z, z > 0, z < LINE - 1)

        @pl.when(inner)
        def _(block=block, slot=slot):
            from_line(block).wait_recv()

            def add(at):
                value = mine[slot, at].astype(F32) + core_in[slot, at].astype(F32)
                value = value + y_in[block, at].astype(F32)
                mine[slot, at] = (value + line_in[block, at].astype(F32)).astype(BF)

            by_rows(rows, add)

        @pl.when(jnp.logical_not(inner))
        def _(block=block, slot=slot):
            def add(at):
                value = mine[slot, at].astype(F32) + core_in[slot, at].astype(F32)
                mine[slot, at] = (value + y_in[block, at].astype(F32)).astype(BF)

            by_rows(rows, add)

        sender(None, functools.partial(to_line, block))

    slot = 2 * z + y
    fetch(slot).wait()
    to_core(slot).wait_recv()
    to_y(z).wait_recv()

    def start(at):
        value = mine[slot, at].astype(F32) + core_in[slot, at].astype(F32)
        total[at] = value + y_in[z, at].astype(F32)

    by_rows(rows, start)
    for condition, source in ((z > 0, z), (z < LINE - 1, LINE)):

        @pl.when(condition)
        def _(source=source):
            from_line(source).wait_recv()

            def add(at):
                total[at] += line_in[source, at].astype(F32)

            by_rows(rows, add)


def gather_scratch(rows, width):
    return [
        pltpu.VMEM((rows, width), BF),
        DMA((1,)),
        DMA((2, 2 * LINE)),
        DMA((2, LINE)),
        DMA((2, LINE + 2)),
    ]


def gather_phase(place, sender, gathered, scratch, between=None, later=None):
    own, local_sem, core_sem, y_sem, line_sem = scratch
    rows = own.shape[0]
    z, y, core = place.z, place.y, place.core

    def spot(block, half):
        return gathered.at[place.rows(block, half, core, rows)]

    def to_core(source, block, half):
        return remote(
            source,
            spot(block, half),
            core_sem.at[0, 2 * block + half],
            core_sem.at[1, 2 * block + half],
            place.at(z, y, 1 - core),
        )

    def to_y(source, block):
        return remote(
            source,
            spot(block, y),
            y_sem.at[0, block],
            y_sem.at[1, block],
            place.at(z, 1 - y, core),
        )

    def to_line(source, block, step, index):
        return remote(
            source,
            spot(block, y),
            line_sem.at[0, index],
            line_sem.at[1, block],
            place.at(z + step, y, core),
        )

    keep = pltpu.make_async_copy(own, spot(z, y), local_sem.at[0])
    keep.start()
    sender(z < LINE - 1, functools.partial(to_line, own, z, 1, LINE))
    sender(z > 0, functools.partial(to_line, own, z, -1, LINE + 1))
    sender(None, functools.partial(to_y, own, z))
    sender(None, functools.partial(to_core, own, z, y))
    if between is not None:
        between()

    def took_y(block):
        remote(
            own,
            spot(block, 1 - y),
            y_sem.at[0, block],
            y_sem.at[1, block],
            place.at(z, 1 - y, core),
        ).wait_recv()

    def across(condition, block):
        guarded(condition, functools.partial(took_y, block))
        sender(condition, lambda: to_core(spot(block, 1 - y), block, 1 - y))

    def along(condition, block, step):
        def took():
            to_line(own, block, step, block).wait_recv()

        guarded(condition, took)
        onward = condition & ((z < LINE - 1) if step > 0 else (z > 0))
        sender(onward, lambda: to_line(spot(block, y), block, step, block))
        sender(condition, lambda: to_y(spot(block, y), block))
        sender(condition, lambda: to_core(spot(block, y), block, y))

    for distance in range(1, LINE + 1):
        if distance < LINE:
            along(z >= distance, z - distance, 1)
            along(z + distance < LINE, z + distance, -1)
        if distance == 1:
            across(None, z)
        else:
            across(z >= distance - 1, z - distance + 1)
            across(z + distance - 1 < LINE, z + distance - 1)
        if distance == 1 and later is not None:
            later()

    keep.wait()
    for block in range(LINE):
        for half in range(2):
            remote(
                own,
                gathered.at[place.rows(block, half, 1 - core, rows)],
                core_sem.at[0, 2 * block + half],
                core_sem.at[1, 2 * block + half],
                place.at(z, y, 1 - core),
            ).wait_recv()


def pair_scratch():
    return [DMA((3,))]


def pair_phase(place, sender, own, pair, scratch):
    (sem,) = scratch
    rows = own.shape[0]
    spot = pair.at[pl.ds(pl.multiple_of(place.core * rows, rows), rows)]
    keep = pltpu.make_async_copy(own, spot, sem.at[0])
    keep.start()

    def send():
        return remote(
            own, spot, sem.at[1], sem.at[2], place.at(place.z, place.y, 1 - place.core)
        )

    sender(None, send)

    def finish():
        keep.wait()
        other = pair.at[pl.ds(pl.multiple_of((1 - place.core) * rows, rows), rows)]
        remote(
            own, other, sem.at[1], sem.at[2], place.at(place.z, place.y, 1 - place.core)
        ).wait_recv()

    return finish


def swap_scratch(count, arrays):
    return [DMA((arrays,)), DMA((2, arrays, count)), DMA((2, arrays, count))]


class Swap:
    def __init__(self, place, pairs, scratch):
        self.place = place
        self.pairs = pairs
        self.local_sem, self.out_sem, self.side_sem = scratch

    def send(self, index, step):
        place = self.place
        source, spot = self.pairs[index]
        target = lax.rem(place.device + step, place.count)
        return remote(
            source(target),
            spot(place.device, place.side),
            self.out_sem.at[0, index, step],
            self.out_sem.at[1, index, step],
            {"fsdp": target},
        )

    def taken(self, index, step, side):
        device = lax.rem(self.place.device + self.place.count - step, self.place.count)
        return self.pairs[index][1](device, side)

    def come(self, index, step):
        place = self.place
        return remote(
            self.pairs[index][0](place.device),
            self.taken(index, step, place.side),
            self.out_sem.at[0, index, step],
            self.out_sem.at[1, index, step],
            place.across(),
        )

    def share(self, index, step, source=None):
        spot = self.taken(index, step, self.place.side)
        return remote(
            spot if source is None else source,
            spot,
            self.side_sem.at[0, index, step],
            self.side_sem.at[1, index, step],
            self.place.across(),
        )

    def shared(self, index, step):
        spot = self.taken(index, step, 1 - self.place.side)
        return remote(
            spot,
            spot,
            self.side_sem.at[0, index, step],
            self.side_sem.at[1, index, step],
            self.place.across(),
        )

    def keep(self, index):
        place = self.place
        source, spot = self.pairs[index]
        return pltpu.make_async_copy(
            source(place.device), spot(place.device, place.side), self.local_sem.at[index]
        )

    def each(self, first, body):
        def step(number, carry):
            for index in range(len(self.pairs)):
                body(index, number)
            return carry

        lax.fori_loop(first, self.place.count, step, 0)

    def start(self):
        self.each(1, lambda index, step: self.send(index, step).start())
        for index, (source, _) in enumerate(self.pairs):
            self.keep(index).start()
            self.share(index, 0, source(self.place.device)).start()

    def pass_on(self):
        def one(index, step):
            self.come(index, step).wait_recv()
            self.share(index, step).start()

        self.each(1, one)

    def finish(self):
        for index in range(len(self.pairs)):
            self.keep(index).wait()
        self.each(0, lambda index, step: self.shared(index, step).wait_recv())
        self.each(1, lambda index, step: self.send(index, step).wait_send())
        self.each(0, lambda index, step: self.share(index, step).wait_send())


def whole_pair(pieces, whole):
    return (lambda target: pieces.at[target], lambda device, side: whole.at[device, side])


def halves_scratch(arrays):
    return [DMA((3, arrays))]


class Halves:
    def __init__(self, place, halves, wholes, scratch):
        self.place = place
        self.pairs = list(zip(halves, wholes))
        (self.sem,) = scratch

    def keep(self, index):
        half, whole = self.pairs[index]
        return pltpu.make_async_copy(half, whole.at[:, self.place.side], self.sem.at[0, index])

    def copy(self, index, side):
        half, whole = self.pairs[index]
        return remote(
            half,
            whole.at[:, side],
            self.sem.at[1, index],
            self.sem.at[2, index],
            self.place.across(),
        )

    def start(self):
        for index in range(len(self.pairs)):
            self.copy(index, self.place.side).start()
            self.keep(index).start()

    def finish(self):
        for index in range(len(self.pairs)):
            self.keep(index).wait()
            self.copy(index, 1 - self.place.side).wait_recv()
            self.copy(index, self.place.side).wait_send()


REDUCE = 9
GATHER = 5


def first_kernel(
    own_ref, query, key, value, out, small, gathered, qkv_all, out_all, small_all, *scratch
):
    place = Place()
    sender = Sender()
    own = scratch[0]
    own[...] = own_ref[...]
    greet_all(place)
    half, columns = qkv_all.shape[2], qkv_all.shape[3] // 3
    out_half = out_all.shape[2]
    rows = pl.ds(pl.multiple_of(place.side * half, half), half)

    def member(target):
        return lax.rem(target, 2 * LINE)

    def column_pair(weight, index):
        def source(target):
            start = pl.multiple_of(member(target) * columns, columns)
            return weight.at[rows, pl.ds(start, columns)]

        def spot(device, side):
            return qkv_all.at[device, side, :, pl.ds(index * columns, columns)]

        return (source, spot)

    def out_source(target):
        start = (2 * member(target) + place.side) * out_half
        return out.at[pl.ds(pl.multiple_of(start, out_half), out_half)]

    pairs = [
        (lambda target: small, lambda device, side: small_all.at[device, side]),
        column_pair(query, 0),
        column_pair(key, 1),
        column_pair(value, 2),
        (out_source, lambda device, side: out_all.at[device, side]),
    ]
    swap = Swap(place, pairs, scratch[GATHER:])
    gather_phase(place, sender, gathered, scratch[:GATHER], swap.start, swap.pass_on)
    swap.finish()
    sender.drain()


def hidden_kernel(
    partial, tokens, gain, pair, down, gathered, branch, hidden, pair_all, down_all, *scratch
):
    place = Place()
    sender = Sender()
    greet(place, True)
    halves = Halves(place, (pair, down), (pair_all, down_all), scratch[REDUCE + GATHER :])
    halves.start()
    reduce_phase(place, sender, partial, scratch[:REDUCE])
    total, own = scratch[4], scratch[REDUCE]
    rows, width = total.shape

    def body(at):
        value = total[at]
        scale = lax.rsqrt(jnp.sum(value * value, axis=1, keepdims=True) / width + EPS)
        result = tokens[at].astype(F32) + value * scale * gain[...]
        branch[at] = value
        hidden[at] = result
        own[at] = result.astype(BF)

    by_rows(rows, body)
    gather_phase(place, sender, gathered, scratch[REDUCE : REDUCE + GATHER])
    halves.finish()
    sender.drain()


def turn_kernel(partial, hidden, cotangent, gain, gathered, outputs, gain_grad, *scratch):
    place = Place()
    sender = Sender()
    greet(place)
    reduce_phase(place, sender, partial, scratch[:REDUCE])
    total, own = scratch[4], scratch[REDUCE]
    out_own = scratch[REDUCE + GATHER]
    rows, width = total.shape
    gain_grad[...] = jnp.zeros_like(gain_grad)

    def body(at):
        value = total[at]
        scale = lax.rsqrt(jnp.sum(value * value, axis=1, keepdims=True) / width + EPS)
        grads = cotangent[at].astype(F32)
        normed = value * scale
        out_own[at] = (hidden[at] + normed * gain[...]).astype(BF)
        gain_grad[...] += jnp.sum(grads * normed, axis=0, keepdims=True)
        gained = gain[...] * grads
        inner = jnp.sum(normed * gained, axis=1, keepdims=True)
        own[at] = (scale * (gained - normed * (inner / width))).astype(BF)

    by_rows(rows, body)
    finish = pair_phase(place, sender, out_own, outputs, scratch[REDUCE + GATHER + 1 :])
    gather_phase(place, sender, gathered, scratch[REDUCE : REDUCE + GATHER])
    finish()
    sender.drain()


def branch_kernel(
    partial,
    branch,
    cotangent,
    gain,
    pair_grad,
    down_grad,
    gathered,
    grad_hidden,
    gain_grad,
    pair_other,
    down_other,
    *scratch,
):
    place = Place()
    sender = Sender()
    greet(place, True)
    (side_sem,) = scratch[REDUCE + GATHER :]
    count = down_other.shape[0]
    rows_out = pl.ds(pl.multiple_of((1 - place.side) * count, count), count)
    sources = (pair_grad.at[:, 1 - place.side], down_grad.at[rows_out])
    crossings = [
        remote(source, target, side_sem.at[0, index], side_sem.at[1, index], place.across())
        for index, (source, target) in enumerate(zip(sources, (pair_other, down_other)))
    ]
    for crossing in crossings:
        crossing.start()
    reduce_phase(place, sender, partial, scratch[:REDUCE])
    total, own = scratch[4], scratch[REDUCE]
    rows, width = total.shape
    gain_grad[...] = jnp.zeros_like(gain_grad)

    def body(at):
        value = branch[at]
        scale = lax.rsqrt(jnp.sum(value * value, axis=1, keepdims=True) / width + EPS)
        grads = cotangent[at].astype(F32) + total[at]
        grad_hidden[at] = grads
        normed = value * scale
        gain_grad[...] += jnp.sum(grads * normed, axis=0, keepdims=True)
        gained = gain[...] * grads
        inner = jnp.sum(normed * gained, axis=1, keepdims=True)
        own[at] = (scale * (gained - normed * (inner / width))).astype(BF)

    by_rows(rows, body)
    gather_phase(place, sender, gathered, scratch[REDUCE : REDUCE + GATHER])
    for crossing in crossings:
        crossing.wait()
    sender.drain()


def last_kernel(
    partial,
    grad_hidden,
    qkv,
    out,
    small,
    down,
    result,
    qkv_all,
    out_all,
    small_all,
    down_all,
    *scratch,
):
    place = Place()
    sender = Sender()
    parts = scratch[REDUCE + 1 :]
    swap_sems, halves_sems, parts = parts[:3], parts[3:4], parts[4:]
    qkv_own, qkv_other, out_own, out_other, small_own, small_other, fetch_sem, side_sem = parts
    greet_all(place)
    fetches, crossings = [], []
    for index, (grad, own, other) in enumerate(
        ((qkv, qkv_own, qkv_other), (out, out_own, out_other))
    ):
        fetches.append(
            pltpu.make_async_copy(grad.at[:, place.side], own, fetch_sem.at[index])
        )
        crossings.append(
            remote(
                grad.at[:, 1 - place.side],
                other,
                side_sem.at[0, index],
                side_sem.at[1, index],
                place.across(),
            )
        )
    crossings.append(
        remote(
            small,
            small_other,
            side_sem.at[0, 2],
            side_sem.at[1, 2],
            place.at(place.z, place.y, 1 - place.core),
        )
    )
    for copy in fetches + crossings:
        copy.start()
    pairs = ((small_own, small_all), (qkv_own, qkv_all), (out_own, out_all))
    swap = Swap(place, [whole_pair(*pair) for pair in pairs], swap_sems)
    halves = Halves(place, (down,), (down_all,), halves_sems)
    shared_rows = 2 * partial.shape[1] // place.count // 128

    def between():
        for fetch in fetches:
            fetch.wait()
        for crossing in crossings:
            crossing.wait()
        small_own[...] = small[...]
        small_own[:, :shared_rows] += small_other[:, :shared_rows]

        def one(index, carry):
            qkv_own[index] = (
                qkv_own[index].astype(F32) + qkv_other[index].astype(F32)
            ).astype(BF)
            out_own[index] = (
                out_own[index].astype(F32) + out_other[index].astype(F32)
            ).astype(BF)
            return carry

        lax.fori_loop(0, place.count, one, 0)
        swap.start()
        halves.start()

    reduce_phase(place, sender, partial, scratch[:REDUCE], between)
    total = scratch[4]

    def body(at):
        total[at] += grad_hidden[at]

    by_rows(total.shape[0], body)
    finish = pair_phase(place, sender, total, result, scratch[REDUCE : REDUCE + 1])
    swap.pass_on()
    finish()
    halves.finish()
    swap.finish()
    sender.drain()


def sum_kernel(carried, value, *rest):
    if carried:
        moved, result, arrived, core_in, y_in, held, line_in, sem, side_sem = rest
    else:
        result, core_in, y_in, held, line_in, sem = rest
    place = Place()
    z, y, core = place.z, place.y, place.core
    barrier = pltpu.get_barrier_semaphore()
    others = [place.at(z, y, 1 - core), place.at(z, 1 - y, core)]
    others += [place.at(lax.rem(z + k, LINE), y, core) for k in range(1, LINE)]
    for device in others + [place.across()] * carried:
        signal(barrier, device)
    pl.semaphore_wait(barrier, len(others) + carried)
    if carried:
        side = remote(moved, arrived, side_sem.at[0], side_sem.at[1], place.across())
        side.start()
    first = remote(value, core_in, sem.at[0, 0], sem.at[1, 0], others[0])
    first.start()
    first.wait_recv()
    held[0] = value[...] + core_in[...]
    second = remote(held.at[0], y_in, sem.at[0, 1], sem.at[1, 1], others[1])
    second.start()
    second.wait_recv()
    held[1] = held[0] + y_in[...]
    sends = [
        remote(held.at[1], line_in.at[k - 1], sem.at[0, 1 + k], sem.at[1, 1 + k], others[1 + k])
        for k in range(1, LINE)
    ]
    for send in sends:
        send.start()
    line_in[LINE - 1] = held[1]
    for send in sends:
        send.wait_recv()
    added = jnp.zeros_like(value)
    for source in range(LINE):
        slot = lax.rem(z - source + 2 * LINE - 1, LINE)
        added = added + line_in[slot]
    result[...] = added
    first.wait_send()
    second.wait_send()
    for send in sends:
        send.wait_send()
    if carried:
        side.wait()


def pack_kernel(side, gate, up, down, pair_out, down_out):
    columns = gate.shape[1]
    pair_out[0, :, :columns] = gate[...]
    pair_out[0, :, columns:] = up[...]
    down_out[0] = down[...]


def unpack_kernel(side, own, other, down, gate_out, up_out, down_out):
    half, columns = own.shape[2], gate_out.shape[1]
    for part, start in ((own, side[0]), (other, 1 - side[0])):
        value = jnp.sum(part[:, 0].astype(F32), axis=0)
        rows = pl.ds(pl.multiple_of(start * half, half), half)
        gate_out[rows] = value[:, :columns]
        up_out[rows] = value[:, columns:]
    down_out[...] = jnp.sum(down[:, 0].astype(F32), axis=0)


def talk(kernel, which, shapes, specs, scratch, microseconds, name=None):
    def call(*operands):
        return pl.pallas_call(
            kernel,
            out_shape=shapes,
            in_specs=specs[0],
            out_specs=specs[1],
            scratch_shapes=scratch,
            compiler_params=pltpu.CompilerParams(
                collective_id=which, has_side_effects=True, vmem_limit_bytes=48 << 20
            ),
            cost_estimate=pl.CostEstimate(
                flops=0, bytes_accessed=int(microseconds * 3.0e6), transcendentals=0
            ),
            name=name or kernel.__name__,
        )(*operands)

    return call


class Team:
    def __init__(self, local_heads, rows, width):
        self.fsdp = lax.axis_size("fsdp")
        self.tensor = lax.axis_size("tensor")
        self.size = 2 * LINE
        self.teams = self.fsdp // self.size
        assert self.fsdp % self.size == 0 and self.tensor == 2 and local_heads % self.size == 0
        self.member = lax.rem(lax.axis_index("fsdp"), self.size)
        self.core = lax.axis_index("tensor")
        self.context = lax.axis_index("context")
        self.groups = None
        if self.teams > 1:
            self.groups = [
                [team * self.size + one for one in range(self.size)] for team in range(self.teams)
            ]
        self.rows = rows
        self.width = width
        self.all_low = jax.ShapeDtypeStruct((2 * self.size * rows, width), BF)
        self.own_wide = jax.ShapeDtypeStruct((rows, width), F32)
        self.line_wide = jax.ShapeDtypeStruct((1, width), F32)
        self.reduces = reduce_scratch(rows, width)
        self.gathers = gather_scratch(rows, width)

    def whole(self, pieces):
        shape = (pieces.shape[0], 2) + pieces.shape[1:]
        return jax.ShapeDtypeStruct(shape, pieces.dtype)

    def first(self, own, weights, out, small):
        rows, columns = weights[0].shape
        rows, columns = rows // 2, columns // self.size
        out_rows = out.shape[0] // self.size // 2
        return talk(
            first_kernel,
            0,
            (
                self.all_low,
                jax.ShapeDtypeStruct((self.fsdp, 2, rows, 3 * columns), BF),
                jax.ShapeDtypeStruct((self.fsdp, 2, out_rows, out.shape[1]), BF),
                jax.ShapeDtypeStruct((self.fsdp, 2) + small.shape, F32),
            ),
            ([VMEM] * 6, (HBM,) * 4),
            self.gathers + swap_scratch(self.fsdp, 5),
            80,
        )(own, *weights, out, small)

    def pack(self, gate, up, down):
        rows, columns = gate.shape
        rows, columns = rows // 2, columns // self.size
        down_rows, down_columns = down.shape
        down_rows = down_rows // self.size // 2

        def column_spec():
            return pl.BlockSpec((rows, columns), lambda d, side: (side[0], d))

        def piece_spec(*shape):
            return pl.BlockSpec((1,) + shape, lambda d, side: (d, 0, 0))

        pair, low = pl.pallas_call(
            pack_kernel,
            grid_spec=pltpu.PrefetchScalarGridSpec(
                num_scalar_prefetch=1,
                grid=(self.size,),
                in_specs=[
                    column_spec(),
                    column_spec(),
                    pl.BlockSpec((down_rows, down_columns), lambda d, side: (2 * d + side[0], 0)),
                ],
                out_specs=[piece_spec(rows, 2 * columns), piece_spec(down_rows, down_columns)],
            ),
            out_shape=[
                jax.ShapeDtypeStruct((self.size, rows, 2 * columns), BF),
                jax.ShapeDtypeStruct((self.size, down_rows, down_columns), BF),
            ],
            name="pack_kernel",
        )(self.context.reshape(1).astype(jnp.int32), gate, up, down)
        return self.repeat(pair), self.repeat(low)

    def hidden(self, partial, tokens, gain, pair, down):
        return talk(
            hidden_kernel,
            1,
            (self.all_low, self.own_wide, self.own_wide, self.whole(pair), self.whole(down)),
            ([HBM, VMEM, VMEM, VMEM, VMEM], (HBM, VMEM, VMEM, HBM, HBM)),
            self.reduces + self.gathers + halves_scratch(2),
            100,
        )(partial, tokens, gain, pair, down)

    def turn(self, partial, hidden, cotangent, gain):
        pair = jax.ShapeDtypeStruct((2 * self.rows, self.width), BF)
        return talk(
            turn_kernel,
            2,
            (self.all_low, pair, self.line_wide),
            ([HBM, VMEM, VMEM, VMEM], (HBM, HBM, VMEM)),
            self.reduces + self.gathers + [pltpu.VMEM((self.rows, self.width), BF)] + pair_scratch(),
            100,
        )(partial, hidden, cotangent, gain)

    def branch(self, partial, branch, cotangent, gain, pair_grad, down_grad):
        shape = pair_grad.shape
        pair_other = jax.ShapeDtypeStruct((shape[0],) + shape[2:], BF)
        down_other = jax.ShapeDtypeStruct((down_grad.shape[0] // 2, down_grad.shape[1]), BF)
        return talk(
            branch_kernel,
            3,
            (self.all_low, self.own_wide, self.line_wide, pair_other, down_other),
            ([HBM, VMEM, VMEM, VMEM, HBM, HBM], (HBM, VMEM, VMEM, HBM, HBM)),
            self.reduces + self.gathers + [DMA((2, 2))],
            100,
        )(partial, branch, cotangent, gain, pair_grad, down_grad)

    def last(self, partial, grad_hidden, qkv, out, small, down):
        both = jax.ShapeDtypeStruct((2 * self.rows, self.width), F32)

        def same(array):
            return jax.ShapeDtypeStruct(array.shape, array.dtype)

        def half(array):
            return pltpu.VMEM((array.shape[0],) + array.shape[2:], array.dtype)

        held = pltpu.VMEM(small.shape, small.dtype)
        return talk(
            last_kernel,
            4,
            (both, same(qkv), same(out), self.whole(small), self.whole(down)),
            ([HBM, VMEM, HBM, HBM, VMEM, VMEM], (HBM,) * 5),
            self.reduces
            + pair_scratch()
            + swap_scratch(self.fsdp, 3)
            + halves_scratch(1)
            + [half(qkv), half(qkv), half(out), half(out), held, held, DMA((2,)), DMA((2, 3))],
            80,
        )(partial, grad_hidden, qkv, out, small, down)

    def total(self, values, moved=None):
        flat = values.reshape(-1, 128)
        carried = int(moved is not None)
        shape = jax.ShapeDtypeStruct(flat.shape, F32)
        scratch = [pltpu.VMEM(flat.shape, F32)] * 2
        scratch += [pltpu.VMEM((2,) + flat.shape, F32), pltpu.VMEM((LINE,) + flat.shape, F32)]
        scratch += [DMA((2, LINE + 1))] + [DMA((2,))] * carried
        which = 5 + self.sums
        self.sums += 1
        kernel = functools.partial(sum_kernel, carried)
        if not carried:
            call = talk(kernel, which, shape, ([VMEM], VMEM), scratch, 10, "sum_kernel")
            return call(flat).reshape(values.shape)
        shapes = (shape, jax.ShapeDtypeStruct(moved.shape, moved.dtype))
        call = talk(kernel, which, shapes, ([VMEM] * 2, (VMEM,) * 2), scratch, 10, "sum_kernel")
        total, came = call(flat, moved)
        return total.reshape(values.shape), came

    sums = 0

    def half(self, array, axis):
        count = array.shape[axis] // 2
        return lax.dynamic_slice_in_dim(array, self.context * count, count, axis)

    def swap(self, pieces):
        return lax.all_to_all(pieces, "fsdp", split_axis=0, concat_axis=0, tiled=True)

    def repeat(self, pieces):
        return jnp.concatenate([pieces] * self.teams, axis=0) if self.teams > 1 else pieces

    def unpack(self, own, down):
        other = lax.ppermute(own, "context", [(0, 1), (1, 0)])
        half, columns = own.shape[1], own.shape[2] // 2
        rows, down_columns = 2 * down.shape[2], down.shape[3]

        def cut(array, *shape):
            return array.reshape((self.teams, self.size) + shape)

        def piece_spec(*shape):
            return pl.BlockSpec((self.teams, 1) + shape, lambda d, side: (0, d, 0, 0))

        wide = pl.BlockSpec((2 * half, columns), lambda d, side: (0, d))
        wide_shape = jax.ShapeDtypeStruct((2 * half, self.size * columns), F32)
        return pl.pallas_call(
            unpack_kernel,
            grid_spec=pltpu.PrefetchScalarGridSpec(
                num_scalar_prefetch=1,
                grid=(self.size,),
                in_specs=[piece_spec(half, 2 * columns)] * 2 + [piece_spec(rows, down_columns)],
                out_specs=[wide, wide, pl.BlockSpec((rows, down_columns), lambda d, side: (d, 0))],
            ),
            out_shape=[
                wide_shape,
                wide_shape,
                jax.ShapeDtypeStruct((self.size * rows, down_columns), F32),
            ],
            name="unpack_kernel",
        )(
            self.context.reshape(1).astype(jnp.int32),
            cut(own, half, 2 * columns),
            cut(other, half, 2 * columns),
            cut(down, rows, down_columns),
        )

    def columns_whole(self, came):
        return came.reshape(-1, came.shape[-1])

    def rows_whole(self, came):
        fsdp, two, rows, columns = came.shape
        return came.transpose(1, 2, 0, 3).reshape(two * rows, fsdp * columns)

    def of_columns(self, grad):
        rows, columns = grad.shape
        return grad.astype(BF).reshape(self.fsdp, 2, rows // self.fsdp // 2, columns)

    def of_rows(self, grad):
        rows, columns = grad.shape
        cut = grad.astype(BF).reshape(2, rows // 2, self.fsdp, columns // self.fsdp)
        return cut.transpose(2, 0, 1, 3)

    def added(self, came):
        if self.teams == 1:
            return came.astype(F32)
        came = came.reshape((self.teams, self.size) + came.shape[1:])
        return jnp.sum(came.astype(F32), axis=0)

    def columns_out(self, came, count):
        size, two, rows, columns = came.shape
        return [
            self.added(part.reshape(size, two * rows, -1))
            .transpose(1, 0, 2)
            .reshape(two * rows, -1)
            for part in jnp.split(came, count, axis=3)
        ]

    def rows_out(self, came):
        return self.added(came).reshape(-1, came.shape[-1])


def local(
    tokens,
    cont_lengths,
    w_query,
    w_key,
    w_value,
    w_output,
    query_gain,
    key_gain,
    attn_gain,
    w_gate,
    w_up,
    w_down,
    mlp_gain,
    cotangent,
):
    rows = tokens.shape[0]
    width = tokens.shape[1]
    fsdp = lax.axis_size("fsdp")
    tensor = lax.axis_size("tensor")
    local_heads = query_gain.shape[0]
    head_size = w_query.shape[1] // local_heads
    own_rows = rows // tensor
    team = Team(local_heads, own_rows, width)
    groups = team.size
    team_rows = groups * rows
    heads = local_heads // team.size
    later = lax.axis_index("context") == 1

    tokens_own = lax.dynamic_slice_in_dim(tokens, team.core * own_rows, own_rows, 0)
    grad_out = lax.dynamic_slice_in_dim(cotangent, team.core * own_rows, own_rows, 0)
    cut = query_gain.size
    share = attn_gain.size
    small = [query_gain.reshape(-1), key_gain.reshape(-1), attn_gain, mlp_gain]
    small = jnp.concatenate([one.astype(F32) for one in small + [cont_lengths.reshape(-1)]])
    small = jnp.pad(small, (0, 8 * 128 - small.size)).reshape(8, 128)
    tokens_all, qkv_came, output_came, small_came = team.first(
        tokens_own, [w_query, w_key, w_value], w_output, small
    )
    qkv_w = team.columns_whole(qkv_came)
    output_w = team.rows_whole(output_came)
    all_small = small_came[:, 0].reshape(fsdp, -1)
    query_gains = all_small[:, :cut].reshape(fsdp, local_heads, -1)
    key_gains = all_small[:, cut : 2 * cut].reshape(fsdp, local_heads, -1)
    query_gains = query_gains.transpose(1, 0, 2).reshape(local_heads, head_size)
    key_gains = key_gains.transpose(1, 0, 2).reshape(local_heads, head_size)
    flat_query = lax.dynamic_slice_in_dim(query_gains, team.member * heads, heads, 0).reshape(-1)
    flat_key = lax.dynamic_slice_in_dim(key_gains, team.member * heads, heads, 0).reshape(-1)
    gain_attn = all_small[:, 2 * cut : 2 * cut + share].reshape(1, -1)
    gain_mlp = all_small[:, 2 * cut + share : 2 * cut + 2 * share].reshape(1, -1)

    conts = cont_lengths.shape[1]
    lengths = all_small[:, 2 * cut + 2 * share : 2 * cut + 2 * share + conts].astype(jnp.int32)
    first_group = lax.axis_index("fsdp") - team.member
    lengths = lax.dynamic_slice_in_dim(lengths, first_group, groups, 0)
    segment, offset = jax.vmap(lambda one: layout(one, rows))(lengths)
    row_index = jnp.arange(rows, dtype=jnp.int32)
    positions = jnp.where(later, rows + offset, row_index[None, :])
    own_segment = jnp.where(later, segment, -1)
    cosine, sine = rotary_tables(positions, head_size)
    cosine = cosine[:, :, None, :]
    sine = sine[:, :, None, :]

    pair_mine, down_mine, tokens_all = lax.optimization_barrier(
        team.pack(w_gate, w_up, w_down) + (tokens_all,)
    )
    pair_came = team.swap(pair_mine)
    down_came = team.swap(down_mine)

    by_head = (groups, rows, heads, head_size)
    raw = product(tokens_all, qkv_w)
    query_raw, key_raw, value_raw = jnp.split(raw, 3, axis=1)
    value_low = value_raw.astype(BF)
    sums, sent_value = team.total(
        jnp.stack([jnp.sum(query_raw * query_raw, axis=1), jnp.sum(key_raw * key_raw, axis=1)]),
        value_low,
    )
    value_low, sent_value = value_low.reshape(by_head), sent_value.reshape(by_head)
    scale_query = lax.rsqrt(sums[0] / width + EPS)[:, None]
    scale_key = lax.rsqrt(sums[1] / width + EPS)[:, None]
    query_norm = query_raw * scale_query * flat_query
    key_norm = key_raw * scale_key * flat_key
    query_low = rotate(query_norm.reshape(by_head), cosine, sine).astype(BF)
    key_low = rotate(key_norm.reshape(by_head), cosine, sine).astype(BF)
    sent_key = lax.ppermute(key_low, "context", [(0, 1)])
    keys_all = jnp.concatenate([sent_key, key_low], axis=1)
    values_all = jnp.concatenate([sent_value, value_low], axis=1)
    key_index = jnp.arange(2 * rows, dtype=jnp.int32)
    key_segment = jnp.concatenate([jnp.full((groups, rows), -2, jnp.int32), own_segment], axis=1)
    remote = (key_index < rows)[None, None, :] & later
    own_keys = (
        (key_index >= rows)[None, None, :]
        & (key_index[None, None, :] - rows <= row_index[None, :, None])
        & (key_segment[:, None, :] == own_segment[:, :, None])
    )
    allowed = (remote | own_keys)[:, None]
    scale = 1.0 / math.sqrt(head_size)
    scores = (
        jnp.einsum("gqhd,gkhd->ghqk", query_low, keys_all, preferred_element_type=F32) * scale
    )
    scores = jnp.where(allowed, scores, -1e30)
    highest = jnp.max(scores, axis=-1, keepdims=True)
    weights = jnp.exp(scores - highest)
    probs = weights / jnp.sum(weights, axis=-1, keepdims=True)
    probs_low = probs.astype(BF)
    mixed = jnp.einsum("ghqk,gkhd->gqhd", probs_low, values_all, preferred_element_type=F32)
    attended_low = mixed.reshape(team_rows, heads * head_size).astype(BF)
    hidden_all, attn_sum, hidden, pair_came, down_came = team.hidden(
        product(attended_low, output_w).astype(BF), tokens_own, gain_attn, pair_came, down_came
    )
    pair_w = team.columns_whole(pair_came)
    down_w = team.rows_whole(down_came)

    gate, upward = jnp.split(product(hidden_all, pair_w), 2, axis=1)
    sigma = jax.nn.sigmoid(gate)
    inner_low = (gate * sigma * upward).astype(BF)
    grad_mlp_all, outputs, grad_mlp_gain = team.turn(
        product(inner_low, down_w).astype(BF), hidden, grad_out, gain_mlp
    )
    down_grad = product_left(inner_low, grad_mlp_all).astype(BF)
    grad_inner = product_right(grad_mlp_all, down_w)
    grad_gate_low = (grad_inner * upward * sigma * (1.0 + gate * (1.0 - sigma))).astype(BF)
    grad_up_low = (grad_inner * gate * sigma).astype(BF)
    grad_pair = jnp.concatenate([grad_gate_low, grad_up_low], axis=1)
    pair_grad = team.of_columns(product_left(hidden_all, grad_pair))
    grad_branch_all, grad_hidden, grad_attn_gain, pair_other, down_other = team.branch(
        product_right(grad_pair, pair_w).astype(BF),
        attn_sum,
        grad_out,
        gain_attn,
        pair_grad,
        down_grad,
    )
    pair_mine = lax.dynamic_index_in_dim(pair_grad, team.context, 1, keepdims=False)
    pair_mine = (pair_mine.astype(F32) + pair_other.astype(F32)).astype(BF)
    down_mine = (team.half(down_grad, 0).astype(F32) + down_other.astype(F32)).astype(BF)
    down_mine = down_mine.reshape(down_mine.shape[0], fsdp, -1).transpose(1, 0, 2)
    pair_came = team.swap(pair_mine)
    output_grad = team.of_rows(product_left(attended_low, grad_branch_all))
    grad_attended = product_right(grad_branch_all, output_w).astype(BF).reshape(by_head)

    grad_probs = jnp.einsum("gqhd,gkhd->ghqk", grad_attended, values_all, preferred_element_type=F32)
    centre = jnp.sum(probs * grad_probs, axis=-1, keepdims=True)
    grad_scores = (probs * (grad_probs - centre)).astype(BF)
    grad_query_rot = (
        jnp.einsum("ghqk,gkhd->gqhd", grad_scores, keys_all, preferred_element_type=F32) * scale
    )
    grad_keys = (
        jnp.einsum("ghqk,gqhd->gkhd", grad_scores, query_low, preferred_element_type=F32) * scale
    )
    grad_values = jnp.einsum("ghqk,gqhd->gkhd", probs_low, grad_attended, preferred_element_type=F32)
    back_value = lax.ppermute(grad_values[:, :rows].astype(BF), "context", [(1, 0)])
    back_key = lax.ppermute(grad_keys[:, :rows].astype(BF), "context", [(1, 0)])
    grad_key_rot = grad_keys[:, rows:] + back_key.astype(F32)
    grad_value_low = (
        (grad_values[:, rows:] + back_value.astype(F32)).reshape(team_rows, -1).astype(BF)
    )
    grad_query_norm = rotate_back(grad_query_rot, cosine, sine).reshape(team_rows, -1)
    grad_key_norm = rotate_back(grad_key_rot, cosine, sine).reshape(team_rows, -1)
    grad_query_gain = jnp.sum(grad_query_norm * query_raw * scale_query, axis=0)
    grad_key_gain = jnp.sum(grad_key_norm * key_raw * scale_key, axis=0)
    totals = team.total(
        jnp.stack(
            [
                jnp.sum(query_raw * flat_query * grad_query_norm, axis=1),
                jnp.sum(key_raw * flat_key * grad_key_norm, axis=1),
            ]
        )
    )
    down_mine, totals = lax.optimization_barrier((down_mine, totals))
    down_came = team.swap(down_mine)
    grad_query_low = norm_back(
        query_raw, scale_query, flat_query, grad_query_norm, totals[0][:, None], width
    ).astype(BF)
    grad_key_low = norm_back(
        key_raw, scale_key, flat_key, grad_key_norm, totals[1][:, None], width
    ).astype(BF)
    grad_qkv = jnp.concatenate([grad_query_low, grad_key_low, grad_value_low], axis=1)
    qkv_grad = team.of_columns(product_left(tokens_all, grad_qkv))
    head_share = head_size // fsdp
    small = [
        grad_attn_gain.reshape(fsdp, share),
        grad_mlp_gain.reshape(fsdp, share),
        grad_query_gain.reshape(heads, fsdp, head_share).transpose(1, 0, 2).reshape(fsdp, -1),
        grad_key_gain.reshape(heads, fsdp, head_share).transpose(1, 0, 2).reshape(fsdp, -1),
    ]
    used = 2 * share + 2 * heads * head_share
    small = jnp.concatenate(small + [jnp.zeros((fsdp, 8 * 128 - used), F32)], axis=1)
    partial, pair_came = lax.optimization_barrier(
        (product_right(grad_qkv, qkv_w).astype(BF), pair_came)
    )
    input_grad, qkv_came, output_came, small_came, down_came = team.last(
        partial,
        grad_hidden,
        qkv_grad,
        output_grad,
        small.reshape(fsdp, 8, 128),
        down_came,
    )
    grad_w_query, grad_w_key, grad_w_value = team.columns_out(qkv_came, 3)
    grad_w_gate, grad_w_up, grad_w_down = team.unpack(pair_came, down_came)
    grad_w_output = team.rows_out(output_came)
    came = jnp.sum(small_came, axis=1).reshape(fsdp, -1)
    row_gains = jnp.sum(came[:, : 2 * share], axis=0).reshape(2, share)
    head_gains = team.added(came[:, 2 * share : used]).reshape(team.size, 2, heads, head_share)
    head_gains = head_gains.transpose(1, 0, 2, 3).reshape(2, local_heads, head_share)
    return (
        outputs,
        input_grad,
        grad_w_query,
        grad_w_key,
        grad_w_value,
        grad_w_output,
        head_gains[0],
        head_gains[1],
        row_gains[0],
        grad_w_gate,
        grad_w_up,
        grad_w_down,
        row_gains[1],
    )


def solution(mesh):
    return jax.shard_map(
        local,
        mesh=mesh,
        in_specs=(
            P(("fsdp", "context"), None),
            P("fsdp", None),
            P("fsdp", "tensor"),
            P("fsdp", "tensor"),
            P("fsdp", "tensor"),
            P("tensor", "fsdp"),
            P("tensor", "fsdp"),
            P("tensor", "fsdp"),
            P("fsdp"),
            P("fsdp", "tensor"),
            P("fsdp", "tensor"),
            P("tensor", "fsdp"),
            P("fsdp"),
            P(("fsdp", "context"), None),
        ),
        out_specs=(
            P(("fsdp", "context"), None),
            P(("fsdp", "context"), None),
            P("fsdp", "tensor"),
            P("fsdp", "tensor"),
            P("fsdp", "tensor"),
            P("tensor", "fsdp"),
            P("tensor", "fsdp"),
            P("tensor", "fsdp"),
            P("fsdp"),
            P("fsdp", "tensor"),
            P("fsdp", "tensor"),
            P("tensor", "fsdp"),
            P("fsdp"),
        ),
        check_vma=False,
    )
```

```python
import functools
import math

import jax
import jax.numpy as jnp
from jax import lax
from jax.experimental import pallas as pl
from jax.experimental.pallas import tpu as pltpu
from jax.sharding import PartitionSpec as P

EPS = 1e-06
THETA = 500000.0
BF = jnp.bfloat16
F32 = jnp.float32


def product(left, right):
    return jnp.dot(left, right, preferred_element_type=F32)


def product_left(left, right):
    return jnp.einsum("rd,rf->df", left, right, preferred_element_type=F32)


def product_right(left, right):
    return jnp.einsum("rf,df->rd", left, right, preferred_element_type=F32)


def rotary_tables(positions, head_size):
    half = head_size // 2
    inverse = jnp.exp(-(2.0 * jnp.arange(half, dtype=F32) / head_size) * math.log(THETA))
    angles = positions.astype(F32)[..., None] * inverse
    angles = jnp.concatenate([angles, angles], axis=-1)
    return (jnp.cos(angles), jnp.sin(angles))


def rotate(values, cosine, sine):
    half = values.shape[-1] // 2
    turned = jnp.concatenate([-values[..., half:], values[..., :half]], axis=-1)
    return values * cosine + turned * sine


def rotate_back(grads, cosine, sine):
    half = grads.shape[-1] // 2
    scaled = grads * sine
    turned = jnp.concatenate([scaled[..., half:], -scaled[..., :half]], axis=-1)
    return grads * cosine + turned


def norm_back(values, scale, gain, grads, total, width):
    return scale * gain * grads - values * scale * scale * scale * (total / width)


def layout(lengths, rows):
    segment_ends = jnp.cumsum(lengths)
    segment_starts = segment_ends - lengths
    row_index = jnp.arange(rows, dtype=jnp.int32)
    segment = jnp.sum((row_index[:, None] >= segment_ends[None, :]).astype(jnp.int32), axis=1)
    chosen = segment[:, None] == jnp.arange(lengths.shape[0], dtype=jnp.int32)[None, :]
    offset = row_index - jnp.sum(jnp.where(chosen, segment_starts[None, :], 0), axis=1)
    return (segment, offset)


LINE = 4
CHUNK = 16
MESH_ID = pl.DeviceIdType.MESH
HBM = pl.BlockSpec(memory_space=pl.ANY)
VMEM = pl.BlockSpec(memory_space=pltpu.VMEM)
DMA = pltpu.SemaphoreType.DMA


class Place:
    def __init__(self):
        device = lax.axis_index("fsdp")
        member = lax.rem(device, 2 * LINE)
        self.base = device - member
        self.z = member // 2
        self.y = lax.rem(member, 2)
        self.core = lax.axis_index("tensor")
        self.side = lax.axis_index("context")
        self.device = device
        self.count = lax.axis_size("fsdp")

    def across(self):
        return {"context": 1 - self.side}

    def at(self, z, y, core):
        return {"fsdp": self.base + 2 * z + y, "tensor": core}

    def near(self):
        yield None, self.at(self.z, self.y, 1 - self.core)
        yield None, self.at(self.z, 1 - self.y, self.core)
        yield self.z > 0, self.at(self.z - 1, self.y, self.core)
        yield self.z < LINE - 1, self.at(self.z + 1, self.y, self.core)

    def rows(self, z, y, core, count):
        start = ((2 * z + y) * 2 + core) * count
        return pl.ds(pl.multiple_of(start, count), count)


def guarded(condition, action):
    if condition is None:
        action()
    else:
        pl.when(condition)(action)


def signal(barrier, device):
    pl.semaphore_signal(barrier, inc=1, device_id=device, device_id_type=MESH_ID)


def greet(place, across=False):
    barrier = pltpu.get_barrier_semaphore()
    for condition, device in place.near():
        guarded(condition, functools.partial(signal, barrier, device))
    if across:
        signal(barrier, place.across())
    inside = (place.z > 0) & (place.z < LINE - 1)
    pl.semaphore_wait(barrier, jnp.where(inside, 4, 3) + int(across))


def greet_all(place):
    barrier = pltpu.get_barrier_semaphore()

    def one(step, carry):
        signal(barrier, {"fsdp": lax.rem(place.device + step, place.count)})
        return carry

    lax.fori_loop(1, place.count, one, 0)
    signal(barrier, place.across())
    signal(barrier, place.at(place.z, place.y, 1 - place.core))
    pl.semaphore_wait(barrier, place.count + 1)


class Sender:
    def __init__(self):
        self.sent = []

    def __call__(self, condition, make):
        def start():
            make().start()

        guarded(condition, start)
        self.sent.append((condition, make))

    def drain(self):
        for condition, make in self.sent:

            def wait(make=make):
                make().wait_send()

            guarded(condition, wait)


def remote(source, target, send, receive, device):
    return pltpu.make_async_remote_copy(
        src_ref=source,
        dst_ref=target,
        send_sem=send,
        recv_sem=receive,
        device_id=device,
        device_id_type=MESH_ID,
    )


def by_rows(rows, body):
    def step(index, carry):
        body(pl.ds(pl.multiple_of(index * CHUNK, CHUNK), CHUNK))
        return carry

    lax.fori_loop(0, rows // CHUNK, step, 0)


def reduce_scratch(rows, width):
    return [
        pltpu.VMEM((2 * LINE, rows, width), BF),
        pltpu.VMEM((2 * LINE, rows, width), BF),
        pltpu.VMEM((LINE, rows, width), BF),
        pltpu.VMEM((LINE + 1, rows, width), BF),
        pltpu.VMEM((rows, width), F32),
        DMA((2 * LINE,)),
        DMA((2, 2 * LINE)),
        DMA((2, LINE)),
        DMA((2, LINE + 1)),
    ]


def reduce_phase(place, sender, partial, scratch, between=None, idle=None):
    mine, core_in, y_in, line_in, total, local_sem, core_sem, y_sem, line_sem = scratch
    rows = total.shape[0]
    z, y, core = place.z, place.y, place.core
    low = z < LINE // 2
    order = []
    for k in range(LINE - 1):
        down = LINE - 1 - k
        down = jnp.where(down <= z, down - 1, down)
        up = jnp.where(k >= z, k + 1, k)
        order.append(jnp.where(low, down, up))
    order.append(z)

    def fetch(slot):
        half = lax.rem(slot, 2)
        return pltpu.make_async_copy(
            partial.at[place.rows(slot // 2, half, core, rows)], mine.at[slot], local_sem.at[slot]
        )

    def to_core(slot):
        half = lax.rem(slot, 2)
        return remote(
            partial.at[place.rows(slot // 2, half, 1 - core, rows)],
            core_in.at[slot],
            core_sem.at[0, slot],
            core_sem.at[1, slot],
            place.at(z, y, 1 - core),
        )

    def to_y(block):
        return remote(
            mine.at[2 * block + 1 - y],
            y_in.at[block],
            y_sem.at[0, block],
            y_sem.at[1, block],
            place.at(z, 1 - y, core),
        )

    def to_line(block):
        step = jnp.where(block > z, 1, -1)
        slot = jnp.where((step < 0) & (block == z - 1), LINE, block)
        return remote(
            mine.at[2 * block + y],
            line_in.at[slot],
            line_sem.at[0, block],
            line_sem.at[1, slot],
            place.at(z + step, y, core),
        )

    def from_line(slot):
        return remote(
            mine.at[0],
            line_in.at[slot],
            line_sem.at[0, 0],
            line_sem.at[1, slot],
            place.at(z, y, 1 - core),
        )

    for half in (1 - y, y):
        for block in order:
            sender(None, functools.partial(to_core, 2 * block + half))
            fetch(2 * block + half).start()

    for block in order:
        slot = 2 * block + 1 - y
        fetch(slot).wait()
        to_core(slot).wait_recv()

        def add(at, slot=slot):
            value = mine[slot, at].astype(F32) + core_in[slot, at].astype(F32)
            mine[slot, at] = value.astype(BF)

        by_rows(rows, add)
        sender(None, functools.partial(to_y, block))

    for number, block in enumerate(order[:-1]):
        if number == LINE - 2 and between is not None:
            between()
        if number < 2 and idle is not None:
            idle(number)
        slot = 2 * block + y
        fetch(slot).wait()
        to_core(slot).wait_recv()
        to_y(block).wait_recv()
        inner = jnp.where(block > z, z > 0, z < LINE - 1)

        @pl.when(inner)
        def _(block=block, slot=slot):
            from_line(block).wait_recv()

            def add(at):
                value = mine[slot, at].astype(F32) + core_in[slot, at].astype(F32)
                value = value + y_in[block, at].astype(F32)
                mine[slot, at] = (value + line_in[block, at].astype(F32)).astype(BF)

            by_rows(rows, add)

        @pl.when(jnp.logical_not(inner))
        def _(block=block, slot=slot):
            def add(at):
                value = mine[slot, at].astype(F32) + core_in[slot, at].astype(F32)
                mine[slot, at] = (value + y_in[block, at].astype(F32)).astype(BF)

            by_rows(rows, add)

        sender(None, functools.partial(to_line, block))

    slot = 2 * z + y
    fetch(slot).wait()
    to_core(slot).wait_recv()
    to_y(z).wait_recv()

    def start(at):
        value = mine[slot, at].astype(F32) + core_in[slot, at].astype(F32)
        total[at] = value + y_in[z, at].astype(F32)

    by_rows(rows, start)
    for condition, source in ((z > 0, z), (z < LINE - 1, LINE)):

        @pl.when(condition)
        def _(source=source):
            from_line(source).wait_recv()

            def add(at):
                total[at] += line_in[source, at].astype(F32)

            by_rows(rows, add)


def gather_scratch(rows, width):
    return [
        pltpu.VMEM((rows, width), BF),
        DMA((1,)),
        DMA((2, 2 * LINE)),
        DMA((2, LINE)),
        DMA((2, LINE + 2)),
    ]


def gather_phase(place, sender, gathered, scratch, between=None, later=None, last=None):
    own, local_sem, core_sem, y_sem, line_sem = scratch
    rows = own.shape[0]
    z, y, core = place.z, place.y, place.core

    def spot(block, half):
        return gathered.at[place.rows(block, half, core, rows)]

    def to_core(source, block, half):
        return remote(
            source,
            spot(block, half),
            core_sem.at[0, 2 * block + half],
            core_sem.at[1, 2 * block + half],
            place.at(z, y, 1 - core),
        )

    def to_y(source, block):
        return remote(
            source,
            spot(block, y),
            y_sem.at[0, block],
            y_sem.at[1, block],
            place.at(z, 1 - y, core),
        )

    def to_line(source, block, step, index):
        return remote(
            source,
            spot(block, y),
            line_sem.at[0, index],
            line_sem.at[1, block],
            place.at(z + step, y, core),
        )

    keep = pltpu.make_async_copy(own, spot(z, y), local_sem.at[0])
    keep.start()
    sender(z < LINE - 1, functools.partial(to_line, own, z, 1, LINE))
    sender(z > 0, functools.partial(to_line, own, z, -1, LINE + 1))
    sender(None, functools.partial(to_y, own, z))
    sender(None, functools.partial(to_core, own, z, y))
    if between is not None:
        between()

    def took_y(block):
        remote(
            own,
            spot(block, 1 - y),
            y_sem.at[0, block],
            y_sem.at[1, block],
            place.at(z, 1 - y, core),
        ).wait_recv()

    def across(condition, block):
        guarded(condition, functools.partial(took_y, block))
        sender(condition, lambda: to_core(spot(block, 1 - y), block, 1 - y))

    def along(condition, block, step):
        def took():
            to_line(own, block, step, block).wait_recv()

        guarded(condition, took)
        onward = condition & ((z < LINE - 1) if step > 0 else (z > 0))
        sender(onward, lambda: to_line(spot(block, y), block, step, block))
        sender(condition, lambda: to_y(spot(block, y), block))
        sender(condition, lambda: to_core(spot(block, y), block, y))

    for distance in range(1, LINE + 1):
        if distance < LINE:
            along(z >= distance, z - distance, 1)
            along(z + distance < LINE, z + distance, -1)
        if distance == 1:
            across(None, z)
        else:
            across(z >= distance - 1, z - distance + 1)
            across(z + distance - 1 < LINE, z + distance - 1)
        if distance == 1 and later is not None:
            later()
        if distance == LINE - 1 and last is not None:
            last()

    keep.wait()
    for block in range(LINE):
        for half in range(2):
            remote(
                own,
                gathered.at[place.rows(block, half, 1 - core, rows)],
                core_sem.at[0, 2 * block + half],
                core_sem.at[1, 2 * block + half],
                place.at(z, y, 1 - core),
            ).wait_recv()


def pair_scratch():
    return [DMA((3,))]


def pair_phase(place, sender, own, pair, scratch):
    (sem,) = scratch
    rows = own.shape[0]
    spot = pair.at[pl.ds(pl.multiple_of(place.core * rows, rows), rows)]
    keep = pltpu.make_async_copy(own, spot, sem.at[0])
    keep.start()

    def send():
        return remote(
            own, spot, sem.at[1], sem.at[2], place.at(place.z, place.y, 1 - place.core)
        )

    sender(None, send)

    def finish():
        keep.wait()
        other = pair.at[pl.ds(pl.multiple_of((1 - place.core) * rows, rows), rows)]
        remote(
            own, other, sem.at[1], sem.at[2], place.at(place.z, place.y, 1 - place.core)
        ).wait_recv()

    return finish


def swap_scratch(count, arrays):
    return [DMA((arrays,)), DMA((2, arrays, count)), DMA((2, arrays, count))]


class Swap:
    def __init__(self, place, pairs, scratch):
        self.place = place
        self.pairs = pairs
        self.local_sem, self.out_sem, self.side_sem = scratch

    def send(self, index, step):
        place = self.place
        source, spot = self.pairs[index]
        target = lax.rem(place.device + step, place.count)
        return remote(
            source(target),
            spot(place.device, place.side),
            self.out_sem.at[0, index, step],
            self.out_sem.at[1, index, step],
            {"fsdp": target},
        )

    def taken(self, index, step, side):
        device = lax.rem(self.place.device + self.place.count - step, self.place.count)
        return self.pairs[index][1](device, side)

    def come(self, index, step):
        place = self.place
        return remote(
            self.pairs[index][0](place.device),
            self.taken(index, step, place.side),
            self.out_sem.at[0, index, step],
            self.out_sem.at[1, index, step],
            place.across(),
        )

    def share(self, index, step, source=None):
        spot = self.taken(index, step, self.place.side)
        return remote(
            spot if source is None else source,
            spot,
            self.side_sem.at[0, index, step],
            self.side_sem.at[1, index, step],
            self.place.across(),
        )

    def shared(self, index, step):
        spot = self.taken(index, step, 1 - self.place.side)
        return remote(
            spot,
            spot,
            self.side_sem.at[0, index, step],
            self.side_sem.at[1, index, step],
            self.place.across(),
        )

    def keep(self, index):
        place = self.place
        source, spot = self.pairs[index]
        return pltpu.make_async_copy(
            source(place.device), spot(place.device, place.side), self.local_sem.at[index]
        )

    def each(self, first, body):
        def step(number, carry):
            for index in range(len(self.pairs)):
                body(index, number)
            return carry

        lax.fori_loop(first, self.place.count, step, 0)

    def start(self):
        self.each(1, lambda index, step: self.send(index, step).start())
        for index, (source, _) in enumerate(self.pairs):
            self.keep(index).start()
            self.share(index, 0, source(self.place.device)).start()

    def pass_on(self):
        def one(index, step):
            self.come(index, step).wait_recv()
            self.share(index, step).start()

        self.each(1, one)

    def finish(self):
        for index in range(len(self.pairs)):
            self.keep(index).wait()
        self.each(0, lambda index, step: self.shared(index, step).wait_recv())
        self.each(1, lambda index, step: self.send(index, step).wait_send())
        self.each(0, lambda index, step: self.share(index, step).wait_send())


def whole_pair(pieces, whole):
    return (lambda target: pieces.at[target], lambda device, side: whole.at[device, side])


def halves_scratch(arrays):
    return [DMA((3, arrays))]


class Halves:
    def __init__(self, place, halves, wholes, scratch):
        self.place = place
        self.pairs = list(zip(halves, wholes))
        (self.sem,) = scratch

    def keep(self, index):
        half, whole = self.pairs[index]
        return pltpu.make_async_copy(half, whole.at[:, self.place.side], self.sem.at[0, index])

    def copy(self, index, side):
        half, whole = self.pairs[index]
        return remote(
            half,
            whole.at[:, side],
            self.sem.at[1, index],
            self.sem.at[2, index],
            self.place.across(),
        )

    def start(self):
        for index in range(len(self.pairs)):
            self.copy(index, self.place.side).start()
            self.keep(index).start()

    def finish(self):
        for index in range(len(self.pairs)):
            self.keep(index).wait()
            self.copy(index, 1 - self.place.side).wait_recv()
            self.copy(index, self.place.side).wait_send()


REDUCE = 9
GATHER = 5
PIECES = 8


def first_kernel(
    own_ref, query, key, value, out, small, gathered, qkv_all, out_all, small_all, *scratch
):
    place = Place()
    sender = Sender()
    own = scratch[0]
    own[...] = own_ref[...]
    greet_all(place)
    half, columns = qkv_all.shape[2], qkv_all.shape[3] // 3
    out_half = out_all.shape[2]
    rows = pl.ds(pl.multiple_of(place.side * half, half), half)

    def member(target):
        return lax.rem(target, 2 * LINE)

    def column_pair(weight, index):
        def source(target):
            start = pl.multiple_of(member(target) * columns, columns)
            return weight.at[rows, pl.ds(start, columns)]

        def spot(device, side):
            return qkv_all.at[device, side, :, pl.ds(index * columns, columns)]

        return (source, spot)

    def out_source(target):
        start = (2 * member(target) + place.side) * out_half
        return out.at[pl.ds(pl.multiple_of(start, out_half), out_half)]

    pairs = [
        (lambda target: small, lambda device, side: small_all.at[device, side]),
        column_pair(query, 0),
        column_pair(key, 1),
        column_pair(value, 2),
        (out_source, lambda device, side: out_all.at[device, side]),
    ]
    swap = Swap(place, pairs, scratch[GATHER:])
    gather_phase(place, sender, gathered, scratch[:GATHER], swap.start, swap.pass_on)
    swap.finish()
    sender.drain()


def hidden_kernel(
    partial, tokens, gain, pair, down, gathered, branch, hidden, pair_all, down_all, *scratch
):
    place = Place()
    sender = Sender()
    greet(place, True)
    halves = Halves(place, (pair, down), (pair_all, down_all), scratch[REDUCE + GATHER :])
    halves.start()
    reduce_phase(place, sender, partial, scratch[:REDUCE])
    total, own = scratch[4], scratch[REDUCE]
    rows, width = total.shape

    def body(at):
        value = total[at]
        scale = lax.rsqrt(jnp.sum(value * value, axis=1, keepdims=True) / width + EPS)
        result = tokens[at].astype(F32) + value * scale * gain[...]
        branch[at] = value
        hidden[at] = result
        own[at] = result.astype(BF)

    by_rows(rows, body)
    gather_phase(place, sender, gathered, scratch[REDUCE : REDUCE + GATHER])
    halves.finish()
    sender.drain()


def turn_kernel(partial, hidden, cotangent, gain, gathered, outputs, gain_grad, *scratch):
    place = Place()
    sender = Sender()
    greet(place)
    reduce_phase(place, sender, partial, scratch[:REDUCE])
    total, own = scratch[4], scratch[REDUCE]
    out_own = scratch[REDUCE + GATHER]
    rows, width = total.shape
    gain_grad[...] = jnp.zeros_like(gain_grad)

    def body(at):
        value = total[at]
        scale = lax.rsqrt(jnp.sum(value * value, axis=1, keepdims=True) / width + EPS)
        grads = cotangent[at].astype(F32)
        normed = value * scale
        out_own[at] = (hidden[at] + normed * gain[...]).astype(BF)
        gain_grad[...] += jnp.sum(grads * normed, axis=0, keepdims=True)
        gained = gain[...] * grads
        inner = jnp.sum(normed * gained, axis=1, keepdims=True)
        own[at] = (scale * (gained - normed * (inner / width))).astype(BF)

    by_rows(rows, body)
    finish = pair_phase(place, sender, out_own, outputs, scratch[REDUCE + GATHER + 1 :])
    gather_phase(place, sender, gathered, scratch[REDUCE : REDUCE + GATHER])
    finish()
    sender.drain()


class WeightGrads:
    def __init__(self, place, arrays, outs, scratch):
        self.place = place
        self.inner, self.grad_mlp, self.hidden, self.grad_pair = arrays
        self.outs = outs
        self.tall, self.turned, self.inner_turned = scratch[:3]
        self.fulls, self.others = scratch[3:5], scratch[5:7]
        self.fetch_sem, self.side_sem = scratch[7:]
        self.piece = self.tall.shape[3]

    def fetch(self, number, slot):
        columns = pl.ds(pl.multiple_of(number * self.piece, self.piece), self.piece)
        return [
            pltpu.make_async_copy(
                array.at[:, columns], self.tall.at[slot, index], self.fetch_sem.at[slot, index]
            )
            for index, array in enumerate((self.hidden, self.grad_mlp))
        ]

    def side_of(self, index, number, side):
        if index == 0:
            return self.fulls[0].at[number, :, side]
        return self.fulls[1].at[number, side]

    def crossing(self, number, index):
        return remote(
            self.side_of(index, number, 1 - self.place.side),
            self.others[index].at[number],
            self.side_sem.at[0, index, number],
            self.side_sem.at[1, index, number],
            self.place.across(),
        )

    def start(self):
        for copy in self.fetch(0, 0):
            copy.start()
        self.inner_turned[...] = self.inner[...].T

    def one(self, number, carry):
        slot = lax.rem(number, 2)
        for copy in self.fetch(number, slot):
            copy.wait()

        @pl.when(number < PIECES - 1)
        def _():
            for copy in self.fetch(number + 1, 1 - slot):
                copy.start()

        full, low = self.fulls
        self.turned[...] = self.tall[slot, 0].T
        columns = self.grad_pair.shape[1]
        step = columns // 4

        def columns_step(index, carry):
            at = pl.ds(pl.multiple_of(index * step, step), step)
            value = product(self.turned[...], self.grad_pair[:, at]).astype(BF)
            full[number, :, :, :, at] = value.reshape(full.shape[1:4] + (step,))
            return carry

        lax.fori_loop(0, 4, columns_step, 0)
        value = product(self.inner_turned[...], self.tall[slot, 1]).astype(BF)
        low[number] = value.reshape(low.shape[1:])
        for index in range(2):
            self.crossing(number, index).start()
        return carry

    def some(self, which):
        half = PIECES // 2
        lax.fori_loop(which * half, which * half + half, self.one, 0)

    def add(self):
        def step(number, carry):
            for index in range(2):
                self.crossing(number, index).wait_recv()
                own = self.side_of(index, number, self.place.side)[...].astype(F32)
                other = self.others[index][number].astype(F32)
                self.outs[index][number] = (own + other).astype(BF)
            return carry

        lax.fori_loop(0, PIECES, step, 0)

    def finish(self):
        def step(number, carry):
            for index in range(2):
                self.crossing(number, index).wait_send()
            return carry

        lax.fori_loop(0, PIECES, step, 0)


def branch_kernel(
    partial,
    branch,
    cotangent,
    gain,
    inner_low,
    grad_mlp,
    hidden_low,
    grad_pair,
    gathered,
    grad_hidden,
    gain_grad,
    pair_mine,
    down_mine,
    *scratch,
):
    place = Place()
    sender = Sender()
    greet(place, True)
    grads = WeightGrads(
        place,
        (inner_low, grad_mlp, hidden_low, grad_pair),
        (pair_mine, down_mine),
        scratch[REDUCE + GATHER :],
    )
    grads.start()
    reduce_phase(place, sender, partial, scratch[:REDUCE], idle=grads.some)
    total, own = scratch[4], scratch[REDUCE]
    rows, width = total.shape
    gain_grad[...] = jnp.zeros_like(gain_grad)

    def body(at):
        value = branch[at]
        scale = lax.rsqrt(jnp.sum(value * value, axis=1, keepdims=True) / width + EPS)
        grads = cotangent[at].astype(F32) + total[at]
        grad_hidden[at] = grads
        normed = value * scale
        gain_grad[...] += jnp.sum(grads * normed, axis=0, keepdims=True)
        gained = gain[...] * grads
        inner = jnp.sum(normed * gained, axis=1, keepdims=True)
        own[at] = (scale * (gained - normed * (inner / width))).astype(BF)

    by_rows(rows, body)
    gather_phase(
        place, sender, gathered, scratch[REDUCE : REDUCE + GATHER], last=grads.add
    )
    grads.finish()
    sender.drain()


def last_kernel(
    partial,
    grad_hidden,
    qkv,
    out,
    small,
    down,
    result,
    qkv_all,
    out_all,
    small_all,
    down_all,
    *scratch,
):
    place = Place()
    sender = Sender()
    parts = scratch[REDUCE + 1 :]
    swap_sems, halves_sems, parts = parts[:3], parts[3:4], parts[4:]
    qkv_own, qkv_other, out_own, out_other, small_own, small_other, fetch_sem, side_sem = parts
    greet_all(place)
    fetches, crossings = [], []
    for index, (grad, own, other) in enumerate(
        ((qkv, qkv_own, qkv_other), (out, out_own, out_other))
    ):
        fetches.append(
            pltpu.make_async_copy(grad.at[:, place.side], own, fetch_sem.at[index])
        )
        crossings.append(
            remote(
                grad.at[:, 1 - place.side],
                other,
                side_sem.at[0, index],
                side_sem.at[1, index],
                place.across(),
            )
        )
    crossings.append(
        remote(
            small,
            small_other,
            side_sem.at[0, 2],
            side_sem.at[1, 2],
            place.at(place.z, place.y, 1 - place.core),
        )
    )
    for copy in fetches + crossings:
        copy.start()
    pairs = ((small_own, small_all), (qkv_own, qkv_all), (out_own, out_all))
    swap = Swap(place, [whole_pair(*pair) for pair in pairs], swap_sems)
    halves = Halves(place, (down,), (down_all,), halves_sems)
    shared_rows = 2 * partial.shape[1] // place.count // 128

    def between():
        for fetch in fetches:
            fetch.wait()
        for crossing in crossings:
            crossing.wait()
        small_own[...] = small[...]
        small_own[:, :shared_rows] += small_other[:, :shared_rows]

        def one(index, carry):
            qkv_own[index] = (
                qkv_own[index].astype(F32) + qkv_other[index].astype(F32)
            ).astype(BF)
            out_own[index] = (
                out_own[index].astype(F32) + out_other[index].astype(F32)
            ).astype(BF)
            return carry

        lax.fori_loop(0, place.count, one, 0)
        swap.start()
        halves.start()

    reduce_phase(place, sender, partial, scratch[:REDUCE], between)
    total = scratch[4]

    def body(at):
        total[at] += grad_hidden[at]

    by_rows(total.shape[0], body)
    finish = pair_phase(place, sender, total, result, scratch[REDUCE : REDUCE + 1])
    swap.pass_on()
    finish()
    halves.finish()
    swap.finish()
    sender.drain()


def sum_kernel(carried, value, *rest):
    if carried:
        moved, result, arrived, core_in, y_in, held, line_in, sem, side_sem = rest
    else:
        result, core_in, y_in, held, line_in, sem = rest
    place = Place()
    z, y, core = place.z, place.y, place.core
    barrier = pltpu.get_barrier_semaphore()
    others = [place.at(z, y, 1 - core), place.at(z, 1 - y, core)]
    others += [place.at(lax.rem(z + k, LINE), y, core) for k in range(1, LINE)]
    for device in others + [place.across()] * carried:
        signal(barrier, device)
    pl.semaphore_wait(barrier, len(others) + carried)
    if carried:
        side = remote(moved, arrived, side_sem.at[0], side_sem.at[1], place.across())
        side.start()
    first = remote(value, core_in, sem.at[0, 0], sem.at[1, 0], others[0])
    first.start()
    first.wait_recv()
    held[0] = value[...] + core_in[...]
    second = remote(held.at[0], y_in, sem.at[0, 1], sem.at[1, 1], others[1])
    second.start()
    second.wait_recv()
    held[1] = held[0] + y_in[...]
    sends = [
        remote(held.at[1], line_in.at[k - 1], sem.at[0, 1 + k], sem.at[1, 1 + k], others[1 + k])
        for k in range(1, LINE)
    ]
    for send in sends:
        send.start()
    line_in[LINE - 1] = held[1]
    for send in sends:
        send.wait_recv()
    added = jnp.zeros_like(value)
    for source in range(LINE):
        slot = lax.rem(z - source + 2 * LINE - 1, LINE)
        added = added + line_in[slot]
    result[...] = added
    first.wait_send()
    second.wait_send()
    for send in sends:
        send.wait_send()
    if carried:
        side.wait()


def pack_kernel(side, gate, up, down, pair_out, down_out):
    columns = gate.shape[1]
    pair_out[0, :, :columns] = gate[...]
    pair_out[0, :, columns:] = up[...]
    down_out[0] = down[...]


def unpack_kernel(side, own, other, down, gate_out, up_out, down_out):
    half, columns = own.shape[2], gate_out.shape[1]
    for part, start in ((own, side[0]), (other, 1 - side[0])):
        value = jnp.sum(part[:, 0].astype(F32), axis=0)
        rows = pl.ds(pl.multiple_of(start * half, half), half)
        gate_out[rows] = value[:, :columns]
        up_out[rows] = value[:, columns:]
    down_out[...] = jnp.sum(down[:, 0].astype(F32), axis=0)


def talk(kernel, which, shapes, specs, scratch, microseconds, name=None):
    def call(*operands):
        return pl.pallas_call(
            kernel,
            out_shape=shapes,
            in_specs=specs[0],
            out_specs=specs[1],
            scratch_shapes=scratch,
            compiler_params=pltpu.CompilerParams(
                collective_id=which, has_side_effects=True, vmem_limit_bytes=48 << 20
            ),
            cost_estimate=pl.CostEstimate(
                flops=0, bytes_accessed=int(microseconds * 3.0e6), transcendentals=0
            ),
            name=name or kernel.__name__,
        )(*operands)

    return call


class Team:
    def __init__(self, local_heads, rows, width):
        self.fsdp = lax.axis_size("fsdp")
        self.tensor = lax.axis_size("tensor")
        self.size = 2 * LINE
        self.teams = self.fsdp // self.size
        assert self.fsdp % self.size == 0 and self.tensor == 2 and local_heads % self.size == 0
        self.member = lax.rem(lax.axis_index("fsdp"), self.size)
        self.core = lax.axis_index("tensor")
        self.context = lax.axis_index("context")
        self.groups = None
        if self.teams > 1:
            self.groups = [
                [team * self.size + one for one in range(self.size)] for team in range(self.teams)
            ]
        self.rows = rows
        self.width = width
        self.all_low = jax.ShapeDtypeStruct((2 * self.size * rows, width), BF)
        self.own_wide = jax.ShapeDtypeStruct((rows, width), F32)
        self.line_wide = jax.ShapeDtypeStruct((1, width), F32)
        self.reduces = reduce_scratch(rows, width)
        self.gathers = gather_scratch(rows, width)

    def whole(self, pieces):
        shape = (pieces.shape[0], 2) + pieces.shape[1:]
        return jax.ShapeDtypeStruct(shape, pieces.dtype)

    def first(self, own, weights, out, small):
        rows, columns = weights[0].shape
        rows, columns = rows // 2, columns // self.size
        out_rows = out.shape[0] // self.size // 2
        return talk(
            first_kernel,
            0,
            (
                self.all_low,
                jax.ShapeDtypeStruct((self.fsdp, 2, rows, 3 * columns), BF),
                jax.ShapeDtypeStruct((self.fsdp, 2, out_rows, out.shape[1]), BF),
                jax.ShapeDtypeStruct((self.fsdp, 2) + small.shape, F32),
            ),
            ([VMEM] * 6, (HBM,) * 4),
            self.gathers + swap_scratch(self.fsdp, 5),
            80,
        )(own, *weights, out, small)

    def pack(self, gate, up, down):
        rows, columns = gate.shape
        rows, columns = rows // 2, columns // self.size
        down_rows, down_columns = down.shape
        down_rows = down_rows // self.size // 2

        def column_spec():
            return pl.BlockSpec((rows, columns), lambda d, side: (side[0], d))

        def piece_spec(*shape):
            return pl.BlockSpec((1,) + shape, lambda d, side: (d, 0, 0))

        pair, low = pl.pallas_call(
            pack_kernel,
            grid_spec=pltpu.PrefetchScalarGridSpec(
                num_scalar_prefetch=1,
                grid=(self.size,),
                in_specs=[
                    column_spec(),
                    column_spec(),
                    pl.BlockSpec((down_rows, down_columns), lambda d, side: (2 * d + side[0], 0)),
                ],
                out_specs=[piece_spec(rows, 2 * columns), piece_spec(down_rows, down_columns)],
            ),
            out_shape=[
                jax.ShapeDtypeStruct((self.size, rows, 2 * columns), BF),
                jax.ShapeDtypeStruct((self.size, down_rows, down_columns), BF),
            ],
            name="pack_kernel",
        )(self.context.reshape(1).astype(jnp.int32), gate, up, down)
        return self.repeat(pair), self.repeat(low)

    def hidden(self, partial, tokens, gain, pair, down):
        return talk(
            hidden_kernel,
            1,
            (self.all_low, self.own_wide, self.own_wide, self.whole(pair), self.whole(down)),
            ([HBM, VMEM, VMEM, VMEM, VMEM], (HBM, VMEM, VMEM, HBM, HBM)),
            self.reduces + self.gathers + halves_scratch(2),
            100,
        )(partial, tokens, gain, pair, down)

    def turn(self, partial, hidden, cotangent, gain):
        pair = jax.ShapeDtypeStruct((2 * self.rows, self.width), BF)
        return talk(
            turn_kernel,
            2,
            (self.all_low, pair, self.line_wide),
            ([HBM, VMEM, VMEM, VMEM], (HBM, HBM, VMEM)),
            self.reduces + self.gathers + [pltpu.VMEM((self.rows, self.width), BF)] + pair_scratch(),
            100,
        )(partial, hidden, cotangent, gain)

    def branch(self, partial, branch, cotangent, gain, inner, grad_mlp, hidden, grad_pair):
        team_rows, units = inner.shape
        columns = grad_pair.shape[1]
        piece = self.width // PIECES
        count = self.fsdp // PIECES
        half = self.width // self.fsdp // 2
        pair_shape = (PIECES, count, half, columns)
        down_shape = (PIECES, units // 2, piece)

        def both(shape):
            return pltpu.VMEM((shape[0], 2) + shape[1:], BF)

        def sides_inside(shape):
            return pltpu.VMEM((shape[0], shape[1], 2) + shape[2:], BF)

        gathered, grad_hidden, gain_grad, pair_mine, down_mine = talk(
            branch_kernel,
            3,
            (
                self.all_low,
                self.own_wide,
                self.line_wide,
                jax.ShapeDtypeStruct(pair_shape, BF),
                jax.ShapeDtypeStruct(down_shape, BF),
            ),
            (
                [HBM, VMEM, VMEM, VMEM, VMEM, HBM, HBM, VMEM],
                (HBM, VMEM, VMEM, VMEM, VMEM),
            ),
            self.reduces
            + self.gathers
            + [
                pltpu.VMEM((2, 2, team_rows, piece), BF),
                pltpu.VMEM((piece, team_rows), BF),
                pltpu.VMEM((units, team_rows), BF),
                sides_inside(pair_shape),
                both(down_shape),
                pltpu.VMEM(pair_shape, BF),
                pltpu.VMEM(down_shape, BF),
                DMA((2, 2)),
                DMA((2, 2, PIECES)),
            ],
            100,
        )(partial, branch, cotangent, gain, inner, grad_mlp, hidden, grad_pair)
        down_mine = down_mine.reshape(PIECES, units // 2, count, piece // count)
        return (
            gathered,
            grad_hidden,
            gain_grad,
            pair_mine.reshape(self.fsdp, half, columns),
            down_mine.transpose(0, 2, 1, 3).reshape(self.fsdp, units // 2, piece // count),
        )

    def last(self, partial, grad_hidden, qkv, out, small, down):
        both = jax.ShapeDtypeStruct((2 * self.rows, self.width), F32)

        def same(array):
            return jax.ShapeDtypeStruct(array.shape, array.dtype)

        def half(array):
            return pltpu.VMEM((array.shape[0],) + array.shape[2:], array.dtype)

        held = pltpu.VMEM(small.shape, small.dtype)
        return talk(
            last_kernel,
            4,
            (both, same(qkv), same(out), self.whole(small), self.whole(down)),
            ([HBM, VMEM, HBM, HBM, VMEM, VMEM], (HBM,) * 5),
            self.reduces
            + pair_scratch()
            + swap_scratch(self.fsdp, 3)
            + halves_scratch(1)
            + [half(qkv), half(qkv), half(out), half(out), held, held, DMA((2,)), DMA((2, 3))],
            80,
        )(partial, grad_hidden, qkv, out, small, down)

    def total(self, values, moved=None):
        flat = values.reshape(-1, 128)
        carried = int(moved is not None)
        shape = jax.ShapeDtypeStruct(flat.shape, F32)
        scratch = [pltpu.VMEM(flat.shape, F32)] * 2
        scratch += [pltpu.VMEM((2,) + flat.shape, F32), pltpu.VMEM((LINE,) + flat.shape, F32)]
        scratch += [DMA((2, LINE + 1))] + [DMA((2,))] * carried
        which = 5 + self.sums
        self.sums += 1
        kernel = functools.partial(sum_kernel, carried)
        if not carried:
            call = talk(kernel, which, shape, ([VMEM], VMEM), scratch, 10, "sum_kernel")
            return call(flat).reshape(values.shape)
        shapes = (shape, jax.ShapeDtypeStruct(moved.shape, moved.dtype))
        call = talk(kernel, which, shapes, ([VMEM] * 2, (VMEM,) * 2), scratch, 10, "sum_kernel")
        total, came = call(flat, moved)
        return total.reshape(values.shape), came

    sums = 0

    def half(self, array, axis):
        count = array.shape[axis] // 2
        return lax.dynamic_slice_in_dim(array, self.context * count, count, axis)

    def swap(self, pieces):
        return lax.all_to_all(pieces, "fsdp", split_axis=0, concat_axis=0, tiled=True)

    def repeat(self, pieces):
        return jnp.concatenate([pieces] * self.teams, axis=0) if self.teams > 1 else pieces

    def unpack(self, own, other, down):
        half, columns = own.shape[1], own.shape[2] // 2
        rows, down_columns = 2 * down.shape[2], down.shape[3]

        def cut(array, *shape):
            return array.reshape((self.teams, self.size) + shape)

        def piece_spec(*shape):
            return pl.BlockSpec((self.teams, 1) + shape, lambda d, side: (0, d, 0, 0))

        wide = pl.BlockSpec((2 * half, columns), lambda d, side: (0, d))
        wide_shape = jax.ShapeDtypeStruct((2 * half, self.size * columns), F32)
        return pl.pallas_call(
            unpack_kernel,
            grid_spec=pltpu.PrefetchScalarGridSpec(
                num_scalar_prefetch=1,
                grid=(self.size,),
                in_specs=[piece_spec(half, 2 * columns)] * 2 + [piece_spec(rows, down_columns)],
                out_specs=[wide, wide, pl.BlockSpec((rows, down_columns), lambda d, side: (d, 0))],
            ),
            out_shape=[
                wide_shape,
                wide_shape,
                jax.ShapeDtypeStruct((self.size * rows, down_columns), F32),
            ],
            name="unpack_kernel",
        )(
            self.context.reshape(1).astype(jnp.int32),
            cut(own, half, 2 * columns),
            cut(other, half, 2 * columns),
            cut(down, rows, down_columns),
        )

    def columns_whole(self, came):
        return came.reshape(-1, came.shape[-1])

    def rows_whole(self, came):
        fsdp, two, rows, columns = came.shape
        return came.transpose(1, 2, 0, 3).reshape(two * rows, fsdp * columns)

    def of_columns(self, grad):
        rows, columns = grad.shape
        return grad.astype(BF).reshape(self.fsdp, 2, rows // self.fsdp // 2, columns)

    def of_rows(self, grad):
        rows, columns = grad.shape
        cut = grad.astype(BF).reshape(2, rows // 2, self.fsdp, columns // self.fsdp)
        return cut.transpose(2, 0, 1, 3)

    def added(self, came):
        if self.teams == 1:
            return came.astype(F32)
        came = came.reshape((self.teams, self.size) + came.shape[1:])
        return jnp.sum(came.astype(F32), axis=0)

    def columns_out(self, came, count):
        size, two, rows, columns = came.shape
        return [
            self.added(part.reshape(size, two * rows, -1))
            .transpose(1, 0, 2)
            .reshape(two * rows, -1)
            for part in jnp.split(came, count, axis=3)
        ]

    def rows_out(self, came):
        return self.added(came).reshape(-1, came.shape[-1])


def local(
    tokens,
    cont_lengths,
    w_query,
    w_key,
    w_value,
    w_output,
    query_gain,
    key_gain,
    attn_gain,
    w_gate,
    w_up,
    w_down,
    mlp_gain,
    cotangent,
):
    rows = tokens.shape[0]
    width = tokens.shape[1]
    fsdp = lax.axis_size("fsdp")
    tensor = lax.axis_size("tensor")
    local_heads = query_gain.shape[0]
    head_size = w_query.shape[1] // local_heads
    own_rows = rows // tensor
    team = Team(local_heads, own_rows, width)
    groups = team.size
    team_rows = groups * rows
    heads = local_heads // team.size
    later = lax.axis_index("context") == 1

    tokens_own = lax.dynamic_slice_in_dim(tokens, team.core * own_rows, own_rows, 0)
    grad_out = lax.dynamic_slice_in_dim(cotangent, team.core * own_rows, own_rows, 0)
    cut = query_gain.size
    share = attn_gain.size
    small = [query_gain.reshape(-1), key_gain.reshape(-1), attn_gain, mlp_gain]
    small = jnp.concatenate([one.astype(F32) for one in small + [cont_lengths.reshape(-1)]])
    small = jnp.pad(small, (0, 8 * 128 - small.size)).reshape(8, 128)
    tokens_all, qkv_came, output_came, small_came = team.first(
        tokens_own, [w_query, w_key, w_value], w_output, small
    )
    qkv_w = team.columns_whole(qkv_came)
    output_w = team.rows_whole(output_came)
    all_small = small_came[:, 0].reshape(fsdp, -1)
    query_gains = all_small[:, :cut].reshape(fsdp, local_heads, -1)
    key_gains = all_small[:, cut : 2 * cut].reshape(fsdp, local_heads, -1)
    query_gains = query_gains.transpose(1, 0, 2).reshape(local_heads, head_size)
    key_gains = key_gains.transpose(1, 0, 2).reshape(local_heads, head_size)
    flat_query = lax.dynamic_slice_in_dim(query_gains, team.member * heads, heads, 0).reshape(-1)
    flat_key = lax.dynamic_slice_in_dim(key_gains, team.member * heads, heads, 0).reshape(-1)
    gain_attn = all_small[:, 2 * cut : 2 * cut + share].reshape(1, -1)
    gain_mlp = all_small[:, 2 * cut + share : 2 * cut + 2 * share].reshape(1, -1)

    conts = cont_lengths.shape[1]
    lengths = all_small[:, 2 * cut + 2 * share : 2 * cut + 2 * share + conts].astype(jnp.int32)
    first_group = lax.axis_index("fsdp") - team.member
    lengths = lax.dynamic_slice_in_dim(lengths, first_group, groups, 0)
    segment, offset = jax.vmap(lambda one: layout(one, rows))(lengths)
    row_index = jnp.arange(rows, dtype=jnp.int32)
    positions = jnp.where(later, rows + offset, row_index[None, :])
    own_segment = jnp.where(later, segment, -1)
    cosine, sine = rotary_tables(positions, head_size)
    cosine = cosine[:, :, None, :]
    sine = sine[:, :, None, :]

    pair_mine, down_mine, tokens_all = lax.optimization_barrier(
        team.pack(w_gate, w_up, w_down) + (tokens_all,)
    )
    pair_came = team.swap(pair_mine)
    down_came = team.swap(down_mine)

    by_head = (groups, rows, heads, head_size)
    raw = product(tokens_all, qkv_w)
    query_raw, key_raw, value_raw = jnp.split(raw, 3, axis=1)
    value_low = value_raw.astype(BF)
    sums, sent_value = team.total(
        jnp.stack([jnp.sum(query_raw * query_raw, axis=1), jnp.sum(key_raw * key_raw, axis=1)]),
        value_low,
    )
    value_low, sent_value = value_low.reshape(by_head), sent_value.reshape(by_head)
    scale_query = lax.rsqrt(sums[0] / width + EPS)[:, None]
    scale_key = lax.rsqrt(sums[1] / width + EPS)[:, None]
    query_norm = query_raw * scale_query * flat_query
    key_norm = key_raw * scale_key * flat_key
    query_low = rotate(query_norm.reshape(by_head), cosine, sine).astype(BF)
    key_low = rotate(key_norm.reshape(by_head), cosine, sine).astype(BF)
    sent_key = lax.ppermute(key_low, "context", [(0, 1)])
    keys_all = jnp.concatenate([sent_key, key_low], axis=1)
    values_all = jnp.concatenate([sent_value, value_low], axis=1)
    key_index = jnp.arange(2 * rows, dtype=jnp.int32)
    key_segment = jnp.concatenate([jnp.full((groups, rows), -2, jnp.int32), own_segment], axis=1)
    remote = (key_index < rows)[None, None, :] & later
    own_keys = (
        (key_index >= rows)[None, None, :]
        & (key_index[None, None, :] - rows <= row_index[None, :, None])
        & (key_segment[:, None, :] == own_segment[:, :, None])
    )
    allowed = (remote | own_keys)[:, None]
    scale = 1.0 / math.sqrt(head_size)
    scores = (
        jnp.einsum("gqhd,gkhd->ghqk", query_low, keys_all, preferred_element_type=F32) * scale
    )
    scores = jnp.where(allowed, scores, -1e30)
    highest = jnp.max(scores, axis=-1, keepdims=True)
    weights = jnp.exp(scores - highest)
    probs = weights / jnp.sum(weights, axis=-1, keepdims=True)
    probs_low = probs.astype(BF)
    mixed = jnp.einsum("ghqk,gkhd->gqhd", probs_low, values_all, preferred_element_type=F32)
    attended_low = mixed.reshape(team_rows, heads * head_size).astype(BF)
    hidden_all, attn_sum, hidden, pair_came, down_came = team.hidden(
        product(attended_low, output_w).astype(BF), tokens_own, gain_attn, pair_came, down_came
    )
    pair_w = team.columns_whole(pair_came)
    down_w = team.rows_whole(down_came)

    gate, upward = jnp.split(product(hidden_all, pair_w), 2, axis=1)
    sigma = jax.nn.sigmoid(gate)
    inner_low = (gate * sigma * upward).astype(BF)
    grad_mlp_all, outputs, grad_mlp_gain = team.turn(
        product(inner_low, down_w).astype(BF), hidden, grad_out, gain_mlp
    )
    grad_inner = product_right(grad_mlp_all, down_w)
    grad_gate_low = (grad_inner * upward * sigma * (1.0 + gate * (1.0 - sigma))).astype(BF)
    grad_up_low = (grad_inner * gate * sigma).astype(BF)
    grad_pair = jnp.concatenate([grad_gate_low, grad_up_low], axis=1)
    grad_branch_all, grad_hidden, grad_attn_gain, pair_mine, down_mine = team.branch(
        product_right(grad_pair, pair_w).astype(BF),
        attn_sum,
        grad_out,
        gain_attn,
        inner_low,
        grad_mlp_all,
        hidden_all,
        grad_pair,
    )
    pair_came = team.swap(pair_mine)
    output_grad = team.of_rows(product_left(attended_low, grad_branch_all))
    grad_attended = product_right(grad_branch_all, output_w).astype(BF).reshape(by_head)

    grad_probs = jnp.einsum("gqhd,gkhd->ghqk", grad_attended, values_all, preferred_element_type=F32)
    centre = jnp.sum(probs * grad_probs, axis=-1, keepdims=True)
    grad_scores = (probs * (grad_probs - centre)).astype(BF)
    grad_query_rot = (
        jnp.einsum("ghqk,gkhd->gqhd", grad_scores, keys_all, preferred_element_type=F32) * scale
    )
    grad_keys = (
        jnp.einsum("ghqk,gqhd->gkhd", grad_scores, query_low, preferred_element_type=F32) * scale
    )
    grad_values = jnp.einsum("ghqk,gqhd->gkhd", probs_low, grad_attended, preferred_element_type=F32)
    back_value = lax.ppermute(grad_values[:, :rows].astype(BF), "context", [(1, 0)])
    back_key = lax.ppermute(grad_keys[:, :rows].astype(BF), "context", [(1, 0)])
    grad_key_rot = grad_keys[:, rows:] + back_key.astype(F32)
    grad_value_low = (
        (grad_values[:, rows:] + back_value.astype(F32)).reshape(team_rows, -1).astype(BF)
    )
    grad_query_norm = rotate_back(grad_query_rot, cosine, sine).reshape(team_rows, -1)
    grad_key_norm = rotate_back(grad_key_rot, cosine, sine).reshape(team_rows, -1)
    grad_query_gain = jnp.sum(grad_query_norm * query_raw * scale_query, axis=0)
    grad_key_gain = jnp.sum(grad_key_norm * key_raw * scale_key, axis=0)
    inner_sums = jnp.stack(
        [
            jnp.sum(query_raw * flat_query * grad_query_norm, axis=1),
            jnp.sum(key_raw * flat_key * grad_key_norm, axis=1),
        ]
    )
    inner_sums, pair_came = lax.optimization_barrier((inner_sums, pair_came))
    pair_other = lax.ppermute(pair_came, "context", [(0, 1), (1, 0)])
    totals = team.total(inner_sums)
    down_mine, totals = lax.optimization_barrier((down_mine, totals))
    down_came = team.swap(down_mine)
    grad_query_low = norm_back(
        query_raw, scale_query, flat_query, grad_query_norm, totals[0][:, None], width
    ).astype(BF)
    grad_key_low = norm_back(
        key_raw, scale_key, flat_key, grad_key_norm, totals[1][:, None], width
    ).astype(BF)
    grad_qkv = jnp.concatenate([grad_query_low, grad_key_low, grad_value_low], axis=1)
    qkv_grad = team.of_columns(product_left(tokens_all, grad_qkv))
    head_share = head_size // fsdp
    small = [
        grad_attn_gain.reshape(fsdp, share),
        grad_mlp_gain.reshape(fsdp, share),
        grad_query_gain.reshape(heads, fsdp, head_share).transpose(1, 0, 2).reshape(fsdp, -1),
        grad_key_gain.reshape(heads, fsdp, head_share).transpose(1, 0, 2).reshape(fsdp, -1),
    ]
    used = 2 * share + 2 * heads * head_share
    small = jnp.concatenate(small + [jnp.zeros((fsdp, 8 * 128 - used), F32)], axis=1)
    partial, pair_other = lax.optimization_barrier(
        (product_right(grad_qkv, qkv_w).astype(BF), pair_other)
    )
    input_grad, qkv_came, output_came, small_came, down_came = team.last(
        partial,
        grad_hidden,
        qkv_grad,
        output_grad,
        small.reshape(fsdp, 8, 128),
        down_came,
    )
    grad_w_query, grad_w_key, grad_w_value = team.columns_out(qkv_came, 3)
    grad_w_gate, grad_w_up, grad_w_down = team.unpack(pair_came, pair_other, down_came)
    grad_w_output = team.rows_out(output_came)
    came = jnp.sum(small_came, axis=1).reshape(fsdp, -1)
    row_gains = jnp.sum(came[:, : 2 * share], axis=0).reshape(2, share)
    head_gains = team.added(came[:, 2 * share : used]).reshape(team.size, 2, heads, head_share)
    head_gains = head_gains.transpose(1, 0, 2, 3).reshape(2, local_heads, head_share)
    return (
        outputs,
        input_grad,
        grad_w_query,
        grad_w_key,
        grad_w_value,
        grad_w_output,
        head_gains[0],
        head_gains[1],
        row_gains[0],
        grad_w_gate,
        grad_w_up,
        grad_w_down,
        row_gains[1],
    )


def solution(mesh):
    return jax.shard_map(
        local,
        mesh=mesh,
        in_specs=(
            P(("fsdp", "context"), None),
            P("fsdp", None),
            P("fsdp", "tensor"),
            P("fsdp", "tensor"),
            P("fsdp", "tensor"),
            P("tensor", "fsdp"),
            P("tensor", "fsdp"),
            P("tensor", "fsdp"),
            P("fsdp"),
            P("fsdp", "tensor"),
            P("fsdp", "tensor"),
            P("tensor", "fsdp"),
            P("fsdp"),
            P(("fsdp", "context"), None),
        ),
        out_specs=(
            P(("fsdp", "context"), None),
            P(("fsdp", "context"), None),
            P("fsdp", "tensor"),
            P("fsdp", "tensor"),
            P("fsdp", "tensor"),
            P("tensor", "fsdp"),
            P("tensor", "fsdp"),
            P("tensor", "fsdp"),
            P("fsdp"),
            P("fsdp", "tensor"),
            P("fsdp", "tensor"),
            P("tensor", "fsdp"),
            P("fsdp"),
        ),
        check_vma=False,
    )
```

```python
import functools
import math

import jax
import jax.numpy as jnp
from jax import lax
from jax.experimental import pallas as pl
from jax.experimental.pallas import tpu as pltpu
from jax.sharding import PartitionSpec as P

EPS = 1e-06
THETA = 500000.0
BF = jnp.bfloat16
F32 = jnp.float32


def product(left, right):
    return jnp.dot(left, right, preferred_element_type=F32)


def product_left(left, right):
    return jnp.einsum("rd,rf->df", left, right, preferred_element_type=F32)


def product_right(left, right):
    return jnp.einsum("rf,df->rd", left, right, preferred_element_type=F32)


def rotary_tables(positions, head_size):
    half = head_size // 2
    inverse = jnp.exp(-(2.0 * jnp.arange(half, dtype=F32) / head_size) * math.log(THETA))
    angles = positions.astype(F32)[..., None] * inverse
    angles = jnp.concatenate([angles, angles], axis=-1)
    return (jnp.cos(angles), jnp.sin(angles))


def rotate(values, cosine, sine):
    half = values.shape[-1] // 2
    turned = jnp.concatenate([-values[..., half:], values[..., :half]], axis=-1)
    return values * cosine + turned * sine


def rotate_back(grads, cosine, sine):
    half = grads.shape[-1] // 2
    scaled = grads * sine
    turned = jnp.concatenate([scaled[..., half:], -scaled[..., :half]], axis=-1)
    return grads * cosine + turned


def norm_back(values, scale, gain, grads, total, width):
    return scale * gain * grads - values * scale * scale * scale * (total / width)


def layout(lengths, rows):
    segment_ends = jnp.cumsum(lengths)
    segment_starts = segment_ends - lengths
    row_index = jnp.arange(rows, dtype=jnp.int32)
    segment = jnp.sum((row_index[:, None] >= segment_ends[None, :]).astype(jnp.int32), axis=1)
    chosen = segment[:, None] == jnp.arange(lengths.shape[0], dtype=jnp.int32)[None, :]
    offset = row_index - jnp.sum(jnp.where(chosen, segment_starts[None, :], 0), axis=1)
    return (segment, offset)


LINE = 4
CHUNK = 16
MESH_ID = pl.DeviceIdType.MESH
HBM = pl.BlockSpec(memory_space=pl.ANY)
VMEM = pl.BlockSpec(memory_space=pltpu.VMEM)
DMA = pltpu.SemaphoreType.DMA


class Place:
    def __init__(self):
        device = lax.axis_index("fsdp")
        member = lax.rem(device, 2 * LINE)
        self.base = device - member
        self.z = member // 2
        self.y = lax.rem(member, 2)
        self.core = lax.axis_index("tensor")
        self.side = lax.axis_index("context")
        self.device = device
        self.count = lax.axis_size("fsdp")

    def across(self):
        return {"context": 1 - self.side}

    def at(self, z, y, core):
        return {"fsdp": self.base + 2 * z + y, "tensor": core}

    def near(self):
        yield None, self.at(self.z, self.y, 1 - self.core)
        yield None, self.at(self.z, 1 - self.y, self.core)
        yield self.z > 0, self.at(self.z - 1, self.y, self.core)
        yield self.z < LINE - 1, self.at(self.z + 1, self.y, self.core)

    def rows(self, z, y, core, count):
        start = ((2 * z + y) * 2 + core) * count
        return pl.ds(pl.multiple_of(start, count), count)


def guarded(condition, action):
    if condition is None:
        action()
    else:
        pl.when(condition)(action)


def signal(barrier, device):
    pl.semaphore_signal(barrier, inc=1, device_id=device, device_id_type=MESH_ID)


def greet(place, across=False):
    barrier = pltpu.get_barrier_semaphore()
    for condition, device in place.near():
        guarded(condition, functools.partial(signal, barrier, device))
    if across:
        signal(barrier, place.across())
    inside = (place.z > 0) & (place.z < LINE - 1)
    pl.semaphore_wait(barrier, jnp.where(inside, 4, 3) + int(across))


def greet_all(place):
    barrier = pltpu.get_barrier_semaphore()

    def one(step, carry):
        signal(barrier, {"fsdp": lax.rem(place.device + step, place.count)})
        return carry

    lax.fori_loop(1, place.count, one, 0)
    signal(barrier, place.across())
    signal(barrier, place.at(place.z, place.y, 1 - place.core))
    pl.semaphore_wait(barrier, place.count + 1)


class Sender:
    def __init__(self):
        self.sent = []

    def __call__(self, condition, make):
        def start():
            make().start()

        guarded(condition, start)
        self.sent.append((condition, make))

    def drain(self):
        for condition, make in self.sent:

            def wait(make=make):
                make().wait_send()

            guarded(condition, wait)


def remote(source, target, send, receive, device):
    return pltpu.make_async_remote_copy(
        src_ref=source,
        dst_ref=target,
        send_sem=send,
        recv_sem=receive,
        device_id=device,
        device_id_type=MESH_ID,
    )


def by_rows(rows, body):
    def step(index, carry):
        body(pl.ds(pl.multiple_of(index * CHUNK, CHUNK), CHUNK))
        return carry

    lax.fori_loop(0, rows // CHUNK, step, 0)


def reduce_scratch(rows, width):
    return [
        pltpu.VMEM((2 * LINE, 2, rows, width), BF),
        pltpu.VMEM((2 * LINE, rows, width), BF),
        pltpu.VMEM((LINE, rows, width), BF),
        pltpu.VMEM((LINE + 1, rows, width), BF),
        pltpu.VMEM((rows, width), F32),
        DMA((2, 2 * LINE)),
        DMA((2, LINE)),
        DMA((2, LINE + 1)),
    ]


def rows_product(left, right, turned):
    def make(slot, made):
        rows, width = made.shape[2:]
        values = left[pl.ds(pl.multiple_of(slot * 2 * rows, 2 * rows), 2 * rows)]
        step = width // 4

        def some(index, carry):
            at = pl.ds(pl.multiple_of(index * step, step), step)
            if turned:
                value = product_right(values, right[at])
            else:
                value = product(values, right[:, at])
            made[slot, :, :, at] = value.astype(BF).reshape(2, rows, step)
            return carry

        lax.fori_loop(0, 4, some, 0)

    return make


def reduce_phase(place, sender, make, scratch, between=None, idle=None):
    made, core_in, y_in, line_in, total, core_sem, y_sem, line_sem = scratch
    rows = total.shape[0]
    z, y, core = place.z, place.y, place.core
    low = z < LINE // 2

    def turn_of(k):
        down = LINE - 1 - k
        down = jnp.where(down <= z, down - 1, down)
        up = jnp.where(k >= z, k + 1, k)
        return jnp.where(k == LINE - 1, z, jnp.where(low, down, up))

    order = [turn_of(jnp.int32(k)) for k in range(LINE)]

    def to_core(slot):
        return remote(
            made.at[slot, 1 - core],
            core_in.at[slot],
            core_sem.at[0, slot],
            core_sem.at[1, slot],
            place.at(z, y, 1 - core),
        )

    def to_y(block):
        return remote(
            made.at[2 * block + 1 - y, core],
            y_in.at[block],
            y_sem.at[0, block],
            y_sem.at[1, block],
            place.at(z, 1 - y, core),
        )

    def to_line(block):
        step = jnp.where(block > z, 1, -1)
        slot = jnp.where((step < 0) & (block == z - 1), LINE, block)
        return remote(
            made.at[2 * block + y, core],
            line_in.at[slot],
            line_sem.at[0, block],
            line_sem.at[1, slot],
            place.at(z + step, y, core),
        )

    def from_line(slot):
        return remote(
            made.at[0, core],
            line_in.at[slot],
            line_sem.at[0, 0],
            line_sem.at[1, slot],
            place.at(z, y, 1 - core),
        )

    def produce(slot):
        make(slot, made)
        to_core(slot).start()

    def pass_y(block):
        slot = 2 * block + 1 - y
        to_core(slot).wait_recv()

        def add(at):
            value = made[slot, core, at].astype(F32) + core_in[slot, at].astype(F32)
            made[slot, core, at] = value.astype(BF)

        by_rows(rows, add)
        to_y(block).start()

    def first_half(k, carry):
        produce(2 * turn_of(k) + 1 - y)

        @pl.when(k > 0)
        def _():
            pass_y(turn_of(k - 1))

        return carry

    def second_half(k, carry):
        produce(2 * turn_of(k) + y)
        return carry

    lax.fori_loop(0, LINE, first_half, 0)
    pass_y(order[LINE - 1])
    lax.fori_loop(0, LINE, second_half, 0)
    sender.sent += [(None, functools.partial(to_core, slot)) for slot in range(2 * LINE)]
    sender.sent += [(None, functools.partial(to_y, block)) for block in range(LINE)]

    for number, block in enumerate(order[:-1]):
        if number == LINE - 2 and between is not None:
            between()
        if number < 2 and idle is not None:
            idle(number)
        slot = 2 * block + y
        to_core(slot).wait_recv()
        to_y(block).wait_recv()
        inner = jnp.where(block > z, z > 0, z < LINE - 1)

        @pl.when(inner)
        def _(block=block, slot=slot):
            from_line(block).wait_recv()

            def add(at):
                value = made[slot, core, at].astype(F32) + core_in[slot, at].astype(F32)
                value = value + y_in[block, at].astype(F32)
                made[slot, core, at] = (value + line_in[block, at].astype(F32)).astype(BF)

            by_rows(rows, add)

        @pl.when(jnp.logical_not(inner))
        def _(block=block, slot=slot):
            def add(at):
                value = made[slot, core, at].astype(F32) + core_in[slot, at].astype(F32)
                made[slot, core, at] = (value + y_in[block, at].astype(F32)).astype(BF)

            by_rows(rows, add)

        sender(None, functools.partial(to_line, block))

    slot = 2 * z + y
    to_core(slot).wait_recv()
    to_y(z).wait_recv()

    def start(at):
        value = made[slot, core, at].astype(F32) + core_in[slot, at].astype(F32)
        total[at] = value + y_in[z, at].astype(F32)

    by_rows(rows, start)
    for condition, source in ((z > 0, z), (z < LINE - 1, LINE)):

        @pl.when(condition)
        def _(source=source):
            from_line(source).wait_recv()

            def add(at):
                total[at] += line_in[source, at].astype(F32)

            by_rows(rows, add)


def gather_scratch(rows, width):
    return [
        pltpu.VMEM((rows, width), BF),
        DMA((1,)),
        DMA((2, 2 * LINE)),
        DMA((2, LINE)),
        DMA((2, LINE + 2)),
    ]


def gather_phase(place, sender, gathered, scratch, between=None, later=None, last=None):
    own, local_sem, core_sem, y_sem, line_sem = scratch
    rows = own.shape[0]
    z, y, core = place.z, place.y, place.core

    def spot(block, half):
        return gathered.at[place.rows(block, half, core, rows)]

    def to_core(source, block, half):
        return remote(
            source,
            spot(block, half),
            core_sem.at[0, 2 * block + half],
            core_sem.at[1, 2 * block + half],
            place.at(z, y, 1 - core),
        )

    def to_y(source, block):
        return remote(
            source,
            spot(block, y),
            y_sem.at[0, block],
            y_sem.at[1, block],
            place.at(z, 1 - y, core),
        )

    def to_line(source, block, step, index):
        return remote(
            source,
            spot(block, y),
            line_sem.at[0, index],
            line_sem.at[1, block],
            place.at(z + step, y, core),
        )

    keep = pltpu.make_async_copy(own, spot(z, y), local_sem.at[0])
    keep.start()
    sender(z < LINE - 1, functools.partial(to_line, own, z, 1, LINE))
    sender(z > 0, functools.partial(to_line, own, z, -1, LINE + 1))
    sender(None, functools.partial(to_y, own, z))
    sender(None, functools.partial(to_core, own, z, y))
    if between is not None:
        between()

    def took_y(block):
        remote(
            own,
            spot(block, 1 - y),
            y_sem.at[0, block],
            y_sem.at[1, block],
            place.at(z, 1 - y, core),
        ).wait_recv()

    def across(condition, block):
        guarded(condition, functools.partial(took_y, block))
        sender(condition, lambda: to_core(spot(block, 1 - y), block, 1 - y))

    def along(condition, block, step):
        def took():
            to_line(own, block, step, block).wait_recv()

        guarded(condition, took)
        onward = condition & ((z < LINE - 1) if step > 0 else (z > 0))
        sender(onward, lambda: to_line(spot(block, y), block, step, block))
        sender(condition, lambda: to_y(spot(block, y), block))
        sender(condition, lambda: to_core(spot(block, y), block, y))

    for distance in range(1, LINE + 1):
        if distance < LINE:
            along(z >= distance, z - distance, 1)
            along(z + distance < LINE, z + distance, -1)
        if distance == 1:
            across(None, z)
        else:
            across(z >= distance - 1, z - distance + 1)
            across(z + distance - 1 < LINE, z + distance - 1)
        if distance == 1 and later is not None:
            later()
        if distance == LINE - 1 and last is not None:
            last()

    keep.wait()
    for block in range(LINE):
        for half in range(2):
            remote(
                own,
                gathered.at[place.rows(block, half, 1 - core, rows)],
                core_sem.at[0, 2 * block + half],
                core_sem.at[1, 2 * block + half],
                place.at(z, y, 1 - core),
            ).wait_recv()


def pair_scratch():
    return [DMA((3,))]


def pair_phase(place, sender, own, pair, scratch):
    (sem,) = scratch
    rows = own.shape[0]
    spot = pair.at[pl.ds(pl.multiple_of(place.core * rows, rows), rows)]
    keep = pltpu.make_async_copy(own, spot, sem.at[0])
    keep.start()

    def send():
        return remote(
            own, spot, sem.at[1], sem.at[2], place.at(place.z, place.y, 1 - place.core)
        )

    sender(None, send)

    def finish():
        keep.wait()
        other = pair.at[pl.ds(pl.multiple_of((1 - place.core) * rows, rows), rows)]
        remote(
            own, other, sem.at[1], sem.at[2], place.at(place.z, place.y, 1 - place.core)
        ).wait_recv()

    return finish


def swap_scratch(count, arrays):
    return [DMA((arrays,)), DMA((2, arrays, count)), DMA((2, arrays, count))]


class Swap:
    def __init__(self, place, pairs, scratch):
        self.place = place
        self.pairs = pairs
        self.local_sem, self.out_sem, self.side_sem = scratch

    def send(self, index, step):
        place = self.place
        source, spot = self.pairs[index]
        target = lax.rem(place.device + step, place.count)
        return remote(
            source(target),
            spot(place.device, place.side),
            self.out_sem.at[0, index, step],
            self.out_sem.at[1, index, step],
            {"fsdp": target},
        )

    def taken(self, index, step, side):
        device = lax.rem(self.place.device + self.place.count - step, self.place.count)
        return self.pairs[index][1](device, side)

    def come(self, index, step):
        place = self.place
        return remote(
            self.pairs[index][0](place.device),
            self.taken(index, step, place.side),
            self.out_sem.at[0, index, step],
            self.out_sem.at[1, index, step],
            place.across(),
        )

    def share(self, index, step, source=None):
        spot = self.taken(index, step, self.place.side)
        return remote(
            spot if source is None else source,
            spot,
            self.side_sem.at[0, index, step],
            self.side_sem.at[1, index, step],
            self.place.across(),
        )

    def shared(self, index, step):
        spot = self.taken(index, step, 1 - self.place.side)
        return remote(
            spot,
            spot,
            self.side_sem.at[0, index, step],
            self.side_sem.at[1, index, step],
            self.place.across(),
        )

    def keep(self, index):
        place = self.place
        source, spot = self.pairs[index]
        return pltpu.make_async_copy(
            source(place.device), spot(place.device, place.side), self.local_sem.at[index]
        )

    def each(self, first, body):
        def step(number, carry):
            for index in range(len(self.pairs)):
                body(index, number)
            return carry

        lax.fori_loop(first, self.place.count, step, 0)

    def start(self):
        self.each(1, lambda index, step: self.send(index, step).start())
        for index, (source, _) in enumerate(self.pairs):
            self.keep(index).start()
            self.share(index, 0, source(self.place.device)).start()

    def pass_on(self):
        def one(index, step):
            self.come(index, step).wait_recv()
            self.share(index, step).start()

        self.each(1, one)

    def finish(self):
        for index in range(len(self.pairs)):
            self.keep(index).wait()
        self.each(0, lambda index, step: self.shared(index, step).wait_recv())
        self.each(1, lambda index, step: self.send(index, step).wait_send())
        self.each(0, lambda index, step: self.share(index, step).wait_send())


def whole_pair(pieces, whole):
    return (lambda target: pieces.at[target], lambda device, side: whole.at[device, side])


def halves_scratch(arrays):
    return [DMA((3, arrays))]


class Halves:
    def __init__(self, place, halves, wholes, scratch):
        self.place = place
        self.pairs = list(zip(halves, wholes))
        (self.sem,) = scratch

    def keep(self, index):
        half, whole = self.pairs[index]
        return pltpu.make_async_copy(half, whole.at[:, self.place.side], self.sem.at[0, index])

    def copy(self, index, side):
        half, whole = self.pairs[index]
        return remote(
            half,
            whole.at[:, side],
            self.sem.at[1, index],
            self.sem.at[2, index],
            self.place.across(),
        )

    def start(self):
        for index in range(len(self.pairs)):
            self.copy(index, self.place.side).start()
            self.keep(index).start()

    def finish(self):
        for index in range(len(self.pairs)):
            self.keep(index).wait()
            self.copy(index, 1 - self.place.side).wait_recv()
            self.copy(index, self.place.side).wait_send()


REDUCE = 8
GATHER = 5
PIECES = 8


def first_kernel(
    own_ref, query, key, value, out, small, gathered, qkv_all, out_all, small_all, *scratch
):
    place = Place()
    sender = Sender()
    own = scratch[0]
    own[...] = own_ref[...]
    greet_all(place)
    half, columns = qkv_all.shape[2], qkv_all.shape[3] // 3
    out_half = out_all.shape[2]
    rows = pl.ds(pl.multiple_of(place.side * half, half), half)

    def member(target):
        return lax.rem(target, 2 * LINE)

    def column_pair(weight, index):
        def source(target):
            start = pl.multiple_of(member(target) * columns, columns)
            return weight.at[rows, pl.ds(start, columns)]

        def spot(device, side):
            return qkv_all.at[device, side, :, pl.ds(index * columns, columns)]

        return (source, spot)

    def out_source(target):
        start = (2 * member(target) + place.side) * out_half
        return out.at[pl.ds(pl.multiple_of(start, out_half), out_half)]

    pairs = [
        (lambda target: small, lambda device, side: small_all.at[device, side]),
        column_pair(query, 0),
        column_pair(key, 1),
        column_pair(value, 2),
        (out_source, lambda device, side: out_all.at[device, side]),
    ]
    swap = Swap(place, pairs, scratch[GATHER:])
    gather_phase(place, sender, gathered, scratch[:GATHER], swap.start, swap.pass_on)
    swap.finish()
    sender.drain()


def hidden_kernel(
    left, right, tokens, gain, pair, down, gathered, branch, hidden, pair_all, down_all, *scratch
):
    place = Place()
    sender = Sender()
    greet(place, True)
    halves = Halves(place, (pair, down), (pair_all, down_all), scratch[REDUCE + GATHER :])
    halves.start()
    reduce_phase(place, sender, rows_product(left, right, False), scratch[:REDUCE])
    total, own = scratch[4], scratch[REDUCE]
    rows, width = total.shape

    def body(at):
        value = total[at]
        scale = lax.rsqrt(jnp.sum(value * value, axis=1, keepdims=True) / width + EPS)
        result = tokens[at].astype(F32) + value * scale * gain[...]
        branch[at] = value
        hidden[at] = result
        own[at] = result.astype(BF)

    by_rows(rows, body)
    gather_phase(place, sender, gathered, scratch[REDUCE : REDUCE + GATHER])
    halves.finish()
    sender.drain()


def turn_kernel(left, right, hidden, cotangent, gain, gathered, outputs, gain_grad, *scratch):
    place = Place()
    sender = Sender()
    greet(place)
    reduce_phase(place, sender, rows_product(left, right, False), scratch[:REDUCE])
    total, own = scratch[4], scratch[REDUCE]
    out_own = scratch[REDUCE + GATHER]
    rows, width = total.shape
    gain_grad[...] = jnp.zeros_like(gain_grad)

    def body(at):
        value = total[at]
        scale = lax.rsqrt(jnp.sum(value * value, axis=1, keepdims=True) / width + EPS)
        grads = cotangent[at].astype(F32)
        normed = value * scale
        out_own[at] = (hidden[at] + normed * gain[...]).astype(BF)
        gain_grad[...] += jnp.sum(grads * normed, axis=0, keepdims=True)
        gained = gain[...] * grads
        inner = jnp.sum(normed * gained, axis=1, keepdims=True)
        own[at] = (scale * (gained - normed * (inner / width))).astype(BF)

    by_rows(rows, body)
    finish = pair_phase(place, sender, out_own, outputs, scratch[REDUCE + GATHER + 1 :])
    gather_phase(place, sender, gathered, scratch[REDUCE : REDUCE + GATHER])
    finish()
    sender.drain()


class WeightGrads:
    def __init__(self, place, arrays, outs, scratch):
        self.place = place
        self.inner, self.grad_mlp, self.hidden, self.grad_pair = arrays
        self.outs = outs
        self.tall, self.turned, self.inner_turned = scratch[:3]
        self.fulls, self.others = scratch[3:5], scratch[5:7]
        self.fetch_sem, self.side_sem = scratch[7:]
        self.piece = self.tall.shape[3]

    def fetch(self, number, slot):
        columns = pl.ds(pl.multiple_of(number * self.piece, self.piece), self.piece)
        return [
            pltpu.make_async_copy(
                array.at[:, columns], self.tall.at[slot, index], self.fetch_sem.at[slot, index]
            )
            for index, array in enumerate((self.hidden, self.grad_mlp))
        ]

    def side_of(self, index, number, side):
        if index == 0:
            return self.fulls[0].at[number, :, side]
        return self.fulls[1].at[number, side]

    def crossing(self, number, index):
        return remote(
            self.side_of(index, number, 1 - self.place.side),
            self.others[index].at[number],
            self.side_sem.at[0, index, number],
            self.side_sem.at[1, index, number],
            self.place.across(),
        )

    def start(self):
        for copy in self.fetch(0, 0):
            copy.start()
        self.inner_turned[...] = self.inner[...].T

    def one(self, number, carry):
        slot = lax.rem(number, 2)
        for copy in self.fetch(number, slot):
            copy.wait()

        @pl.when(number < PIECES - 1)
        def _():
            for copy in self.fetch(number + 1, 1 - slot):
                copy.start()

        full, low = self.fulls
        self.turned[...] = self.tall[slot, 0].T
        columns = self.grad_pair.shape[1]
        step = columns // 4

        def columns_step(index, carry):
            at = pl.ds(pl.multiple_of(index * step, step), step)
            value = product(self.turned[...], self.grad_pair[:, at]).astype(BF)
            full[number, :, :, :, at] = value.reshape(full.shape[1:4] + (step,))
            return carry

        lax.fori_loop(0, 4, columns_step, 0)
        value = product(self.inner_turned[...], self.tall[slot, 1]).astype(BF)
        low[number] = value.reshape(low.shape[1:])
        for index in range(2):
            self.crossing(number, index).start()
        return carry

    def some(self, which):
        half = PIECES // 2
        lax.fori_loop(which * half, which * half + half, self.one, 0)

    def add(self):
        def step(number, carry):
            for index in range(2):
                self.crossing(number, index).wait_recv()
                own = self.side_of(index, number, self.place.side)[...].astype(F32)
                other = self.others[index][number].astype(F32)
                self.outs[index][number] = (own + other).astype(BF)
            return carry

        lax.fori_loop(0, PIECES, step, 0)

    def finish(self):
        def step(number, carry):
            for index in range(2):
                self.crossing(number, index).wait_send()
            return carry

        lax.fori_loop(0, PIECES, step, 0)


def branch_kernel(
    weights,
    branch,
    cotangent,
    gain,
    inner_low,
    grad_mlp,
    hidden_low,
    grad_pair,
    gathered,
    grad_hidden,
    gain_grad,
    pair_mine,
    down_mine,
    *scratch,
):
    place = Place()
    sender = Sender()
    greet(place, True)
    grads = WeightGrads(
        place,
        (inner_low, grad_mlp, hidden_low, grad_pair),
        (pair_mine, down_mine),
        scratch[REDUCE + GATHER :],
    )
    grads.start()
    make = rows_product(grad_pair, weights, True)
    reduce_phase(place, sender, make, scratch[:REDUCE], idle=grads.some)
    total, own = scratch[4], scratch[REDUCE]
    rows, width = total.shape
    gain_grad[...] = jnp.zeros_like(gain_grad)

    def body(at):
        value = branch[at]
        scale = lax.rsqrt(jnp.sum(value * value, axis=1, keepdims=True) / width + EPS)
        grads = cotangent[at].astype(F32) + total[at]
        grad_hidden[at] = grads
        normed = value * scale
        gain_grad[...] += jnp.sum(grads * normed, axis=0, keepdims=True)
        gained = gain[...] * grads
        inner = jnp.sum(normed * gained, axis=1, keepdims=True)
        own[at] = (scale * (gained - normed * (inner / width))).astype(BF)

    by_rows(rows, body)
    gather_phase(
        place, sender, gathered, scratch[REDUCE : REDUCE + GATHER], last=grads.add
    )
    grads.finish()
    sender.drain()


def last_kernel(
    left,
    right,
    grad_hidden,
    qkv,
    out,
    small,
    down,
    pair,
    result,
    qkv_all,
    out_all,
    small_all,
    down_all,
    pair_rest,
    *scratch,
):
    place = Place()
    sender = Sender()
    parts = scratch[REDUCE + 1 :]
    swap_sems, halves_sems, parts = parts[:3], parts[3:4], parts[4:]
    qkv_own, qkv_other, out_own, out_other, small_own, small_other = parts[:6]
    fetch_sem, side_sem, rest_sem = parts[6:]
    rest = pair_rest.shape[1]
    resting = remote(
        pair.at[:, pl.ds(rest, rest)], pair_rest, rest_sem.at[0], rest_sem.at[1], place.across()
    )
    greet_all(place)
    fetches, crossings = [], []
    for index, (grad, own, other) in enumerate(
        ((qkv, qkv_own, qkv_other), (out, out_own, out_other))
    ):
        fetches.append(
            pltpu.make_async_copy(grad.at[:, place.side], own, fetch_sem.at[index])
        )
        crossings.append(
            remote(
                grad.at[:, 1 - place.side],
                other,
                side_sem.at[0, index],
                side_sem.at[1, index],
                place.across(),
            )
        )
    crossings.append(
        remote(
            small,
            small_other,
            side_sem.at[0, 2],
            side_sem.at[1, 2],
            place.at(place.z, place.y, 1 - place.core),
        )
    )
    for copy in fetches + crossings:
        copy.start()
    pairs = ((small_own, small_all), (qkv_own, qkv_all), (out_own, out_all))
    swap = Swap(place, [whole_pair(*pair) for pair in pairs], swap_sems)
    halves = Halves(place, (down,), (down_all,), halves_sems)
    shared_rows = 2 * right.shape[0] // place.count // 128

    def between():
        for fetch in fetches:
            fetch.wait()
        for crossing in crossings:
            crossing.wait()
        small_own[...] = small[...]
        small_own[:, :shared_rows] += small_other[:, :shared_rows]

        def one(index, carry):
            qkv_own[index] = (
                qkv_own[index].astype(F32) + qkv_other[index].astype(F32)
            ).astype(BF)
            out_own[index] = (
                out_own[index].astype(F32) + out_other[index].astype(F32)
            ).astype(BF)
            return carry

        lax.fori_loop(0, place.count, one, 0)
        swap.start()
        halves.start()
        resting.start()

    reduce_phase(place, sender, rows_product(left, right, True), scratch[:REDUCE], between)
    total = scratch[4]

    def body(at):
        total[at] += grad_hidden[at]

    by_rows(total.shape[0], body)
    finish = pair_phase(place, sender, total, result, scratch[REDUCE : REDUCE + 1])
    swap.pass_on()
    finish()
    halves.finish()
    resting.wait()
    swap.finish()
    sender.drain()


def sum_kernel(carried, value, *rest):
    if carried:
        moved, result, arrived, core_in, y_in, held, line_in, sem, side_sem = rest
    else:
        result, core_in, y_in, held, line_in, sem = rest
    place = Place()
    z, y, core = place.z, place.y, place.core
    barrier = pltpu.get_barrier_semaphore()
    others = [place.at(z, y, 1 - core), place.at(z, 1 - y, core)]
    others += [place.at(lax.rem(z + k, LINE), y, core) for k in range(1, LINE)]
    for device in others + [place.across()] * carried:
        signal(barrier, device)
    pl.semaphore_wait(barrier, len(others) + carried)
    if carried:
        side = remote(moved, arrived, side_sem.at[0], side_sem.at[1], place.across())
        side.start()
    first = remote(value, core_in, sem.at[0, 0], sem.at[1, 0], others[0])
    first.start()
    first.wait_recv()
    held[0] = value[...] + core_in[...]
    second = remote(held.at[0], y_in, sem.at[0, 1], sem.at[1, 1], others[1])
    second.start()
    second.wait_recv()
    held[1] = held[0] + y_in[...]
    sends = [
        remote(held.at[1], line_in.at[k - 1], sem.at[0, 1 + k], sem.at[1, 1 + k], others[1 + k])
        for k in range(1, LINE)
    ]
    for send in sends:
        send.start()
    line_in[LINE - 1] = held[1]
    for send in sends:
        send.wait_recv()
    added = jnp.zeros_like(value)
    for source in range(LINE):
        slot = lax.rem(z - source + 2 * LINE - 1, LINE)
        added = added + line_in[slot]
    result[...] = added
    first.wait_send()
    second.wait_send()
    for send in sends:
        send.wait_send()
    if carried:
        side.wait()


def pack_kernel(side, gate, up, down, pair_out, down_out):
    columns = gate.shape[1]
    pair_out[0, :, :columns] = gate[...]
    pair_out[0, :, columns:] = up[...]
    down_out[0] = down[...]


def unpack_kernel(side, own, other, rest, down, gate_out, up_out, down_out):
    half, columns = own.shape[2], gate_out.shape[1]
    quarter = half // 2
    other_start = (1 - side[0]) * half
    parts = ((own, side[0] * half), (other, other_start), (rest, other_start + quarter))
    for part, start in parts:
        value = jnp.sum(part[:, 0].astype(F32), axis=0)
        rows = pl.ds(pl.multiple_of(start, quarter), part.shape[2])
        gate_out[rows] = value[:, :columns]
        up_out[rows] = value[:, columns:]
    down_out[...] = jnp.sum(down[:, 0].astype(F32), axis=0)


def talk(kernel, which, shapes, specs, scratch, microseconds, name=None):
    def call(*operands):
        return pl.pallas_call(
            kernel,
            out_shape=shapes,
            in_specs=specs[0],
            out_specs=specs[1],
            scratch_shapes=scratch,
            compiler_params=pltpu.CompilerParams(
                collective_id=which, has_side_effects=True, vmem_limit_bytes=56 << 20
            ),
            cost_estimate=pl.CostEstimate(
                flops=0, bytes_accessed=int(microseconds * 3.0e6), transcendentals=0
            ),
            name=name or kernel.__name__,
        )(*operands)

    return call


class Team:
    def __init__(self, local_heads, rows, width):
        self.fsdp = lax.axis_size("fsdp")
        self.tensor = lax.axis_size("tensor")
        self.size = 2 * LINE
        self.teams = self.fsdp // self.size
        assert self.fsdp % self.size == 0 and self.tensor == 2 and local_heads % self.size == 0
        self.member = lax.rem(lax.axis_index("fsdp"), self.size)
        self.core = lax.axis_index("tensor")
        self.context = lax.axis_index("context")
        self.groups = None
        if self.teams > 1:
            self.groups = [
                [team * self.size + one for one in range(self.size)] for team in range(self.teams)
            ]
        self.rows = rows
        self.width = width
        self.all_low = jax.ShapeDtypeStruct((2 * self.size * rows, width), BF)
        self.own_wide = jax.ShapeDtypeStruct((rows, width), F32)
        self.line_wide = jax.ShapeDtypeStruct((1, width), F32)
        self.reduces = reduce_scratch(rows, width)
        self.gathers = gather_scratch(rows, width)

    def whole(self, pieces):
        shape = (pieces.shape[0], 2) + pieces.shape[1:]
        return jax.ShapeDtypeStruct(shape, pieces.dtype)

    def first(self, own, weights, out, small):
        rows, columns = weights[0].shape
        rows, columns = rows // 2, columns // self.size
        out_rows = out.shape[0] // self.size // 2
        return talk(
            first_kernel,
            0,
            (
                self.all_low,
                jax.ShapeDtypeStruct((self.fsdp, 2, rows, 3 * columns), BF),
                jax.ShapeDtypeStruct((self.fsdp, 2, out_rows, out.shape[1]), BF),
                jax.ShapeDtypeStruct((self.fsdp, 2) + small.shape, F32),
            ),
            ([VMEM] * 6, (HBM,) * 4),
            self.gathers + swap_scratch(self.fsdp, 5),
            80,
        )(own, *weights, out, small)

    def pack(self, gate, up, down):
        rows, columns = gate.shape
        rows, columns = rows // 2, columns // self.size
        down_rows, down_columns = down.shape
        down_rows = down_rows // self.size // 2

        def column_spec():
            return pl.BlockSpec((rows, columns), lambda d, side: (side[0], d))

        def piece_spec(*shape):
            return pl.BlockSpec((1,) + shape, lambda d, side: (d, 0, 0))

        pair, low = pl.pallas_call(
            pack_kernel,
            grid_spec=pltpu.PrefetchScalarGridSpec(
                num_scalar_prefetch=1,
                grid=(self.size,),
                in_specs=[
                    column_spec(),
                    column_spec(),
                    pl.BlockSpec((down_rows, down_columns), lambda d, side: (2 * d + side[0], 0)),
                ],
                out_specs=[piece_spec(rows, 2 * columns), piece_spec(down_rows, down_columns)],
            ),
            out_shape=[
                jax.ShapeDtypeStruct((self.size, rows, 2 * columns), BF),
                jax.ShapeDtypeStruct((self.size, down_rows, down_columns), BF),
            ],
            name="pack_kernel",
        )(self.context.reshape(1).astype(jnp.int32), gate, up, down)
        return self.repeat(pair), self.repeat(low)

    def hidden(self, left, right, tokens, gain, pair, down):
        return talk(
            hidden_kernel,
            1,
            (self.all_low, self.own_wide, self.own_wide, self.whole(pair), self.whole(down)),
            ([VMEM] * 6, (HBM, VMEM, VMEM, HBM, HBM)),
            self.reduces + self.gathers + halves_scratch(2),
            100,
        )(left, right, tokens, gain, pair, down)

    def turn(self, left, right, hidden, cotangent, gain):
        pair = jax.ShapeDtypeStruct((2 * self.rows, self.width), BF)
        return talk(
            turn_kernel,
            2,
            (self.all_low, pair, self.line_wide),
            ([VMEM] * 5, (HBM, HBM, VMEM)),
            self.reduces + self.gathers + [pltpu.VMEM((self.rows, self.width), BF)] + pair_scratch(),
            100,
        )(left, right, hidden, cotangent, gain)

    def branch(self, weights, branch, cotangent, gain, inner, grad_mlp, hidden, grad_pair):
        team_rows, units = inner.shape
        columns = grad_pair.shape[1]
        piece = self.width // PIECES
        count = self.fsdp // PIECES
        half = self.width // self.fsdp // 2
        pair_shape = (PIECES, count, half, columns)
        down_shape = (PIECES, units // 2, piece)

        def both(shape):
            return pltpu.VMEM((shape[0], 2) + shape[1:], BF)

        def sides_inside(shape):
            return pltpu.VMEM((shape[0], shape[1], 2) + shape[2:], BF)

        gathered, grad_hidden, gain_grad, pair_mine, down_mine = talk(
            branch_kernel,
            3,
            (
                self.all_low,
                self.own_wide,
                self.line_wide,
                jax.ShapeDtypeStruct(pair_shape, BF),
                jax.ShapeDtypeStruct(down_shape, BF),
            ),
            (
                [VMEM, VMEM, VMEM, VMEM, VMEM, HBM, HBM, VMEM],
                (HBM, VMEM, VMEM, VMEM, VMEM),
            ),
            self.reduces
            + self.gathers
            + [
                pltpu.VMEM((2, 2, team_rows, piece), BF),
                pltpu.VMEM((piece, team_rows), BF),
                pltpu.VMEM((units, team_rows), BF),
                sides_inside(pair_shape),
                both(down_shape),
                pltpu.VMEM(pair_shape, BF),
                pltpu.VMEM(down_shape, BF),
                DMA((2, 2)),
                DMA((2, 2, PIECES)),
            ],
            100,
        )(weights, branch, cotangent, gain, inner, grad_mlp, hidden, grad_pair)
        down_mine = down_mine.reshape(PIECES, units // 2, count, piece // count)
        return (
            gathered,
            grad_hidden,
            gain_grad,
            pair_mine.reshape(self.fsdp, half, columns),
            down_mine.transpose(0, 2, 1, 3).reshape(self.fsdp, units // 2, piece // count),
        )

    def last(self, left, right, grad_hidden, qkv, out, small, down, pair):
        both = jax.ShapeDtypeStruct((2 * self.rows, self.width), F32)

        def same(array):
            return jax.ShapeDtypeStruct(array.shape, array.dtype)

        def half(array):
            return pltpu.VMEM((array.shape[0],) + array.shape[2:], array.dtype)

        held = pltpu.VMEM(small.shape, small.dtype)
        return talk(
            last_kernel,
            4,
            (
                both,
                same(qkv),
                same(out),
                self.whole(small),
                self.whole(down),
                jax.ShapeDtypeStruct((pair.shape[0], pair.shape[1] // 2, pair.shape[2]), BF),
            ),
            ([VMEM, VMEM, VMEM, HBM, HBM, VMEM, VMEM, HBM], (HBM,) * 6),
            self.reduces
            + pair_scratch()
            + swap_scratch(self.fsdp, 3)
            + halves_scratch(1)
            + [half(qkv), half(qkv), half(out), half(out), held, held]
            + [DMA((2,)), DMA((2, 3)), DMA((2,))],
            80,
        )(left, right, grad_hidden, qkv, out, small, down, pair)

    def total(self, values, moved=None):
        flat = values.reshape(-1, 128)
        carried = int(moved is not None)
        shape = jax.ShapeDtypeStruct(flat.shape, F32)
        scratch = [pltpu.VMEM(flat.shape, F32)] * 2
        scratch += [pltpu.VMEM((2,) + flat.shape, F32), pltpu.VMEM((LINE,) + flat.shape, F32)]
        scratch += [DMA((2, LINE + 1))] + [DMA((2,))] * carried
        which = 5 + self.sums
        self.sums += 1
        kernel = functools.partial(sum_kernel, carried)
        if not carried:
            call = talk(kernel, which, shape, ([VMEM], VMEM), scratch, 10, "sum_kernel")
            return call(flat).reshape(values.shape)
        shapes = (shape, jax.ShapeDtypeStruct(moved.shape, moved.dtype))
        call = talk(kernel, which, shapes, ([VMEM] * 2, (VMEM,) * 2), scratch, 10, "sum_kernel")
        total, came = call(flat, moved)
        return total.reshape(values.shape), came

    sums = 0

    def half(self, array, axis):
        count = array.shape[axis] // 2
        return lax.dynamic_slice_in_dim(array, self.context * count, count, axis)

    def swap(self, pieces):
        return lax.all_to_all(pieces, "fsdp", split_axis=0, concat_axis=0, tiled=True)

    def repeat(self, pieces):
        return jnp.concatenate([pieces] * self.teams, axis=0) if self.teams > 1 else pieces

    def unpack(self, own, other, rest, down):
        half, columns = own.shape[1], own.shape[2] // 2
        rows, down_columns = 2 * down.shape[2], down.shape[3]

        def cut(array, *shape):
            return array.reshape((self.teams, self.size) + shape)

        def piece_spec(*shape):
            return pl.BlockSpec((self.teams, 1) + shape, lambda d, side: (0, d, 0, 0))

        wide = pl.BlockSpec((2 * half, columns), lambda d, side: (0, d))
        wide_shape = jax.ShapeDtypeStruct((2 * half, self.size * columns), F32)
        return pl.pallas_call(
            unpack_kernel,
            grid_spec=pltpu.PrefetchScalarGridSpec(
                num_scalar_prefetch=1,
                grid=(self.size,),
                in_specs=[piece_spec(half, 2 * columns)]
                + [piece_spec(half // 2, 2 * columns)] * 2
                + [piece_spec(rows, down_columns)],
                out_specs=[wide, wide, pl.BlockSpec((rows, down_columns), lambda d, side: (d, 0))],
            ),
            out_shape=[
                wide_shape,
                wide_shape,
                jax.ShapeDtypeStruct((self.size * rows, down_columns), F32),
            ],
            name="unpack_kernel",
        )(
            self.context.reshape(1).astype(jnp.int32),
            cut(own, half, 2 * columns),
            cut(other, half // 2, 2 * columns),
            cut(rest, half // 2, 2 * columns),
            cut(down, rows, down_columns),
        )

    def columns_whole(self, came):
        return came.reshape(-1, came.shape[-1])

    def rows_whole(self, came):
        fsdp, two, rows, columns = came.shape
        return came.transpose(1, 2, 0, 3).reshape(two * rows, fsdp * columns)

    def of_columns(self, grad):
        rows, columns = grad.shape
        return grad.astype(BF).reshape(self.fsdp, 2, rows // self.fsdp // 2, columns)

    def of_rows(self, grad):
        rows, columns = grad.shape
        cut = grad.astype(BF).reshape(2, rows // 2, self.fsdp, columns // self.fsdp)
        return cut.transpose(2, 0, 1, 3)

    def added(self, came):
        if self.teams == 1:
            return came.astype(F32)
        came = came.reshape((self.teams, self.size) + came.shape[1:])
        return jnp.sum(came.astype(F32), axis=0)

    def columns_out(self, came, count):
        size, two, rows, columns = came.shape
        return [
            self.added(part.reshape(size, two * rows, -1))
            .transpose(1, 0, 2)
            .reshape(two * rows, -1)
            for part in jnp.split(came, count, axis=3)
        ]

    def rows_out(self, came):
        return self.added(came).reshape(-1, came.shape[-1])


def local(
    tokens,
    cont_lengths,
    w_query,
    w_key,
    w_value,
    w_output,
    query_gain,
    key_gain,
    attn_gain,
    w_gate,
    w_up,
    w_down,
    mlp_gain,
    cotangent,
):
    rows = tokens.shape[0]
    width = tokens.shape[1]
    fsdp = lax.axis_size("fsdp")
    tensor = lax.axis_size("tensor")
    local_heads = query_gain.shape[0]
    head_size = w_query.shape[1] // local_heads
    own_rows = rows // tensor
    team = Team(local_heads, own_rows, width)
    groups = team.size
    team_rows = groups * rows
    heads = local_heads // team.size
    later = lax.axis_index("context") == 1

    tokens_own = lax.dynamic_slice_in_dim(tokens, team.core * own_rows, own_rows, 0)
    grad_out = lax.dynamic_slice_in_dim(cotangent, team.core * own_rows, own_rows, 0)
    cut = query_gain.size
    share = attn_gain.size
    small = [query_gain.reshape(-1), key_gain.reshape(-1), attn_gain, mlp_gain]
    small = jnp.concatenate([one.astype(F32) for one in small + [cont_lengths.reshape(-1)]])
    small = jnp.pad(small, (0, 8 * 128 - small.size)).reshape(8, 128)
    tokens_all, qkv_came, output_came, small_came = team.first(
        tokens_own, [w_query, w_key, w_value], w_output, small
    )
    qkv_w = team.columns_whole(qkv_came)
    output_w = team.rows_whole(output_came)
    all_small = small_came[:, 0].reshape(fsdp, -1)
    query_gains = all_small[:, :cut].reshape(fsdp, local_heads, -1)
    key_gains = all_small[:, cut : 2 * cut].reshape(fsdp, local_heads, -1)
    query_gains = query_gains.transpose(1, 0, 2).reshape(local_heads, head_size)
    key_gains = key_gains.transpose(1, 0, 2).reshape(local_heads, head_size)
    flat_query = lax.dynamic_slice_in_dim(query_gains, team.member * heads, heads, 0).reshape(-1)
    flat_key = lax.dynamic_slice_in_dim(key_gains, team.member * heads, heads, 0).reshape(-1)
    gain_attn = all_small[:, 2 * cut : 2 * cut + share].reshape(1, -1)
    gain_mlp = all_small[:, 2 * cut + share : 2 * cut + 2 * share].reshape(1, -1)

    conts = cont_lengths.shape[1]
    lengths = all_small[:, 2 * cut + 2 * share : 2 * cut + 2 * share + conts].astype(jnp.int32)
    first_group = lax.axis_index("fsdp") - team.member
    lengths = lax.dynamic_slice_in_dim(lengths, first_group, groups, 0)
    segment, offset = jax.vmap(lambda one: layout(one, rows))(lengths)
    row_index = jnp.arange(rows, dtype=jnp.int32)
    positions = jnp.where(later, rows + offset, row_index[None, :])
    own_segment = jnp.where(later, segment, -1)
    cosine, sine = rotary_tables(positions, head_size)
    cosine = cosine[:, :, None, :]
    sine = sine[:, :, None, :]

    pair_mine, down_mine, tokens_all = lax.optimization_barrier(
        team.pack(w_gate, w_up, w_down) + (tokens_all,)
    )
    pair_came = team.swap(pair_mine)
    down_came = team.swap(down_mine)

    by_head = (groups, rows, heads, head_size)
    raw = product(tokens_all, qkv_w)
    query_raw, key_raw, value_raw = jnp.split(raw, 3, axis=1)
    value_low = value_raw.astype(BF)
    sums, sent_value = team.total(
        jnp.stack([jnp.sum(query_raw * query_raw, axis=1), jnp.sum(key_raw * key_raw, axis=1)]),
        value_low,
    )
    value_low, sent_value = value_low.reshape(by_head), sent_value.reshape(by_head)
    scale_query = lax.rsqrt(sums[0] / width + EPS)[:, None]
    scale_key = lax.rsqrt(sums[1] / width + EPS)[:, None]
    query_norm = query_raw * scale_query * flat_query
    key_norm = key_raw * scale_key * flat_key
    query_low = rotate(query_norm.reshape(by_head), cosine, sine).astype(BF)
    key_low = rotate(key_norm.reshape(by_head), cosine, sine).astype(BF)
    sent_key = lax.ppermute(key_low, "context", [(0, 1)])
    keys_all = jnp.concatenate([sent_key, key_low], axis=1)
    values_all = jnp.concatenate([sent_value, value_low], axis=1)
    key_index = jnp.arange(2 * rows, dtype=jnp.int32)
    key_segment = jnp.concatenate([jnp.full((groups, rows), -2, jnp.int32), own_segment], axis=1)
    remote = (key_index < rows)[None, None, :] & later
    own_keys = (
        (key_index >= rows)[None, None, :]
        & (key_index[None, None, :] - rows <= row_index[None, :, None])
        & (key_segment[:, None, :] == own_segment[:, :, None])
    )
    allowed = (remote | own_keys)[:, None]
    scale = 1.0 / math.sqrt(head_size)
    scores = (
        jnp.einsum("gqhd,gkhd->ghqk", query_low, keys_all, preferred_element_type=F32) * scale
    )
    scores = jnp.where(allowed, scores, -1e30)
    highest = jnp.max(scores, axis=-1, keepdims=True)
    weights = jnp.exp(scores - highest)
    probs = weights / jnp.sum(weights, axis=-1, keepdims=True)
    probs_low = probs.astype(BF)
    mixed = jnp.einsum("ghqk,gkhd->gqhd", probs_low, values_all, preferred_element_type=F32)
    attended_low = mixed.reshape(team_rows, heads * head_size).astype(BF)
    hidden_all, attn_sum, hidden, pair_came, down_came = team.hidden(
        attended_low, output_w, tokens_own, gain_attn, pair_came, down_came
    )
    pair_w = team.columns_whole(pair_came)
    down_w = team.rows_whole(down_came)

    gate, upward = jnp.split(product(hidden_all, pair_w), 2, axis=1)
    sigma = jax.nn.sigmoid(gate)
    inner_low = (gate * sigma * upward).astype(BF)
    grad_mlp_all, outputs, grad_mlp_gain = team.turn(
        inner_low, down_w, hidden, grad_out, gain_mlp
    )
    grad_inner = product_right(grad_mlp_all, down_w)
    grad_gate_low = (grad_inner * upward * sigma * (1.0 + gate * (1.0 - sigma))).astype(BF)
    grad_up_low = (grad_inner * gate * sigma).astype(BF)
    grad_pair = jnp.concatenate([grad_gate_low, grad_up_low], axis=1)
    grad_branch_all, grad_hidden, grad_attn_gain, pair_mine, down_mine = team.branch(
        pair_w,
        attn_sum,
        grad_out,
        gain_attn,
        inner_low,
        grad_mlp_all,
        hidden_all,
        grad_pair,
    )
    pair_came = team.swap(pair_mine)
    output_grad = team.of_rows(product_left(attended_low, grad_branch_all))
    grad_attended = product_right(grad_branch_all, output_w).astype(BF).reshape(by_head)

    grad_probs = jnp.einsum("gqhd,gkhd->ghqk", grad_attended, values_all, preferred_element_type=F32)
    centre = jnp.sum(probs * grad_probs, axis=-1, keepdims=True)
    grad_scores = (probs * (grad_probs - centre)).astype(BF)
    grad_query_rot = (
        jnp.einsum("ghqk,gkhd->gqhd", grad_scores, keys_all, preferred_element_type=F32) * scale
    )
    grad_keys = (
        jnp.einsum("ghqk,gqhd->gkhd", grad_scores, query_low, preferred_element_type=F32) * scale
    )
    grad_values = jnp.einsum("ghqk,gqhd->gkhd", probs_low, grad_attended, preferred_element_type=F32)
    back_value = lax.ppermute(grad_values[:, :rows].astype(BF), "context", [(1, 0)])
    back_key = lax.ppermute(grad_keys[:, :rows].astype(BF), "context", [(1, 0)])
    grad_key_rot = grad_keys[:, rows:] + back_key.astype(F32)
    grad_value_low = (
        (grad_values[:, rows:] + back_value.astype(F32)).reshape(team_rows, -1).astype(BF)
    )
    grad_query_norm = rotate_back(grad_query_rot, cosine, sine).reshape(team_rows, -1)
    grad_key_norm = rotate_back(grad_key_rot, cosine, sine).reshape(team_rows, -1)
    grad_query_gain = jnp.sum(grad_query_norm * query_raw * scale_query, axis=0)
    grad_key_gain = jnp.sum(grad_key_norm * key_raw * scale_key, axis=0)
    inner_sums = jnp.stack(
        [
            jnp.sum(query_raw * flat_query * grad_query_norm, axis=1),
            jnp.sum(key_raw * flat_key * grad_key_norm, axis=1),
        ]
    )
    inner_sums, pair_came = lax.optimization_barrier((inner_sums, pair_came))
    pair_other = lax.ppermute(
        pair_came[:, : pair_came.shape[1] // 2], "context", [(0, 1), (1, 0)]
    )
    totals = team.total(inner_sums)
    down_mine, totals = lax.optimization_barrier((down_mine, totals))
    down_came = team.swap(down_mine)
    grad_query_low = norm_back(
        query_raw, scale_query, flat_query, grad_query_norm, totals[0][:, None], width
    ).astype(BF)
    grad_key_low = norm_back(
        key_raw, scale_key, flat_key, grad_key_norm, totals[1][:, None], width
    ).astype(BF)
    grad_qkv = jnp.concatenate([grad_query_low, grad_key_low, grad_value_low], axis=1)
    qkv_grad = team.of_columns(product_left(tokens_all, grad_qkv))
    head_share = head_size // fsdp
    small = [
        grad_attn_gain.reshape(fsdp, share),
        grad_mlp_gain.reshape(fsdp, share),
        grad_query_gain.reshape(heads, fsdp, head_share).transpose(1, 0, 2).reshape(fsdp, -1),
        grad_key_gain.reshape(heads, fsdp, head_share).transpose(1, 0, 2).reshape(fsdp, -1),
    ]
    used = 2 * share + 2 * heads * head_share
    small = jnp.concatenate(small + [jnp.zeros((fsdp, 8 * 128 - used), F32)], axis=1)
    grad_qkv, pair_other = lax.optimization_barrier((grad_qkv, pair_other))
    input_grad, qkv_came, output_came, small_came, down_came, pair_rest = team.last(
        grad_qkv,
        qkv_w,
        grad_hidden,
        qkv_grad,
        output_grad,
        small.reshape(fsdp, 8, 128),
        down_came,
        pair_came,
    )
    grad_w_query, grad_w_key, grad_w_value = team.columns_out(qkv_came, 3)
    grad_w_gate, grad_w_up, grad_w_down = team.unpack(
        pair_came, pair_other, pair_rest, down_came
    )
    grad_w_output = team.rows_out(output_came)
    came = jnp.sum(small_came, axis=1).reshape(fsdp, -1)
    row_gains = jnp.sum(came[:, : 2 * share], axis=0).reshape(2, share)
    head_gains = team.added(came[:, 2 * share : used]).reshape(team.size, 2, heads, head_share)
    head_gains = head_gains.transpose(1, 0, 2, 3).reshape(2, local_heads, head_share)
    return (
        outputs,
        input_grad,
        grad_w_query,
        grad_w_key,
        grad_w_value,
        grad_w_output,
        head_gains[0],
        head_gains[1],
        row_gains[0],
        grad_w_gate,
        grad_w_up,
        grad_w_down,
        row_gains[1],
    )


def solution(mesh):
    return jax.shard_map(
        local,
        mesh=mesh,
        in_specs=(
            P(("fsdp", "context"), None),
            P("fsdp", None),
            P("fsdp", "tensor"),
            P("fsdp", "tensor"),
            P("fsdp", "tensor"),
            P("tensor", "fsdp"),
            P("tensor", "fsdp"),
            P("tensor", "fsdp"),
            P("fsdp"),
            P("fsdp", "tensor"),
            P("fsdp", "tensor"),
            P("tensor", "fsdp"),
            P("fsdp"),
            P(("fsdp", "context"), None),
        ),
        out_specs=(
            P(("fsdp", "context"), None),
            P(("fsdp", "context"), None),
            P("fsdp", "tensor"),
            P("fsdp", "tensor"),
            P("fsdp", "tensor"),
            P("tensor", "fsdp"),
            P("tensor", "fsdp"),
            P("tensor", "fsdp"),
            P("fsdp"),
            P("fsdp", "tensor"),
            P("fsdp", "tensor"),
            P("tensor", "fsdp"),
            P("fsdp"),
        ),
        check_vma=False,
    )
```

```python
import functools
import math

import jax
import jax.numpy as jnp
from jax import lax
from jax.experimental import pallas as pl
from jax.experimental.pallas import tpu as pltpu
from jax.sharding import PartitionSpec as P

EPS = 1e-06
THETA = 500000.0
BF = jnp.bfloat16
F32 = jnp.float32


def product(left, right):
    return jnp.dot(left, right, preferred_element_type=F32)


def product_left(left, right):
    return jnp.einsum("rd,rf->df", left, right, preferred_element_type=F32)


def product_right(left, right):
    return jnp.einsum("rf,df->rd", left, right, preferred_element_type=F32)


def rotary_tables(positions, head_size):
    half = head_size // 2
    inverse = jnp.exp(-(2.0 * jnp.arange(half, dtype=F32) / head_size) * math.log(THETA))
    angles = positions.astype(F32)[..., None] * inverse
    angles = jnp.concatenate([angles, angles], axis=-1)
    return (jnp.cos(angles), jnp.sin(angles))


def rotate(values, cosine, sine):
    half = values.shape[-1] // 2
    turned = jnp.concatenate([-values[..., half:], values[..., :half]], axis=-1)
    return values * cosine + turned * sine


def rotate_back(grads, cosine, sine):
    half = grads.shape[-1] // 2
    scaled = grads * sine
    turned = jnp.concatenate([scaled[..., half:], -scaled[..., :half]], axis=-1)
    return grads * cosine + turned


def norm_back(values, scale, gain, grads, total, width):
    return scale * gain * grads - values * scale * scale * scale * (total / width)


def layout(lengths, rows):
    segment_ends = jnp.cumsum(lengths)
    segment_starts = segment_ends - lengths
    row_index = jnp.arange(rows, dtype=jnp.int32)
    segment = jnp.sum((row_index[:, None] >= segment_ends[None, :]).astype(jnp.int32), axis=1)
    chosen = segment[:, None] == jnp.arange(lengths.shape[0], dtype=jnp.int32)[None, :]
    offset = row_index - jnp.sum(jnp.where(chosen, segment_starts[None, :], 0), axis=1)
    return (segment, offset)


LINE = 4
CHUNK = 16
MESH_ID = pl.DeviceIdType.MESH
HBM = pl.BlockSpec(memory_space=pl.ANY)
VMEM = pl.BlockSpec(memory_space=pltpu.VMEM)
DMA = pltpu.SemaphoreType.DMA


class Place:
    def __init__(self):
        device = lax.axis_index("fsdp")
        member = lax.rem(device, 2 * LINE)
        self.base = device - member
        self.z = member // 2
        self.y = lax.rem(member, 2)
        self.core = lax.axis_index("tensor")
        self.side = lax.axis_index("context")
        self.device = device
        self.count = lax.axis_size("fsdp")

    def across(self):
        return {"context": 1 - self.side}

    def at(self, z, y, core):
        return {"fsdp": self.base + 2 * z + y, "tensor": core}

    def near(self):
        yield None, self.at(self.z, self.y, 1 - self.core)
        yield None, self.at(self.z, 1 - self.y, self.core)
        yield self.z > 0, self.at(self.z - 1, self.y, self.core)
        yield self.z < LINE - 1, self.at(self.z + 1, self.y, self.core)

    def rows(self, z, y, core, count):
        start = ((2 * z + y) * 2 + core) * count
        return pl.ds(pl.multiple_of(start, count), count)


def guarded(condition, action):
    if condition is None:
        action()
    else:
        pl.when(condition)(action)


def signal(barrier, device):
    pl.semaphore_signal(barrier, inc=1, device_id=device, device_id_type=MESH_ID)


def greet(place, across=False):
    barrier = pltpu.get_barrier_semaphore()
    for condition, device in place.near():
        guarded(condition, functools.partial(signal, barrier, device))
    if across:
        signal(barrier, place.across())
    inside = (place.z > 0) & (place.z < LINE - 1)
    pl.semaphore_wait(barrier, jnp.where(inside, 4, 3) + int(across))


def greet_all(place):
    barrier = pltpu.get_barrier_semaphore()

    def one(step, carry):
        signal(barrier, {"fsdp": lax.rem(place.device + step, place.count)})
        return carry

    lax.fori_loop(1, place.count, one, 0)
    signal(barrier, place.across())
    signal(barrier, place.at(place.z, place.y, 1 - place.core))
    pl.semaphore_wait(barrier, place.count + 1)


class Sender:
    def __init__(self):
        self.sent = []

    def __call__(self, condition, make):
        def start():
            make().start()

        guarded(condition, start)
        self.sent.append((condition, make))

    def drain(self):
        for condition, make in self.sent:

            def wait(make=make):
                make().wait_send()

            guarded(condition, wait)


def remote(source, target, send, receive, device):
    return pltpu.make_async_remote_copy(
        src_ref=source,
        dst_ref=target,
        send_sem=send,
        recv_sem=receive,
        device_id=device,
        device_id_type=MESH_ID,
    )


def by_rows(rows, body):
    def step(index, carry):
        body(pl.ds(pl.multiple_of(index * CHUNK, CHUNK), CHUNK))
        return carry

    lax.fori_loop(0, rows // CHUNK, step, 0)


def reduce_scratch(rows, width):
    return [
        pltpu.VMEM((2 * LINE, 2, rows, width), BF),
        pltpu.VMEM((2 * LINE, rows, width), BF),
        pltpu.VMEM((LINE, rows, width), BF),
        pltpu.VMEM((LINE + 1, rows, width), BF),
        pltpu.VMEM((rows, width), F32),
        DMA((2, 2 * LINE)),
        DMA((2, LINE)),
        DMA((2, LINE + 1)),
    ]


def rows_product(left, right):
    def make(slot, made):
        rows, width = made.shape[2:]
        values = left[pl.ds(pl.multiple_of(slot * 2 * rows, 2 * rows), 2 * rows)]
        step = width // 4

        def some(index, carry):
            at = pl.ds(pl.multiple_of(index * step, step), step)
            value = product(values, right[:, at])
            made[slot, :, :, at] = value.astype(BF).reshape(2, rows, step)
            return carry

        lax.fori_loop(0, 4, some, 0)

    return make


def rows_fetch(partial, made, sem):
    def fetch(slot):
        return pltpu.make_async_copy(partial.at[slot], made.at[slot], sem.at[slot])

    lax.fori_loop(0, 2 * LINE, lambda slot, carry: (fetch(slot).start(), carry)[1], 0)
    return lambda slot, made: fetch(slot).wait()


def reduce_phase(place, sender, make, scratch, between=None, idle=None):
    made, core_in, y_in, line_in, total, core_sem, y_sem, line_sem = scratch
    rows = total.shape[0]
    z, y, core = place.z, place.y, place.core
    low = z < LINE // 2

    def turn_of(k):
        down = LINE - 1 - k
        down = jnp.where(down <= z, down - 1, down)
        up = jnp.where(k >= z, k + 1, k)
        return jnp.where(k == LINE - 1, z, jnp.where(low, down, up))

    order = [turn_of(jnp.int32(k)) for k in range(LINE)]

    def to_core(slot):
        return remote(
            made.at[slot, 1 - core],
            core_in.at[slot],
            core_sem.at[0, slot],
            core_sem.at[1, slot],
            place.at(z, y, 1 - core),
        )

    def to_y(block):
        return remote(
            made.at[2 * block + 1 - y, core],
            y_in.at[block],
            y_sem.at[0, block],
            y_sem.at[1, block],
            place.at(z, 1 - y, core),
        )

    def to_line(block):
        step = jnp.where(block > z, 1, -1)
        slot = jnp.where((step < 0) & (block == z - 1), LINE, block)
        return remote(
            made.at[2 * block + y, core],
            line_in.at[slot],
            line_sem.at[0, block],
            line_sem.at[1, slot],
            place.at(z + step, y, core),
        )

    def from_line(slot):
        return remote(
            made.at[0, core],
            line_in.at[slot],
            line_sem.at[0, 0],
            line_sem.at[1, slot],
            place.at(z, y, 1 - core),
        )

    def produce(slot):
        make(slot, made)
        to_core(slot).start()

    def pass_y(block):
        slot = 2 * block + 1 - y
        to_core(slot).wait_recv()

        def add(at):
            value = made[slot, core, at].astype(F32) + core_in[slot, at].astype(F32)
            made[slot, core, at] = value.astype(BF)

        by_rows(rows, add)
        to_y(block).start()

    def first_half(k, carry):
        produce(2 * turn_of(k) + 1 - y)

        @pl.when(k > 0)
        def _():
            pass_y(turn_of(k - 1))

        return carry

    def second_half(k, carry):
        produce(2 * turn_of(k) + y)
        return carry

    lax.fori_loop(0, LINE, first_half, 0)
    pass_y(order[LINE - 1])
    lax.fori_loop(0, LINE, second_half, 0)
    sender.sent += [(None, functools.partial(to_core, slot)) for slot in range(2 * LINE)]
    sender.sent += [(None, functools.partial(to_y, block)) for block in range(LINE)]

    for number, block in enumerate(order[:-1]):
        if number == LINE - 2 and between is not None:
            between()
        if number < 2 and idle is not None:
            idle(number)
        slot = 2 * block + y
        to_core(slot).wait_recv()
        to_y(block).wait_recv()
        inner = jnp.where(block > z, z > 0, z < LINE - 1)

        @pl.when(inner)
        def _(block=block, slot=slot):
            from_line(block).wait_recv()

            def add(at):
                value = made[slot, core, at].astype(F32) + core_in[slot, at].astype(F32)
                value = value + y_in[block, at].astype(F32)
                made[slot, core, at] = (value + line_in[block, at].astype(F32)).astype(BF)

            by_rows(rows, add)

        @pl.when(jnp.logical_not(inner))
        def _(block=block, slot=slot):
            def add(at):
                value = made[slot, core, at].astype(F32) + core_in[slot, at].astype(F32)
                made[slot, core, at] = (value + y_in[block, at].astype(F32)).astype(BF)

            by_rows(rows, add)

        sender(None, functools.partial(to_line, block))

    slot = 2 * z + y
    to_core(slot).wait_recv()
    to_y(z).wait_recv()

    def start(at):
        value = made[slot, core, at].astype(F32) + core_in[slot, at].astype(F32)
        total[at] = value + y_in[z, at].astype(F32)

    by_rows(rows, start)
    for condition, source in ((z > 0, z), (z < LINE - 1, LINE)):

        @pl.when(condition)
        def _(source=source):
            from_line(source).wait_recv()

            def add(at):
                total[at] += line_in[source, at].astype(F32)

            by_rows(rows, add)


def gather_scratch(rows, width):
    return [
        pltpu.VMEM((rows, width), BF),
        DMA((1,)),
        DMA((2, 2 * LINE)),
        DMA((2, LINE)),
        DMA((2, LINE + 2)),
    ]


def gather_phase(place, sender, gathered, scratch, between=None, later=None, last=None):
    own, local_sem, core_sem, y_sem, line_sem = scratch
    rows = own.shape[0]
    z, y, core = place.z, place.y, place.core

    def spot(block, half):
        return gathered.at[place.rows(block, half, core, rows)]

    def to_core(source, block, half):
        return remote(
            source,
            spot(block, half),
            core_sem.at[0, 2 * block + half],
            core_sem.at[1, 2 * block + half],
            place.at(z, y, 1 - core),
        )

    def to_y(source, block):
        return remote(
            source,
            spot(block, y),
            y_sem.at[0, block],
            y_sem.at[1, block],
            place.at(z, 1 - y, core),
        )

    def to_line(source, block, step, index):
        return remote(
            source,
            spot(block, y),
            line_sem.at[0, index],
            line_sem.at[1, block],
            place.at(z + step, y, core),
        )

    keep = pltpu.make_async_copy(own, spot(z, y), local_sem.at[0])
    keep.start()
    sender(z < LINE - 1, functools.partial(to_line, own, z, 1, LINE))
    sender(z > 0, functools.partial(to_line, own, z, -1, LINE + 1))
    sender(None, functools.partial(to_y, own, z))
    sender(None, functools.partial(to_core, own, z, y))
    if between is not None:
        between()

    def took_y(block):
        remote(
            own,
            spot(block, 1 - y),
            y_sem.at[0, block],
            y_sem.at[1, block],
            place.at(z, 1 - y, core),
        ).wait_recv()

    def across(condition, block):
        guarded(condition, functools.partial(took_y, block))
        sender(condition, lambda: to_core(spot(block, 1 - y), block, 1 - y))

    def along(condition, block, step):
        def took():
            to_line(own, block, step, block).wait_recv()

        guarded(condition, took)
        onward = condition & ((z < LINE - 1) if step > 0 else (z > 0))
        sender(onward, lambda: to_line(spot(block, y), block, step, block))
        sender(condition, lambda: to_y(spot(block, y), block))
        sender(condition, lambda: to_core(spot(block, y), block, y))

    for distance in range(1, LINE + 1):
        if distance < LINE:
            along(z >= distance, z - distance, 1)
            along(z + distance < LINE, z + distance, -1)
        if distance == 1:
            across(None, z)
        else:
            across(z >= distance - 1, z - distance + 1)
            across(z + distance - 1 < LINE, z + distance - 1)
        if distance == 1 and later is not None:
            later()
        if distance == LINE - 1 and last is not None:
            last()

    keep.wait()
    for block in range(LINE):
        for half in range(2):
            remote(
                own,
                gathered.at[place.rows(block, half, 1 - core, rows)],
                core_sem.at[0, 2 * block + half],
                core_sem.at[1, 2 * block + half],
                place.at(z, y, 1 - core),
            ).wait_recv()


def pair_scratch():
    return [DMA((3,))]


def pair_phase(place, sender, own, pair, scratch):
    (sem,) = scratch
    rows = own.shape[0]
    spot = pair.at[pl.ds(pl.multiple_of(place.core * rows, rows), rows)]
    keep = pltpu.make_async_copy(own, spot, sem.at[0])
    keep.start()

    def send():
        return remote(
            own, spot, sem.at[1], sem.at[2], place.at(place.z, place.y, 1 - place.core)
        )

    sender(None, send)

    def finish():
        keep.wait()
        other = pair.at[pl.ds(pl.multiple_of((1 - place.core) * rows, rows), rows)]
        remote(
            own, other, sem.at[1], sem.at[2], place.at(place.z, place.y, 1 - place.core)
        ).wait_recv()

    return finish


def swap_scratch(count, arrays):
    return [DMA((arrays,)), DMA((2, arrays, count)), DMA((2, arrays, count))]


class Swap:
    def __init__(self, place, pairs, scratch):
        self.place = place
        self.pairs = pairs
        self.local_sem, self.out_sem, self.side_sem = scratch

    def send(self, index, step):
        place = self.place
        source, spot = self.pairs[index]
        target = lax.rem(place.device + step, place.count)
        return remote(
            source(target),
            spot(place.device, place.side),
            self.out_sem.at[0, index, step],
            self.out_sem.at[1, index, step],
            {"fsdp": target},
        )

    def taken(self, index, step, side):
        device = lax.rem(self.place.device + self.place.count - step, self.place.count)
        return self.pairs[index][1](device, side)

    def come(self, index, step):
        place = self.place
        return remote(
            self.pairs[index][0](place.device),
            self.taken(index, step, place.side),
            self.out_sem.at[0, index, step],
            self.out_sem.at[1, index, step],
            place.across(),
        )

    def share(self, index, step, source=None):
        spot = self.taken(index, step, self.place.side)
        return remote(
            spot if source is None else source,
            spot,
            self.side_sem.at[0, index, step],
            self.side_sem.at[1, index, step],
            self.place.across(),
        )

    def shared(self, index, step):
        spot = self.taken(index, step, 1 - self.place.side)
        return remote(
            spot,
            spot,
            self.side_sem.at[0, index, step],
            self.side_sem.at[1, index, step],
            self.place.across(),
        )

    def keep(self, index):
        place = self.place
        source, spot = self.pairs[index]
        return pltpu.make_async_copy(
            source(place.device), spot(place.device, place.side), self.local_sem.at[index]
        )

    def each(self, first, body):
        def step(number, carry):
            for index in range(len(self.pairs)):
                body(index, number)
            return carry

        lax.fori_loop(first, self.place.count, step, 0)

    def start(self):
        self.each(1, lambda index, step: self.send(index, step).start())
        for index, (source, _) in enumerate(self.pairs):
            self.keep(index).start()
            self.share(index, 0, source(self.place.device)).start()

    def pass_on(self):
        def one(index, step):
            self.come(index, step).wait_recv()
            self.share(index, step).start()

        self.each(1, one)

    def finish(self):
        for index in range(len(self.pairs)):
            self.keep(index).wait()
        self.each(0, lambda index, step: self.shared(index, step).wait_recv())
        self.each(1, lambda index, step: self.send(index, step).wait_send())
        self.each(0, lambda index, step: self.share(index, step).wait_send())


def whole_pair(pieces, whole):
    return (lambda target: pieces.at[target], lambda device, side: whole.at[device, side])


def halves_scratch(arrays):
    return [DMA((3, arrays))]


class Halves:
    def __init__(self, place, halves, wholes, scratch):
        self.place = place
        self.pairs = list(zip(halves, wholes))
        (self.sem,) = scratch

    def keep(self, index):
        half, whole = self.pairs[index]
        return pltpu.make_async_copy(half, whole.at[:, self.place.side], self.sem.at[0, index])

    def copy(self, index, side):
        half, whole = self.pairs[index]
        return remote(
            half,
            whole.at[:, side],
            self.sem.at[1, index],
            self.sem.at[2, index],
            self.place.across(),
        )

    def start(self):
        for index in range(len(self.pairs)):
            self.copy(index, self.place.side).start()
            self.keep(index).start()

    def finish(self):
        for index in range(len(self.pairs)):
            self.keep(index).wait()
            self.copy(index, 1 - self.place.side).wait_recv()
            self.copy(index, self.place.side).wait_send()


REDUCE = 8
GATHER = 5
PIECES = 8


def first_kernel(
    own_ref, query, key, value, out, small, gathered, qkv_all, out_all, small_all, *scratch
):
    place = Place()
    sender = Sender()
    own = scratch[0]
    own[...] = own_ref[...]
    greet_all(place)
    half, columns = qkv_all.shape[2], qkv_all.shape[3] // 3
    out_half = out_all.shape[2]
    rows = pl.ds(pl.multiple_of(place.side * half, half), half)

    def member(target):
        return lax.rem(target, 2 * LINE)

    def column_pair(weight, index):
        def source(target):
            start = pl.multiple_of(member(target) * columns, columns)
            return weight.at[rows, pl.ds(start, columns)]

        def spot(device, side):
            return qkv_all.at[device, side, :, pl.ds(index * columns, columns)]

        return (source, spot)

    def out_source(target):
        start = (2 * member(target) + place.side) * out_half
        return out.at[pl.ds(pl.multiple_of(start, out_half), out_half)]

    pairs = [
        (lambda target: small, lambda device, side: small_all.at[device, side]),
        column_pair(query, 0),
        column_pair(key, 1),
        column_pair(value, 2),
        (out_source, lambda device, side: out_all.at[device, side]),
    ]
    swap = Swap(place, pairs, scratch[GATHER:])
    gather_phase(place, sender, gathered, scratch[:GATHER], swap.start, swap.pass_on)
    swap.finish()
    sender.drain()


def hidden_kernel(
    left, right, tokens, gain, pair, down, gathered, branch, hidden, pair_all, down_all, *scratch
):
    place = Place()
    sender = Sender()
    greet(place, True)
    halves = Halves(place, (pair, down), (pair_all, down_all), scratch[REDUCE + GATHER :])
    halves.start()
    reduce_phase(place, sender, rows_product(left, right), scratch[:REDUCE])
    total, own = scratch[4], scratch[REDUCE]
    rows, width = total.shape

    def body(at):
        value = total[at]
        scale = lax.rsqrt(jnp.sum(value * value, axis=1, keepdims=True) / width + EPS)
        result = tokens[at].astype(F32) + value * scale * gain[...]
        branch[at] = value
        hidden[at] = result
        own[at] = result.astype(BF)

    by_rows(rows, body)
    gather_phase(place, sender, gathered, scratch[REDUCE : REDUCE + GATHER])
    halves.finish()
    sender.drain()


def turn_kernel(left, right, hidden, cotangent, gain, gathered, outputs, gain_grad, *scratch):
    place = Place()
    sender = Sender()
    greet(place)
    reduce_phase(place, sender, rows_product(left, right), scratch[:REDUCE])
    total, own = scratch[4], scratch[REDUCE]
    out_own = scratch[REDUCE + GATHER]
    rows, width = total.shape
    gain_grad[...] = jnp.zeros_like(gain_grad)

    def body(at):
        value = total[at]
        scale = lax.rsqrt(jnp.sum(value * value, axis=1, keepdims=True) / width + EPS)
        grads = cotangent[at].astype(F32)
        normed = value * scale
        out_own[at] = (hidden[at] + normed * gain[...]).astype(BF)
        gain_grad[...] += jnp.sum(grads * normed, axis=0, keepdims=True)
        gained = gain[...] * grads
        inner = jnp.sum(normed * gained, axis=1, keepdims=True)
        own[at] = (scale * (gained - normed * (inner / width))).astype(BF)

    by_rows(rows, body)
    finish = pair_phase(place, sender, out_own, outputs, scratch[REDUCE + GATHER + 1 :])
    gather_phase(place, sender, gathered, scratch[REDUCE : REDUCE + GATHER])
    finish()
    sender.drain()


class WeightGrads:
    def __init__(self, place, arrays, outs, scratch):
        self.place = place
        self.inner, self.grad_mlp, self.hidden, self.grad_pair = arrays
        self.outs = outs
        self.tall, self.turned, self.inner_turned = scratch[:3]
        self.fulls, self.others = scratch[3:5], scratch[5:7]
        self.fetch_sem, self.side_sem = scratch[7:]
        self.piece = self.tall.shape[3]

    def fetch(self, number, slot):
        columns = pl.ds(pl.multiple_of(number * self.piece, self.piece), self.piece)
        return [
            pltpu.make_async_copy(
                array.at[:, columns], self.tall.at[slot, index], self.fetch_sem.at[slot, index]
            )
            for index, array in enumerate((self.hidden, self.grad_mlp))
        ]

    def side_of(self, index, number, side):
        if index == 0:
            return self.fulls[0].at[number, :, side]
        return self.fulls[1].at[number, side]

    def crossing(self, number, index):
        return remote(
            self.side_of(index, number, 1 - self.place.side),
            self.others[index].at[number],
            self.side_sem.at[0, index, number],
            self.side_sem.at[1, index, number],
            self.place.across(),
        )

    def start(self):
        for copy in self.fetch(0, 0):
            copy.start()
        self.inner_turned[...] = self.inner[...].T

    def one(self, number, carry):
        slot = lax.rem(number, 2)
        for copy in self.fetch(number, slot):
            copy.wait()

        @pl.when(number < PIECES - 1)
        def _():
            for copy in self.fetch(number + 1, 1 - slot):
                copy.start()

        full, low = self.fulls
        self.turned[...] = self.tall[slot, 0].T
        columns = self.grad_pair.shape[1]
        step = columns // 4

        def columns_step(index, carry):
            at = pl.ds(pl.multiple_of(index * step, step), step)
            value = product(self.turned[...], self.grad_pair[:, at]).astype(BF)
            full[number, :, :, :, at] = value.reshape(full.shape[1:4] + (step,))
            return carry

        lax.fori_loop(0, 4, columns_step, 0)
        value = product(self.inner_turned[...], self.tall[slot, 1]).astype(BF)
        low[number] = value.reshape(low.shape[1:])
        for index in range(2):
            self.crossing(number, index).start()
        return carry

    def some(self, which):
        half = PIECES // 2
        lax.fori_loop(which * half, which * half + half, self.one, 0)

    def add(self):
        def step(number, carry):
            for index in range(2):
                self.crossing(number, index).wait_recv()
                own = self.side_of(index, number, self.place.side)[...].astype(F32)
                other = self.others[index][number].astype(F32)
                self.outs[index][number] = (own + other).astype(BF)
            return carry

        lax.fori_loop(0, PIECES, step, 0)

    def finish(self):
        def step(number, carry):
            for index in range(2):
                self.crossing(number, index).wait_send()
            return carry

        lax.fori_loop(0, PIECES, step, 0)


def branch_kernel(
    partial,
    branch,
    cotangent,
    gain,
    inner_low,
    grad_mlp,
    hidden_low,
    grad_pair,
    gathered,
    grad_hidden,
    gain_grad,
    pair_mine,
    down_mine,
    *scratch,
):
    place = Place()
    sender = Sender()
    greet(place, True)
    grads = WeightGrads(
        place,
        (inner_low, grad_mlp, hidden_low, grad_pair),
        (pair_mine, down_mine),
        scratch[REDUCE + GATHER : -1],
    )
    rows_sem = scratch[-1]
    grads.start()
    make = rows_fetch(partial, scratch[0], rows_sem)
    reduce_phase(place, sender, make, scratch[:REDUCE], idle=grads.some)
    total, own = scratch[4], scratch[REDUCE]
    rows, width = total.shape
    gain_grad[...] = jnp.zeros_like(gain_grad)

    def body(at):
        value = branch[at]
        scale = lax.rsqrt(jnp.sum(value * value, axis=1, keepdims=True) / width + EPS)
        grads = cotangent[at].astype(F32) + total[at]
        grad_hidden[at] = grads
        normed = value * scale
        gain_grad[...] += jnp.sum(grads * normed, axis=0, keepdims=True)
        gained = gain[...] * grads
        inner = jnp.sum(normed * gained, axis=1, keepdims=True)
        own[at] = (scale * (gained - normed * (inner / width))).astype(BF)

    by_rows(rows, body)
    gather_phase(
        place, sender, gathered, scratch[REDUCE : REDUCE + GATHER], last=grads.add
    )
    grads.finish()
    sender.drain()


def last_kernel(
    partial,
    grad_hidden,
    qkv,
    out,
    small,
    down,
    pair,
    result,
    qkv_all,
    out_all,
    small_all,
    down_all,
    pair_rest,
    *scratch,
):
    place = Place()
    sender = Sender()
    parts = scratch[REDUCE + 1 :]
    swap_sems, halves_sems, parts = parts[:3], parts[3:4], parts[4:]
    qkv_own, qkv_other, out_own, out_other, small_own, small_other = parts[:6]
    fetch_sem, side_sem, rest_sem, rows_sem = parts[6:]
    rest = pair_rest.shape[1]
    resting = remote(
        pair.at[:, pl.ds(rest, rest)], pair_rest, rest_sem.at[0], rest_sem.at[1], place.across()
    )
    greet_all(place)
    fetches, crossings = [], []
    for index, (grad, own, other) in enumerate(
        ((qkv, qkv_own, qkv_other), (out, out_own, out_other))
    ):
        fetches.append(
            pltpu.make_async_copy(grad.at[:, place.side], own, fetch_sem.at[index])
        )
        crossings.append(
            remote(
                grad.at[:, 1 - place.side],
                other,
                side_sem.at[0, index],
                side_sem.at[1, index],
                place.across(),
            )
        )
    crossings.append(
        remote(
            small,
            small_other,
            side_sem.at[0, 2],
            side_sem.at[1, 2],
            place.at(place.z, place.y, 1 - place.core),
        )
    )
    for copy in fetches + crossings:
        copy.start()
    pairs = ((small_own, small_all), (qkv_own, qkv_all), (out_own, out_all))
    swap = Swap(place, [whole_pair(*pair) for pair in pairs], swap_sems)
    halves = Halves(place, (down,), (down_all,), halves_sems)
    shared_rows = 2 * partial.shape[3] // place.count // 128

    def between():
        for fetch in fetches:
            fetch.wait()
        for crossing in crossings:
            crossing.wait()
        small_own[...] = small[...]
        small_own[:, :shared_rows] += small_other[:, :shared_rows]

        def one(index, carry):
            qkv_own[index] = (
                qkv_own[index].astype(F32) + qkv_other[index].astype(F32)
            ).astype(BF)
            out_own[index] = (
                out_own[index].astype(F32) + out_other[index].astype(F32)
            ).astype(BF)
            return carry

        lax.fori_loop(0, place.count, one, 0)
        swap.start()
        halves.start()
        resting.start()

    make = rows_fetch(partial, scratch[0], rows_sem)
    reduce_phase(place, sender, make, scratch[:REDUCE], between)
    total = scratch[4]

    def body(at):
        total[at] += grad_hidden[at]

    by_rows(total.shape[0], body)
    finish = pair_phase(place, sender, total, result, scratch[REDUCE : REDUCE + 1])
    swap.pass_on()
    finish()
    halves.finish()
    resting.wait()
    swap.finish()
    sender.drain()


def sum_kernel(carried, value, *rest):
    if carried:
        moved, result, arrived, core_in, y_in, held, line_in, sem, side_sem = rest
    else:
        result, core_in, y_in, held, line_in, sem = rest
    place = Place()
    z, y, core = place.z, place.y, place.core
    barrier = pltpu.get_barrier_semaphore()
    others = [place.at(z, y, 1 - core), place.at(z, 1 - y, core)]
    others += [place.at(lax.rem(z + k, LINE), y, core) for k in range(1, LINE)]
    for device in others + [place.across()] * carried:
        signal(barrier, device)
    pl.semaphore_wait(barrier, len(others) + carried)
    if carried:
        side = remote(moved, arrived, side_sem.at[0], side_sem.at[1], place.across())
        side.start()
    first = remote(value, core_in, sem.at[0, 0], sem.at[1, 0], others[0])
    first.start()
    first.wait_recv()
    held[0] = value[...] + core_in[...]
    second = remote(held.at[0], y_in, sem.at[0, 1], sem.at[1, 1], others[1])
    second.start()
    second.wait_recv()
    held[1] = held[0] + y_in[...]
    sends = [
        remote(held.at[1], line_in.at[k - 1], sem.at[0, 1 + k], sem.at[1, 1 + k], others[1 + k])
        for k in range(1, LINE)
    ]
    for send in sends:
        send.start()
    line_in[LINE - 1] = held[1]
    for send in sends:
        send.wait_recv()
    added = jnp.zeros_like(value)
    for source in range(LINE):
        slot = lax.rem(z - source + 2 * LINE - 1, LINE)
        added = added + line_in[slot]
    result[...] = added
    first.wait_send()
    second.wait_send()
    for send in sends:
        send.wait_send()
    if carried:
        side.wait()


def pack_kernel(side, gate, up, down, pair_out, down_out):
    columns = gate.shape[1]
    pair_out[0, :, :columns] = gate[...]
    pair_out[0, :, columns:] = up[...]
    down_out[0] = down[...]


def unpack_kernel(side, own, other, rest, down, gate_out, up_out, down_out):
    half, columns = own.shape[2], gate_out.shape[1]
    quarter = half // 2
    other_start = (1 - side[0]) * half
    parts = ((own, side[0] * half), (other, other_start), (rest, other_start + quarter))
    for part, start in parts:
        value = jnp.sum(part[:, 0].astype(F32), axis=0)
        rows = pl.ds(pl.multiple_of(start, quarter), part.shape[2])
        gate_out[rows] = value[:, :columns]
        up_out[rows] = value[:, columns:]
    down_out[...] = jnp.sum(down[:, 0].astype(F32), axis=0)


def talk(kernel, which, shapes, specs, scratch, microseconds, name=None):
    def call(*operands):
        return pl.pallas_call(
            kernel,
            out_shape=shapes,
            in_specs=specs[0],
            out_specs=specs[1],
            scratch_shapes=scratch,
            compiler_params=pltpu.CompilerParams(
                collective_id=which, has_side_effects=True, vmem_limit_bytes=56 << 20
            ),
            cost_estimate=pl.CostEstimate(
                flops=0, bytes_accessed=int(microseconds * 3.0e6), transcendentals=0
            ),
            name=name or kernel.__name__,
        )(*operands)

    return call


class Team:
    def __init__(self, local_heads, rows, width):
        self.fsdp = lax.axis_size("fsdp")
        self.tensor = lax.axis_size("tensor")
        self.size = 2 * LINE
        self.teams = self.fsdp // self.size
        assert self.fsdp % self.size == 0 and self.tensor == 2 and local_heads % self.size == 0
        self.member = lax.rem(lax.axis_index("fsdp"), self.size)
        self.core = lax.axis_index("tensor")
        self.context = lax.axis_index("context")
        self.groups = None
        if self.teams > 1:
            self.groups = [
                [team * self.size + one for one in range(self.size)] for team in range(self.teams)
            ]
        self.rows = rows
        self.width = width
        self.all_low = jax.ShapeDtypeStruct((2 * self.size * rows, width), BF)
        self.own_wide = jax.ShapeDtypeStruct((rows, width), F32)
        self.line_wide = jax.ShapeDtypeStruct((1, width), F32)
        self.reduces = reduce_scratch(rows, width)
        self.gathers = gather_scratch(rows, width)

    def whole(self, pieces):
        shape = (pieces.shape[0], 2) + pieces.shape[1:]
        return jax.ShapeDtypeStruct(shape, pieces.dtype)

    def first(self, own, weights, out, small):
        rows, columns = weights[0].shape
        rows, columns = rows // 2, columns // self.size
        out_rows = out.shape[0] // self.size // 2
        return talk(
            first_kernel,
            0,
            (
                self.all_low,
                jax.ShapeDtypeStruct((self.fsdp, 2, rows, 3 * columns), BF),
                jax.ShapeDtypeStruct((self.fsdp, 2, out_rows, out.shape[1]), BF),
                jax.ShapeDtypeStruct((self.fsdp, 2) + small.shape, F32),
            ),
            ([VMEM] * 6, (HBM,) * 4),
            self.gathers + swap_scratch(self.fsdp, 5),
            80,
        )(own, *weights, out, small)

    def cut(self, partial):
        return partial.reshape(self.size, 2, self.rows, self.width)

    def pack(self, gate, up, down):
        rows, columns = gate.shape
        rows, columns = rows // 2, columns // self.size
        down_rows, down_columns = down.shape
        down_rows = down_rows // self.size // 2

        def column_spec():
            return pl.BlockSpec((rows, columns), lambda d, side: (side[0], d))

        def piece_spec(*shape):
            return pl.BlockSpec((1,) + shape, lambda d, side: (d, 0, 0))

        pair, low = pl.pallas_call(
            pack_kernel,
            grid_spec=pltpu.PrefetchScalarGridSpec(
                num_scalar_prefetch=1,
                grid=(self.size,),
                in_specs=[
                    column_spec(),
                    column_spec(),
                    pl.BlockSpec((down_rows, down_columns), lambda d, side: (2 * d + side[0], 0)),
                ],
                out_specs=[piece_spec(rows, 2 * columns), piece_spec(down_rows, down_columns)],
            ),
            out_shape=[
                jax.ShapeDtypeStruct((self.size, rows, 2 * columns), BF),
                jax.ShapeDtypeStruct((self.size, down_rows, down_columns), BF),
            ],
            name="pack_kernel",
        )(self.context.reshape(1).astype(jnp.int32), gate, up, down)
        return self.repeat(pair), self.repeat(low)

    def hidden(self, left, right, tokens, gain, pair, down):
        return talk(
            hidden_kernel,
            1,
            (self.all_low, self.own_wide, self.own_wide, self.whole(pair), self.whole(down)),
            ([VMEM] * 6, (HBM, VMEM, VMEM, HBM, HBM)),
            self.reduces + self.gathers + halves_scratch(2),
            100,
        )(left, right, tokens, gain, pair, down)

    def turn(self, left, right, hidden, cotangent, gain):
        pair = jax.ShapeDtypeStruct((2 * self.rows, self.width), BF)
        return talk(
            turn_kernel,
            2,
            (self.all_low, pair, self.line_wide),
            ([VMEM] * 5, (HBM, HBM, VMEM)),
            self.reduces + self.gathers + [pltpu.VMEM((self.rows, self.width), BF)] + pair_scratch(),
            100,
        )(left, right, hidden, cotangent, gain)

    def branch(self, partial, branch, cotangent, gain, inner, grad_mlp, hidden, grad_pair):
        team_rows, units = inner.shape
        columns = grad_pair.shape[1]
        piece = self.width // PIECES
        count = self.fsdp // PIECES
        half = self.width // self.fsdp // 2
        pair_shape = (PIECES, count, half, columns)
        down_shape = (PIECES, units // 2, piece)

        def both(shape):
            return pltpu.VMEM((shape[0], 2) + shape[1:], BF)

        def sides_inside(shape):
            return pltpu.VMEM((shape[0], shape[1], 2) + shape[2:], BF)

        gathered, grad_hidden, gain_grad, pair_mine, down_mine = talk(
            branch_kernel,
            3,
            (
                self.all_low,
                self.own_wide,
                self.line_wide,
                jax.ShapeDtypeStruct(pair_shape, BF),
                jax.ShapeDtypeStruct(down_shape, BF),
            ),
            (
                [HBM, VMEM, VMEM, VMEM, VMEM, HBM, HBM, VMEM],
                (HBM, VMEM, VMEM, VMEM, VMEM),
            ),
            self.reduces
            + self.gathers
            + [
                pltpu.VMEM((2, 2, team_rows, piece), BF),
                pltpu.VMEM((piece, team_rows), BF),
                pltpu.VMEM((units, team_rows), BF),
                sides_inside(pair_shape),
                both(down_shape),
                pltpu.VMEM(pair_shape, BF),
                pltpu.VMEM(down_shape, BF),
                DMA((2, 2)),
                DMA((2, 2, PIECES)),
                DMA((2 * LINE,)),
            ],
            100,
        )(self.cut(partial), branch, cotangent, gain, inner, grad_mlp, hidden, grad_pair)
        down_mine = down_mine.reshape(PIECES, units // 2, count, piece // count)
        return (
            gathered,
            grad_hidden,
            gain_grad,
            pair_mine.reshape(self.fsdp, half, columns),
            down_mine.transpose(0, 2, 1, 3).reshape(self.fsdp, units // 2, piece // count),
        )

    def last(self, partial, grad_hidden, qkv, out, small, down, pair):
        both = jax.ShapeDtypeStruct((2 * self.rows, self.width), F32)

        def same(array):
            return jax.ShapeDtypeStruct(array.shape, array.dtype)

        def half(array):
            return pltpu.VMEM((array.shape[0],) + array.shape[2:], array.dtype)

        held = pltpu.VMEM(small.shape, small.dtype)
        return talk(
            last_kernel,
            4,
            (
                both,
                same(qkv),
                same(out),
                self.whole(small),
                self.whole(down),
                jax.ShapeDtypeStruct((pair.shape[0], pair.shape[1] // 2, pair.shape[2]), BF),
            ),
            ([HBM, VMEM, HBM, HBM, VMEM, VMEM, HBM], (HBM,) * 6),
            self.reduces
            + pair_scratch()
            + swap_scratch(self.fsdp, 3)
            + halves_scratch(1)
            + [half(qkv), half(qkv), half(out), half(out), held, held]
            + [DMA((2,)), DMA((2, 3)), DMA((2,)), DMA((2 * LINE,))],
            80,
        )(self.cut(partial), grad_hidden, qkv, out, small, down, pair)

    def total(self, values, moved=None):
        flat = values.reshape(-1, 128)
        carried = int(moved is not None)
        shape = jax.ShapeDtypeStruct(flat.shape, F32)
        scratch = [pltpu.VMEM(flat.shape, F32)] * 2
        scratch += [pltpu.VMEM((2,) + flat.shape, F32), pltpu.VMEM((LINE,) + flat.shape, F32)]
        scratch += [DMA((2, LINE + 1))] + [DMA((2,))] * carried
        which = 5 + self.sums
        self.sums += 1
        kernel = functools.partial(sum_kernel, carried)
        if not carried:
            call = talk(kernel, which, shape, ([VMEM], VMEM), scratch, 10, "sum_kernel")
            return call(flat).reshape(values.shape)
        shapes = (shape, jax.ShapeDtypeStruct(moved.shape, moved.dtype))
        call = talk(kernel, which, shapes, ([VMEM] * 2, (VMEM,) * 2), scratch, 10, "sum_kernel")
        total, came = call(flat, moved)
        return total.reshape(values.shape), came

    sums = 0

    def half(self, array, axis):
        count = array.shape[axis] // 2
        return lax.dynamic_slice_in_dim(array, self.context * count, count, axis)

    def swap(self, pieces):
        return lax.all_to_all(pieces, "fsdp", split_axis=0, concat_axis=0, tiled=True)

    def repeat(self, pieces):
        return jnp.concatenate([pieces] * self.teams, axis=0) if self.teams > 1 else pieces

    def unpack(self, own, other, rest, down):
        half, columns = own.shape[1], own.shape[2] // 2
        rows, down_columns = 2 * down.shape[2], down.shape[3]

        def cut(array, *shape):
            return array.reshape((self.teams, self.size) + shape)

        def piece_spec(*shape):
            return pl.BlockSpec((self.teams, 1) + shape, lambda d, side: (0, d, 0, 0))

        wide = pl.BlockSpec((2 * half, columns), lambda d, side: (0, d))
        wide_shape = jax.ShapeDtypeStruct((2 * half, self.size * columns), F32)
        return pl.pallas_call(
            unpack_kernel,
            grid_spec=pltpu.PrefetchScalarGridSpec(
                num_scalar_prefetch=1,
                grid=(self.size,),
                in_specs=[piece_spec(half, 2 * columns)]
                + [piece_spec(half // 2, 2 * columns)] * 2
                + [piece_spec(rows, down_columns)],
                out_specs=[wide, wide, pl.BlockSpec((rows, down_columns), lambda d, side: (d, 0))],
            ),
            out_shape=[
                wide_shape,
                wide_shape,
                jax.ShapeDtypeStruct((self.size * rows, down_columns), F32),
            ],
            name="unpack_kernel",
        )(
            self.context.reshape(1).astype(jnp.int32),
            cut(own, half, 2 * columns),
            cut(other, half // 2, 2 * columns),
            cut(rest, half // 2, 2 * columns),
            cut(down, rows, down_columns),
        )

    def columns_whole(self, came):
        return came.reshape(-1, came.shape[-1])

    def rows_whole(self, came):
        fsdp, two, rows, columns = came.shape
        return came.transpose(1, 2, 0, 3).reshape(two * rows, fsdp * columns)

    def of_columns(self, grad):
        rows, columns = grad.shape
        return grad.astype(BF).reshape(self.fsdp, 2, rows // self.fsdp // 2, columns)

    def of_rows(self, grad):
        rows, columns = grad.shape
        cut = grad.astype(BF).reshape(2, rows // 2, self.fsdp, columns // self.fsdp)
        return cut.transpose(2, 0, 1, 3)

    def added(self, came):
        if self.teams == 1:
            return came.astype(F32)
        came = came.reshape((self.teams, self.size) + came.shape[1:])
        return jnp.sum(came.astype(F32), axis=0)

    def columns_out(self, came, count):
        size, two, rows, columns = came.shape
        return [
            self.added(part.reshape(size, two * rows, -1))
            .transpose(1, 0, 2)
            .reshape(two * rows, -1)
            for part in jnp.split(came, count, axis=3)
        ]

    def rows_out(self, came):
        return self.added(came).reshape(-1, came.shape[-1])


def local(
    tokens,
    cont_lengths,
    w_query,
    w_key,
    w_value,
    w_output,
    query_gain,
    key_gain,
    attn_gain,
    w_gate,
    w_up,
    w_down,
    mlp_gain,
    cotangent,
):
    rows = tokens.shape[0]
    width = tokens.shape[1]
    fsdp = lax.axis_size("fsdp")
    tensor = lax.axis_size("tensor")
    local_heads = query_gain.shape[0]
    head_size = w_query.shape[1] // local_heads
    own_rows = rows // tensor
    team = Team(local_heads, own_rows, width)
    groups = team.size
    team_rows = groups * rows
    heads = local_heads // team.size
    later = lax.axis_index("context") == 1

    tokens_own = lax.dynamic_slice_in_dim(tokens, team.core * own_rows, own_rows, 0)
    grad_out = lax.dynamic_slice_in_dim(cotangent, team.core * own_rows, own_rows, 0)
    cut = query_gain.size
    share = attn_gain.size
    small = [query_gain.reshape(-1), key_gain.reshape(-1), attn_gain, mlp_gain]
    small = jnp.concatenate([one.astype(F32) for one in small + [cont_lengths.reshape(-1)]])
    small = jnp.pad(small, (0, 8 * 128 - small.size)).reshape(8, 128)
    tokens_all, qkv_came, output_came, small_came = team.first(
        tokens_own, [w_query, w_key, w_value], w_output, small
    )
    qkv_w = team.columns_whole(qkv_came)
    output_w = team.rows_whole(output_came)
    all_small = small_came[:, 0].reshape(fsdp, -1)
    query_gains = all_small[:, :cut].reshape(fsdp, local_heads, -1)
    key_gains = all_small[:, cut : 2 * cut].reshape(fsdp, local_heads, -1)
    query_gains = query_gains.transpose(1, 0, 2).reshape(local_heads, head_size)
    key_gains = key_gains.transpose(1, 0, 2).reshape(local_heads, head_size)
    flat_query = lax.dynamic_slice_in_dim(query_gains, team.member * heads, heads, 0).reshape(-1)
    flat_key = lax.dynamic_slice_in_dim(key_gains, team.member * heads, heads, 0).reshape(-1)
    gain_attn = all_small[:, 2 * cut : 2 * cut + share].reshape(1, -1)
    gain_mlp = all_small[:, 2 * cut + share : 2 * cut + 2 * share].reshape(1, -1)

    conts = cont_lengths.shape[1]
    lengths = all_small[:, 2 * cut + 2 * share : 2 * cut + 2 * share + conts].astype(jnp.int32)
    first_group = lax.axis_index("fsdp") - team.member
    lengths = lax.dynamic_slice_in_dim(lengths, first_group, groups, 0)
    segment, offset = jax.vmap(lambda one: layout(one, rows))(lengths)
    row_index = jnp.arange(rows, dtype=jnp.int32)
    positions = jnp.where(later, rows + offset, row_index[None, :])
    own_segment = jnp.where(later, segment, -1)
    cosine, sine = rotary_tables(positions, head_size)
    cosine = cosine[:, :, None, :]
    sine = sine[:, :, None, :]

    pair_mine, down_mine, tokens_all = lax.optimization_barrier(
        team.pack(w_gate, w_up, w_down) + (tokens_all,)
    )
    pair_came = team.swap(pair_mine)
    down_came = team.swap(down_mine)

    by_head = (groups, rows, heads, head_size)
    raw = product(tokens_all, qkv_w)
    query_raw, key_raw, value_raw = jnp.split(raw, 3, axis=1)
    value_low = value_raw.astype(BF)
    sums, sent_value = team.total(
        jnp.stack([jnp.sum(query_raw * query_raw, axis=1), jnp.sum(key_raw * key_raw, axis=1)]),
        value_low,
    )
    value_low, sent_value = value_low.reshape(by_head), sent_value.reshape(by_head)
    scale_query = lax.rsqrt(sums[0] / width + EPS)[:, None]
    scale_key = lax.rsqrt(sums[1] / width + EPS)[:, None]
    query_norm = query_raw * scale_query * flat_query
    key_norm = key_raw * scale_key * flat_key
    query_low = rotate(query_norm.reshape(by_head), cosine, sine).astype(BF)
    key_low = rotate(key_norm.reshape(by_head), cosine, sine).astype(BF)
    sent_key = lax.ppermute(key_low, "context", [(0, 1)])
    keys_all = jnp.concatenate([sent_key, key_low], axis=1)
    values_all = jnp.concatenate([sent_value, value_low], axis=1)
    key_index = jnp.arange(2 * rows, dtype=jnp.int32)
    key_segment = jnp.concatenate([jnp.full((groups, rows), -2, jnp.int32), own_segment], axis=1)
    remote = (key_index < rows)[None, None, :] & later
    own_keys = (
        (key_index >= rows)[None, None, :]
        & (key_index[None, None, :] - rows <= row_index[None, :, None])
        & (key_segment[:, None, :] == own_segment[:, :, None])
    )
    allowed = (remote | own_keys)[:, None]
    scale = 1.0 / math.sqrt(head_size)
    scores = (
        jnp.einsum("gqhd,gkhd->ghqk", query_low, keys_all, preferred_element_type=F32) * scale
    )
    scores = jnp.where(allowed, scores, -1e30)
    highest = jnp.max(scores, axis=-1, keepdims=True)
    weights = jnp.exp(scores - highest)
    probs = weights / jnp.sum(weights, axis=-1, keepdims=True)
    probs_low = probs.astype(BF)
    mixed = jnp.einsum("ghqk,gkhd->gqhd", probs_low, values_all, preferred_element_type=F32)
    attended_low = mixed.reshape(team_rows, heads * head_size).astype(BF)
    hidden_all, attn_sum, hidden, pair_came, down_came = team.hidden(
        attended_low, output_w, tokens_own, gain_attn, pair_came, down_came
    )
    pair_w = team.columns_whole(pair_came)
    down_w = team.rows_whole(down_came)

    gate, upward = jnp.split(product(hidden_all, pair_w), 2, axis=1)
    sigma = jax.nn.sigmoid(gate)
    inner_low = (gate * sigma * upward).astype(BF)
    grad_mlp_all, outputs, grad_mlp_gain = team.turn(
        inner_low, down_w, hidden, grad_out, gain_mlp
    )
    grad_inner = product_right(grad_mlp_all, down_w)
    grad_gate_low = (grad_inner * upward * sigma * (1.0 + gate * (1.0 - sigma))).astype(BF)
    grad_up_low = (grad_inner * gate * sigma).astype(BF)
    grad_pair = jnp.concatenate([grad_gate_low, grad_up_low], axis=1)
    grad_branch_all, grad_hidden, grad_attn_gain, pair_mine, down_mine = team.branch(
        product_right(grad_pair, pair_w).astype(BF),
        attn_sum,
        grad_out,
        gain_attn,
        inner_low,
        grad_mlp_all,
        hidden_all,
        grad_pair,
    )
    pair_came = team.swap(pair_mine)
    output_grad = team.of_rows(product_left(attended_low, grad_branch_all))
    grad_attended = product_right(grad_branch_all, output_w).astype(BF).reshape(by_head)

    grad_probs = jnp.einsum("gqhd,gkhd->ghqk", grad_attended, values_all, preferred_element_type=F32)
    centre = jnp.sum(probs * grad_probs, axis=-1, keepdims=True)
    grad_scores = (probs * (grad_probs - centre)).astype(BF)
    grad_query_rot = (
        jnp.einsum("ghqk,gkhd->gqhd", grad_scores, keys_all, preferred_element_type=F32) * scale
    )
    grad_keys = (
        jnp.einsum("ghqk,gqhd->gkhd", grad_scores, query_low, preferred_element_type=F32) * scale
    )
    grad_values = jnp.einsum("ghqk,gqhd->gkhd", probs_low, grad_attended, preferred_element_type=F32)
    back_value = lax.ppermute(grad_values[:, :rows].astype(BF), "context", [(1, 0)])
    back_key = lax.ppermute(grad_keys[:, :rows].astype(BF), "context", [(1, 0)])
    grad_key_rot = grad_keys[:, rows:] + back_key.astype(F32)
    grad_value_low = (
        (grad_values[:, rows:] + back_value.astype(F32)).reshape(team_rows, -1).astype(BF)
    )
    grad_query_norm = rotate_back(grad_query_rot, cosine, sine).reshape(team_rows, -1)
    grad_key_norm = rotate_back(grad_key_rot, cosine, sine).reshape(team_rows, -1)
    grad_query_gain = jnp.sum(grad_query_norm * query_raw * scale_query, axis=0)
    grad_key_gain = jnp.sum(grad_key_norm * key_raw * scale_key, axis=0)
    inner_sums = jnp.stack(
        [
            jnp.sum(query_raw * flat_query * grad_query_norm, axis=1),
            jnp.sum(key_raw * flat_key * grad_key_norm, axis=1),
        ]
    )
    inner_sums, pair_came = lax.optimization_barrier((inner_sums, pair_came))
    pair_other = lax.ppermute(
        pair_came[:, : pair_came.shape[1] // 2], "context", [(0, 1), (1, 0)]
    )
    totals = team.total(inner_sums)
    down_mine, totals = lax.optimization_barrier((down_mine, totals))
    down_came = team.swap(down_mine)
    grad_query_low = norm_back(
        query_raw, scale_query, flat_query, grad_query_norm, totals[0][:, None], width
    ).astype(BF)
    grad_key_low = norm_back(
        key_raw, scale_key, flat_key, grad_key_norm, totals[1][:, None], width
    ).astype(BF)
    grad_qkv = jnp.concatenate([grad_query_low, grad_key_low, grad_value_low], axis=1)
    qkv_grad = team.of_columns(product_left(tokens_all, grad_qkv))
    head_share = head_size // fsdp
    small = [
        grad_attn_gain.reshape(fsdp, share),
        grad_mlp_gain.reshape(fsdp, share),
        grad_query_gain.reshape(heads, fsdp, head_share).transpose(1, 0, 2).reshape(fsdp, -1),
        grad_key_gain.reshape(heads, fsdp, head_share).transpose(1, 0, 2).reshape(fsdp, -1),
    ]
    used = 2 * share + 2 * heads * head_share
    small = jnp.concatenate(small + [jnp.zeros((fsdp, 8 * 128 - used), F32)], axis=1)
    partial, pair_other = lax.optimization_barrier(
        (product_right(grad_qkv, qkv_w).astype(BF), pair_other)
    )
    input_grad, qkv_came, output_came, small_came, down_came, pair_rest = team.last(
        partial,
        grad_hidden,
        qkv_grad,
        output_grad,
        small.reshape(fsdp, 8, 128),
        down_came,
        pair_came,
    )
    grad_w_query, grad_w_key, grad_w_value = team.columns_out(qkv_came, 3)
    grad_w_gate, grad_w_up, grad_w_down = team.unpack(
        pair_came, pair_other, pair_rest, down_came
    )
    grad_w_output = team.rows_out(output_came)
    came = jnp.sum(small_came, axis=1).reshape(fsdp, -1)
    row_gains = jnp.sum(came[:, : 2 * share], axis=0).reshape(2, share)
    head_gains = team.added(came[:, 2 * share : used]).reshape(team.size, 2, heads, head_share)
    head_gains = head_gains.transpose(1, 0, 2, 3).reshape(2, local_heads, head_share)
    return (
        outputs,
        input_grad,
        grad_w_query,
        grad_w_key,
        grad_w_value,
        grad_w_output,
        head_gains[0],
        head_gains[1],
        row_gains[0],
        grad_w_gate,
        grad_w_up,
        grad_w_down,
        row_gains[1],
    )


def solution(mesh):
    return jax.shard_map(
        local,
        mesh=mesh,
        in_specs=(
            P(("fsdp", "context"), None),
            P("fsdp", None),
            P("fsdp", "tensor"),
            P("fsdp", "tensor"),
            P("fsdp", "tensor"),
            P("tensor", "fsdp"),
            P("tensor", "fsdp"),
            P("tensor", "fsdp"),
            P("fsdp"),
            P("fsdp", "tensor"),
            P("fsdp", "tensor"),
            P("tensor", "fsdp"),
            P("fsdp"),
            P(("fsdp", "context"), None),
        ),
        out_specs=(
            P(("fsdp", "context"), None),
            P(("fsdp", "context"), None),
            P("fsdp", "tensor"),
            P("fsdp", "tensor"),
            P("fsdp", "tensor"),
            P("tensor", "fsdp"),
            P("tensor", "fsdp"),
            P("tensor", "fsdp"),
            P("fsdp"),
            P("fsdp", "tensor"),
            P("fsdp", "tensor"),
            P("tensor", "fsdp"),
            P("fsdp"),
        ),
        check_vma=False,
    )
```

```python
import functools
import math

import jax
import jax.numpy as jnp
from jax import lax
from jax.experimental import pallas as pl
from jax.experimental.pallas import tpu as pltpu
from jax.sharding import PartitionSpec as P

EPS = 1e-06
THETA = 500000.0
BF = jnp.bfloat16
F32 = jnp.float32


def product(left, right):
    return jnp.dot(left, right, preferred_element_type=F32)


def product_left(left, right):
    return jnp.einsum("rd,rf->df", left, right, preferred_element_type=F32)


def product_right(left, right):
    return jnp.einsum("rf,df->rd", left, right, preferred_element_type=F32)


def rotary_tables(positions, head_size):
    half = head_size // 2
    inverse = jnp.exp(-(2.0 * jnp.arange(half, dtype=F32) / head_size) * math.log(THETA))
    angles = positions.astype(F32)[..., None] * inverse
    angles = jnp.concatenate([angles, angles], axis=-1)
    return (jnp.cos(angles), jnp.sin(angles))


def rotate(values, cosine, sine):
    half = values.shape[-1] // 2
    turned = jnp.concatenate([-values[..., half:], values[..., :half]], axis=-1)
    return values * cosine + turned * sine


def rotate_back(grads, cosine, sine):
    half = grads.shape[-1] // 2
    scaled = grads * sine
    turned = jnp.concatenate([scaled[..., half:], -scaled[..., :half]], axis=-1)
    return grads * cosine + turned


def norm_back(values, scale, gain, grads, total, width):
    return scale * gain * grads - values * scale * scale * scale * (total / width)


def layout(lengths, rows):
    segment_ends = jnp.cumsum(lengths)
    segment_starts = segment_ends - lengths
    row_index = jnp.arange(rows, dtype=jnp.int32)
    segment = jnp.sum((row_index[:, None] >= segment_ends[None, :]).astype(jnp.int32), axis=1)
    chosen = segment[:, None] == jnp.arange(lengths.shape[0], dtype=jnp.int32)[None, :]
    offset = row_index - jnp.sum(jnp.where(chosen, segment_starts[None, :], 0), axis=1)
    return (segment, offset)


LINE = 4
CHUNK = 16
MESH_ID = pl.DeviceIdType.MESH
HBM = pl.BlockSpec(memory_space=pl.ANY)
VMEM = pl.BlockSpec(memory_space=pltpu.VMEM)
DMA = pltpu.SemaphoreType.DMA


class Place:
    def __init__(self):
        device = lax.axis_index("fsdp")
        member = lax.rem(device, 2 * LINE)
        self.base = device - member
        self.z = member // 2
        self.y = lax.rem(member, 2)
        self.core = lax.axis_index("tensor")
        self.side = lax.axis_index("context")
        self.device = device
        self.count = lax.axis_size("fsdp")

    def across(self):
        return {"context": 1 - self.side}

    def at(self, z, y, core):
        return {"fsdp": self.base + 2 * z + y, "tensor": core}

    def near(self):
        yield None, self.at(self.z, self.y, 1 - self.core)
        yield None, self.at(self.z, 1 - self.y, self.core)
        yield self.z > 0, self.at(self.z - 1, self.y, self.core)
        yield self.z < LINE - 1, self.at(self.z + 1, self.y, self.core)

    def rows(self, z, y, core, count):
        start = ((2 * z + y) * 2 + core) * count
        return pl.ds(pl.multiple_of(start, count), count)


def guarded(condition, action):
    if condition is None:
        action()
    else:
        pl.when(condition)(action)


def signal(barrier, device):
    pl.semaphore_signal(barrier, inc=1, device_id=device, device_id_type=MESH_ID)


def greet(place, across=False):
    barrier = pltpu.get_barrier_semaphore()
    for condition, device in place.near():
        guarded(condition, functools.partial(signal, barrier, device))
    if across:
        signal(barrier, place.across())
    inside = (place.z > 0) & (place.z < LINE - 1)
    pl.semaphore_wait(barrier, jnp.where(inside, 4, 3) + int(across))


def greet_all(place):
    barrier = pltpu.get_barrier_semaphore()

    def one(step, carry):
        signal(barrier, {"fsdp": lax.rem(place.device + step, place.count)})
        return carry

    lax.fori_loop(1, place.count, one, 0)
    signal(barrier, place.across())
    signal(barrier, place.at(place.z, place.y, 1 - place.core))
    pl.semaphore_wait(barrier, place.count + 1)


class Sender:
    def __init__(self):
        self.sent = []

    def __call__(self, condition, make):
        def start():
            make().start()

        guarded(condition, start)
        self.sent.append((condition, make))

    def drain(self):
        for condition, make in self.sent:

            def wait(make=make):
                make().wait_send()

            guarded(condition, wait)


def remote(source, target, send, receive, device):
    return pltpu.make_async_remote_copy(
        src_ref=source,
        dst_ref=target,
        send_sem=send,
        recv_sem=receive,
        device_id=device,
        device_id_type=MESH_ID,
    )


def by_rows(rows, body):
    def step(index, carry):
        body(pl.ds(pl.multiple_of(index * CHUNK, CHUNK), CHUNK))
        return carry

    lax.fori_loop(0, rows // CHUNK, step, 0)


def reduce_scratch(rows, width):
    return [
        pltpu.VMEM((2 * LINE, rows, width), BF),
        pltpu.VMEM((2 * LINE, rows, width), BF),
        pltpu.VMEM((LINE, rows, width), BF),
        pltpu.VMEM((LINE + 1, rows, width), BF),
        pltpu.VMEM((rows, width), F32),
        DMA((2 * LINE,)),
        DMA((2, 2 * LINE)),
        DMA((2, LINE)),
        DMA((2, LINE + 1)),
    ]


def reduce_phase(place, sender, partial, scratch, between=None, idle=None, late=None):
    mine, core_in, y_in, line_in, total, local_sem, core_sem, y_sem, line_sem = scratch
    rows = total.shape[0]
    z, y, core = place.z, place.y, place.core
    low = z < LINE // 2
    order = []
    for k in range(LINE - 1):
        down = LINE - 1 - k
        down = jnp.where(down <= z, down - 1, down)
        up = jnp.where(k >= z, k + 1, k)
        order.append(jnp.where(low, down, up))
    order.append(z)

    def fetch(slot):
        half = lax.rem(slot, 2)
        return pltpu.make_async_copy(
            partial.at[place.rows(slot // 2, half, core, rows)], mine.at[slot], local_sem.at[slot]
        )

    def to_core(slot):
        half = lax.rem(slot, 2)
        return remote(
            partial.at[place.rows(slot // 2, half, 1 - core, rows)],
            core_in.at[slot],
            core_sem.at[0, slot],
            core_sem.at[1, slot],
            place.at(z, y, 1 - core),
        )

    def to_y(block):
        return remote(
            mine.at[2 * block + 1 - y],
            y_in.at[block],
            y_sem.at[0, block],
            y_sem.at[1, block],
            place.at(z, 1 - y, core),
        )

    def to_line(block):
        step = jnp.where(block > z, 1, -1)
        slot = jnp.where((step < 0) & (block == z - 1), LINE, block)
        return remote(
            mine.at[2 * block + y],
            line_in.at[slot],
            line_sem.at[0, block],
            line_sem.at[1, slot],
            place.at(z + step, y, core),
        )

    def from_line(slot):
        return remote(
            mine.at[0],
            line_in.at[slot],
            line_sem.at[0, 0],
            line_sem.at[1, slot],
            place.at(z, y, 1 - core),
        )

    for half in (1 - y, y):
        for block in order:
            sender(None, functools.partial(to_core, 2 * block + half))
            fetch(2 * block + half).start()

    for block in order:
        slot = 2 * block + 1 - y
        fetch(slot).wait()
        to_core(slot).wait_recv()

        def add(at, slot=slot):
            value = mine[slot, at].astype(F32) + core_in[slot, at].astype(F32)
            mine[slot, at] = value.astype(BF)

        by_rows(rows, add)
        sender(None, functools.partial(to_y, block))

    for number, block in enumerate(order[:-1]):
        if number == LINE - 2 and between is not None:
            between()
        if number < 2 and idle is not None:
            idle(number)
        slot = 2 * block + y
        fetch(slot).wait()
        to_core(slot).wait_recv()
        to_y(block).wait_recv()
        inner = jnp.where(block > z, z > 0, z < LINE - 1)

        @pl.when(inner)
        def _(block=block, slot=slot):
            from_line(block).wait_recv()

            def add(at):
                value = mine[slot, at].astype(F32) + core_in[slot, at].astype(F32)
                value = value + y_in[block, at].astype(F32)
                mine[slot, at] = (value + line_in[block, at].astype(F32)).astype(BF)

            by_rows(rows, add)

        @pl.when(jnp.logical_not(inner))
        def _(block=block, slot=slot):
            def add(at):
                value = mine[slot, at].astype(F32) + core_in[slot, at].astype(F32)
                mine[slot, at] = (value + y_in[block, at].astype(F32)).astype(BF)

            by_rows(rows, add)

        sender(None, functools.partial(to_line, block))

    if late is not None:
        late()
    slot = 2 * z + y
    fetch(slot).wait()
    to_core(slot).wait_recv()
    to_y(z).wait_recv()

    def start(at):
        value = mine[slot, at].astype(F32) + core_in[slot, at].astype(F32)
        total[at] = value + y_in[z, at].astype(F32)

    by_rows(rows, start)
    for condition, source in ((z > 0, z), (z < LINE - 1, LINE)):

        @pl.when(condition)
        def _(source=source):
            from_line(source).wait_recv()

            def add(at):
                total[at] += line_in[source, at].astype(F32)

            by_rows(rows, add)


def gather_scratch(rows, width):
    return [
        pltpu.VMEM((rows, width), BF),
        DMA((1,)),
        DMA((2, 2 * LINE)),
        DMA((2, LINE)),
        DMA((2, LINE + 2)),
    ]


def gather_phase(place, sender, gathered, scratch, between=None, later=None, last=None):
    own, local_sem, core_sem, y_sem, line_sem = scratch
    rows = own.shape[0]
    z, y, core = place.z, place.y, place.core

    def spot(block, half):
        return gathered.at[place.rows(block, half, core, rows)]

    def to_core(source, block, half):
        return remote(
            source,
            spot(block, half),
            core_sem.at[0, 2 * block + half],
            core_sem.at[1, 2 * block + half],
            place.at(z, y, 1 - core),
        )

    def to_y(source, block):
        return remote(
            source,
            spot(block, y),
            y_sem.at[0, block],
            y_sem.at[1, block],
            place.at(z, 1 - y, core),
        )

    def to_line(source, block, step, index):
        return remote(
            source,
            spot(block, y),
            line_sem.at[0, index],
            line_sem.at[1, block],
            place.at(z + step, y, core),
        )

    keep = pltpu.make_async_copy(own, spot(z, y), local_sem.at[0])
    keep.start()
    sender(z < LINE - 1, functools.partial(to_line, own, z, 1, LINE))
    sender(z > 0, functools.partial(to_line, own, z, -1, LINE + 1))
    sender(None, functools.partial(to_y, own, z))
    sender(None, functools.partial(to_core, own, z, y))
    if between is not None:
        between()

    def took_y(block):
        remote(
            own,
            spot(block, 1 - y),
            y_sem.at[0, block],
            y_sem.at[1, block],
            place.at(z, 1 - y, core),
        ).wait_recv()

    def across(condition, block):
        guarded(condition, functools.partial(took_y, block))
        sender(condition, lambda: to_core(spot(block, 1 - y), block, 1 - y))

    def along(condition, block, step):
        def took():
            to_line(own, block, step, block).wait_recv()

        guarded(condition, took)
        onward = condition & ((z < LINE - 1) if step > 0 else (z > 0))
        sender(onward, lambda: to_line(spot(block, y), block, step, block))
        sender(condition, lambda: to_y(spot(block, y), block))
        sender(condition, lambda: to_core(spot(block, y), block, y))

    for distance in range(1, LINE + 1):
        if distance < LINE:
            along(z >= distance, z - distance, 1)
            along(z + distance < LINE, z + distance, -1)
        if distance == 1:
            across(None, z)
        else:
            across(z >= distance - 1, z - distance + 1)
            across(z + distance - 1 < LINE, z + distance - 1)
        if distance == 1 and later is not None:
            later()
        if distance == LINE - 1 and last is not None:
            last()

    keep.wait()
    for block in range(LINE):
        for half in range(2):
            remote(
                own,
                gathered.at[place.rows(block, half, 1 - core, rows)],
                core_sem.at[0, 2 * block + half],
                core_sem.at[1, 2 * block + half],
                place.at(z, y, 1 - core),
            ).wait_recv()


def pair_scratch():
    return [DMA((3,))]


def pair_phase(place, sender, own, pair, scratch):
    (sem,) = scratch
    rows = own.shape[0]
    spot = pair.at[pl.ds(pl.multiple_of(place.core * rows, rows), rows)]
    keep = pltpu.make_async_copy(own, spot, sem.at[0])
    keep.start()

    def send():
        return remote(
            own, spot, sem.at[1], sem.at[2], place.at(place.z, place.y, 1 - place.core)
        )

    sender(None, send)

    def finish():
        keep.wait()
        other = pair.at[pl.ds(pl.multiple_of((1 - place.core) * rows, rows), rows)]
        remote(
            own, other, sem.at[1], sem.at[2], place.at(place.z, place.y, 1 - place.core)
        ).wait_recv()

    return finish


def swap_scratch(count, arrays):
    return [DMA((arrays,)), DMA((2, arrays, count)), DMA((2, arrays, count))]


class Swap:
    def __init__(self, place, pairs, scratch):
        self.place = place
        self.pairs = pairs
        self.local_sem, self.out_sem, self.side_sem = scratch

    def send(self, index, step):
        place = self.place
        source, spot = self.pairs[index]
        target = lax.rem(place.device + step, place.count)
        return remote(
            source(target),
            spot(place.device, place.side),
            self.out_sem.at[0, index, step],
            self.out_sem.at[1, index, step],
            {"fsdp": target},
        )

    def taken(self, index, step, side):
        device = lax.rem(self.place.device + self.place.count - step, self.place.count)
        return self.pairs[index][1](device, side)

    def come(self, index, step):
        place = self.place
        return remote(
            self.pairs[index][0](place.device),
            self.taken(index, step, place.side),
            self.out_sem.at[0, index, step],
            self.out_sem.at[1, index, step],
            place.across(),
        )

    def share(self, index, step, source=None):
        spot = self.taken(index, step, self.place.side)
        return remote(
            spot if source is None else source,
            spot,
            self.side_sem.at[0, index, step],
            self.side_sem.at[1, index, step],
            self.place.across(),
        )

    def shared(self, index, step):
        spot = self.taken(index, step, 1 - self.place.side)
        return remote(
            spot,
            spot,
            self.side_sem.at[0, index, step],
            self.side_sem.at[1, index, step],
            self.place.across(),
        )

    def keep(self, index):
        place = self.place
        source, spot = self.pairs[index]
        return pltpu.make_async_copy(
            source(place.device), spot(place.device, place.side), self.local_sem.at[index]
        )

    def each(self, first, body):
        def step(number, carry):
            for index in range(len(self.pairs)):
                body(index, number)
            return carry

        lax.fori_loop(first, self.place.count, step, 0)

    def start(self):
        self.each(1, lambda index, step: self.send(index, step).start())
        for index, (source, _) in enumerate(self.pairs):
            self.keep(index).start()
            self.share(index, 0, source(self.place.device)).start()

    def pass_on(self):
        def one(index, step):
            self.come(index, step).wait_recv()
            self.share(index, step).start()

        self.each(1, one)

    def finish(self):
        for index in range(len(self.pairs)):
            self.keep(index).wait()
        self.each(0, lambda index, step: self.shared(index, step).wait_recv())
        self.each(1, lambda index, step: self.send(index, step).wait_send())
        self.each(0, lambda index, step: self.share(index, step).wait_send())


def whole_pair(pieces, whole):
    return (lambda target: pieces.at[target], lambda device, side: whole.at[device, side])


def halves_scratch(arrays):
    return [DMA((3, arrays))]


class Halves:
    def __init__(self, place, halves, wholes, scratch):
        self.place = place
        self.pairs = list(zip(halves, wholes))
        (self.sem,) = scratch

    def keep(self, index):
        half, whole = self.pairs[index]
        return pltpu.make_async_copy(half, whole.at[:, self.place.side], self.sem.at[0, index])

    def copy(self, index, side):
        half, whole = self.pairs[index]
        return remote(
            half,
            whole.at[:, side],
            self.sem.at[1, index],
            self.sem.at[2, index],
            self.place.across(),
        )

    def start(self):
        for index in range(len(self.pairs)):
            self.copy(index, self.place.side).start()
            self.keep(index).start()

    def finish(self):
        for index in range(len(self.pairs)):
            self.keep(index).wait()
            self.copy(index, 1 - self.place.side).wait_recv()
            self.copy(index, self.place.side).wait_send()


REDUCE = 9
GATHER = 5
PIECES = 8


def first_kernel(
    own_ref, query, key, value, out, small, gathered, qkv_all, out_all, small_all, *scratch
):
    place = Place()
    sender = Sender()
    own = scratch[0]
    own[...] = own_ref[...]
    greet_all(place)
    half, columns = qkv_all.shape[2], qkv_all.shape[3] // 3
    out_half = out_all.shape[2]
    rows = pl.ds(pl.multiple_of(place.side * half, half), half)

    def member(target):
        return lax.rem(target, 2 * LINE)

    def column_pair(weight, index):
        def source(target):
            start = pl.multiple_of(member(target) * columns, columns)
            return weight.at[rows, pl.ds(start, columns)]

        def spot(device, side):
            return qkv_all.at[device, side, :, pl.ds(index * columns, columns)]

        return (source, spot)

    def out_source(target):
        start = (2 * member(target) + place.side) * out_half
        return out.at[pl.ds(pl.multiple_of(start, out_half), out_half)]

    pairs = [
        (lambda target: small, lambda device, side: small_all.at[device, side]),
        column_pair(query, 0),
        column_pair(key, 1),
        column_pair(value, 2),
        (out_source, lambda device, side: out_all.at[device, side]),
    ]
    swap = Swap(place, pairs, scratch[GATHER:])
    gather_phase(place, sender, gathered, scratch[:GATHER], swap.start, swap.pass_on)
    swap.finish()
    sender.drain()


def hidden_kernel(
    partial, tokens, gain, pair, down, gathered, branch, hidden, pair_all, down_all, *scratch
):
    place = Place()
    sender = Sender()
    greet(place, True)
    halves = Halves(place, (pair, down), (pair_all, down_all), scratch[REDUCE + GATHER :])
    halves.start()
    reduce_phase(place, sender, partial, scratch[:REDUCE])
    total, own = scratch[4], scratch[REDUCE]
    rows, width = total.shape

    def body(at):
        value = total[at]
        scale = lax.rsqrt(jnp.sum(value * value, axis=1, keepdims=True) / width + EPS)
        result = tokens[at].astype(F32) + value * scale * gain[...]
        branch[at] = value
        hidden[at] = result
        own[at] = result.astype(BF)

    by_rows(rows, body)
    gather_phase(place, sender, gathered, scratch[REDUCE : REDUCE + GATHER])
    halves.finish()
    sender.drain()


def turn_kernel(partial, hidden, cotangent, gain, gathered, outputs, gain_grad, *scratch):
    place = Place()
    sender = Sender()
    greet(place)
    reduce_phase(place, sender, partial, scratch[:REDUCE])
    total, own = scratch[4], scratch[REDUCE]
    out_own = scratch[REDUCE + GATHER]
    rows, width = total.shape
    gain_grad[...] = jnp.zeros_like(gain_grad)

    def body(at):
        value = total[at]
        scale = lax.rsqrt(jnp.sum(value * value, axis=1, keepdims=True) / width + EPS)
        grads = cotangent[at].astype(F32)
        normed = value * scale
        out_own[at] = (hidden[at] + normed * gain[...]).astype(BF)
        gain_grad[...] += jnp.sum(grads * normed, axis=0, keepdims=True)
        gained = gain[...] * grads
        inner = jnp.sum(normed * gained, axis=1, keepdims=True)
        own[at] = (scale * (gained - normed * (inner / width))).astype(BF)

    by_rows(rows, body)
    finish = pair_phase(place, sender, out_own, outputs, scratch[REDUCE + GATHER + 1 :])
    gather_phase(place, sender, gathered, scratch[REDUCE : REDUCE + GATHER])
    finish()
    sender.drain()


class WeightGrads:
    def __init__(self, place, arrays, outs, scratch):
        self.place = place
        self.inner, self.grad_mlp, self.hidden, self.grad_pair = arrays
        self.outs = outs
        self.tall, self.turned, self.inner_turned = scratch[:3]
        self.fulls, self.others = scratch[3:5], scratch[5:7]
        self.fetch_sem, self.side_sem = scratch[7:]
        self.piece = self.tall.shape[3]

    def fetch(self, number, slot):
        columns = pl.ds(pl.multiple_of(number * self.piece, self.piece), self.piece)
        return [
            pltpu.make_async_copy(
                array.at[:, columns], self.tall.at[slot, index], self.fetch_sem.at[slot, index]
            )
            for index, array in enumerate((self.hidden, self.grad_mlp))
        ]

    def side_of(self, index, number, side):
        if index == 0:
            return self.fulls[0].at[number, :, side]
        return self.fulls[1].at[number, side]

    def crossing(self, number, index):
        return remote(
            self.side_of(index, number, 1 - self.place.side),
            self.others[index].at[number],
            self.side_sem.at[0, index, number],
            self.side_sem.at[1, index, number],
            self.place.across(),
        )

    def start(self):
        for copy in self.fetch(0, 0):
            copy.start()
        self.inner_turned[...] = self.inner[...].T

    def one(self, number, carry):
        slot = lax.rem(number, 2)
        for copy in self.fetch(number, slot):
            copy.wait()

        @pl.when(number < PIECES - 1)
        def _():
            for copy in self.fetch(number + 1, 1 - slot):
                copy.start()

        full, low = self.fulls
        self.turned[...] = self.tall[slot, 0].T
        columns = self.grad_pair.shape[1]
        step = columns // 4

        def columns_step(index, carry):
            at = pl.ds(pl.multiple_of(index * step, step), step)
            value = product(self.turned[...], self.grad_pair[:, at]).astype(BF)
            full[number, :, :, :, at] = value.reshape(full.shape[1:4] + (step,))
            return carry

        lax.fori_loop(0, 4, columns_step, 0)
        value = product(self.inner_turned[...], self.tall[slot, 1]).astype(BF)
        low[number] = value.reshape(low.shape[1:])
        for index in range(2):
            self.crossing(number, index).start()
        return carry

    def some(self, which):
        half = PIECES // 2
        lax.fori_loop(which * half, which * half + half, self.one, 0)

    def add(self):
        def step(number, carry):
            for index in range(2):
                self.crossing(number, index).wait_recv()
                own = self.side_of(index, number, self.place.side)[...].astype(F32)
                other = self.others[index][number].astype(F32)
                self.outs[index][number] = (own + other).astype(BF)
            return carry

        lax.fori_loop(0, PIECES, step, 0)

    def finish(self):
        def step(number, carry):
            for index in range(2):
                self.crossing(number, index).wait_send()
            return carry

        lax.fori_loop(0, PIECES, step, 0)


def branch_kernel(
    partial,
    branch,
    cotangent,
    gain,
    inner_low,
    grad_mlp,
    hidden_low,
    grad_pair,
    gathered,
    grad_hidden,
    gain_grad,
    pair_mine,
    down_mine,
    *scratch,
):
    place = Place()
    sender = Sender()
    greet(place, True)
    grads = WeightGrads(
        place,
        (inner_low, grad_mlp, hidden_low, grad_pair),
        (pair_mine, down_mine),
        scratch[REDUCE + GATHER :],
    )
    grads.start()
    reduce_phase(place, sender, partial, scratch[:REDUCE], idle=grads.some)
    total, own = scratch[4], scratch[REDUCE]
    rows, width = total.shape
    gain_grad[...] = jnp.zeros_like(gain_grad)

    def body(at):
        value = branch[at]
        scale = lax.rsqrt(jnp.sum(value * value, axis=1, keepdims=True) / width + EPS)
        grads = cotangent[at].astype(F32) + total[at]
        grad_hidden[at] = grads
        normed = value * scale
        gain_grad[...] += jnp.sum(grads * normed, axis=0, keepdims=True)
        gained = gain[...] * grads
        inner = jnp.sum(normed * gained, axis=1, keepdims=True)
        own[at] = (scale * (gained - normed * (inner / width))).astype(BF)

    by_rows(rows, body)
    gather_phase(
        place, sender, gathered, scratch[REDUCE : REDUCE + GATHER], last=grads.add
    )
    grads.finish()
    sender.drain()


def last_kernel(
    partial,
    grad_hidden,
    qkv,
    out,
    small,
    down,
    result,
    qkv_all,
    out_all,
    small_all,
    down_all,
    *scratch,
):
    place = Place()
    sender = Sender()
    parts = scratch[REDUCE + 1 :]
    swap_sems, halves_sems, parts = parts[:3], parts[3:4], parts[4:]
    qkv_own, qkv_other, out_own, out_other, small_own, small_other, fetch_sem, side_sem = parts
    greet_all(place)
    fetches, crossings = [], []
    for index, (grad, own, other) in enumerate(
        ((qkv, qkv_own, qkv_other), (out, out_own, out_other))
    ):
        fetches.append(
            pltpu.make_async_copy(grad.at[:, place.side], own, fetch_sem.at[index])
        )
        crossings.append(
            remote(
                grad.at[:, 1 - place.side],
                other,
                side_sem.at[0, index],
                side_sem.at[1, index],
                place.across(),
            )
        )
    crossings.append(
        remote(
            small,
            small_other,
            side_sem.at[0, 2],
            side_sem.at[1, 2],
            place.at(place.z, place.y, 1 - place.core),
        )
    )
    for copy in fetches + crossings:
        copy.start()
    pairs = ((small_own, small_all), (qkv_own, qkv_all), (out_own, out_all))
    swap = Swap(place, [whole_pair(*pair) for pair in pairs], swap_sems)
    halves = Halves(place, (down,), (down_all,), halves_sems)
    shared_rows = 2 * partial.shape[1] // place.count // 128

    def between():
        for fetch in fetches:
            fetch.wait()
        for crossing in crossings:
            crossing.wait()
        small_own[...] = small[...]
        small_own[:, :shared_rows] += small_other[:, :shared_rows]

        def one(index, carry):
            qkv_own[index] = (
                qkv_own[index].astype(F32) + qkv_other[index].astype(F32)
            ).astype(BF)
            out_own[index] = (
                out_own[index].astype(F32) + out_other[index].astype(F32)
            ).astype(BF)
            return carry

        lax.fori_loop(0, place.count, one, 0)
        swap.start()
        halves.start()

    reduce_phase(place, sender, partial, scratch[:REDUCE], between, late=swap.pass_on)
    total = scratch[4]

    def body(at):
        total[at] += grad_hidden[at]

    by_rows(total.shape[0], body)
    finish = pair_phase(place, sender, total, result, scratch[REDUCE : REDUCE + 1])
    finish()
    halves.finish()
    swap.finish()
    sender.drain()


def sum_kernel(carried, value, *rest):
    if carried:
        moved, result, arrived, core_in, y_in, held, line_in, sem, side_sem = rest
    else:
        result, core_in, y_in, held, line_in, sem = rest
    place = Place()
    z, y, core = place.z, place.y, place.core
    barrier = pltpu.get_barrier_semaphore()
    others = [place.at(z, y, 1 - core), place.at(z, 1 - y, core)]
    others += [place.at(lax.rem(z + k, LINE), y, core) for k in range(1, LINE)]
    for device in others + [place.across()] * carried:
        signal(barrier, device)
    pl.semaphore_wait(barrier, len(others) + carried)
    if carried:
        side = remote(moved, arrived, side_sem.at[0], side_sem.at[1], place.across())
        side.start()
    first = remote(value, core_in, sem.at[0, 0], sem.at[1, 0], others[0])
    first.start()
    first.wait_recv()
    held[0] = value[...] + core_in[...]
    second = remote(held.at[0], y_in, sem.at[0, 1], sem.at[1, 1], others[1])
    second.start()
    second.wait_recv()
    held[1] = held[0] + y_in[...]
    sends = [
        remote(held.at[1], line_in.at[k - 1], sem.at[0, 1 + k], sem.at[1, 1 + k], others[1 + k])
        for k in range(1, LINE)
    ]
    for send in sends:
        send.start()
    line_in[LINE - 1] = held[1]
    for send in sends:
        send.wait_recv()
    added = jnp.zeros_like(value)
    for source in range(LINE):
        slot = lax.rem(z - source + 2 * LINE - 1, LINE)
        added = added + line_in[slot]
    result[...] = added
    first.wait_send()
    second.wait_send()
    for send in sends:
        send.wait_send()
    if carried:
        side.wait()


def pack_kernel(side, gate, up, down, pair_out, down_out):
    columns = gate.shape[1]
    pair_out[0, :, :columns] = gate[...]
    pair_out[0, :, columns:] = up[...]
    down_out[0] = down[...]


def unpack_kernel(side, own, other, rest, down, gate_out, up_out, down_out):
    half, columns = own.shape[2], gate_out.shape[1]
    first = other.shape[2]
    other_start = (1 - side[0]) * half
    parts = ((own, side[0] * half), (other, other_start), (rest, other_start + first))
    for part, start in parts:
        value = jnp.sum(part[:, 0].astype(F32), axis=0)
        rows = pl.ds(pl.multiple_of(start, first), part.shape[2])
        gate_out[rows] = value[:, :columns]
        up_out[rows] = value[:, columns:]
    down_out[...] = jnp.sum(down[:, 0].astype(F32), axis=0)


def talk(kernel, which, shapes, specs, scratch, microseconds, name=None):
    def call(*operands):
        return pl.pallas_call(
            kernel,
            out_shape=shapes,
            in_specs=specs[0],
            out_specs=specs[1],
            scratch_shapes=scratch,
            compiler_params=pltpu.CompilerParams(
                collective_id=which, has_side_effects=True, vmem_limit_bytes=48 << 20
            ),
            cost_estimate=pl.CostEstimate(
                flops=0, bytes_accessed=int(microseconds * 3.0e6), transcendentals=0
            ),
            name=name or kernel.__name__,
        )(*operands)

    return call


class Team:
    def __init__(self, local_heads, rows, width):
        self.fsdp = lax.axis_size("fsdp")
        self.tensor = lax.axis_size("tensor")
        self.size = 2 * LINE
        self.teams = self.fsdp // self.size
        assert self.fsdp % self.size == 0 and self.tensor == 2 and local_heads % self.size == 0
        self.member = lax.rem(lax.axis_index("fsdp"), self.size)
        self.core = lax.axis_index("tensor")
        self.context = lax.axis_index("context")
        self.groups = None
        if self.teams > 1:
            self.groups = [
                [team * self.size + one for one in range(self.size)] for team in range(self.teams)
            ]
        self.rows = rows
        self.width = width
        self.all_low = jax.ShapeDtypeStruct((2 * self.size * rows, width), BF)
        self.own_wide = jax.ShapeDtypeStruct((rows, width), F32)
        self.line_wide = jax.ShapeDtypeStruct((1, width), F32)
        self.reduces = reduce_scratch(rows, width)
        self.gathers = gather_scratch(rows, width)

    def whole(self, pieces):
        shape = (pieces.shape[0], 2) + pieces.shape[1:]
        return jax.ShapeDtypeStruct(shape, pieces.dtype)

    def first(self, own, weights, out, small):
        rows, columns = weights[0].shape
        rows, columns = rows // 2, columns // self.size
        out_rows = out.shape[0] // self.size // 2
        return talk(
            first_kernel,
            0,
            (
                self.all_low,
                jax.ShapeDtypeStruct((self.fsdp, 2, rows, 3 * columns), BF),
                jax.ShapeDtypeStruct((self.fsdp, 2, out_rows, out.shape[1]), BF),
                jax.ShapeDtypeStruct((self.fsdp, 2) + small.shape, F32),
            ),
            ([VMEM] * 6, (HBM,) * 4),
            self.gathers + swap_scratch(self.fsdp, 5),
            80,
        )(own, *weights, out, small)

    def pack(self, gate, up, down):
        rows, columns = gate.shape
        rows, columns = rows // 2, columns // self.size
        down_rows, down_columns = down.shape
        down_rows = down_rows // self.size // 2

        def column_spec():
            return pl.BlockSpec((rows, columns), lambda d, side: (side[0], d))

        def piece_spec(*shape):
            return pl.BlockSpec((1,) + shape, lambda d, side: (d, 0, 0))

        pair, low = pl.pallas_call(
            pack_kernel,
            grid_spec=pltpu.PrefetchScalarGridSpec(
                num_scalar_prefetch=1,
                grid=(self.size,),
                in_specs=[
                    column_spec(),
                    column_spec(),
                    pl.BlockSpec((down_rows, down_columns), lambda d, side: (2 * d + side[0], 0)),
                ],
                out_specs=[piece_spec(rows, 2 * columns), piece_spec(down_rows, down_columns)],
            ),
            out_shape=[
                jax.ShapeDtypeStruct((self.size, rows, 2 * columns), BF),
                jax.ShapeDtypeStruct((self.size, down_rows, down_columns), BF),
            ],
            name="pack_kernel",
        )(self.context.reshape(1).astype(jnp.int32), gate, up, down)
        return self.repeat(pair), self.repeat(low)

    def hidden(self, partial, tokens, gain, pair, down):
        return talk(
            hidden_kernel,
            1,
            (self.all_low, self.own_wide, self.own_wide, self.whole(pair), self.whole(down)),
            ([HBM, VMEM, VMEM, VMEM, VMEM], (HBM, VMEM, VMEM, HBM, HBM)),
            self.reduces + self.gathers + halves_scratch(2),
            100,
        )(partial, tokens, gain, pair, down)

    def turn(self, partial, hidden, cotangent, gain):
        pair = jax.ShapeDtypeStruct((2 * self.rows, self.width), BF)
        return talk(
            turn_kernel,
            2,
            (self.all_low, pair, self.line_wide),
            ([HBM, VMEM, VMEM, VMEM], (HBM, HBM, VMEM)),
            self.reduces + self.gathers + [pltpu.VMEM((self.rows, self.width), BF)] + pair_scratch(),
            100,
        )(partial, hidden, cotangent, gain)

    def branch(self, partial, branch, cotangent, gain, inner, grad_mlp, hidden, grad_pair):
        team_rows, units = inner.shape
        columns = grad_pair.shape[1]
        piece = self.width // PIECES
        count = self.fsdp // PIECES
        half = self.width // self.fsdp // 2
        pair_shape = (PIECES, count, half, columns)
        down_shape = (PIECES, units // 2, piece)

        def both(shape):
            return pltpu.VMEM((shape[0], 2) + shape[1:], BF)

        def sides_inside(shape):
            return pltpu.VMEM((shape[0], shape[1], 2) + shape[2:], BF)

        gathered, grad_hidden, gain_grad, pair_mine, down_mine = talk(
            branch_kernel,
            3,
            (
                self.all_low,
                self.own_wide,
                self.line_wide,
                jax.ShapeDtypeStruct(pair_shape, BF),
                jax.ShapeDtypeStruct(down_shape, BF),
            ),
            (
                [HBM, VMEM, VMEM, VMEM, VMEM, HBM, HBM, VMEM],
                (HBM, VMEM, VMEM, VMEM, VMEM),
            ),
            self.reduces
            + self.gathers
            + [
                pltpu.VMEM((2, 2, team_rows, piece), BF),
                pltpu.VMEM((piece, team_rows), BF),
                pltpu.VMEM((units, team_rows), BF),
                sides_inside(pair_shape),
                both(down_shape),
                pltpu.VMEM(pair_shape, BF),
                pltpu.VMEM(down_shape, BF),
                DMA((2, 2)),
                DMA((2, 2, PIECES)),
            ],
            100,
        )(partial, branch, cotangent, gain, inner, grad_mlp, hidden, grad_pair)
        down_mine = down_mine.reshape(PIECES, units // 2, count, piece // count)
        return (
            gathered,
            grad_hidden,
            gain_grad,
            pair_mine.reshape(self.fsdp, half, columns),
            down_mine.transpose(0, 2, 1, 3).reshape(self.fsdp, units // 2, piece // count),
        )

    def last(self, partial, grad_hidden, qkv, out, small, down):
        both = jax.ShapeDtypeStruct((2 * self.rows, self.width), F32)

        def same(array):
            return jax.ShapeDtypeStruct(array.shape, array.dtype)

        def half(array):
            return pltpu.VMEM((array.shape[0],) + array.shape[2:], array.dtype)

        held = pltpu.VMEM(small.shape, small.dtype)
        return talk(
            last_kernel,
            4,
            (both, same(qkv), same(out), self.whole(small), self.whole(down)),
            ([HBM, VMEM, HBM, HBM, VMEM, VMEM], (HBM,) * 5),
            self.reduces
            + pair_scratch()
            + swap_scratch(self.fsdp, 3)
            + halves_scratch(1)
            + [half(qkv), half(qkv), half(out), half(out), held, held, DMA((2,)), DMA((2, 3))],
            80,
        )(partial, grad_hidden, qkv, out, small, down)

    def total(self, values, moved=None):
        flat = values.reshape(-1, 128)
        carried = int(moved is not None)
        shape = jax.ShapeDtypeStruct(flat.shape, F32)
        scratch = [pltpu.VMEM(flat.shape, F32)] * 2
        scratch += [pltpu.VMEM((2,) + flat.shape, F32), pltpu.VMEM((LINE,) + flat.shape, F32)]
        scratch += [DMA((2, LINE + 1))] + [DMA((2,))] * carried
        which = 5 + self.sums
        self.sums += 1
        kernel = functools.partial(sum_kernel, carried)
        if not carried:
            call = talk(kernel, which, shape, ([VMEM], VMEM), scratch, 10, "sum_kernel")
            return call(flat).reshape(values.shape)
        shapes = (shape, jax.ShapeDtypeStruct(moved.shape, moved.dtype))
        call = talk(kernel, which, shapes, ([VMEM] * 2, (VMEM,) * 2), scratch, 10, "sum_kernel")
        total, came = call(flat, moved)
        return total.reshape(values.shape), came

    sums = 0

    def half(self, array, axis):
        count = array.shape[axis] // 2
        return lax.dynamic_slice_in_dim(array, self.context * count, count, axis)

    def swap(self, pieces):
        return lax.all_to_all(pieces, "fsdp", split_axis=0, concat_axis=0, tiled=True)

    def repeat(self, pieces):
        return jnp.concatenate([pieces] * self.teams, axis=0) if self.teams > 1 else pieces

    def unpack(self, own, other, rest, down):
        half, columns = own.shape[1], own.shape[2] // 2
        rows, down_columns = 2 * down.shape[2], down.shape[3]

        def cut(array, *shape):
            return array.reshape((self.teams, self.size) + shape)

        def piece_spec(*shape):
            return pl.BlockSpec((self.teams, 1) + shape, lambda d, side: (0, d, 0, 0))

        wide = pl.BlockSpec((2 * half, columns), lambda d, side: (0, d))
        wide_shape = jax.ShapeDtypeStruct((2 * half, self.size * columns), F32)
        return pl.pallas_call(
            unpack_kernel,
            grid_spec=pltpu.PrefetchScalarGridSpec(
                num_scalar_prefetch=1,
                grid=(self.size,),
                in_specs=[
                    piece_spec(half, 2 * columns),
                    piece_spec(other.shape[1], 2 * columns),
                    piece_spec(rest.shape[1], 2 * columns),
                    piece_spec(rows, down_columns),
                ],
                out_specs=[wide, wide, pl.BlockSpec((rows, down_columns), lambda d, side: (d, 0))],
            ),
            out_shape=[
                wide_shape,
                wide_shape,
                jax.ShapeDtypeStruct((self.size * rows, down_columns), F32),
            ],
            name="unpack_kernel",
        )(
            self.context.reshape(1).astype(jnp.int32),
            cut(own, half, 2 * columns),
            cut(other, other.shape[1], 2 * columns),
            cut(rest, rest.shape[1], 2 * columns),
            cut(down, rows, down_columns),
        )

    def columns_whole(self, came):
        return came.reshape(-1, came.shape[-1])

    def rows_whole(self, came):
        fsdp, two, rows, columns = came.shape
        return came.transpose(1, 2, 0, 3).reshape(two * rows, fsdp * columns)

    def of_columns(self, grad):
        rows, columns = grad.shape
        return grad.astype(BF).reshape(self.fsdp, 2, rows // self.fsdp // 2, columns)

    def of_rows(self, grad):
        rows, columns = grad.shape
        cut = grad.astype(BF).reshape(2, rows // 2, self.fsdp, columns // self.fsdp)
        return cut.transpose(2, 0, 1, 3)

    def added(self, came):
        if self.teams == 1:
            return came.astype(F32)
        came = came.reshape((self.teams, self.size) + came.shape[1:])
        return jnp.sum(came.astype(F32), axis=0)

    def columns_out(self, came, count):
        size, two, rows, columns = came.shape
        return [
            self.added(part.reshape(size, two * rows, -1))
            .transpose(1, 0, 2)
            .reshape(two * rows, -1)
            for part in jnp.split(came, count, axis=3)
        ]

    def rows_out(self, came):
        return self.added(came).reshape(-1, came.shape[-1])


def local(
    tokens,
    cont_lengths,
    w_query,
    w_key,
    w_value,
    w_output,
    query_gain,
    key_gain,
    attn_gain,
    w_gate,
    w_up,
    w_down,
    mlp_gain,
    cotangent,
):
    rows = tokens.shape[0]
    width = tokens.shape[1]
    fsdp = lax.axis_size("fsdp")
    tensor = lax.axis_size("tensor")
    local_heads = query_gain.shape[0]
    head_size = w_query.shape[1] // local_heads
    own_rows = rows // tensor
    team = Team(local_heads, own_rows, width)
    groups = team.size
    team_rows = groups * rows
    heads = local_heads // team.size
    later = lax.axis_index("context") == 1

    tokens_own = lax.dynamic_slice_in_dim(tokens, team.core * own_rows, own_rows, 0)
    grad_out = lax.dynamic_slice_in_dim(cotangent, team.core * own_rows, own_rows, 0)
    cut = query_gain.size
    share = attn_gain.size
    small = [query_gain.reshape(-1), key_gain.reshape(-1), attn_gain, mlp_gain]
    small = jnp.concatenate([one.astype(F32) for one in small + [cont_lengths.reshape(-1)]])
    small = jnp.pad(small, (0, 8 * 128 - small.size)).reshape(8, 128)
    tokens_all, qkv_came, output_came, small_came = team.first(
        tokens_own, [w_query, w_key, w_value], w_output, small
    )
    qkv_w = team.columns_whole(qkv_came)
    output_w = team.rows_whole(output_came)
    all_small = small_came[:, 0].reshape(fsdp, -1)
    query_gains = all_small[:, :cut].reshape(fsdp, local_heads, -1)
    key_gains = all_small[:, cut : 2 * cut].reshape(fsdp, local_heads, -1)
    query_gains = query_gains.transpose(1, 0, 2).reshape(local_heads, head_size)
    key_gains = key_gains.transpose(1, 0, 2).reshape(local_heads, head_size)
    flat_query = lax.dynamic_slice_in_dim(query_gains, team.member * heads, heads, 0).reshape(-1)
    flat_key = lax.dynamic_slice_in_dim(key_gains, team.member * heads, heads, 0).reshape(-1)
    gain_attn = all_small[:, 2 * cut : 2 * cut + share].reshape(1, -1)
    gain_mlp = all_small[:, 2 * cut + share : 2 * cut + 2 * share].reshape(1, -1)

    conts = cont_lengths.shape[1]
    lengths = all_small[:, 2 * cut + 2 * share : 2 * cut + 2 * share + conts].astype(jnp.int32)
    first_group = lax.axis_index("fsdp") - team.member
    lengths = lax.dynamic_slice_in_dim(lengths, first_group, groups, 0)
    segment, offset = jax.vmap(lambda one: layout(one, rows))(lengths)
    row_index = jnp.arange(rows, dtype=jnp.int32)
    positions = jnp.where(later, rows + offset, row_index[None, :])
    own_segment = jnp.where(later, segment, -1)
    cosine, sine = rotary_tables(positions, head_size)
    cosine = cosine[:, :, None, :]
    sine = sine[:, :, None, :]

    pair_mine, down_mine, tokens_all = lax.optimization_barrier(
        team.pack(w_gate, w_up, w_down) + (tokens_all,)
    )
    pair_came = team.swap(pair_mine)
    down_came = team.swap(down_mine)

    by_head = (groups, rows, heads, head_size)
    raw = product(tokens_all, qkv_w)
    query_raw, key_raw, value_raw = jnp.split(raw, 3, axis=1)
    value_low = value_raw.astype(BF)
    sums, sent_value = team.total(
        jnp.stack([jnp.sum(query_raw * query_raw, axis=1), jnp.sum(key_raw * key_raw, axis=1)]),
        value_low,
    )
    value_low, sent_value = value_low.reshape(by_head), sent_value.reshape(by_head)
    scale_query = lax.rsqrt(sums[0] / width + EPS)[:, None]
    scale_key = lax.rsqrt(sums[1] / width + EPS)[:, None]
    query_norm = query_raw * scale_query * flat_query
    key_norm = key_raw * scale_key * flat_key
    query_low = rotate(query_norm.reshape(by_head), cosine, sine).astype(BF)
    key_low = rotate(key_norm.reshape(by_head), cosine, sine).astype(BF)
    sent_key = lax.ppermute(key_low, "context", [(0, 1)])
    keys_all = jnp.concatenate([sent_key, key_low], axis=1)
    values_all = jnp.concatenate([sent_value, value_low], axis=1)
    key_index = jnp.arange(2 * rows, dtype=jnp.int32)
    key_segment = jnp.concatenate([jnp.full((groups, rows), -2, jnp.int32), own_segment], axis=1)
    remote = (key_index < rows)[None, None, :] & later
    own_keys = (
        (key_index >= rows)[None, None, :]
        & (key_index[None, None, :] - rows <= row_index[None, :, None])
        & (key_segment[:, None, :] == own_segment[:, :, None])
    )
    allowed = (remote | own_keys)[:, None]
    scale = 1.0 / math.sqrt(head_size)
    scores = (
        jnp.einsum("gqhd,gkhd->ghqk", query_low, keys_all, preferred_element_type=F32) * scale
    )
    scores = jnp.where(allowed, scores, -1e30)
    highest = jnp.max(scores, axis=-1, keepdims=True)
    weights = jnp.exp(scores - highest)
    probs = weights / jnp.sum(weights, axis=-1, keepdims=True)
    probs_low = probs.astype(BF)
    mixed = jnp.einsum("ghqk,gkhd->gqhd", probs_low, values_all, preferred_element_type=F32)
    attended_low = mixed.reshape(team_rows, heads * head_size).astype(BF)
    hidden_all, attn_sum, hidden, pair_came, down_came = team.hidden(
        product(attended_low, output_w).astype(BF), tokens_own, gain_attn, pair_came, down_came
    )
    pair_w = team.columns_whole(pair_came)
    down_w = team.rows_whole(down_came)

    gate, upward = jnp.split(product(hidden_all, pair_w), 2, axis=1)
    sigma = jax.nn.sigmoid(gate)
    inner_low = (gate * sigma * upward).astype(BF)
    grad_mlp_all, outputs, grad_mlp_gain = team.turn(
        product(inner_low, down_w).astype(BF), hidden, grad_out, gain_mlp
    )
    grad_inner = product_right(grad_mlp_all, down_w)
    grad_gate_low = (grad_inner * upward * sigma * (1.0 + gate * (1.0 - sigma))).astype(BF)
    grad_up_low = (grad_inner * gate * sigma).astype(BF)
    grad_pair = jnp.concatenate([grad_gate_low, grad_up_low], axis=1)
    grad_branch_all, grad_hidden, grad_attn_gain, pair_mine, down_mine = team.branch(
        product_right(grad_pair, pair_w).astype(BF),
        attn_sum,
        grad_out,
        gain_attn,
        inner_low,
        grad_mlp_all,
        hidden_all,
        grad_pair,
    )
    pair_came = team.swap(pair_mine)
    output_grad = team.of_rows(product_left(attended_low, grad_branch_all))
    grad_attended = product_right(grad_branch_all, output_w).astype(BF).reshape(by_head)

    grad_probs = jnp.einsum("gqhd,gkhd->ghqk", grad_attended, values_all, preferred_element_type=F32)
    centre = jnp.sum(probs * grad_probs, axis=-1, keepdims=True)
    grad_scores = (probs * (grad_probs - centre)).astype(BF)
    grad_query_rot = (
        jnp.einsum("ghqk,gkhd->gqhd", grad_scores, keys_all, preferred_element_type=F32) * scale
    )
    grad_keys = (
        jnp.einsum("ghqk,gqhd->gkhd", grad_scores, query_low, preferred_element_type=F32) * scale
    )
    grad_values = jnp.einsum("ghqk,gqhd->gkhd", probs_low, grad_attended, preferred_element_type=F32)
    back_value = lax.ppermute(grad_values[:, :rows].astype(BF), "context", [(1, 0)])
    back_key = lax.ppermute(grad_keys[:, :rows].astype(BF), "context", [(1, 0)])
    grad_key_rot = grad_keys[:, rows:] + back_key.astype(F32)
    grad_value_low = (
        (grad_values[:, rows:] + back_value.astype(F32)).reshape(team_rows, -1).astype(BF)
    )
    grad_query_norm = rotate_back(grad_query_rot, cosine, sine).reshape(team_rows, -1)
    grad_key_norm = rotate_back(grad_key_rot, cosine, sine).reshape(team_rows, -1)
    grad_query_gain = jnp.sum(grad_query_norm * query_raw * scale_query, axis=0)
    grad_key_gain = jnp.sum(grad_key_norm * key_raw * scale_key, axis=0)
    inner_sums = jnp.stack(
        [
            jnp.sum(query_raw * flat_query * grad_query_norm, axis=1),
            jnp.sum(key_raw * flat_key * grad_key_norm, axis=1),
        ]
    )
    inner_sums, pair_came = lax.optimization_barrier((inner_sums, pair_came))
    first = pair_came.shape[1] // 4
    pair_rest = lax.ppermute(pair_came[:, first:], "context", [(0, 1), (1, 0)])
    totals, pair_other = team.total(inner_sums, pair_came[:, :first])
    down_mine, totals = lax.optimization_barrier((down_mine, totals))
    down_came = team.swap(down_mine)
    grad_query_low = norm_back(
        query_raw, scale_query, flat_query, grad_query_norm, totals[0][:, None], width
    ).astype(BF)
    grad_key_low = norm_back(
        key_raw, scale_key, flat_key, grad_key_norm, totals[1][:, None], width
    ).astype(BF)
    grad_qkv = jnp.concatenate([grad_query_low, grad_key_low, grad_value_low], axis=1)
    qkv_grad = team.of_columns(product_left(tokens_all, grad_qkv))
    head_share = head_size // fsdp
    small = [
        grad_attn_gain.reshape(fsdp, share),
        grad_mlp_gain.reshape(fsdp, share),
        grad_query_gain.reshape(heads, fsdp, head_share).transpose(1, 0, 2).reshape(fsdp, -1),
        grad_key_gain.reshape(heads, fsdp, head_share).transpose(1, 0, 2).reshape(fsdp, -1),
    ]
    used = 2 * share + 2 * heads * head_share
    small = jnp.concatenate(small + [jnp.zeros((fsdp, 8 * 128 - used), F32)], axis=1)
    partial, pair_rest = lax.optimization_barrier(
        (product_right(grad_qkv, qkv_w).astype(BF), pair_rest)
    )
    input_grad, qkv_came, output_came, small_came, down_came = team.last(
        partial,
        grad_hidden,
        qkv_grad,
        output_grad,
        small.reshape(fsdp, 8, 128),
        down_came,
    )
    grad_w_query, grad_w_key, grad_w_value = team.columns_out(qkv_came, 3)
    grad_w_gate, grad_w_up, grad_w_down = team.unpack(
        pair_came, pair_other, pair_rest, down_came
    )
    grad_w_output = team.rows_out(output_came)
    came = jnp.sum(small_came, axis=1).reshape(fsdp, -1)
    row_gains = jnp.sum(came[:, : 2 * share], axis=0).reshape(2, share)
    head_gains = team.added(came[:, 2 * share : used]).reshape(team.size, 2, heads, head_share)
    head_gains = head_gains.transpose(1, 0, 2, 3).reshape(2, local_heads, head_share)
    return (
        outputs,
        input_grad,
        grad_w_query,
        grad_w_key,
        grad_w_value,
        grad_w_output,
        head_gains[0],
        head_gains[1],
        row_gains[0],
        grad_w_gate,
        grad_w_up,
        grad_w_down,
        row_gains[1],
    )


def solution(mesh):
    return jax.shard_map(
        local,
        mesh=mesh,
        in_specs=(
            P(("fsdp", "context"), None),
            P("fsdp", None),
            P("fsdp", "tensor"),
            P("fsdp", "tensor"),
            P("fsdp", "tensor"),
            P("tensor", "fsdp"),
            P("tensor", "fsdp"),
            P("tensor", "fsdp"),
            P("fsdp"),
            P("fsdp", "tensor"),
            P("fsdp", "tensor"),
            P("tensor", "fsdp"),
            P("fsdp"),
            P(("fsdp", "context"), None),
        ),
        out_specs=(
            P(("fsdp", "context"), None),
            P(("fsdp", "context"), None),
            P("fsdp", "tensor"),
            P("fsdp", "tensor"),
            P("fsdp", "tensor"),
            P("tensor", "fsdp"),
            P("tensor", "fsdp"),
            P("tensor", "fsdp"),
            P("fsdp"),
            P("fsdp", "tensor"),
            P("fsdp", "tensor"),
            P("tensor", "fsdp"),
            P("fsdp"),
        ),
        check_vma=False,
    )
```

```python
import functools
import math

import jax
import jax.numpy as jnp
from jax import lax
from jax.experimental import pallas as pl
from jax.experimental.pallas import tpu as pltpu
from jax.sharding import PartitionSpec as P

EPS = 1e-06
THETA = 500000.0
BF = jnp.bfloat16
F32 = jnp.float32


def product(left, right):
    return jnp.dot(left, right, preferred_element_type=F32)


def product_left(left, right):
    return jnp.einsum("rd,rf->df", left, right, preferred_element_type=F32)


def product_right(left, right):
    return jnp.einsum("rf,df->rd", left, right, preferred_element_type=F32)


def rotary_tables(positions, head_size):
    half = head_size // 2
    inverse = jnp.exp(-(2.0 * jnp.arange(half, dtype=F32) / head_size) * math.log(THETA))
    angles = positions.astype(F32)[..., None] * inverse
    angles = jnp.concatenate([angles, angles], axis=-1)
    return (jnp.cos(angles), jnp.sin(angles))


def rotate(values, cosine, sine):
    half = values.shape[-1] // 2
    turned = jnp.concatenate([-values[..., half:], values[..., :half]], axis=-1)
    return values * cosine + turned * sine


def rotate_back(grads, cosine, sine):
    half = grads.shape[-1] // 2
    scaled = grads * sine
    turned = jnp.concatenate([scaled[..., half:], -scaled[..., :half]], axis=-1)
    return grads * cosine + turned


def norm_back(values, scale, gain, grads, total, width):
    return scale * gain * grads - values * scale * scale * scale * (total / width)


def layout(lengths, rows):
    segment_ends = jnp.cumsum(lengths)
    segment_starts = segment_ends - lengths
    row_index = jnp.arange(rows, dtype=jnp.int32)
    segment = jnp.sum((row_index[:, None] >= segment_ends[None, :]).astype(jnp.int32), axis=1)
    chosen = segment[:, None] == jnp.arange(lengths.shape[0], dtype=jnp.int32)[None, :]
    offset = row_index - jnp.sum(jnp.where(chosen, segment_starts[None, :], 0), axis=1)
    return (segment, offset)


LINE = 4
CHUNK = 16
FEW = 8
MESH_ID = pl.DeviceIdType.MESH
HBM = pl.BlockSpec(memory_space=pl.ANY)
VMEM = pl.BlockSpec(memory_space=pltpu.VMEM)
DMA = pltpu.SemaphoreType.DMA


class Place:
    def __init__(self):
        device = lax.axis_index("fsdp")
        member = lax.rem(device, 2 * LINE)
        self.base = device - member
        self.z = member // 2
        self.y = lax.rem(member, 2)
        self.core = lax.axis_index("tensor")
        self.side = lax.axis_index("context")
        self.device = device
        self.count = lax.axis_size("fsdp")

    def across(self):
        return {"context": 1 - self.side}

    def at(self, z, y, core):
        return {"fsdp": self.base + 2 * z + y, "tensor": core}

    def near(self):
        yield None, self.at(self.z, self.y, 1 - self.core)
        yield None, self.at(self.z, 1 - self.y, self.core)
        yield self.z > 0, self.at(self.z - 1, self.y, self.core)
        yield self.z < LINE - 1, self.at(self.z + 1, self.y, self.core)

    def rows(self, z, y, core, count):
        start = ((2 * z + y) * 2 + core) * count
        return pl.ds(pl.multiple_of(start, count), count)


def guarded(condition, action):
    if condition is None:
        action()
    else:
        pl.when(condition)(action)


def signal(barrier, device):
    pl.semaphore_signal(barrier, inc=1, device_id=device, device_id_type=MESH_ID)


def greet(place, across=False):
    barrier = pltpu.get_barrier_semaphore()
    for condition, device in place.near():
        guarded(condition, functools.partial(signal, barrier, device))
    if across:
        signal(barrier, place.across())
    inside = (place.z > 0) & (place.z < LINE - 1)
    pl.semaphore_wait(barrier, jnp.where(inside, 4, 3) + int(across))


def greet_all(place):
    barrier = pltpu.get_barrier_semaphore()

    def one(step, carry):
        signal(barrier, {"fsdp": lax.rem(place.device + step, place.count)})
        return carry

    lax.fori_loop(1, place.count, one, 0)
    signal(barrier, place.across())
    signal(barrier, place.at(place.z, place.y, 1 - place.core))
    pl.semaphore_wait(barrier, place.count + 1)


class Sender:
    def __init__(self):
        self.sent = []

    def __call__(self, condition, make):
        def start():
            make().start()

        guarded(condition, start)
        self.sent.append((condition, make))

    def drain(self):
        for condition, make in self.sent:

            def wait(make=make):
                make().wait_send()

            guarded(condition, wait)


def remote(source, target, send, receive, device):
    return pltpu.make_async_remote_copy(
        src_ref=source,
        dst_ref=target,
        send_sem=send,
        recv_sem=receive,
        device_id=device,
        device_id_type=MESH_ID,
    )


def by_rows(rows, body, first=0):
    def step(index, carry):
        body(pl.ds(pl.multiple_of(index * CHUNK, CHUNK), CHUNK))
        return carry

    lax.fori_loop(first // CHUNK, rows // CHUNK, step, 0)


def reduce_scratch(rows, width):
    return [
        pltpu.VMEM((2 * LINE, rows, width), BF),
        pltpu.VMEM((2 * LINE, rows, width), BF),
        pltpu.VMEM((LINE, rows, width), BF),
        pltpu.VMEM((LINE + 1, rows, width), BF),
        pltpu.VMEM((rows, width), F32),
        DMA((2 * LINE,)),
        DMA((2, 2 * LINE)),
        DMA((2, LINE)),
        DMA((2, LINE + 1)),
        pltpu.VMEM((LINE + 1, rows // FEW, width), BF),
        DMA((2, LINE + 1)),
    ]


def reduce_phase(place, sender, partial, scratch, between=None, idle=None, late=None):
    mine, core_in, y_in, line_in, total, local_sem, core_sem, y_sem, line_sem = scratch[:9]
    few_in, few_sem = scratch[9:]
    rows = total.shape[0]
    few = rows // FEW
    z, y, core = place.z, place.y, place.core
    low = z < LINE // 2
    order = []
    for k in range(LINE - 1):
        down = LINE - 1 - k
        down = jnp.where(down <= z, down - 1, down)
        up = jnp.where(k >= z, k + 1, k)
        order.append(jnp.where(low, down, up))
    order.append(z)

    def fetch(slot):
        half = lax.rem(slot, 2)
        return pltpu.make_async_copy(
            partial.at[place.rows(slot // 2, half, core, rows)], mine.at[slot], local_sem.at[slot]
        )

    def to_core(slot):
        half = lax.rem(slot, 2)
        return remote(
            partial.at[place.rows(slot // 2, half, 1 - core, rows)],
            core_in.at[slot],
            core_sem.at[0, slot],
            core_sem.at[1, slot],
            place.at(z, y, 1 - core),
        )

    def to_y(block, first):
        at = pl.ds(first, rows - first)
        return remote(
            mine.at[2 * block + 1 - y, at],
            y_in.at[block, at],
            y_sem.at[0, block],
            y_sem.at[1, block],
            place.at(z, 1 - y, core),
        )

    def few_along(block):
        step = jnp.where(block > z, 1, -1)
        slot = jnp.where((step < 0) & (block == z - 1), LINE, block)
        return remote(
            mine.at[2 * block + 1 - y, pl.ds(0, few)],
            few_in.at[slot],
            few_sem.at[0, block],
            few_sem.at[1, slot],
            place.at(z + step, y, core),
        )

    def add_few(slot, source):
        remote(
            mine.at[0, pl.ds(0, few)],
            few_in.at[source],
            few_sem.at[0, 0],
            few_sem.at[1, source],
            place.at(z, y, 1 - core),
        ).wait_recv()

        def add(at):
            value = mine[slot, at].astype(F32) + few_in[source, at].astype(F32)
            mine[slot, at] = value.astype(BF)

        by_rows(few, add)

    def to_line(block):
        step = jnp.where(block > z, 1, -1)
        slot = jnp.where((step < 0) & (block == z - 1), LINE, block)
        return remote(
            mine.at[2 * block + y],
            line_in.at[slot],
            line_sem.at[0, block],
            line_sem.at[1, slot],
            place.at(z + step, y, core),
        )

    def from_line(slot):
        return remote(
            mine.at[0],
            line_in.at[slot],
            line_sem.at[0, 0],
            line_sem.at[1, slot],
            place.at(z, y, 1 - core),
        )

    for half in (1 - y, y):
        for block in order:
            sender(None, functools.partial(to_core, 2 * block + half))
            fetch(2 * block + half).start()

    for number, block in enumerate(order):
        slot = 2 * block + 1 - y
        fetch(slot).wait()
        to_core(slot).wait_recv()

        def add(at, slot=slot):
            value = mine[slot, at].astype(F32) + core_in[slot, at].astype(F32)
            mine[slot, at] = value.astype(BF)

        by_rows(rows, add)
        if number == LINE - 1:
            pl.when(z > 0)(functools.partial(add_few, slot, z))
            pl.when(z < LINE - 1)(functools.partial(add_few, slot, LINE))
            sender(None, functools.partial(to_y, block, 0))
        else:
            sender(None, functools.partial(to_y, block, few))
            inner = jnp.where(block > z, z > 0, z < LINE - 1)
            pl.when(inner)(functools.partial(add_few, slot, block))
            sender(None, functools.partial(few_along, block))

    for number, block in enumerate(order[:-1]):
        if number == LINE - 2 and between is not None:
            between()
        if number < 2 and idle is not None:
            idle(number)
        slot = 2 * block + y
        fetch(slot).wait()
        to_core(slot).wait_recv()
        to_y(block, few).wait_recv()
        inner = jnp.where(block > z, z > 0, z < LINE - 1)

        @pl.when(inner)
        def _(block=block, slot=slot):
            from_line(block).wait_recv()

            def add_first(at):
                value = mine[slot, at].astype(F32) + core_in[slot, at].astype(F32)
                mine[slot, at] = (value + line_in[block, at].astype(F32)).astype(BF)

            def add(at):
                value = mine[slot, at].astype(F32) + core_in[slot, at].astype(F32)
                value = value + y_in[block, at].astype(F32)
                mine[slot, at] = (value + line_in[block, at].astype(F32)).astype(BF)

            by_rows(few, add_first)
            by_rows(rows, add, few)

        @pl.when(jnp.logical_not(inner))
        def _(block=block, slot=slot):
            def add_first(at):
                value = mine[slot, at].astype(F32) + core_in[slot, at].astype(F32)
                mine[slot, at] = value.astype(BF)

            def add(at):
                value = mine[slot, at].astype(F32) + core_in[slot, at].astype(F32)
                mine[slot, at] = (value + y_in[block, at].astype(F32)).astype(BF)

            by_rows(few, add_first)
            by_rows(rows, add, few)

        sender(None, functools.partial(to_line, block))

    if late is not None:
        late()
    slot = 2 * z + y
    fetch(slot).wait()
    to_core(slot).wait_recv()
    to_y(z, 0).wait_recv()

    def start(at):
        value = mine[slot, at].astype(F32) + core_in[slot, at].astype(F32)
        total[at] = value + y_in[z, at].astype(F32)

    by_rows(rows, start)
    for condition, source in ((z > 0, z), (z < LINE - 1, LINE)):

        @pl.when(condition)
        def _(source=source):
            from_line(source).wait_recv()

            def add(at):
                total[at] += line_in[source, at].astype(F32)

            by_rows(rows, add)


def gather_scratch(rows, width):
    return [
        pltpu.VMEM((rows, width), BF),
        DMA((1,)),
        DMA((2, 2 * LINE)),
        DMA((2, LINE)),
        DMA((2, LINE + 2)),
        DMA((2, LINE + 2)),
    ]


def gather_phase(place, sender, gathered, scratch, between=None, later=None, last=None):
    own, local_sem, core_sem, y_sem, line_sem, few_sem = scratch
    rows = own.shape[0]
    few = rows // FEW
    z, y, core = place.z, place.y, place.core

    def spot(block, half):
        return gathered.at[place.rows(block, half, core, rows)]

    def to_core(source, block, half):
        return remote(
            source,
            spot(block, half),
            core_sem.at[0, 2 * block + half],
            core_sem.at[1, 2 * block + half],
            place.at(z, y, 1 - core),
        )

    def to_y(source, block):
        return remote(
            source,
            spot(block, y),
            y_sem.at[0, block],
            y_sem.at[1, block],
            place.at(z, 1 - y, core),
        )

    def to_line(source, block, step, index):
        return remote(
            source,
            spot(block, y),
            line_sem.at[0, index],
            line_sem.at[1, block],
            place.at(z + step, y, core),
        )

    def some(block, half, first, count):
        start = ((2 * block + half) * 2 + core) * rows + first
        return gathered.at[pl.ds(pl.multiple_of(start, few), count)]

    def rest_to_y(half, block):
        return remote(
            some(block, half, few, rows - few),
            some(block, half, few, rows - few),
            y_sem.at[0, block],
            y_sem.at[1, block],
            place.at(z, 1 - y, core),
        )

    def few_along(block, step, index):
        return remote(
            some(block, 1 - y, 0, few),
            some(block, 1 - y, 0, few),
            few_sem.at[0, index],
            few_sem.at[1, block],
            place.at(z + step, y, core),
        )

    keep = pltpu.make_async_copy(own, spot(z, y), local_sem.at[0])
    keep.start()
    sender(z < LINE - 1, functools.partial(to_line, own, z, 1, LINE))
    sender(z > 0, functools.partial(to_line, own, z, -1, LINE + 1))
    sender(None, functools.partial(to_y, own, z))
    sender(None, functools.partial(to_core, own, z, y))
    if between is not None:
        between()

    def took_y(block):
        remote(
            own,
            spot(block, 1 - y),
            y_sem.at[0, block],
            y_sem.at[1, block],
            place.at(z, 1 - y, core),
        ).wait_recv()

    def across_own():
        took_y(z)
        sender(z < LINE - 1, functools.partial(few_along, z, 1, LINE))
        sender(z > 0, functools.partial(few_along, z, -1, LINE + 1))
        sender(None, lambda: to_core(spot(z, 1 - y), z, 1 - y))

    def across(condition, block, step):
        guarded(condition, lambda: few_along(block, step, block).wait_recv())
        onward = condition & ((z < LINE - 1) if step > 0 else (z > 0))
        sender(onward, functools.partial(few_along, block, step, block))
        guarded(condition, lambda: rest_to_y(1 - y, block).wait_recv())
        sender(condition, lambda: to_core(spot(block, 1 - y), block, 1 - y))

    def along(condition, block, step):
        def took():
            to_line(own, block, step, block).wait_recv()

        guarded(condition, took)
        onward = condition & ((z < LINE - 1) if step > 0 else (z > 0))
        sender(onward, lambda: to_line(spot(block, y), block, step, block))
        sender(condition, lambda: rest_to_y(y, block))
        sender(condition, lambda: to_core(spot(block, y), block, y))

    for distance in range(1, LINE + 1):
        if distance < LINE:
            along(z >= distance, z - distance, 1)
            along(z + distance < LINE, z + distance, -1)
        if distance == 1:
            across_own()
        else:
            across(z >= distance - 1, z - distance + 1, 1)
            across(z + distance - 1 < LINE, z + distance - 1, -1)
        if distance == 1 and later is not None:
            later()
        if distance == LINE - 1 and last is not None:
            last()

    keep.wait()
    for block in range(LINE):
        for half in range(2):
            remote(
                own,
                gathered.at[place.rows(block, half, 1 - core, rows)],
                core_sem.at[0, 2 * block + half],
                core_sem.at[1, 2 * block + half],
                place.at(z, y, 1 - core),
            ).wait_recv()


def pair_scratch():
    return [DMA((3,))]


def pair_phase(place, sender, own, pair, scratch):
    (sem,) = scratch
    rows = own.shape[0]
    spot = pair.at[pl.ds(pl.multiple_of(place.core * rows, rows), rows)]
    keep = pltpu.make_async_copy(own, spot, sem.at[0])
    keep.start()

    def send():
        return remote(
            own, spot, sem.at[1], sem.at[2], place.at(place.z, place.y, 1 - place.core)
        )

    sender(None, send)

    def finish():
        keep.wait()
        other = pair.at[pl.ds(pl.multiple_of((1 - place.core) * rows, rows), rows)]
        remote(
            own, other, sem.at[1], sem.at[2], place.at(place.z, place.y, 1 - place.core)
        ).wait_recv()

    return finish


def swap_scratch(count, arrays):
    return [DMA((arrays,)), DMA((2, arrays, count)), DMA((2, arrays, count))]


class Swap:
    def __init__(self, place, pairs, scratch):
        self.place = place
        self.pairs = pairs
        self.local_sem, self.out_sem, self.side_sem = scratch

    def send(self, index, step):
        place = self.place
        source, spot = self.pairs[index]
        target = lax.rem(place.device + step, place.count)
        return remote(
            source(target),
            spot(place.device, place.side),
            self.out_sem.at[0, index, step],
            self.out_sem.at[1, index, step],
            {"fsdp": target},
        )

    def taken(self, index, step, side):
        device = lax.rem(self.place.device + self.place.count - step, self.place.count)
        return self.pairs[index][1](device, side)

    def come(self, index, step):
        place = self.place
        return remote(
            self.pairs[index][0](place.device),
            self.taken(index, step, place.side),
            self.out_sem.at[0, index, step],
            self.out_sem.at[1, index, step],
            place.across(),
        )

    def share(self, index, step, source=None):
        spot = self.taken(index, step, self.place.side)
        return remote(
            spot if source is None else source,
            spot,
            self.side_sem.at[0, index, step],
            self.side_sem.at[1, index, step],
            self.place.across(),
        )

    def shared(self, index, step):
        spot = self.taken(index, step, 1 - self.place.side)
        return remote(
            spot,
            spot,
            self.side_sem.at[0, index, step],
            self.side_sem.at[1, index, step],
            self.place.across(),
        )

    def keep(self, index):
        place = self.place
        source, spot = self.pairs[index]
        return pltpu.make_async_copy(
            source(place.device), spot(place.device, place.side), self.local_sem.at[index]
        )

    def each(self, first, body):
        def step(number, carry):
            for index in range(len(self.pairs)):
                body(index, number)
            return carry

        lax.fori_loop(first, self.place.count, step, 0)

    def start(self):
        self.each(1, lambda index, step: self.send(index, step).start())
        for index, (source, _) in enumerate(self.pairs):
            self.keep(index).start()
            self.share(index, 0, source(self.place.device)).start()

    def pass_on(self):
        def one(index, step):
            self.come(index, step).wait_recv()
            self.share(index, step).start()

        self.each(1, one)

    def finish(self):
        for index in range(len(self.pairs)):
            self.keep(index).wait()
        self.each(0, lambda index, step: self.shared(index, step).wait_recv())
        self.each(1, lambda index, step: self.send(index, step).wait_send())
        self.each(0, lambda index, step: self.share(index, step).wait_send())


def whole_pair(pieces, whole):
    return (lambda target: pieces.at[target], lambda device, side: whole.at[device, side])


def halves_scratch(arrays):
    return [DMA((3, arrays))]


class Halves:
    def __init__(self, place, halves, wholes, scratch):
        self.place = place
        self.pairs = list(zip(halves, wholes))
        (self.sem,) = scratch

    def keep(self, index):
        half, whole = self.pairs[index]
        return pltpu.make_async_copy(half, whole.at[:, self.place.side], self.sem.at[0, index])

    def copy(self, index, side):
        half, whole = self.pairs[index]
        return remote(
            half,
            whole.at[:, side],
            self.sem.at[1, index],
            self.sem.at[2, index],
            self.place.across(),
        )

    def start(self):
        for index in range(len(self.pairs)):
            self.copy(index, self.place.side).start()
            self.keep(index).start()

    def finish(self):
        for index in range(len(self.pairs)):
            self.keep(index).wait()
            self.copy(index, 1 - self.place.side).wait_recv()
            self.copy(index, self.place.side).wait_send()


REDUCE = 11
GATHER = 6
PIECES = 8


def first_kernel(
    own_ref, query, key, value, out, small, gathered, qkv_all, out_all, small_all, *scratch
):
    place = Place()
    sender = Sender()
    own = scratch[0]
    own[...] = own_ref[...]
    greet_all(place)
    half, columns = qkv_all.shape[2], qkv_all.shape[3] // 3
    out_half = out_all.shape[2]
    rows = pl.ds(pl.multiple_of(place.side * half, half), half)

    def member(target):
        return lax.rem(target, 2 * LINE)

    def column_pair(weight, index):
        def source(target):
            start = pl.multiple_of(member(target) * columns, columns)
            return weight.at[rows, pl.ds(start, columns)]

        def spot(device, side):
            return qkv_all.at[device, side, :, pl.ds(index * columns, columns)]

        return (source, spot)

    def out_source(target):
        start = (2 * member(target) + place.side) * out_half
        return out.at[pl.ds(pl.multiple_of(start, out_half), out_half)]

    pairs = [
        (lambda target: small, lambda device, side: small_all.at[device, side]),
        column_pair(query, 0),
        column_pair(key, 1),
        column_pair(value, 2),
        (out_source, lambda device, side: out_all.at[device, side]),
    ]
    swap = Swap(place, pairs, scratch[GATHER:])
    gather_phase(place, sender, gathered, scratch[:GATHER], swap.start, swap.pass_on)
    swap.finish()
    sender.drain()


def hidden_kernel(
    partial, tokens, gain, pair, down, gathered, branch, hidden, pair_all, down_all, *scratch
):
    place = Place()
    sender = Sender()
    greet(place, True)
    halves = Halves(place, (pair, down), (pair_all, down_all), scratch[REDUCE + GATHER :])
    halves.start()
    reduce_phase(place, sender, partial, scratch[:REDUCE])
    total, own = scratch[4], scratch[REDUCE]
    rows, width = total.shape

    def body(at):
        value = total[at]
        scale = lax.rsqrt(jnp.sum(value * value, axis=1, keepdims=True) / width + EPS)
        result = tokens[at].astype(F32) + value * scale * gain[...]
        branch[at] = value
        hidden[at] = result
        own[at] = result.astype(BF)

    by_rows(rows, body)
    gather_phase(place, sender, gathered, scratch[REDUCE : REDUCE + GATHER])
    halves.finish()
    sender.drain()


def turn_kernel(partial, hidden, cotangent, gain, gathered, outputs, gain_grad, *scratch):
    place = Place()
    sender = Sender()
    greet(place)
    reduce_phase(place, sender, partial, scratch[:REDUCE])
    total, own = scratch[4], scratch[REDUCE]
    out_own = scratch[REDUCE + GATHER]
    rows, width = total.shape
    gain_grad[...] = jnp.zeros_like(gain_grad)

    def body(at):
        value = total[at]
        scale = lax.rsqrt(jnp.sum(value * value, axis=1, keepdims=True) / width + EPS)
        grads = cotangent[at].astype(F32)
        normed = value * scale
        out_own[at] = (hidden[at] + normed * gain[...]).astype(BF)
        gain_grad[...] += jnp.sum(grads * normed, axis=0, keepdims=True)
        gained = gain[...] * grads
        inner = jnp.sum(normed * gained, axis=1, keepdims=True)
        own[at] = (scale * (gained - normed * (inner / width))).astype(BF)

    by_rows(rows, body)
    finish = pair_phase(place, sender, out_own, outputs, scratch[REDUCE + GATHER + 1 :])
    gather_phase(place, sender, gathered, scratch[REDUCE : REDUCE + GATHER])
    finish()
    sender.drain()


class WeightGrads:
    def __init__(self, place, arrays, outs, scratch):
        self.place = place
        self.inner, self.grad_mlp, self.hidden, self.grad_pair = arrays
        self.outs = outs
        self.tall, self.turned, self.inner_turned = scratch[:3]
        self.fulls, self.others = scratch[3:5], scratch[5:7]
        self.fetch_sem, self.side_sem = scratch[7:]
        self.piece = self.tall.shape[3]

    def fetch(self, number, slot):
        columns = pl.ds(pl.multiple_of(number * self.piece, self.piece), self.piece)
        return [
            pltpu.make_async_copy(
                array.at[:, columns], self.tall.at[slot, index], self.fetch_sem.at[slot, index]
            )
            for index, array in enumerate((self.hidden, self.grad_mlp))
        ]

    def side_of(self, index, number, side):
        if index == 0:
            return self.fulls[0].at[number, :, side]
        return self.fulls[1].at[number, side]

    def crossing(self, number, index):
        return remote(
            self.side_of(index, number, 1 - self.place.side),
            self.others[index].at[number],
            self.side_sem.at[0, index, number],
            self.side_sem.at[1, index, number],
            self.place.across(),
        )

    def start(self):
        for copy in self.fetch(0, 0):
            copy.start()
        self.inner_turned[...] = self.inner[...].T

    def one(self, number, carry):
        slot = lax.rem(number, 2)
        for copy in self.fetch(number, slot):
            copy.wait()

        @pl.when(number < PIECES - 1)
        def _():
            for copy in self.fetch(number + 1, 1 - slot):
                copy.start()

        full, low = self.fulls
        self.turned[...] = self.tall[slot, 0].T
        columns = self.grad_pair.shape[1]
        step = columns // 4

        def columns_step(index, carry):
            at = pl.ds(pl.multiple_of(index * step, step), step)
            value = product(self.turned[...], self.grad_pair[:, at]).astype(BF)
            full[number, :, :, :, at] = value.reshape(full.shape[1:4] + (step,))
            return carry

        lax.fori_loop(0, 4, columns_step, 0)
        value = product(self.inner_turned[...], self.tall[slot, 1]).astype(BF)
        low[number] = value.reshape(low.shape[1:])
        for index in range(2):
            self.crossing(number, index).start()
        return carry

    def some(self, which):
        half = PIECES // 2
        lax.fori_loop(which * half, which * half + half, self.one, 0)

    def add(self):
        def step(number, carry):
            for index in range(2):
                self.crossing(number, index).wait_recv()
                own = self.side_of(index, number, self.place.side)[...].astype(F32)
                other = self.others[index][number].astype(F32)
                self.outs[index][number] = (own + other).astype(BF)
            return carry

        lax.fori_loop(0, PIECES, step, 0)

    def finish(self):
        def step(number, carry):
            for index in range(2):
                self.crossing(number, index).wait_send()
            return carry

        lax.fori_loop(0, PIECES, step, 0)


def branch_kernel(
    partial,
    branch,
    cotangent,
    gain,
    inner_low,
    grad_mlp,
    hidden_low,
    grad_pair,
    gathered,
    grad_hidden,
    gain_grad,
    pair_mine,
    down_mine,
    *scratch,
):
    place = Place()
    sender = Sender()
    greet(place, True)
    grads = WeightGrads(
        place,
        (inner_low, grad_mlp, hidden_low, grad_pair),
        (pair_mine, down_mine),
        scratch[REDUCE + GATHER :],
    )
    grads.start()
    reduce_phase(place, sender, partial, scratch[:REDUCE], idle=grads.some)
    total, own = scratch[4], scratch[REDUCE]
    rows, width = total.shape
    gain_grad[...] = jnp.zeros_like(gain_grad)

    def body(at):
        value = branch[at]
        scale = lax.rsqrt(jnp.sum(value * value, axis=1, keepdims=True) / width + EPS)
        grads = cotangent[at].astype(F32) + total[at]
        grad_hidden[at] = grads
        normed = value * scale
        gain_grad[...] += jnp.sum(grads * normed, axis=0, keepdims=True)
        gained = gain[...] * grads
        inner = jnp.sum(normed * gained, axis=1, keepdims=True)
        own[at] = (scale * (gained - normed * (inner / width))).astype(BF)

    by_rows(rows, body)
    gather_phase(
        place, sender, gathered, scratch[REDUCE : REDUCE + GATHER], last=grads.add
    )
    grads.finish()
    sender.drain()


def last_kernel(
    partial,
    grad_hidden,
    qkv,
    out,
    small,
    down,
    result,
    qkv_all,
    out_all,
    small_all,
    down_all,
    *scratch,
):
    place = Place()
    sender = Sender()
    parts = scratch[REDUCE + 1 :]
    swap_sems, halves_sems, parts = parts[:3], parts[3:4], parts[4:]
    qkv_own, qkv_other, out_own, out_other, small_own, small_other, fetch_sem, side_sem = parts
    greet_all(place)
    fetches, crossings = [], []
    for index, (grad, own, other) in enumerate(
        ((qkv, qkv_own, qkv_other), (out, out_own, out_other))
    ):
        fetches.append(
            pltpu.make_async_copy(grad.at[:, place.side], own, fetch_sem.at[index])
        )
        crossings.append(
            remote(
                grad.at[:, 1 - place.side],
                other,
                side_sem.at[0, index],
                side_sem.at[1, index],
                place.across(),
            )
        )
    crossings.append(
        remote(
            small,
            small_other,
            side_sem.at[0, 2],
            side_sem.at[1, 2],
            place.at(place.z, place.y, 1 - place.core),
        )
    )
    for copy in fetches + crossings:
        copy.start()
    pairs = ((small_own, small_all), (qkv_own, qkv_all), (out_own, out_all))
    swap = Swap(place, [whole_pair(*pair) for pair in pairs], swap_sems)
    halves = Halves(place, (down,), (down_all,), halves_sems)
    shared_rows = 2 * partial.shape[1] // place.count // 128

    def between():
        for fetch in fetches:
            fetch.wait()
        for crossing in crossings:
            crossing.wait()
        small_own[...] = small[...]
        small_own[:, :shared_rows] += small_other[:, :shared_rows]

        def one(index, carry):
            qkv_own[index] = (
                qkv_own[index].astype(F32) + qkv_other[index].astype(F32)
            ).astype(BF)
            out_own[index] = (
                out_own[index].astype(F32) + out_other[index].astype(F32)
            ).astype(BF)
            return carry

        lax.fori_loop(0, place.count, one, 0)
        swap.start()
        halves.start()

    reduce_phase(place, sender, partial, scratch[:REDUCE], between, late=swap.pass_on)
    total = scratch[4]

    def body(at):
        total[at] += grad_hidden[at]

    by_rows(total.shape[0], body)
    finish = pair_phase(place, sender, total, result, scratch[REDUCE : REDUCE + 1])
    finish()
    halves.finish()
    swap.finish()
    sender.drain()


def sum_kernel(carried, value, *rest):
    if carried:
        moved, result, arrived, core_in, y_in, held, line_in, sem, side_sem = rest
    else:
        result, core_in, y_in, held, line_in, sem = rest
    place = Place()
    z, y, core = place.z, place.y, place.core
    barrier = pltpu.get_barrier_semaphore()
    others = [place.at(z, y, 1 - core), place.at(z, 1 - y, core)]
    others += [place.at(lax.rem(z + k, LINE), y, core) for k in range(1, LINE)]
    for device in others + [place.across()] * carried:
        signal(barrier, device)
    pl.semaphore_wait(barrier, len(others) + carried)
    if carried:
        side = remote(moved, arrived, side_sem.at[0], side_sem.at[1], place.across())
        side.start()
    first = remote(value, core_in, sem.at[0, 0], sem.at[1, 0], others[0])
    first.start()
    first.wait_recv()
    held[0] = value[...] + core_in[...]
    second = remote(held.at[0], y_in, sem.at[0, 1], sem.at[1, 1], others[1])
    second.start()
    second.wait_recv()
    held[1] = held[0] + y_in[...]
    sends = [
        remote(held.at[1], line_in.at[k - 1], sem.at[0, 1 + k], sem.at[1, 1 + k], others[1 + k])
        for k in range(1, LINE)
    ]
    for send in sends:
        send.start()
    line_in[LINE - 1] = held[1]
    for send in sends:
        send.wait_recv()
    added = jnp.zeros_like(value)
    for source in range(LINE):
        slot = lax.rem(z - source + 2 * LINE - 1, LINE)
        added = added + line_in[slot]
    result[...] = added
    first.wait_send()
    second.wait_send()
    for send in sends:
        send.wait_send()
    if carried:
        side.wait()


def pack_kernel(side, gate, up, down, pair_out, down_out):
    columns = gate.shape[1]
    pair_out[0, :, :columns] = gate[...]
    pair_out[0, :, columns:] = up[...]
    down_out[0] = down[...]


def unpack_kernel(side, own, other, rest, down, gate_out, up_out, down_out):
    half, columns = own.shape[2], gate_out.shape[1]
    first = other.shape[2]
    other_start = (1 - side[0]) * half
    parts = ((own, side[0] * half), (other, other_start), (rest, other_start + first))
    for part, start in parts:
        value = jnp.sum(part[:, 0].astype(F32), axis=0)
        rows = pl.ds(pl.multiple_of(start, first), part.shape[2])
        gate_out[rows] = value[:, :columns]
        up_out[rows] = value[:, columns:]
    down_out[...] = jnp.sum(down[:, 0].astype(F32), axis=0)


def talk(kernel, which, shapes, specs, scratch, microseconds, name=None):
    def call(*operands):
        return pl.pallas_call(
            kernel,
            out_shape=shapes,
            in_specs=specs[0],
            out_specs=specs[1],
            scratch_shapes=scratch,
            compiler_params=pltpu.CompilerParams(
                collective_id=which, has_side_effects=True, vmem_limit_bytes=48 << 20
            ),
            cost_estimate=pl.CostEstimate(
                flops=0, bytes_accessed=int(microseconds * 3.0e6), transcendentals=0
            ),
            name=name or kernel.__name__,
        )(*operands)

    return call


class Team:
    def __init__(self, local_heads, rows, width):
        self.fsdp = lax.axis_size("fsdp")
        self.tensor = lax.axis_size("tensor")
        self.size = 2 * LINE
        self.teams = self.fsdp // self.size
        assert self.fsdp % self.size == 0 and self.tensor == 2 and local_heads % self.size == 0
        self.member = lax.rem(lax.axis_index("fsdp"), self.size)
        self.core = lax.axis_index("tensor")
        self.context = lax.axis_index("context")
        self.groups = None
        if self.teams > 1:
            self.groups = [
                [team * self.size + one for one in range(self.size)] for team in range(self.teams)
            ]
        self.rows = rows
        self.width = width
        self.all_low = jax.ShapeDtypeStruct((2 * self.size * rows, width), BF)
        self.own_wide = jax.ShapeDtypeStruct((rows, width), F32)
        self.line_wide = jax.ShapeDtypeStruct((1, width), F32)
        self.reduces = reduce_scratch(rows, width)
        self.gathers = gather_scratch(rows, width)

    def whole(self, pieces):
        shape = (pieces.shape[0], 2) + pieces.shape[1:]
        return jax.ShapeDtypeStruct(shape, pieces.dtype)

    def first(self, own, weights, out, small):
        rows, columns = weights[0].shape
        rows, columns = rows // 2, columns // self.size
        out_rows = out.shape[0] // self.size // 2
        return talk(
            first_kernel,
            0,
            (
                self.all_low,
                jax.ShapeDtypeStruct((self.fsdp, 2, rows, 3 * columns), BF),
                jax.ShapeDtypeStruct((self.fsdp, 2, out_rows, out.shape[1]), BF),
                jax.ShapeDtypeStruct((self.fsdp, 2) + small.shape, F32),
            ),
            ([VMEM] * 6, (HBM,) * 4),
            self.gathers + swap_scratch(self.fsdp, 5),
            80,
        )(own, *weights, out, small)

    def pack(self, gate, up, down):
        rows, columns = gate.shape
        rows, columns = rows // 2, columns // self.size
        down_rows, down_columns = down.shape
        down_rows = down_rows // self.size // 2

        def column_spec():
            return pl.BlockSpec((rows, columns), lambda d, side: (side[0], d))

        def piece_spec(*shape):
            return pl.BlockSpec((1,) + shape, lambda d, side: (d, 0, 0))

        pair, low = pl.pallas_call(
            pack_kernel,
            grid_spec=pltpu.PrefetchScalarGridSpec(
                num_scalar_prefetch=1,
                grid=(self.size,),
                in_specs=[
                    column_spec(),
                    column_spec(),
                    pl.BlockSpec((down_rows, down_columns), lambda d, side: (2 * d + side[0], 0)),
                ],
                out_specs=[piece_spec(rows, 2 * columns), piece_spec(down_rows, down_columns)],
            ),
            out_shape=[
                jax.ShapeDtypeStruct((self.size, rows, 2 * columns), BF),
                jax.ShapeDtypeStruct((self.size, down_rows, down_columns), BF),
            ],
            name="pack_kernel",
        )(self.context.reshape(1).astype(jnp.int32), gate, up, down)
        return self.repeat(pair), self.repeat(low)

    def hidden(self, partial, tokens, gain, pair, down):
        return talk(
            hidden_kernel,
            1,
            (self.all_low, self.own_wide, self.own_wide, self.whole(pair), self.whole(down)),
            ([HBM, VMEM, VMEM, VMEM, VMEM], (HBM, VMEM, VMEM, HBM, HBM)),
            self.reduces + self.gathers + halves_scratch(2),
            100,
        )(partial, tokens, gain, pair, down)

    def turn(self, partial, hidden, cotangent, gain):
        pair = jax.ShapeDtypeStruct((2 * self.rows, self.width), BF)
        return talk(
            turn_kernel,
            2,
            (self.all_low, pair, self.line_wide),
            ([HBM, VMEM, VMEM, VMEM], (HBM, HBM, VMEM)),
            self.reduces + self.gathers + [pltpu.VMEM((self.rows, self.width), BF)] + pair_scratch(),
            100,
        )(partial, hidden, cotangent, gain)

    def branch(self, partial, branch, cotangent, gain, inner, grad_mlp, hidden, grad_pair):
        team_rows, units = inner.shape
        columns = grad_pair.shape[1]
        piece = self.width // PIECES
        count = self.fsdp // PIECES
        half = self.width // self.fsdp // 2
        pair_shape = (PIECES, count, half, columns)
        down_shape = (PIECES, units // 2, piece)

        def both(shape):
            return pltpu.VMEM((shape[0], 2) + shape[1:], BF)

        def sides_inside(shape):
            return pltpu.VMEM((shape[0], shape[1], 2) + shape[2:], BF)

        gathered, grad_hidden, gain_grad, pair_mine, down_mine = talk(
            branch_kernel,
            3,
            (
                self.all_low,
                self.own_wide,
                self.line_wide,
                jax.ShapeDtypeStruct(pair_shape, BF),
                jax.ShapeDtypeStruct(down_shape, BF),
            ),
            (
                [HBM, VMEM, VMEM, VMEM, VMEM, HBM, HBM, VMEM],
                (HBM, VMEM, VMEM, VMEM, VMEM),
            ),
            self.reduces
            + self.gathers
            + [
                pltpu.VMEM((2, 2, team_rows, piece), BF),
                pltpu.VMEM((piece, team_rows), BF),
                pltpu.VMEM((units, team_rows), BF),
                sides_inside(pair_shape),
                both(down_shape),
                pltpu.VMEM(pair_shape, BF),
                pltpu.VMEM(down_shape, BF),
                DMA((2, 2)),
                DMA((2, 2, PIECES)),
            ],
            100,
        )(partial, branch, cotangent, gain, inner, grad_mlp, hidden, grad_pair)
        down_mine = down_mine.reshape(PIECES, units // 2, count, piece // count)
        return (
            gathered,
            grad_hidden,
            gain_grad,
            pair_mine.reshape(self.fsdp, half, columns),
            down_mine.transpose(0, 2, 1, 3).reshape(self.fsdp, units // 2, piece // count),
        )

    def last(self, partial, grad_hidden, qkv, out, small, down):
        both = jax.ShapeDtypeStruct((2 * self.rows, self.width), F32)

        def same(array):
            return jax.ShapeDtypeStruct(array.shape, array.dtype)

        def half(array):
            return pltpu.VMEM((array.shape[0],) + array.shape[2:], array.dtype)

        held = pltpu.VMEM(small.shape, small.dtype)
        return talk(
            last_kernel,
            4,
            (both, same(qkv), same(out), self.whole(small), self.whole(down)),
            ([HBM, VMEM, HBM, HBM, VMEM, VMEM], (HBM,) * 5),
            self.reduces
            + pair_scratch()
            + swap_scratch(self.fsdp, 3)
            + halves_scratch(1)
            + [half(qkv), half(qkv), half(out), half(out), held, held, DMA((2,)), DMA((2, 3))],
            80,
        )(partial, grad_hidden, qkv, out, small, down)

    def total(self, values, moved=None):
        flat = values.reshape(-1, 128)
        carried = int(moved is not None)
        shape = jax.ShapeDtypeStruct(flat.shape, F32)
        scratch = [pltpu.VMEM(flat.shape, F32)] * 2
        scratch += [pltpu.VMEM((2,) + flat.shape, F32), pltpu.VMEM((LINE,) + flat.shape, F32)]
        scratch += [DMA((2, LINE + 1))] + [DMA((2,))] * carried
        which = 5 + self.sums
        self.sums += 1
        kernel = functools.partial(sum_kernel, carried)
        if not carried:
            call = talk(kernel, which, shape, ([VMEM], VMEM), scratch, 10, "sum_kernel")
            return call(flat).reshape(values.shape)
        shapes = (shape, jax.ShapeDtypeStruct(moved.shape, moved.dtype))
        call = talk(kernel, which, shapes, ([VMEM] * 2, (VMEM,) * 2), scratch, 10, "sum_kernel")
        total, came = call(flat, moved)
        return total.reshape(values.shape), came

    sums = 0

    def half(self, array, axis):
        count = array.shape[axis] // 2
        return lax.dynamic_slice_in_dim(array, self.context * count, count, axis)

    def swap(self, pieces):
        return lax.all_to_all(pieces, "fsdp", split_axis=0, concat_axis=0, tiled=True)

    def repeat(self, pieces):
        return jnp.concatenate([pieces] * self.teams, axis=0) if self.teams > 1 else pieces

    def unpack(self, own, other, rest, down):
        half, columns = own.shape[1], own.shape[2] // 2
        rows, down_columns = 2 * down.shape[2], down.shape[3]

        def cut(array, *shape):
            return array.reshape((self.teams, self.size) + shape)

        def piece_spec(*shape):
            return pl.BlockSpec((self.teams, 1) + shape, lambda d, side: (0, d, 0, 0))

        wide = pl.BlockSpec((2 * half, columns), lambda d, side: (0, d))
        wide_shape = jax.ShapeDtypeStruct((2 * half, self.size * columns), F32)
        return pl.pallas_call(
            unpack_kernel,
            grid_spec=pltpu.PrefetchScalarGridSpec(
                num_scalar_prefetch=1,
                grid=(self.size,),
                in_specs=[
                    piece_spec(half, 2 * columns),
                    piece_spec(other.shape[1], 2 * columns),
                    piece_spec(rest.shape[1], 2 * columns),
                    piece_spec(rows, down_columns),
                ],
                out_specs=[wide, wide, pl.BlockSpec((rows, down_columns), lambda d, side: (d, 0))],
            ),
            out_shape=[
                wide_shape,
                wide_shape,
                jax.ShapeDtypeStruct((self.size * rows, down_columns), F32),
            ],
            name="unpack_kernel",
        )(
            self.context.reshape(1).astype(jnp.int32),
            cut(own, half, 2 * columns),
            cut(other, other.shape[1], 2 * columns),
            cut(rest, rest.shape[1], 2 * columns),
            cut(down, rows, down_columns),
        )

    def columns_whole(self, came):
        return came.reshape(-1, came.shape[-1])

    def rows_whole(self, came):
        fsdp, two, rows, columns = came.shape
        return came.transpose(1, 2, 0, 3).reshape(two * rows, fsdp * columns)

    def of_columns(self, grad):
        rows, columns = grad.shape
        return grad.astype(BF).reshape(self.fsdp, 2, rows // self.fsdp // 2, columns)

    def of_rows(self, grad):
        rows, columns = grad.shape
        cut = grad.astype(BF).reshape(2, rows // 2, self.fsdp, columns // self.fsdp)
        return cut.transpose(2, 0, 1, 3)

    def added(self, came):
        if self.teams == 1:
            return came.astype(F32)
        came = came.reshape((self.teams, self.size) + came.shape[1:])
        return jnp.sum(came.astype(F32), axis=0)

    def columns_out(self, came, count):
        size, two, rows, columns = came.shape
        return [
            self.added(part.reshape(size, two * rows, -1))
            .transpose(1, 0, 2)
            .reshape(two * rows, -1)
            for part in jnp.split(came, count, axis=3)
        ]

    def rows_out(self, came):
        return self.added(came).reshape(-1, came.shape[-1])


def local(
    tokens,
    cont_lengths,
    w_query,
    w_key,
    w_value,
    w_output,
    query_gain,
    key_gain,
    attn_gain,
    w_gate,
    w_up,
    w_down,
    mlp_gain,
    cotangent,
):
    rows = tokens.shape[0]
    width = tokens.shape[1]
    fsdp = lax.axis_size("fsdp")
    tensor = lax.axis_size("tensor")
    local_heads = query_gain.shape[0]
    head_size = w_query.shape[1] // local_heads
    own_rows = rows // tensor
    team = Team(local_heads, own_rows, width)
    groups = team.size
    team_rows = groups * rows
    heads = local_heads // team.size
    later = lax.axis_index("context") == 1

    tokens_own = lax.dynamic_slice_in_dim(tokens, team.core * own_rows, own_rows, 0)
    grad_out = lax.dynamic_slice_in_dim(cotangent, team.core * own_rows, own_rows, 0)
    cut = query_gain.size
    share = attn_gain.size
    small = [query_gain.reshape(-1), key_gain.reshape(-1), attn_gain, mlp_gain]
    small = jnp.concatenate([one.astype(F32) for one in small + [cont_lengths.reshape(-1)]])
    small = jnp.pad(small, (0, 8 * 128 - small.size)).reshape(8, 128)
    tokens_all, qkv_came, output_came, small_came = team.first(
        tokens_own, [w_query, w_key, w_value], w_output, small
    )
    qkv_w = team.columns_whole(qkv_came)
    output_w = team.rows_whole(output_came)
    all_small = small_came[:, 0].reshape(fsdp, -1)
    query_gains = all_small[:, :cut].reshape(fsdp, local_heads, -1)
    key_gains = all_small[:, cut : 2 * cut].reshape(fsdp, local_heads, -1)
    query_gains = query_gains.transpose(1, 0, 2).reshape(local_heads, head_size)
    key_gains = key_gains.transpose(1, 0, 2).reshape(local_heads, head_size)
    flat_query = lax.dynamic_slice_in_dim(query_gains, team.member * heads, heads, 0).reshape(-1)
    flat_key = lax.dynamic_slice_in_dim(key_gains, team.member * heads, heads, 0).reshape(-1)
    gain_attn = all_small[:, 2 * cut : 2 * cut + share].reshape(1, -1)
    gain_mlp = all_small[:, 2 * cut + share : 2 * cut + 2 * share].reshape(1, -1)

    conts = cont_lengths.shape[1]
    lengths = all_small[:, 2 * cut + 2 * share : 2 * cut + 2 * share + conts].astype(jnp.int32)
    first_group = lax.axis_index("fsdp") - team.member
    lengths = lax.dynamic_slice_in_dim(lengths, first_group, groups, 0)
    segment, offset = jax.vmap(lambda one: layout(one, rows))(lengths)
    row_index = jnp.arange(rows, dtype=jnp.int32)
    positions = jnp.where(later, rows + offset, row_index[None, :])
    own_segment = jnp.where(later, segment, -1)
    cosine, sine = rotary_tables(positions, head_size)
    cosine = cosine[:, :, None, :]
    sine = sine[:, :, None, :]

    pair_mine, down_mine, tokens_all = lax.optimization_barrier(
        team.pack(w_gate, w_up, w_down) + (tokens_all,)
    )
    pair_came = team.swap(pair_mine)
    down_came = team.swap(down_mine)

    by_head = (groups, rows, heads, head_size)
    raw = product(tokens_all, qkv_w)
    query_raw, key_raw, value_raw = jnp.split(raw, 3, axis=1)
    value_low = value_raw.astype(BF)
    sums, sent_value = team.total(
        jnp.stack([jnp.sum(query_raw * query_raw, axis=1), jnp.sum(key_raw * key_raw, axis=1)]),
        value_low,
    )
    value_low, sent_value = value_low.reshape(by_head), sent_value.reshape(by_head)
    scale_query = lax.rsqrt(sums[0] / width + EPS)[:, None]
    scale_key = lax.rsqrt(sums[1] / width + EPS)[:, None]
    query_norm = query_raw * scale_query * flat_query
    key_norm = key_raw * scale_key * flat_key
    query_low = rotate(query_norm.reshape(by_head), cosine, sine).astype(BF)
    key_low = rotate(key_norm.reshape(by_head), cosine, sine).astype(BF)
    sent_key = lax.ppermute(key_low, "context", [(0, 1)])
    keys_all = jnp.concatenate([sent_key, key_low], axis=1)
    values_all = jnp.concatenate([sent_value, value_low], axis=1)
    key_index = jnp.arange(2 * rows, dtype=jnp.int32)
    key_segment = jnp.concatenate([jnp.full((groups, rows), -2, jnp.int32), own_segment], axis=1)
    remote = (key_index < rows)[None, None, :] & later
    own_keys = (
        (key_index >= rows)[None, None, :]
        & (key_index[None, None, :] - rows <= row_index[None, :, None])
        & (key_segment[:, None, :] == own_segment[:, :, None])
    )
    allowed = (remote | own_keys)[:, None]
    scale = 1.0 / math.sqrt(head_size)
    scores = (
        jnp.einsum("gqhd,gkhd->ghqk", query_low, keys_all, preferred_element_type=F32) * scale
    )
    scores = jnp.where(allowed, scores, -1e30)
    highest = jnp.max(scores, axis=-1, keepdims=True)
    weights = jnp.exp(scores - highest)
    probs = weights / jnp.sum(weights, axis=-1, keepdims=True)
    probs_low = probs.astype(BF)
    mixed = jnp.einsum("ghqk,gkhd->gqhd", probs_low, values_all, preferred_element_type=F32)
    attended_low = mixed.reshape(team_rows, heads * head_size).astype(BF)
    hidden_all, attn_sum, hidden, pair_came, down_came = team.hidden(
        product(attended_low, output_w).astype(BF), tokens_own, gain_attn, pair_came, down_came
    )
    pair_w = team.columns_whole(pair_came)
    down_w = team.rows_whole(down_came)

    gate, upward = jnp.split(product(hidden_all, pair_w), 2, axis=1)
    sigma = jax.nn.sigmoid(gate)
    inner_low = (gate * sigma * upward).astype(BF)
    grad_mlp_all, outputs, grad_mlp_gain = team.turn(
        product(inner_low, down_w).astype(BF), hidden, grad_out, gain_mlp
    )
    grad_inner = product_right(grad_mlp_all, down_w)
    grad_gate_low = (grad_inner * upward * sigma * (1.0 + gate * (1.0 - sigma))).astype(BF)
    grad_up_low = (grad_inner * gate * sigma).astype(BF)
    grad_pair = jnp.concatenate([grad_gate_low, grad_up_low], axis=1)
    grad_branch_all, grad_hidden, grad_attn_gain, pair_mine, down_mine = team.branch(
        product_right(grad_pair, pair_w).astype(BF),
        attn_sum,
        grad_out,
        gain_attn,
        inner_low,
        grad_mlp_all,
        hidden_all,
        grad_pair,
    )
    pair_came = team.swap(pair_mine)
    output_grad = team.of_rows(product_left(attended_low, grad_branch_all))
    grad_attended = product_right(grad_branch_all, output_w).astype(BF).reshape(by_head)

    grad_probs = jnp.einsum("gqhd,gkhd->ghqk", grad_attended, values_all, preferred_element_type=F32)
    centre = jnp.sum(probs * grad_probs, axis=-1, keepdims=True)
    grad_scores = (probs * (grad_probs - centre)).astype(BF)
    grad_query_rot = (
        jnp.einsum("ghqk,gkhd->gqhd", grad_scores, keys_all, preferred_element_type=F32) * scale
    )
    grad_keys = (
        jnp.einsum("ghqk,gqhd->gkhd", grad_scores, query_low, preferred_element_type=F32) * scale
    )
    grad_values = jnp.einsum("ghqk,gqhd->gkhd", probs_low, grad_attended, preferred_element_type=F32)
    back_value = lax.ppermute(grad_values[:, :rows].astype(BF), "context", [(1, 0)])
    back_key = lax.ppermute(grad_keys[:, :rows].astype(BF), "context", [(1, 0)])
    grad_key_rot = grad_keys[:, rows:] + back_key.astype(F32)
    grad_value_low = (
        (grad_values[:, rows:] + back_value.astype(F32)).reshape(team_rows, -1).astype(BF)
    )
    grad_query_norm = rotate_back(grad_query_rot, cosine, sine).reshape(team_rows, -1)
    grad_key_norm = rotate_back(grad_key_rot, cosine, sine).reshape(team_rows, -1)
    grad_query_gain = jnp.sum(grad_query_norm * query_raw * scale_query, axis=0)
    grad_key_gain = jnp.sum(grad_key_norm * key_raw * scale_key, axis=0)
    inner_sums = jnp.stack(
        [
            jnp.sum(query_raw * flat_query * grad_query_norm, axis=1),
            jnp.sum(key_raw * flat_key * grad_key_norm, axis=1),
        ]
    )
    inner_sums, pair_came = lax.optimization_barrier((inner_sums, pair_came))
    first = pair_came.shape[1] // 4
    pair_rest = lax.ppermute(pair_came[:, first:], "context", [(0, 1), (1, 0)])
    totals, pair_other = team.total(inner_sums, pair_came[:, :first])
    down_mine, totals = lax.optimization_barrier((down_mine, totals))
    down_came = team.swap(down_mine)
    grad_query_low = norm_back(
        query_raw, scale_query, flat_query, grad_query_norm, totals[0][:, None], width
    ).astype(BF)
    grad_key_low = norm_back(
        key_raw, scale_key, flat_key, grad_key_norm, totals[1][:, None], width
    ).astype(BF)
    grad_qkv = jnp.concatenate([grad_query_low, grad_key_low, grad_value_low], axis=1)
    qkv_grad = team.of_columns(product_left(tokens_all, grad_qkv))
    head_share = head_size // fsdp
    small = [
        grad_attn_gain.reshape(fsdp, share),
        grad_mlp_gain.reshape(fsdp, share),
        grad_query_gain.reshape(heads, fsdp, head_share).transpose(1, 0, 2).reshape(fsdp, -1),
        grad_key_gain.reshape(heads, fsdp, head_share).transpose(1, 0, 2).reshape(fsdp, -1),
    ]
    used = 2 * share + 2 * heads * head_share
    small = jnp.concatenate(small + [jnp.zeros((fsdp, 8 * 128 - used), F32)], axis=1)
    partial, pair_rest = lax.optimization_barrier(
        (product_right(grad_qkv, qkv_w).astype(BF), pair_rest)
    )
    input_grad, qkv_came, output_came, small_came, down_came = team.last(
        partial,
        grad_hidden,
        qkv_grad,
        output_grad,
        small.reshape(fsdp, 8, 128),
        down_came,
    )
    grad_w_query, grad_w_key, grad_w_value = team.columns_out(qkv_came, 3)
    grad_w_gate, grad_w_up, grad_w_down = team.unpack(
        pair_came, pair_other, pair_rest, down_came
    )
    grad_w_output = team.rows_out(output_came)
    came = jnp.sum(small_came, axis=1).reshape(fsdp, -1)
    row_gains = jnp.sum(came[:, : 2 * share], axis=0).reshape(2, share)
    head_gains = team.added(came[:, 2 * share : used]).reshape(team.size, 2, heads, head_share)
    head_gains = head_gains.transpose(1, 0, 2, 3).reshape(2, local_heads, head_share)
    return (
        outputs,
        input_grad,
        grad_w_query,
        grad_w_key,
        grad_w_value,
        grad_w_output,
        head_gains[0],
        head_gains[1],
        row_gains[0],
        grad_w_gate,
        grad_w_up,
        grad_w_down,
        row_gains[1],
    )


def solution(mesh):
    return jax.shard_map(
        local,
        mesh=mesh,
        in_specs=(
            P(("fsdp", "context"), None),
            P("fsdp", None),
            P("fsdp", "tensor"),
            P("fsdp", "tensor"),
            P("fsdp", "tensor"),
            P("tensor", "fsdp"),
            P("tensor", "fsdp"),
            P("tensor", "fsdp"),
            P("fsdp"),
            P("fsdp", "tensor"),
            P("fsdp", "tensor"),
            P("tensor", "fsdp"),
            P("fsdp"),
            P(("fsdp", "context"), None),
        ),
        out_specs=(
            P(("fsdp", "context"), None),
            P(("fsdp", "context"), None),
            P("fsdp", "tensor"),
            P("fsdp", "tensor"),
            P("fsdp", "tensor"),
            P("tensor", "fsdp"),
            P("tensor", "fsdp"),
            P("tensor", "fsdp"),
            P("fsdp"),
            P("fsdp", "tensor"),
            P("fsdp", "tensor"),
            P("tensor", "fsdp"),
            P("fsdp"),
        ),
        check_vma=False,
    )
```

```python
import functools
import math

import jax
import jax.numpy as jnp
from jax import lax
from jax.experimental import pallas as pl
from jax.experimental.pallas import tpu as pltpu
from jax.sharding import PartitionSpec as P

EPS = 1e-06
THETA = 500000.0
BF = jnp.bfloat16
F32 = jnp.float32


def product(left, right):
    return jnp.dot(left, right, preferred_element_type=F32)


def product_left(left, right):
    return jnp.einsum("rd,rf->df", left, right, preferred_element_type=F32)


def product_right(left, right):
    return jnp.einsum("rf,df->rd", left, right, preferred_element_type=F32)


def rotary_tables(positions, head_size):
    half = head_size // 2
    inverse = jnp.exp(-(2.0 * jnp.arange(half, dtype=F32) / head_size) * math.log(THETA))
    angles = positions.astype(F32)[..., None] * inverse
    angles = jnp.concatenate([angles, angles], axis=-1)
    return (jnp.cos(angles), jnp.sin(angles))


def rotate(values, cosine, sine):
    half = values.shape[-1] // 2
    turned = jnp.concatenate([-values[..., half:], values[..., :half]], axis=-1)
    return values * cosine + turned * sine


def rotate_back(grads, cosine, sine):
    half = grads.shape[-1] // 2
    scaled = grads * sine
    turned = jnp.concatenate([scaled[..., half:], -scaled[..., :half]], axis=-1)
    return grads * cosine + turned


def norm_back(values, scale, gain, grads, total, width):
    return scale * gain * grads - values * scale * scale * scale * (total / width)


def layout(lengths, rows):
    segment_ends = jnp.cumsum(lengths)
    segment_starts = segment_ends - lengths
    row_index = jnp.arange(rows, dtype=jnp.int32)
    segment = jnp.sum((row_index[:, None] >= segment_ends[None, :]).astype(jnp.int32), axis=1)
    chosen = segment[:, None] == jnp.arange(lengths.shape[0], dtype=jnp.int32)[None, :]
    offset = row_index - jnp.sum(jnp.where(chosen, segment_starts[None, :], 0), axis=1)
    return (segment, offset)


LINE = 4
CHUNK = 16
FEW = 8
MESH_ID = pl.DeviceIdType.MESH
HBM = pl.BlockSpec(memory_space=pl.ANY)
VMEM = pl.BlockSpec(memory_space=pltpu.VMEM)
DMA = pltpu.SemaphoreType.DMA


class Place:
    def __init__(self):
        device = lax.axis_index("fsdp")
        member = lax.rem(device, 2 * LINE)
        self.base = device - member
        self.z = member // 2
        self.y = lax.rem(member, 2)
        self.core = lax.axis_index("tensor")
        self.side = lax.axis_index("context")
        self.device = device
        self.count = lax.axis_size("fsdp")

    def across(self):
        return {"context": 1 - self.side}

    def at(self, z, y, core):
        return {"fsdp": self.base + 2 * z + y, "tensor": core}

    def near(self):
        yield None, self.at(self.z, self.y, 1 - self.core)
        yield None, self.at(self.z, 1 - self.y, self.core)
        yield self.z > 0, self.at(self.z - 1, self.y, self.core)
        yield self.z < LINE - 1, self.at(self.z + 1, self.y, self.core)

    def rows(self, z, y, core, count):
        start = ((2 * z + y) * 2 + core) * count
        return pl.ds(pl.multiple_of(start, count), count)


def guarded(condition, action):
    if condition is None:
        action()
    else:
        pl.when(condition)(action)


def signal(barrier, device):
    pl.semaphore_signal(barrier, inc=1, device_id=device, device_id_type=MESH_ID)


def greet(place, across=False):
    barrier = pltpu.get_barrier_semaphore()
    for condition, device in place.near():
        guarded(condition, functools.partial(signal, barrier, device))
    if across:
        signal(barrier, place.across())
    inside = (place.z > 0) & (place.z < LINE - 1)
    pl.semaphore_wait(barrier, jnp.where(inside, 4, 3) + int(across))


def greet_all(place):
    barrier = pltpu.get_barrier_semaphore()

    def one(step, carry):
        signal(barrier, {"fsdp": lax.rem(place.device + step, place.count)})
        return carry

    lax.fori_loop(1, place.count, one, 0)
    signal(barrier, place.across())
    signal(barrier, place.at(place.z, place.y, 1 - place.core))
    pl.semaphore_wait(barrier, place.count + 1)


class Sender:
    def __init__(self):
        self.sent = []

    def __call__(self, condition, make):
        def start():
            make().start()

        guarded(condition, start)
        self.sent.append((condition, make))

    def drain(self):
        for condition, make in self.sent:

            def wait(make=make):
                make().wait_send()

            guarded(condition, wait)


def remote(source, target, send, receive, device):
    return pltpu.make_async_remote_copy(
        src_ref=source,
        dst_ref=target,
        send_sem=send,
        recv_sem=receive,
        device_id=device,
        device_id_type=MESH_ID,
    )


def by_rows(rows, body, first=0):
    def step(index, carry):
        body(pl.ds(pl.multiple_of(index * CHUNK, CHUNK), CHUNK))
        return carry

    lax.fori_loop(first // CHUNK, rows // CHUNK, step, 0)


def reduce_scratch(rows, width):
    return [
        pltpu.VMEM((2 * LINE, rows, width), BF),
        pltpu.VMEM((2 * LINE, rows, width), BF),
        pltpu.VMEM((LINE, rows, width), BF),
        pltpu.VMEM((LINE + 1, rows, width), BF),
        pltpu.VMEM((rows, width), F32),
        DMA((2 * LINE,)),
        DMA((2, 2 * LINE)),
        DMA((2, LINE)),
        DMA((2, LINE + 1)),
        pltpu.VMEM((LINE + 1, rows // FEW, width), BF),
        DMA((2, LINE + 1)),
    ]


def reduce_phase(place, sender, partial, scratch, between=None, idle=None, late=None):
    mine, core_in, y_in, line_in, total, local_sem, core_sem, y_sem, line_sem = scratch[:9]
    few_in, few_sem = scratch[9:]
    rows = total.shape[0]
    few = rows // FEW
    z, y, core = place.z, place.y, place.core
    low = z < LINE // 2
    order = []
    for k in range(LINE - 1):
        down = LINE - 1 - k
        down = jnp.where(down <= z, down - 1, down)
        up = jnp.where(k >= z, k + 1, k)
        order.append(jnp.where(low, down, up))
    order.append(z)

    def fetch(slot):
        half = lax.rem(slot, 2)
        return pltpu.make_async_copy(
            partial.at[place.rows(slot // 2, half, core, rows)], mine.at[slot], local_sem.at[slot]
        )

    def to_core(slot):
        half = lax.rem(slot, 2)
        return remote(
            partial.at[place.rows(slot // 2, half, 1 - core, rows)],
            core_in.at[slot],
            core_sem.at[0, slot],
            core_sem.at[1, slot],
            place.at(z, y, 1 - core),
        )

    def to_y(block, first):
        at = pl.ds(first, rows - first)
        return remote(
            mine.at[2 * block + 1 - y, at],
            y_in.at[block, at],
            y_sem.at[0, block],
            y_sem.at[1, block],
            place.at(z, 1 - y, core),
        )

    def few_along(block):
        step = jnp.where(block > z, 1, -1)
        slot = jnp.where((step < 0) & (block == z - 1), LINE, block)
        return remote(
            mine.at[2 * block + 1 - y, pl.ds(0, few)],
            few_in.at[slot],
            few_sem.at[0, block],
            few_sem.at[1, slot],
            place.at(z + step, y, core),
        )

    def add_few(slot, source):
        remote(
            mine.at[0, pl.ds(0, few)],
            few_in.at[source],
            few_sem.at[0, 0],
            few_sem.at[1, source],
            place.at(z, y, 1 - core),
        ).wait_recv()

        def add(at):
            value = mine[slot, at].astype(F32) + few_in[source, at].astype(F32)
            mine[slot, at] = value.astype(BF)

        by_rows(few, add)

    def to_line(block):
        step = jnp.where(block > z, 1, -1)
        slot = jnp.where((step < 0) & (block == z - 1), LINE, block)
        return remote(
            mine.at[2 * block + y],
            line_in.at[slot],
            line_sem.at[0, block],
            line_sem.at[1, slot],
            place.at(z + step, y, core),
        )

    def from_line(slot):
        return remote(
            mine.at[0],
            line_in.at[slot],
            line_sem.at[0, 0],
            line_sem.at[1, slot],
            place.at(z, y, 1 - core),
        )

    for half in (1 - y, y):
        for block in order:
            sender(None, functools.partial(to_core, 2 * block + half))
            fetch(2 * block + half).start()

    for number, block in enumerate(order):
        slot = 2 * block + 1 - y
        fetch(slot).wait()
        to_core(slot).wait_recv()

        def add(at, slot=slot):
            value = mine[slot, at].astype(F32) + core_in[slot, at].astype(F32)
            mine[slot, at] = value.astype(BF)

        by_rows(rows, add)
        if number == LINE - 1:
            pl.when(z > 0)(functools.partial(add_few, slot, z))
            pl.when(z < LINE - 1)(functools.partial(add_few, slot, LINE))
            sender(None, functools.partial(to_y, block, 0))
        else:
            sender(None, functools.partial(to_y, block, few))
            inner = jnp.where(block > z, z > 0, z < LINE - 1)
            pl.when(inner)(functools.partial(add_few, slot, block))
            sender(None, functools.partial(few_along, block))

    for number, block in enumerate(order[:-1]):
        if number == LINE - 2 and between is not None:
            between()
        if number < 2 and idle is not None:
            idle(number)
        slot = 2 * block + y
        fetch(slot).wait()
        to_core(slot).wait_recv()
        to_y(block, few).wait_recv()
        inner = jnp.where(block > z, z > 0, z < LINE - 1)

        @pl.when(inner)
        def _(block=block, slot=slot):
            from_line(block).wait_recv()

            def add_first(at):
                value = mine[slot, at].astype(F32) + core_in[slot, at].astype(F32)
                mine[slot, at] = (value + line_in[block, at].astype(F32)).astype(BF)

            def add(at):
                value = mine[slot, at].astype(F32) + core_in[slot, at].astype(F32)
                value = value + y_in[block, at].astype(F32)
                mine[slot, at] = (value + line_in[block, at].astype(F32)).astype(BF)

            by_rows(few, add_first)
            by_rows(rows, add, few)

        @pl.when(jnp.logical_not(inner))
        def _(block=block, slot=slot):
            def add_first(at):
                value = mine[slot, at].astype(F32) + core_in[slot, at].astype(F32)
                mine[slot, at] = value.astype(BF)

            def add(at):
                value = mine[slot, at].astype(F32) + core_in[slot, at].astype(F32)
                mine[slot, at] = (value + y_in[block, at].astype(F32)).astype(BF)

            by_rows(few, add_first)
            by_rows(rows, add, few)

        sender(None, functools.partial(to_line, block))

    if late is not None:
        late()
    slot = 2 * z + y
    fetch(slot).wait()
    to_core(slot).wait_recv()
    to_y(z, 0).wait_recv()

    def start(at):
        value = mine[slot, at].astype(F32) + core_in[slot, at].astype(F32)
        total[at] = value + y_in[z, at].astype(F32)

    by_rows(rows, start)
    for condition, source in ((z > 0, z), (z < LINE - 1, LINE)):

        @pl.when(condition)
        def _(source=source):
            from_line(source).wait_recv()

            def add(at):
                total[at] += line_in[source, at].astype(F32)

            by_rows(rows, add)


def gather_scratch(rows, width):
    return [
        pltpu.VMEM((rows, width), BF),
        DMA((1,)),
        DMA((2, 2 * LINE)),
        DMA((2, LINE)),
        DMA((2, LINE + 2)),
        DMA((2, LINE + 2)),
    ]


def gather_phase(place, sender, gathered, scratch, between=None, later=None, last=None):
    own, local_sem, core_sem, y_sem, line_sem, few_sem = scratch
    rows = own.shape[0]
    few = rows // FEW
    z, y, core = place.z, place.y, place.core

    def spot(block, half):
        return gathered.at[place.rows(block, half, core, rows)]

    def to_core(source, block, half):
        return remote(
            source,
            spot(block, half),
            core_sem.at[0, 2 * block + half],
            core_sem.at[1, 2 * block + half],
            place.at(z, y, 1 - core),
        )

    def to_y(source, block):
        return remote(
            source,
            spot(block, y),
            y_sem.at[0, block],
            y_sem.at[1, block],
            place.at(z, 1 - y, core),
        )

    def to_line(source, block, step, index):
        return remote(
            source,
            spot(block, y),
            line_sem.at[0, index],
            line_sem.at[1, block],
            place.at(z + step, y, core),
        )

    def some(block, half, first, count):
        start = ((2 * block + half) * 2 + core) * rows + first
        return gathered.at[pl.ds(pl.multiple_of(start, few), count)]

    def rest_to_y(half, block):
        return remote(
            some(block, half, few, rows - few),
            some(block, half, few, rows - few),
            y_sem.at[0, block],
            y_sem.at[1, block],
            place.at(z, 1 - y, core),
        )

    def few_along(block, step, index):
        return remote(
            some(block, 1 - y, 0, few),
            some(block, 1 - y, 0, few),
            few_sem.at[0, index],
            few_sem.at[1, block],
            place.at(z + step, y, core),
        )

    keep = pltpu.make_async_copy(own, spot(z, y), local_sem.at[0])
    keep.start()
    sender(z < LINE - 1, functools.partial(to_line, own, z, 1, LINE))
    sender(z > 0, functools.partial(to_line, own, z, -1, LINE + 1))
    sender(None, functools.partial(to_y, own, z))
    sender(None, functools.partial(to_core, own, z, y))
    if between is not None:
        between()

    def took_y(block):
        remote(
            own,
            spot(block, 1 - y),
            y_sem.at[0, block],
            y_sem.at[1, block],
            place.at(z, 1 - y, core),
        ).wait_recv()

    def across_own():
        took_y(z)
        sender(z < LINE - 1, functools.partial(few_along, z, 1, LINE))
        sender(z > 0, functools.partial(few_along, z, -1, LINE + 1))
        sender(None, lambda: to_core(spot(z, 1 - y), z, 1 - y))

    def across(condition, block, step):
        guarded(condition, lambda: few_along(block, step, block).wait_recv())
        onward = condition & ((z < LINE - 1) if step > 0 else (z > 0))
        sender(onward, functools.partial(few_along, block, step, block))
        guarded(condition, lambda: rest_to_y(1 - y, block).wait_recv())
        sender(condition, lambda: to_core(spot(block, 1 - y), block, 1 - y))

    def along(condition, block, step):
        def took():
            to_line(own, block, step, block).wait_recv()

        guarded(condition, took)
        onward = condition & ((z < LINE - 1) if step > 0 else (z > 0))
        sender(onward, lambda: to_line(spot(block, y), block, step, block))
        sender(condition, lambda: rest_to_y(y, block))
        sender(condition, lambda: to_core(spot(block, y), block, y))

    for distance in range(1, LINE + 1):
        if distance < LINE:
            along(z >= distance, z - distance, 1)
            along(z + distance < LINE, z + distance, -1)
        if distance == 1:
            across_own()
        else:
            across(z >= distance - 1, z - distance + 1, 1)
            across(z + distance - 1 < LINE, z + distance - 1, -1)
        if distance == 1 and later is not None:
            later()
        if distance == LINE - 1 and last is not None:
            last()

    keep.wait()
    for block in range(LINE):
        for half in range(2):
            remote(
                own,
                gathered.at[place.rows(block, half, 1 - core, rows)],
                core_sem.at[0, 2 * block + half],
                core_sem.at[1, 2 * block + half],
                place.at(z, y, 1 - core),
            ).wait_recv()


def pair_scratch():
    return [DMA((3,))]


def pair_phase(place, sender, own, pair, scratch):
    (sem,) = scratch
    rows = own.shape[0]
    spot = pair.at[pl.ds(pl.multiple_of(place.core * rows, rows), rows)]
    keep = pltpu.make_async_copy(own, spot, sem.at[0])
    keep.start()

    def send():
        return remote(
            own, spot, sem.at[1], sem.at[2], place.at(place.z, place.y, 1 - place.core)
        )

    sender(None, send)

    def finish():
        keep.wait()
        other = pair.at[pl.ds(pl.multiple_of((1 - place.core) * rows, rows), rows)]
        remote(
            own, other, sem.at[1], sem.at[2], place.at(place.z, place.y, 1 - place.core)
        ).wait_recv()

    return finish


def swap_scratch(count, arrays):
    return [DMA((arrays,)), DMA((2, arrays, count)), DMA((2, arrays, count))]


class Swap:
    def __init__(self, place, pairs, scratch):
        self.place = place
        self.pairs = pairs
        self.local_sem, self.out_sem, self.side_sem = scratch

    def send(self, index, step):
        place = self.place
        source, spot = self.pairs[index]
        target = lax.rem(place.device + step, place.count)
        return remote(
            source(target),
            spot(place.device, place.side),
            self.out_sem.at[0, index, step],
            self.out_sem.at[1, index, step],
            {"fsdp": target},
        )

    def taken(self, index, step, side):
        device = lax.rem(self.place.device + self.place.count - step, self.place.count)
        return self.pairs[index][1](device, side)

    def come(self, index, step):
        place = self.place
        return remote(
            self.pairs[index][0](place.device),
            self.taken(index, step, place.side),
            self.out_sem.at[0, index, step],
            self.out_sem.at[1, index, step],
            place.across(),
        )

    def share(self, index, step, source=None):
        spot = self.taken(index, step, self.place.side)
        return remote(
            spot if source is None else source,
            spot,
            self.side_sem.at[0, index, step],
            self.side_sem.at[1, index, step],
            self.place.across(),
        )

    def shared(self, index, step):
        spot = self.taken(index, step, 1 - self.place.side)
        return remote(
            spot,
            spot,
            self.side_sem.at[0, index, step],
            self.side_sem.at[1, index, step],
            self.place.across(),
        )

    def keep(self, index):
        place = self.place
        source, spot = self.pairs[index]
        return pltpu.make_async_copy(
            source(place.device), spot(place.device, place.side), self.local_sem.at[index]
        )

    def each(self, first, body):
        def step(number, carry):
            for index in range(len(self.pairs)):
                body(index, number)
            return carry

        lax.fori_loop(first, self.place.count, step, 0)

    def start(self):
        self.each(1, lambda index, step: self.send(index, step).start())
        for index, (source, _) in enumerate(self.pairs):
            self.keep(index).start()
            self.share(index, 0, source(self.place.device)).start()

    def pass_on(self):
        def one(index, step):
            self.come(index, step).wait_recv()
            self.share(index, step).start()

        self.each(1, one)

    def finish(self):
        for index in range(len(self.pairs)):
            self.keep(index).wait()
        self.each(0, lambda index, step: self.shared(index, step).wait_recv())
        self.each(1, lambda index, step: self.send(index, step).wait_send())
        self.each(0, lambda index, step: self.share(index, step).wait_send())


def whole_pair(pieces, whole):
    return (lambda target: pieces.at[target], lambda device, side: whole.at[device, side])


def halves_scratch(arrays):
    return [DMA((3, arrays))]


class Halves:
    def __init__(self, place, halves, wholes, scratch):
        self.place = place
        self.pairs = list(zip(halves, wholes))
        (self.sem,) = scratch

    def keep(self, index):
        half, whole = self.pairs[index]
        return pltpu.make_async_copy(half, whole.at[:, self.place.side], self.sem.at[0, index])

    def copy(self, index, side):
        half, whole = self.pairs[index]
        return remote(
            half,
            whole.at[:, side],
            self.sem.at[1, index],
            self.sem.at[2, index],
            self.place.across(),
        )

    def start(self):
        for index in range(len(self.pairs)):
            self.copy(index, self.place.side).start()
            self.keep(index).start()

    def finish(self):
        for index in range(len(self.pairs)):
            self.keep(index).wait()
            self.copy(index, 1 - self.place.side).wait_recv()
            self.copy(index, self.place.side).wait_send()


REDUCE = 11
GATHER = 6
PIECES = 8


class Pack:
    def __init__(self, place, weights, outs, scratch):
        gate, up, down = weights
        pair, low = outs
        held_gate, held_up, held_down, in_sem, out_sem = scratch
        half, columns = held_gate.shape[0], pair.shape[2] // 2
        down_half = held_down.shape[1]
        rows = pl.ds(pl.multiple_of(place.side * half, half), half)
        self.ins = [
            pltpu.make_async_copy(gate.at[rows], held_gate, in_sem.at[0]),
            pltpu.make_async_copy(up.at[rows], held_up, in_sem.at[1]),
        ]
        self.outs = []
        for member in range(2 * LINE):
            start = (2 * member + place.side) * down_half
            down_rows = pl.ds(pl.multiple_of(start, down_half), down_half)
            self.ins.append(
                pltpu.make_async_copy(
                    down.at[down_rows], held_down.at[member], in_sem.at[2 + member]
                )
            )
            at = pl.ds(member * columns, columns)
            for index, (source, target) in enumerate(
                (
                    (held_gate.at[:, at], pair.at[member, :, pl.ds(0, columns)]),
                    (held_up.at[:, at], pair.at[member, :, pl.ds(columns, columns)]),
                    (held_down.at[member], low.at[member]),
                )
            ):
                sem = out_sem.at[index, member]
                self.outs.append(pltpu.make_async_copy(source, target, sem))

    def fetch(self):
        for copy in self.ins:
            copy.start()

    def put(self):
        for copy in self.ins:
            copy.wait()
        for copy in self.outs:
            copy.start()

    def finish(self):
        for copy in self.outs:
            copy.wait()


def first_kernel(
    own_ref,
    query,
    key,
    value,
    out,
    small,
    gate,
    up,
    down,
    gathered,
    qkv_all,
    out_all,
    small_all,
    pair,
    low,
    *scratch,
):
    place = Place()
    sender = Sender()
    own = scratch[0]
    own[...] = own_ref[...]
    greet_all(place)
    half, columns = qkv_all.shape[2], qkv_all.shape[3] // 3
    out_half = out_all.shape[2]
    rows = pl.ds(pl.multiple_of(place.side * half, half), half)

    def member(target):
        return lax.rem(target, 2 * LINE)

    def column_pair(weight, index):
        def source(target):
            start = pl.multiple_of(member(target) * columns, columns)
            return weight.at[rows, pl.ds(start, columns)]

        def spot(device, side):
            return qkv_all.at[device, side, :, pl.ds(index * columns, columns)]

        return (source, spot)

    def out_source(target):
        start = (2 * member(target) + place.side) * out_half
        return out.at[pl.ds(pl.multiple_of(start, out_half), out_half)]

    pairs = [
        (lambda target: small, lambda device, side: small_all.at[device, side]),
        column_pair(query, 0),
        column_pair(key, 1),
        column_pair(value, 2),
        (out_source, lambda device, side: out_all.at[device, side]),
    ]
    swap = Swap(place, pairs, scratch[GATHER : GATHER + 3])
    pack = Pack(place, (gate, up, down), (pair, low), scratch[GATHER + 3 :])

    def begin():
        swap.start()
        pack.fetch()

    def later():
        pack.put()
        swap.pass_on()

    gather_phase(place, sender, gathered, scratch[:GATHER], begin, later)
    swap.finish()
    pack.finish()
    sender.drain()


def hidden_kernel(
    partial, tokens, gain, pair, down, gathered, branch, hidden, pair_all, down_all, *scratch
):
    place = Place()
    sender = Sender()
    greet(place, True)
    halves = Halves(place, (pair, down), (pair_all, down_all), scratch[REDUCE + GATHER :])
    halves.start()
    reduce_phase(place, sender, partial, scratch[:REDUCE])
    total, own = scratch[4], scratch[REDUCE]
    rows, width = total.shape

    def body(at):
        value = total[at]
        scale = lax.rsqrt(jnp.sum(value * value, axis=1, keepdims=True) / width + EPS)
        result = tokens[at].astype(F32) + value * scale * gain[...]
        branch[at] = value
        hidden[at] = result
        own[at] = result.astype(BF)

    by_rows(rows, body)
    gather_phase(place, sender, gathered, scratch[REDUCE : REDUCE + GATHER])
    halves.finish()
    sender.drain()


def turn_kernel(partial, hidden, cotangent, gain, gathered, outputs, gain_grad, *scratch):
    place = Place()
    sender = Sender()
    greet(place)
    reduce_phase(place, sender, partial, scratch[:REDUCE])
    total, own = scratch[4], scratch[REDUCE]
    out_own = scratch[REDUCE + GATHER]
    rows, width = total.shape
    gain_grad[...] = jnp.zeros_like(gain_grad)

    def body(at):
        value = total[at]
        scale = lax.rsqrt(jnp.sum(value * value, axis=1, keepdims=True) / width + EPS)
        grads = cotangent[at].astype(F32)
        normed = value * scale
        out_own[at] = (hidden[at] + normed * gain[...]).astype(BF)
        gain_grad[...] += jnp.sum(grads * normed, axis=0, keepdims=True)
        gained = gain[...] * grads
        inner = jnp.sum(normed * gained, axis=1, keepdims=True)
        own[at] = (scale * (gained - normed * (inner / width))).astype(BF)

    by_rows(rows, body)
    finish = pair_phase(place, sender, out_own, outputs, scratch[REDUCE + GATHER + 1 :])
    gather_phase(place, sender, gathered, scratch[REDUCE : REDUCE + GATHER])
    finish()
    sender.drain()


class WeightGrads:
    def __init__(self, place, arrays, outs, scratch):
        self.place = place
        self.inner, self.grad_mlp, self.hidden, self.grad_pair = arrays
        self.outs = outs
        self.tall, self.turned, self.inner_turned = scratch[:3]
        self.fulls, self.others = scratch[3:5], scratch[5:7]
        self.fetch_sem, self.side_sem = scratch[7:]
        self.piece = self.tall.shape[3]

    def fetch(self, number, slot):
        columns = pl.ds(pl.multiple_of(number * self.piece, self.piece), self.piece)
        return [
            pltpu.make_async_copy(
                array.at[:, columns], self.tall.at[slot, index], self.fetch_sem.at[slot, index]
            )
            for index, array in enumerate((self.hidden, self.grad_mlp))
        ]

    def side_of(self, index, number, side):
        if index == 0:
            return self.fulls[0].at[number, :, side]
        return self.fulls[1].at[number, side]

    def crossing(self, number, index):
        return remote(
            self.side_of(index, number, 1 - self.place.side),
            self.others[index].at[number],
            self.side_sem.at[0, index, number],
            self.side_sem.at[1, index, number],
            self.place.across(),
        )

    def start(self):
        for copy in self.fetch(0, 0):
            copy.start()
        self.inner_turned[...] = self.inner[...].T

    def one(self, number, carry):
        slot = lax.rem(number, 2)
        for copy in self.fetch(number, slot):
            copy.wait()

        @pl.when(number < PIECES - 1)
        def _():
            for copy in self.fetch(number + 1, 1 - slot):
                copy.start()

        full, low = self.fulls
        self.turned[...] = self.tall[slot, 0].T
        columns = self.grad_pair.shape[1]
        step = columns // 4

        def columns_step(index, carry):
            at = pl.ds(pl.multiple_of(index * step, step), step)
            value = product(self.turned[...], self.grad_pair[:, at]).astype(BF)
            full[number, :, :, :, at] = value.reshape(full.shape[1:4] + (step,))
            return carry

        lax.fori_loop(0, 4, columns_step, 0)
        value = product(self.inner_turned[...], self.tall[slot, 1]).astype(BF)
        low[number] = value.reshape(low.shape[1:])
        for index in range(2):
            self.crossing(number, index).start()
        return carry

    def some(self, which):
        half = PIECES // 2
        lax.fori_loop(which * half, which * half + half, self.one, 0)

    def add(self):
        def step(number, carry):
            for index in range(2):
                self.crossing(number, index).wait_recv()
                own = self.side_of(index, number, self.place.side)[...].astype(F32)
                other = self.others[index][number].astype(F32)
                self.outs[index][number] = (own + other).astype(BF)
            return carry

        lax.fori_loop(0, PIECES, step, 0)

    def finish(self):
        def step(number, carry):
            for index in range(2):
                self.crossing(number, index).wait_send()
            return carry

        lax.fori_loop(0, PIECES, step, 0)


def branch_kernel(
    partial,
    branch,
    cotangent,
    gain,
    inner_low,
    grad_mlp,
    hidden_low,
    grad_pair,
    gathered,
    grad_hidden,
    gain_grad,
    pair_mine,
    down_mine,
    *scratch,
):
    place = Place()
    sender = Sender()
    greet(place, True)
    grads = WeightGrads(
        place,
        (inner_low, grad_mlp, hidden_low, grad_pair),
        (pair_mine, down_mine),
        scratch[REDUCE + GATHER :],
    )
    grads.start()
    reduce_phase(place, sender, partial, scratch[:REDUCE], idle=grads.some)
    total, own = scratch[4], scratch[REDUCE]
    rows, width = total.shape
    gain_grad[...] = jnp.zeros_like(gain_grad)

    def body(at):
        value = branch[at]
        scale = lax.rsqrt(jnp.sum(value * value, axis=1, keepdims=True) / width + EPS)
        grads = cotangent[at].astype(F32) + total[at]
        grad_hidden[at] = grads
        normed = value * scale
        gain_grad[...] += jnp.sum(grads * normed, axis=0, keepdims=True)
        gained = gain[...] * grads
        inner = jnp.sum(normed * gained, axis=1, keepdims=True)
        own[at] = (scale * (gained - normed * (inner / width))).astype(BF)

    by_rows(rows, body)
    gather_phase(
        place, sender, gathered, scratch[REDUCE : REDUCE + GATHER], last=grads.add
    )
    grads.finish()
    sender.drain()


def last_kernel(
    partial,
    grad_hidden,
    qkv,
    out,
    small,
    down,
    result,
    qkv_all,
    out_all,
    small_all,
    down_all,
    *scratch,
):
    place = Place()
    sender = Sender()
    parts = scratch[REDUCE + 1 :]
    swap_sems, halves_sems, parts = parts[:3], parts[3:4], parts[4:]
    qkv_own, qkv_other, out_own, out_other, small_own, small_other, fetch_sem, side_sem = parts
    greet_all(place)
    fetches, crossings = [], []
    for index, (grad, own, other) in enumerate(
        ((qkv, qkv_own, qkv_other), (out, out_own, out_other))
    ):
        fetches.append(
            pltpu.make_async_copy(grad.at[:, place.side], own, fetch_sem.at[index])
        )
        crossings.append(
            remote(
                grad.at[:, 1 - place.side],
                other,
                side_sem.at[0, index],
                side_sem.at[1, index],
                place.across(),
            )
        )
    crossings.append(
        remote(
            small,
            small_other,
            side_sem.at[0, 2],
            side_sem.at[1, 2],
            place.at(place.z, place.y, 1 - place.core),
        )
    )
    for copy in fetches + crossings:
        copy.start()
    pairs = ((small_own, small_all), (qkv_own, qkv_all), (out_own, out_all))
    swap = Swap(place, [whole_pair(*pair) for pair in pairs], swap_sems)
    halves = Halves(place, (down,), (down_all,), halves_sems)
    shared_rows = 2 * partial.shape[1] // place.count // 128

    def between():
        for fetch in fetches:
            fetch.wait()
        for crossing in crossings:
            crossing.wait()
        small_own[...] = small[...]
        small_own[:, :shared_rows] += small_other[:, :shared_rows]

        def one(index, carry):
            qkv_own[index] = (
                qkv_own[index].astype(F32) + qkv_other[index].astype(F32)
            ).astype(BF)
            out_own[index] = (
                out_own[index].astype(F32) + out_other[index].astype(F32)
            ).astype(BF)
            return carry

        lax.fori_loop(0, place.count, one, 0)
        swap.start()
        halves.start()

    reduce_phase(place, sender, partial, scratch[:REDUCE], between, late=swap.pass_on)
    total = scratch[4]

    def body(at):
        total[at] += grad_hidden[at]

    by_rows(total.shape[0], body)
    finish = pair_phase(place, sender, total, result, scratch[REDUCE : REDUCE + 1])
    finish()
    halves.finish()
    swap.finish()
    sender.drain()


def sum_kernel(carried, value, *rest):
    if carried:
        moved, result, arrived, core_in, y_in, held, line_in, sem, side_sem = rest
    else:
        result, core_in, y_in, held, line_in, sem = rest
    place = Place()
    z, y, core = place.z, place.y, place.core
    barrier = pltpu.get_barrier_semaphore()
    others = [place.at(z, y, 1 - core), place.at(z, 1 - y, core)]
    others += [place.at(lax.rem(z + k, LINE), y, core) for k in range(1, LINE)]
    for device in others + [place.across()] * carried:
        signal(barrier, device)
    pl.semaphore_wait(barrier, len(others) + carried)
    if carried:
        side = remote(moved, arrived, side_sem.at[0], side_sem.at[1], place.across())
        side.start()
    first = remote(value, core_in, sem.at[0, 0], sem.at[1, 0], others[0])
    first.start()
    first.wait_recv()
    held[0] = value[...] + core_in[...]
    second = remote(held.at[0], y_in, sem.at[0, 1], sem.at[1, 1], others[1])
    second.start()
    second.wait_recv()
    held[1] = held[0] + y_in[...]
    sends = [
        remote(held.at[1], line_in.at[k - 1], sem.at[0, 1 + k], sem.at[1, 1 + k], others[1 + k])
        for k in range(1, LINE)
    ]
    for send in sends:
        send.start()
    line_in[LINE - 1] = held[1]
    for send in sends:
        send.wait_recv()
    added = jnp.zeros_like(value)
    for source in range(LINE):
        slot = lax.rem(z - source + 2 * LINE - 1, LINE)
        added = added + line_in[slot]
    result[...] = added
    first.wait_send()
    second.wait_send()
    for send in sends:
        send.wait_send()
    if carried:
        side.wait()


def widen_own_kernel(side, own, gate_out, up_out):
    columns = gate_out.shape[1]
    value = jnp.sum(own[:, 0].astype(F32), axis=0)
    gate_out[...] = value[:, :columns]
    up_out[...] = value[:, columns:]


def widen_other_kernel(side, gate, up, other, rest, down, gate_out, up_out, down_out):
    columns = gate_out.shape[1]
    first = other.shape[2]
    for part, start in ((other, 0), (rest, first)):
        value = jnp.sum(part[:, 0].astype(F32), axis=0)
        rows = pl.ds(start, part.shape[2])
        gate_out[rows] = value[:, :columns]
        up_out[rows] = value[:, columns:]
    down_out[...] = jnp.sum(down[:, 0].astype(F32), axis=0)


def talk(kernel, which, shapes, specs, scratch, microseconds, name=None):
    def call(*operands):
        return pl.pallas_call(
            kernel,
            out_shape=shapes,
            in_specs=specs[0],
            out_specs=specs[1],
            scratch_shapes=scratch,
            compiler_params=pltpu.CompilerParams(
                collective_id=which, has_side_effects=True, vmem_limit_bytes=48 << 20
            ),
            cost_estimate=pl.CostEstimate(
                flops=0, bytes_accessed=int(microseconds * 3.0e6), transcendentals=0
            ),
            name=name or kernel.__name__,
        )(*operands)

    return call


class Team:
    def __init__(self, local_heads, rows, width):
        self.fsdp = lax.axis_size("fsdp")
        self.tensor = lax.axis_size("tensor")
        self.size = 2 * LINE
        self.teams = self.fsdp // self.size
        assert self.fsdp % self.size == 0 and self.tensor == 2 and local_heads % self.size == 0
        self.member = lax.rem(lax.axis_index("fsdp"), self.size)
        self.core = lax.axis_index("tensor")
        self.context = lax.axis_index("context")
        self.groups = None
        if self.teams > 1:
            self.groups = [
                [team * self.size + one for one in range(self.size)] for team in range(self.teams)
            ]
        self.rows = rows
        self.width = width
        self.all_low = jax.ShapeDtypeStruct((2 * self.size * rows, width), BF)
        self.own_wide = jax.ShapeDtypeStruct((rows, width), F32)
        self.line_wide = jax.ShapeDtypeStruct((1, width), F32)
        self.reduces = reduce_scratch(rows, width)
        self.gathers = gather_scratch(rows, width)

    def whole(self, pieces):
        shape = (pieces.shape[0], 2) + pieces.shape[1:]
        return jax.ShapeDtypeStruct(shape, pieces.dtype)

    def first(self, own, weights, out, small, gate, up, down):
        rows, columns = weights[0].shape
        rows, columns = rows // 2, columns // self.size
        out_rows = out.shape[0] // self.size // 2
        wide = gate.shape[1]
        low = (self.size, down.shape[0] // self.size // 2, down.shape[1])
        *results, pair, low = talk(
            first_kernel,
            0,
            (
                self.all_low,
                jax.ShapeDtypeStruct((self.fsdp, 2, rows, 3 * columns), BF),
                jax.ShapeDtypeStruct((self.fsdp, 2, out_rows, out.shape[1]), BF),
                jax.ShapeDtypeStruct((self.fsdp, 2) + small.shape, F32),
                jax.ShapeDtypeStruct((self.size, rows, 2 * wide // self.size), BF),
                jax.ShapeDtypeStruct(low, BF),
            ),
            ([VMEM] * 6 + [HBM] * 3, (HBM,) * 6),
            self.gathers
            + swap_scratch(self.fsdp, 5)
            + [
                pltpu.VMEM((rows, wide), BF),
                pltpu.VMEM((rows, wide), BF),
                pltpu.VMEM(low, BF),
                DMA((2 + self.size,)),
                DMA((3, self.size)),
            ],
            80,
        )(own, *weights, out, small, gate, up, down)
        return *results, self.repeat(pair), self.repeat(low)

    def hidden(self, partial, tokens, gain, pair, down):
        return talk(
            hidden_kernel,
            1,
            (self.all_low, self.own_wide, self.own_wide, self.whole(pair), self.whole(down)),
            ([HBM, VMEM, VMEM, VMEM, VMEM], (HBM, VMEM, VMEM, HBM, HBM)),
            self.reduces + self.gathers + halves_scratch(2),
            100,
        )(partial, tokens, gain, pair, down)

    def turn(self, partial, hidden, cotangent, gain):
        pair = jax.ShapeDtypeStruct((2 * self.rows, self.width), BF)
        return talk(
            turn_kernel,
            2,
            (self.all_low, pair, self.line_wide),
            ([HBM, VMEM, VMEM, VMEM], (HBM, HBM, VMEM)),
            self.reduces + self.gathers + [pltpu.VMEM((self.rows, self.width), BF)] + pair_scratch(),
            100,
        )(partial, hidden, cotangent, gain)

    def branch(self, partial, branch, cotangent, gain, inner, grad_mlp, hidden, grad_pair):
        team_rows, units = inner.shape
        columns = grad_pair.shape[1]
        piece = self.width // PIECES
        count = self.fsdp // PIECES
        half = self.width // self.fsdp // 2
        pair_shape = (PIECES, count, half, columns)
        down_shape = (PIECES, units // 2, piece)

        def both(shape):
            return pltpu.VMEM((shape[0], 2) + shape[1:], BF)

        def sides_inside(shape):
            return pltpu.VMEM((shape[0], shape[1], 2) + shape[2:], BF)

        gathered, grad_hidden, gain_grad, pair_mine, down_mine = talk(
            branch_kernel,
            3,
            (
                self.all_low,
                self.own_wide,
                self.line_wide,
                jax.ShapeDtypeStruct(pair_shape, BF),
                jax.ShapeDtypeStruct(down_shape, BF),
            ),
            (
                [HBM, VMEM, VMEM, VMEM, VMEM, HBM, HBM, VMEM],
                (HBM, VMEM, VMEM, VMEM, VMEM),
            ),
            self.reduces
            + self.gathers
            + [
                pltpu.VMEM((2, 2, team_rows, piece), BF),
                pltpu.VMEM((piece, team_rows), BF),
                pltpu.VMEM((units, team_rows), BF),
                sides_inside(pair_shape),
                both(down_shape),
                pltpu.VMEM(pair_shape, BF),
                pltpu.VMEM(down_shape, BF),
                DMA((2, 2)),
                DMA((2, 2, PIECES)),
            ],
            100,
        )(partial, branch, cotangent, gain, inner, grad_mlp, hidden, grad_pair)
        down_mine = down_mine.reshape(PIECES, units // 2, count, piece // count)
        return (
            gathered,
            grad_hidden,
            gain_grad,
            pair_mine.reshape(self.fsdp, half, columns),
            down_mine.transpose(0, 2, 1, 3).reshape(self.fsdp, units // 2, piece // count),
        )

    def last(self, partial, grad_hidden, qkv, out, small, down):
        both = jax.ShapeDtypeStruct((2 * self.rows, self.width), F32)

        def same(array):
            return jax.ShapeDtypeStruct(array.shape, array.dtype)

        def half(array):
            return pltpu.VMEM((array.shape[0],) + array.shape[2:], array.dtype)

        held = pltpu.VMEM(small.shape, small.dtype)
        return talk(
            last_kernel,
            4,
            (both, same(qkv), same(out), self.whole(small), self.whole(down)),
            ([HBM, VMEM, HBM, HBM, VMEM, VMEM], (HBM,) * 5),
            self.reduces
            + pair_scratch()
            + swap_scratch(self.fsdp, 3)
            + halves_scratch(1)
            + [half(qkv), half(qkv), half(out), half(out), held, held, DMA((2,)), DMA((2, 3))],
            80,
        )(partial, grad_hidden, qkv, out, small, down)

    def total(self, values, moved=None):
        flat = values.reshape(-1, 128)
        carried = int(moved is not None)
        shape = jax.ShapeDtypeStruct(flat.shape, F32)
        scratch = [pltpu.VMEM(flat.shape, F32)] * 2
        scratch += [pltpu.VMEM((2,) + flat.shape, F32), pltpu.VMEM((LINE,) + flat.shape, F32)]
        scratch += [DMA((2, LINE + 1))] + [DMA((2,))] * carried
        which = 5 + self.sums
        self.sums += 1
        kernel = functools.partial(sum_kernel, carried)
        if not carried:
            call = talk(kernel, which, shape, ([VMEM], VMEM), scratch, 10, "sum_kernel")
            return call(flat).reshape(values.shape)
        shapes = (shape, jax.ShapeDtypeStruct(moved.shape, moved.dtype))
        call = talk(kernel, which, shapes, ([VMEM] * 2, (VMEM,) * 2), scratch, 10, "sum_kernel")
        total, came = call(flat, moved)
        return total.reshape(values.shape), came

    sums = 0

    def half(self, array, axis):
        count = array.shape[axis] // 2
        return lax.dynamic_slice_in_dim(array, self.context * count, count, axis)

    def swap(self, pieces):
        return lax.all_to_all(pieces, "fsdp", split_axis=0, concat_axis=0, tiled=True)

    def repeat(self, pieces):
        return jnp.concatenate([pieces] * self.teams, axis=0) if self.teams > 1 else pieces

    def pieces(self, array):
        shape = (-1,) + array.shape[-2:] if array.ndim == 3 else (-1, 2 * array.shape[2], array.shape[3])
        array = array.reshape(shape)
        cut = array.reshape((self.teams, self.size) + array.shape[1:])
        spec = pl.BlockSpec((self.teams, 1) + array.shape[1:], lambda d, side: (0, d, 0, 0))
        return cut, spec

    def widen_own(self, own):
        half, columns = own.shape[1], own.shape[2] // 2
        cut, spec = self.pieces(own)
        wide = pl.BlockSpec((half, columns), lambda d, side: (side[0], d))
        return pl.pallas_call(
            widen_own_kernel,
            grid_spec=pltpu.PrefetchScalarGridSpec(
                num_scalar_prefetch=1, grid=(self.size,), in_specs=[spec], out_specs=[wide] * 2
            ),
            out_shape=[jax.ShapeDtypeStruct((2 * half, self.size * columns), F32)] * 2,
            name="widen_own_kernel",
        )(self.context.reshape(1).astype(jnp.int32), cut)

    def widen_other(self, gate, up, other, rest, down):
        half, columns = other.shape[1] + rest.shape[1], other.shape[2] // 2
        cuts, specs = zip(*[self.pieces(one) for one in (other, rest, down)])
        rows, down_columns = cuts[2].shape[2:]
        wide = pl.BlockSpec((half, columns), lambda d, side: (1 - side[0], d))
        return pl.pallas_call(
            widen_other_kernel,
            grid_spec=pltpu.PrefetchScalarGridSpec(
                num_scalar_prefetch=1,
                grid=(self.size,),
                in_specs=[HBM, HBM] + list(specs),
                out_specs=[wide, wide, pl.BlockSpec((rows, down_columns), lambda d, side: (d, 0))],
            ),
            out_shape=[
                jax.ShapeDtypeStruct(gate.shape, F32),
                jax.ShapeDtypeStruct(up.shape, F32),
                jax.ShapeDtypeStruct((self.size * rows, down_columns), F32),
            ],
            input_output_aliases={1: 0, 2: 1},
            name="widen_other_kernel",
        )(self.context.reshape(1).astype(jnp.int32), gate, up, *cuts)

    def columns_whole(self, came):
        return came.reshape(-1, came.shape[-1])

    def rows_whole(self, came):
        fsdp, two, rows, columns = came.shape
        return came.transpose(1, 2, 0, 3).reshape(two * rows, fsdp * columns)

    def of_columns(self, grad):
        rows, columns = grad.shape
        return grad.astype(BF).reshape(self.fsdp, 2, rows // self.fsdp // 2, columns)

    def of_rows(self, grad):
        rows, columns = grad.shape
        cut = grad.astype(BF).reshape(2, rows // 2, self.fsdp, columns // self.fsdp)
        return cut.transpose(2, 0, 1, 3)

    def added(self, came):
        if self.teams == 1:
            return came.astype(F32)
        came = came.reshape((self.teams, self.size) + came.shape[1:])
        return jnp.sum(came.astype(F32), axis=0)

    def columns_out(self, came, count):
        size, two, rows, columns = came.shape
        return [
            self.added(part.reshape(size, two * rows, -1))
            .transpose(1, 0, 2)
            .reshape(two * rows, -1)
            for part in jnp.split(came, count, axis=3)
        ]

    def rows_out(self, came):
        return self.added(came).reshape(-1, came.shape[-1])


def local(
    tokens,
    cont_lengths,
    w_query,
    w_key,
    w_value,
    w_output,
    query_gain,
    key_gain,
    attn_gain,
    w_gate,
    w_up,
    w_down,
    mlp_gain,
    cotangent,
):
    rows = tokens.shape[0]
    width = tokens.shape[1]
    fsdp = lax.axis_size("fsdp")
    tensor = lax.axis_size("tensor")
    local_heads = query_gain.shape[0]
    head_size = w_query.shape[1] // local_heads
    own_rows = rows // tensor
    team = Team(local_heads, own_rows, width)
    groups = team.size
    team_rows = groups * rows
    heads = local_heads // team.size
    later = lax.axis_index("context") == 1

    tokens_own = lax.dynamic_slice_in_dim(tokens, team.core * own_rows, own_rows, 0)
    grad_out = lax.dynamic_slice_in_dim(cotangent, team.core * own_rows, own_rows, 0)
    cut = query_gain.size
    share = attn_gain.size
    small = [query_gain.reshape(-1), key_gain.reshape(-1), attn_gain, mlp_gain]
    small = jnp.concatenate([one.astype(F32) for one in small + [cont_lengths.reshape(-1)]])
    small = jnp.pad(small, (0, 8 * 128 - small.size)).reshape(8, 128)
    tokens_all, qkv_came, output_came, small_came, pair_mine, down_mine = team.first(
        tokens_own, [w_query, w_key, w_value], w_output, small, w_gate, w_up, w_down
    )
    qkv_w = team.columns_whole(qkv_came)
    output_w = team.rows_whole(output_came)
    all_small = small_came[:, 0].reshape(fsdp, -1)
    query_gains = all_small[:, :cut].reshape(fsdp, local_heads, -1)
    key_gains = all_small[:, cut : 2 * cut].reshape(fsdp, local_heads, -1)
    query_gains = query_gains.transpose(1, 0, 2).reshape(local_heads, head_size)
    key_gains = key_gains.transpose(1, 0, 2).reshape(local_heads, head_size)
    flat_query = lax.dynamic_slice_in_dim(query_gains, team.member * heads, heads, 0).reshape(-1)
    flat_key = lax.dynamic_slice_in_dim(key_gains, team.member * heads, heads, 0).reshape(-1)
    gain_attn = all_small[:, 2 * cut : 2 * cut + share].reshape(1, -1)
    gain_mlp = all_small[:, 2 * cut + share : 2 * cut + 2 * share].reshape(1, -1)

    conts = cont_lengths.shape[1]
    lengths = all_small[:, 2 * cut + 2 * share : 2 * cut + 2 * share + conts].astype(jnp.int32)
    first_group = lax.axis_index("fsdp") - team.member
    lengths = lax.dynamic_slice_in_dim(lengths, first_group, groups, 0)
    segment, offset = jax.vmap(lambda one: layout(one, rows))(lengths)
    row_index = jnp.arange(rows, dtype=jnp.int32)
    positions = jnp.where(later, rows + offset, row_index[None, :])
    own_segment = jnp.where(later, segment, -1)
    cosine, sine = rotary_tables(positions, head_size)
    cosine = cosine[:, :, None, :]
    sine = sine[:, :, None, :]

    pair_came = team.swap(pair_mine)
    down_came = team.swap(down_mine)

    by_head = (groups, rows, heads, head_size)
    raw = product(tokens_all, qkv_w)
    query_raw, key_raw, value_raw = jnp.split(raw, 3, axis=1)
    value_low = value_raw.astype(BF)
    sums, sent_value = team.total(
        jnp.stack([jnp.sum(query_raw * query_raw, axis=1), jnp.sum(key_raw * key_raw, axis=1)]),
        value_low,
    )
    value_low, sent_value = value_low.reshape(by_head), sent_value.reshape(by_head)
    scale_query = lax.rsqrt(sums[0] / width + EPS)[:, None]
    scale_key = lax.rsqrt(sums[1] / width + EPS)[:, None]
    query_norm = query_raw * scale_query * flat_query
    key_norm = key_raw * scale_key * flat_key
    query_low = rotate(query_norm.reshape(by_head), cosine, sine).astype(BF)
    key_low = rotate(key_norm.reshape(by_head), cosine, sine).astype(BF)
    sent_key = lax.ppermute(key_low, "context", [(0, 1)])
    keys_all = jnp.concatenate([sent_key, key_low], axis=1)
    values_all = jnp.concatenate([sent_value, value_low], axis=1)
    key_index = jnp.arange(2 * rows, dtype=jnp.int32)
    key_segment = jnp.concatenate([jnp.full((groups, rows), -2, jnp.int32), own_segment], axis=1)
    remote = (key_index < rows)[None, None, :] & later
    own_keys = (
        (key_index >= rows)[None, None, :]
        & (key_index[None, None, :] - rows <= row_index[None, :, None])
        & (key_segment[:, None, :] == own_segment[:, :, None])
    )
    allowed = (remote | own_keys)[:, None]
    scale = 1.0 / math.sqrt(head_size)
    scores = (
        jnp.einsum("gqhd,gkhd->ghqk", query_low, keys_all, preferred_element_type=F32) * scale
    )
    scores = jnp.where(allowed, scores, -1e30)
    highest = jnp.max(scores, axis=-1, keepdims=True)
    weights = jnp.exp(scores - highest)
    probs = weights / jnp.sum(weights, axis=-1, keepdims=True)
    probs_low = probs.astype(BF)
    mixed = jnp.einsum("ghqk,gkhd->gqhd", probs_low, values_all, preferred_element_type=F32)
    attended_low = mixed.reshape(team_rows, heads * head_size).astype(BF)
    hidden_all, attn_sum, hidden, pair_came, down_came = team.hidden(
        product(attended_low, output_w).astype(BF), tokens_own, gain_attn, pair_came, down_came
    )
    pair_w = team.columns_whole(pair_came)
    down_w = team.rows_whole(down_came)

    gate, upward = jnp.split(product(hidden_all, pair_w), 2, axis=1)
    sigma = jax.nn.sigmoid(gate)
    inner_low = (gate * sigma * upward).astype(BF)
    grad_mlp_all, outputs, grad_mlp_gain = team.turn(
        product(inner_low, down_w).astype(BF), hidden, grad_out, gain_mlp
    )
    grad_inner = product_right(grad_mlp_all, down_w)
    grad_gate_low = (grad_inner * upward * sigma * (1.0 + gate * (1.0 - sigma))).astype(BF)
    grad_up_low = (grad_inner * gate * sigma).astype(BF)
    grad_pair = jnp.concatenate([grad_gate_low, grad_up_low], axis=1)
    grad_branch_all, grad_hidden, grad_attn_gain, pair_mine, down_mine = team.branch(
        product_right(grad_pair, pair_w).astype(BF),
        attn_sum,
        grad_out,
        gain_attn,
        inner_low,
        grad_mlp_all,
        hidden_all,
        grad_pair,
    )
    pair_came = team.swap(pair_mine)
    output_grad = team.of_rows(product_left(attended_low, grad_branch_all))
    grad_attended = product_right(grad_branch_all, output_w).astype(BF).reshape(by_head)

    grad_probs = jnp.einsum("gqhd,gkhd->ghqk", grad_attended, values_all, preferred_element_type=F32)
    centre = jnp.sum(probs * grad_probs, axis=-1, keepdims=True)
    grad_scores = (probs * (grad_probs - centre)).astype(BF)
    grad_query_rot = (
        jnp.einsum("ghqk,gkhd->gqhd", grad_scores, keys_all, preferred_element_type=F32) * scale
    )
    grad_keys = (
        jnp.einsum("ghqk,gqhd->gkhd", grad_scores, query_low, preferred_element_type=F32) * scale
    )
    grad_values = jnp.einsum("ghqk,gqhd->gkhd", probs_low, grad_attended, preferred_element_type=F32)
    back_value = lax.ppermute(grad_values[:, :rows].astype(BF), "context", [(1, 0)])
    back_key = lax.ppermute(grad_keys[:, :rows].astype(BF), "context", [(1, 0)])
    grad_key_rot = grad_keys[:, rows:] + back_key.astype(F32)
    grad_value_low = (
        (grad_values[:, rows:] + back_value.astype(F32)).reshape(team_rows, -1).astype(BF)
    )
    grad_query_norm = rotate_back(grad_query_rot, cosine, sine).reshape(team_rows, -1)
    grad_key_norm = rotate_back(grad_key_rot, cosine, sine).reshape(team_rows, -1)
    grad_query_gain = jnp.sum(grad_query_norm * query_raw * scale_query, axis=0)
    grad_key_gain = jnp.sum(grad_key_norm * key_raw * scale_key, axis=0)
    inner_sums = jnp.stack(
        [
            jnp.sum(query_raw * flat_query * grad_query_norm, axis=1),
            jnp.sum(key_raw * flat_key * grad_key_norm, axis=1),
        ]
    )
    inner_sums, pair_came = lax.optimization_barrier((inner_sums, pair_came))
    first = pair_came.shape[1] // 4
    pair_rest = lax.ppermute(pair_came[:, first:], "context", [(0, 1), (1, 0)])
    totals, pair_other = team.total(inner_sums, pair_came[:, :first])
    down_mine, totals = lax.optimization_barrier((down_mine, totals))
    down_came = team.swap(down_mine)
    grad_query_low = norm_back(
        query_raw, scale_query, flat_query, grad_query_norm, totals[0][:, None], width
    ).astype(BF)
    grad_key_low = norm_back(
        key_raw, scale_key, flat_key, grad_key_norm, totals[1][:, None], width
    ).astype(BF)
    grad_qkv = jnp.concatenate([grad_query_low, grad_key_low, grad_value_low], axis=1)
    qkv_grad = team.of_columns(product_left(tokens_all, grad_qkv))
    head_share = head_size // fsdp
    small = [
        grad_attn_gain.reshape(fsdp, share),
        grad_mlp_gain.reshape(fsdp, share),
        grad_query_gain.reshape(heads, fsdp, head_share).transpose(1, 0, 2).reshape(fsdp, -1),
        grad_key_gain.reshape(heads, fsdp, head_share).transpose(1, 0, 2).reshape(fsdp, -1),
    ]
    used = 2 * share + 2 * heads * head_share
    small = jnp.concatenate(small + [jnp.zeros((fsdp, 8 * 128 - used), F32)], axis=1)
    gate_own, up_own = team.widen_own(pair_came)
    partial, pair_rest, gate_own, up_own = lax.optimization_barrier(
        (product_right(grad_qkv, qkv_w).astype(BF), pair_rest, gate_own, up_own)
    )
    input_grad, qkv_came, output_came, small_came, down_came = team.last(
        partial,
        grad_hidden,
        qkv_grad,
        output_grad,
        small.reshape(fsdp, 8, 128),
        down_came,
    )
    grad_w_query, grad_w_key, grad_w_value = team.columns_out(qkv_came, 3)
    grad_w_gate, grad_w_up, grad_w_down = team.widen_other(
        gate_own, up_own, pair_other, pair_rest, down_came
    )
    grad_w_output = team.rows_out(output_came)
    came = jnp.sum(small_came, axis=1).reshape(fsdp, -1)
    row_gains = jnp.sum(came[:, : 2 * share], axis=0).reshape(2, share)
    head_gains = team.added(came[:, 2 * share : used]).reshape(team.size, 2, heads, head_share)
    head_gains = head_gains.transpose(1, 0, 2, 3).reshape(2, local_heads, head_share)
    return (
        outputs,
        input_grad,
        grad_w_query,
        grad_w_key,
        grad_w_value,
        grad_w_output,
        head_gains[0],
        head_gains[1],
        row_gains[0],
        grad_w_gate,
        grad_w_up,
        grad_w_down,
        row_gains[1],
    )


def solution(mesh):
    return jax.shard_map(
        local,
        mesh=mesh,
        in_specs=(
            P(("fsdp", "context"), None),
            P("fsdp", None),
            P("fsdp", "tensor"),
            P("fsdp", "tensor"),
            P("fsdp", "tensor"),
            P("tensor", "fsdp"),
            P("tensor", "fsdp"),
            P("tensor", "fsdp"),
            P("fsdp"),
            P("fsdp", "tensor"),
            P("fsdp", "tensor"),
            P("tensor", "fsdp"),
            P("fsdp"),
            P(("fsdp", "context"), None),
        ),
        out_specs=(
            P(("fsdp", "context"), None),
            P(("fsdp", "context"), None),
            P("fsdp", "tensor"),
            P("fsdp", "tensor"),
            P("fsdp", "tensor"),
            P("tensor", "fsdp"),
            P("tensor", "fsdp"),
            P("tensor", "fsdp"),
            P("fsdp"),
            P("fsdp", "tensor"),
            P("fsdp", "tensor"),
            P("tensor", "fsdp"),
            P("fsdp"),
        ),
        check_vma=False,
    )
```

```python
import functools
import math

import jax
import jax.numpy as jnp
from jax import lax
from jax.experimental import pallas as pl
from jax.experimental.pallas import tpu as pltpu
from jax.sharding import PartitionSpec as P

EPS = 1e-06
THETA = 500000.0
BF = jnp.bfloat16
F32 = jnp.float32


def product(left, right):
    return jnp.dot(left, right, preferred_element_type=F32)


def product_left(left, right):
    return jnp.einsum("rd,rf->df", left, right, preferred_element_type=F32)


def product_right(left, right):
    return jnp.einsum("rf,df->rd", left, right, preferred_element_type=F32)


def rotary_tables(positions, head_size):
    half = head_size // 2
    inverse = jnp.exp(-(2.0 * jnp.arange(half, dtype=F32) / head_size) * math.log(THETA))
    angles = positions.astype(F32)[..., None] * inverse
    angles = jnp.concatenate([angles, angles], axis=-1)
    return (jnp.cos(angles), jnp.sin(angles))


def rotate(values, cosine, sine):
    half = values.shape[-1] // 2
    turned = jnp.concatenate([-values[..., half:], values[..., :half]], axis=-1)
    return values * cosine + turned * sine


def rotate_back(grads, cosine, sine):
    half = grads.shape[-1] // 2
    scaled = grads * sine
    turned = jnp.concatenate([scaled[..., half:], -scaled[..., :half]], axis=-1)
    return grads * cosine + turned


def norm_back(values, scale, gain, grads, total, width):
    return scale * gain * grads - values * scale * scale * scale * (total / width)


def layout(lengths, rows):
    segment_ends = jnp.cumsum(lengths)
    segment_starts = segment_ends - lengths
    row_index = jnp.arange(rows, dtype=jnp.int32)
    segment = jnp.sum((row_index[:, None] >= segment_ends[None, :]).astype(jnp.int32), axis=1)
    chosen = segment[:, None] == jnp.arange(lengths.shape[0], dtype=jnp.int32)[None, :]
    offset = row_index - jnp.sum(jnp.where(chosen, segment_starts[None, :], 0), axis=1)
    return (segment, offset)


LINE = 4
CHUNK = 16
FEW = 8
MESH_ID = pl.DeviceIdType.MESH
HBM = pl.BlockSpec(memory_space=pl.ANY)
VMEM = pl.BlockSpec(memory_space=pltpu.VMEM)
DMA = pltpu.SemaphoreType.DMA


class Place:
    def __init__(self):
        device = lax.axis_index("fsdp")
        member = lax.rem(device, 2 * LINE)
        self.base = device - member
        self.z = member // 2
        self.y = lax.rem(member, 2)
        self.core = lax.axis_index("tensor")
        self.side = lax.axis_index("context")
        self.device = device
        self.count = lax.axis_size("fsdp")

    def across(self):
        return {"context": 1 - self.side}

    def at(self, z, y, core):
        return {"fsdp": self.base + 2 * z + y, "tensor": core}

    def near(self):
        yield None, self.at(self.z, self.y, 1 - self.core)
        yield None, self.at(self.z, 1 - self.y, self.core)
        yield self.z > 0, self.at(self.z - 1, self.y, self.core)
        yield self.z < LINE - 1, self.at(self.z + 1, self.y, self.core)

    def rows(self, z, y, core, count):
        start = ((2 * z + y) * 2 + core) * count
        return pl.ds(pl.multiple_of(start, count), count)


def guarded(condition, action):
    if condition is None:
        action()
    else:
        pl.when(condition)(action)


def signal(barrier, device):
    pl.semaphore_signal(barrier, inc=1, device_id=device, device_id_type=MESH_ID)


def greet(place, across=False):
    barrier = pltpu.get_barrier_semaphore()
    for condition, device in place.near():
        guarded(condition, functools.partial(signal, barrier, device))
    if across:
        signal(barrier, place.across())
    inside = (place.z > 0) & (place.z < LINE - 1)
    pl.semaphore_wait(barrier, jnp.where(inside, 4, 3) + int(across))


def greet_all(place):
    barrier = pltpu.get_barrier_semaphore()

    def one(step, carry):
        signal(barrier, {"fsdp": lax.rem(place.device + step, place.count)})
        return carry

    lax.fori_loop(1, place.count, one, 0)
    signal(barrier, place.across())
    signal(barrier, place.at(place.z, place.y, 1 - place.core))
    pl.semaphore_wait(barrier, place.count + 1)


class Sender:
    def __init__(self):
        self.sent = []

    def __call__(self, condition, make):
        def start():
            make().start()

        guarded(condition, start)
        self.sent.append((condition, make))

    def drain(self):
        for condition, make in self.sent:

            def wait(make=make):
                make().wait_send()

            guarded(condition, wait)


def remote(source, target, send, receive, device):
    return pltpu.make_async_remote_copy(
        src_ref=source,
        dst_ref=target,
        send_sem=send,
        recv_sem=receive,
        device_id=device,
        device_id_type=MESH_ID,
    )


def by_rows(rows, body, first=0):
    def step(index, carry):
        body(pl.ds(pl.multiple_of(index * CHUNK, CHUNK), CHUNK))
        return carry

    lax.fori_loop(first // CHUNK, rows // CHUNK, step, 0)


def reduce_scratch(rows, width):
    return [
        pltpu.VMEM((2 * LINE, rows, width), BF),
        pltpu.VMEM((2 * LINE, rows, width), BF),
        pltpu.VMEM((LINE, rows, width), BF),
        pltpu.VMEM((LINE + 1, rows, width), BF),
        pltpu.VMEM((rows, width), F32),
        DMA((2 * LINE,)),
        DMA((2, 2 * LINE)),
        DMA((2, LINE)),
        DMA((2, LINE + 1)),
        pltpu.VMEM((LINE + 1, rows // FEW, width), BF),
        DMA((2, LINE + 1)),
    ]


def reduce_phase(place, sender, partial, scratch, between=None, idle=None, late=None):
    mine, core_in, y_in, line_in, total, local_sem, core_sem, y_sem, line_sem = scratch[:9]
    few_in, few_sem = scratch[9:]
    rows = total.shape[0]
    few = rows // FEW
    z, y, core = place.z, place.y, place.core
    low = z < LINE // 2
    order = []
    for k in range(LINE - 1):
        down = LINE - 1 - k
        down = jnp.where(down <= z, down - 1, down)
        up = jnp.where(k >= z, k + 1, k)
        order.append(jnp.where(low, down, up))
    order.append(z)

    def fetch(slot):
        half = lax.rem(slot, 2)
        return pltpu.make_async_copy(
            partial.at[place.rows(slot // 2, half, core, rows)], mine.at[slot], local_sem.at[slot]
        )

    def to_core(slot):
        half = lax.rem(slot, 2)
        return remote(
            partial.at[place.rows(slot // 2, half, 1 - core, rows)],
            core_in.at[slot],
            core_sem.at[0, slot],
            core_sem.at[1, slot],
            place.at(z, y, 1 - core),
        )

    def to_y(block, first):
        at = pl.ds(first, rows - first)
        return remote(
            mine.at[2 * block + 1 - y, at],
            y_in.at[block, at],
            y_sem.at[0, block],
            y_sem.at[1, block],
            place.at(z, 1 - y, core),
        )

    def few_along(block):
        step = jnp.where(block > z, 1, -1)
        slot = jnp.where((step < 0) & (block == z - 1), LINE, block)
        return remote(
            mine.at[2 * block + 1 - y, pl.ds(0, few)],
            few_in.at[slot],
            few_sem.at[0, block],
            few_sem.at[1, slot],
            place.at(z + step, y, core),
        )

    def add_few(slot, source):
        remote(
            mine.at[0, pl.ds(0, few)],
            few_in.at[source],
            few_sem.at[0, 0],
            few_sem.at[1, source],
            place.at(z, y, 1 - core),
        ).wait_recv()

        def add(at):
            value = mine[slot, at].astype(F32) + few_in[source, at].astype(F32)
            mine[slot, at] = value.astype(BF)

        by_rows(few, add)

    def to_line(block):
        step = jnp.where(block > z, 1, -1)
        slot = jnp.where((step < 0) & (block == z - 1), LINE, block)
        return remote(
            mine.at[2 * block + y],
            line_in.at[slot],
            line_sem.at[0, block],
            line_sem.at[1, slot],
            place.at(z + step, y, core),
        )

    def from_line(slot):
        return remote(
            mine.at[0],
            line_in.at[slot],
            line_sem.at[0, 0],
            line_sem.at[1, slot],
            place.at(z, y, 1 - core),
        )

    for half in (1 - y, y):
        for block in order:
            sender(None, functools.partial(to_core, 2 * block + half))
            fetch(2 * block + half).start()

    for number, block in enumerate(order):
        slot = 2 * block + 1 - y
        fetch(slot).wait()
        to_core(slot).wait_recv()

        def add(at, slot=slot):
            value = mine[slot, at].astype(F32) + core_in[slot, at].astype(F32)
            mine[slot, at] = value.astype(BF)

        by_rows(rows, add)
        if number == LINE - 1:
            pl.when(z > 0)(functools.partial(add_few, slot, z))
            pl.when(z < LINE - 1)(functools.partial(add_few, slot, LINE))
            sender(None, functools.partial(to_y, block, 0))
        else:
            sender(None, functools.partial(to_y, block, few))
            inner = jnp.where(block > z, z > 0, z < LINE - 1)
            pl.when(inner)(functools.partial(add_few, slot, block))
            sender(None, functools.partial(few_along, block))

    for number, block in enumerate(order[:-1]):
        if number == LINE - 2 and between is not None:
            between()
        if number < 2 and idle is not None:
            idle(number)
        slot = 2 * block + y
        fetch(slot).wait()
        to_core(slot).wait_recv()
        to_y(block, few).wait_recv()
        inner = jnp.where(block > z, z > 0, z < LINE - 1)

        @pl.when(inner)
        def _(block=block, slot=slot):
            from_line(block).wait_recv()

            def add_first(at):
                value = mine[slot, at].astype(F32) + core_in[slot, at].astype(F32)
                mine[slot, at] = (value + line_in[block, at].astype(F32)).astype(BF)

            def add(at):
                value = mine[slot, at].astype(F32) + core_in[slot, at].astype(F32)
                value = value + y_in[block, at].astype(F32)
                mine[slot, at] = (value + line_in[block, at].astype(F32)).astype(BF)

            by_rows(few, add_first)
            by_rows(rows, add, few)

        @pl.when(jnp.logical_not(inner))
        def _(block=block, slot=slot):
            def add_first(at):
                value = mine[slot, at].astype(F32) + core_in[slot, at].astype(F32)
                mine[slot, at] = value.astype(BF)

            def add(at):
                value = mine[slot, at].astype(F32) + core_in[slot, at].astype(F32)
                mine[slot, at] = (value + y_in[block, at].astype(F32)).astype(BF)

            by_rows(few, add_first)
            by_rows(rows, add, few)

        sender(None, functools.partial(to_line, block))

    if late is not None:
        late()
    slot = 2 * z + y
    fetch(slot).wait()
    to_core(slot).wait_recv()
    to_y(z, 0).wait_recv()

    def start(at):
        value = mine[slot, at].astype(F32) + core_in[slot, at].astype(F32)
        total[at] = value + y_in[z, at].astype(F32)

    by_rows(rows, start)
    for condition, source in ((z > 0, z), (z < LINE - 1, LINE)):

        @pl.when(condition)
        def _(source=source):
            from_line(source).wait_recv()

            def add(at):
                total[at] += line_in[source, at].astype(F32)

            by_rows(rows, add)


def gather_scratch(rows, width):
    return [
        pltpu.VMEM((rows, width), BF),
        DMA((1,)),
        DMA((2, 2 * LINE)),
        DMA((2, LINE)),
        DMA((2, LINE + 2)),
        DMA((2, LINE + 2)),
    ]


def gather_phase(place, sender, gathered, scratch, between=None, later=None, last=None):
    own, local_sem, core_sem, y_sem, line_sem, few_sem = scratch
    rows = own.shape[0]
    few = rows // FEW
    z, y, core = place.z, place.y, place.core

    def spot(block, half):
        return gathered.at[place.rows(block, half, core, rows)]

    def to_core(source, block, half):
        return remote(
            source,
            spot(block, half),
            core_sem.at[0, 2 * block + half],
            core_sem.at[1, 2 * block + half],
            place.at(z, y, 1 - core),
        )

    def to_y(source, block):
        return remote(
            source,
            spot(block, y),
            y_sem.at[0, block],
            y_sem.at[1, block],
            place.at(z, 1 - y, core),
        )

    def to_line(source, block, step, index):
        return remote(
            source,
            spot(block, y),
            line_sem.at[0, index],
            line_sem.at[1, block],
            place.at(z + step, y, core),
        )

    def some(block, half, first, count):
        start = ((2 * block + half) * 2 + core) * rows + first
        return gathered.at[pl.ds(pl.multiple_of(start, few), count)]

    def rest_to_y(half, block):
        return remote(
            some(block, half, few, rows - few),
            some(block, half, few, rows - few),
            y_sem.at[0, block],
            y_sem.at[1, block],
            place.at(z, 1 - y, core),
        )

    def few_along(block, step, index):
        return remote(
            some(block, 1 - y, 0, few),
            some(block, 1 - y, 0, few),
            few_sem.at[0, index],
            few_sem.at[1, block],
            place.at(z + step, y, core),
        )

    keep = pltpu.make_async_copy(own, spot(z, y), local_sem.at[0])
    keep.start()
    sender(z < LINE - 1, functools.partial(to_line, own, z, 1, LINE))
    sender(z > 0, functools.partial(to_line, own, z, -1, LINE + 1))
    sender(None, functools.partial(to_y, own, z))
    sender(None, functools.partial(to_core, own, z, y))
    if between is not None:
        between()

    def took_y(block):
        remote(
            own,
            spot(block, 1 - y),
            y_sem.at[0, block],
            y_sem.at[1, block],
            place.at(z, 1 - y, core),
        ).wait_recv()

    def across_own():
        took_y(z)
        sender(z < LINE - 1, functools.partial(few_along, z, 1, LINE))
        sender(z > 0, functools.partial(few_along, z, -1, LINE + 1))
        sender(None, lambda: to_core(spot(z, 1 - y), z, 1 - y))

    def across(condition, block, step):
        guarded(condition, lambda: few_along(block, step, block).wait_recv())
        onward = condition & ((z < LINE - 1) if step > 0 else (z > 0))
        sender(onward, functools.partial(few_along, block, step, block))
        guarded(condition, lambda: rest_to_y(1 - y, block).wait_recv())
        sender(condition, lambda: to_core(spot(block, 1 - y), block, 1 - y))

    def along(condition, block, step):
        def took():
            to_line(own, block, step, block).wait_recv()

        guarded(condition, took)
        onward = condition & ((z < LINE - 1) if step > 0 else (z > 0))
        sender(onward, lambda: to_line(spot(block, y), block, step, block))
        sender(condition, lambda: rest_to_y(y, block))
        sender(condition, lambda: to_core(spot(block, y), block, y))

    for distance in range(1, LINE + 1):
        if distance < LINE:
            along(z >= distance, z - distance, 1)
            along(z + distance < LINE, z + distance, -1)
        if distance == 1:
            across_own()
        else:
            across(z >= distance - 1, z - distance + 1, 1)
            across(z + distance - 1 < LINE, z + distance - 1, -1)
        if distance == 1 and later is not None:
            later()
        if distance == LINE - 1 and last is not None:
            last()

    keep.wait()
    for block in range(LINE):
        for half in range(2):
            remote(
                own,
                gathered.at[place.rows(block, half, 1 - core, rows)],
                core_sem.at[0, 2 * block + half],
                core_sem.at[1, 2 * block + half],
                place.at(z, y, 1 - core),
            ).wait_recv()


def pair_scratch():
    return [DMA((3,))]


def pair_phase(place, sender, own, pair, scratch):
    (sem,) = scratch
    rows = own.shape[0]
    spot = pair.at[pl.ds(pl.multiple_of(place.core * rows, rows), rows)]
    keep = pltpu.make_async_copy(own, spot, sem.at[0])
    keep.start()

    def send():
        return remote(
            own, spot, sem.at[1], sem.at[2], place.at(place.z, place.y, 1 - place.core)
        )

    sender(None, send)

    def finish():
        keep.wait()
        other = pair.at[pl.ds(pl.multiple_of((1 - place.core) * rows, rows), rows)]
        remote(
            own, other, sem.at[1], sem.at[2], place.at(place.z, place.y, 1 - place.core)
        ).wait_recv()

    return finish


def swap_scratch(count, arrays):
    return [DMA((arrays,)), DMA((2, arrays, count)), DMA((2, arrays, count))]


class Swap:
    def __init__(self, place, pairs, scratch):
        self.place = place
        self.pairs = pairs
        self.local_sem, self.out_sem, self.side_sem = scratch

    def send(self, index, step):
        place = self.place
        source, spot = self.pairs[index]
        target = lax.rem(place.device + step, place.count)
        return remote(
            source(target),
            spot(place.device, place.side),
            self.out_sem.at[0, index, step],
            self.out_sem.at[1, index, step],
            {"fsdp": target},
        )

    def taken(self, index, step, side):
        device = lax.rem(self.place.device + self.place.count - step, self.place.count)
        return self.pairs[index][1](device, side)

    def come(self, index, step):
        place = self.place
        return remote(
            self.pairs[index][0](place.device),
            self.taken(index, step, place.side),
            self.out_sem.at[0, index, step],
            self.out_sem.at[1, index, step],
            place.across(),
        )

    def share(self, index, step, source=None):
        spot = self.taken(index, step, self.place.side)
        return remote(
            spot if source is None else source,
            spot,
            self.side_sem.at[0, index, step],
            self.side_sem.at[1, index, step],
            self.place.across(),
        )

    def shared(self, index, step):
        spot = self.taken(index, step, 1 - self.place.side)
        return remote(
            spot,
            spot,
            self.side_sem.at[0, index, step],
            self.side_sem.at[1, index, step],
            self.place.across(),
        )

    def keep(self, index):
        place = self.place
        source, spot = self.pairs[index]
        return pltpu.make_async_copy(
            source(place.device), spot(place.device, place.side), self.local_sem.at[index]
        )

    def each(self, first, body):
        def step(number, carry):
            for index in range(len(self.pairs)):
                body(index, number)
            return carry

        lax.fori_loop(first, self.place.count, step, 0)

    def start(self):
        self.each(1, lambda index, step: self.send(index, step).start())
        for index, (source, _) in enumerate(self.pairs):
            self.keep(index).start()
            self.share(index, 0, source(self.place.device)).start()

    def pass_on(self):
        def one(index, step):
            self.come(index, step).wait_recv()
            self.share(index, step).start()

        self.each(1, one)

    def finish(self):
        for index in range(len(self.pairs)):
            self.keep(index).wait()
        self.each(0, lambda index, step: self.shared(index, step).wait_recv())
        self.each(1, lambda index, step: self.send(index, step).wait_send())
        self.each(0, lambda index, step: self.share(index, step).wait_send())


def whole_pair(pieces, whole):
    return (lambda target: pieces.at[target], lambda device, side: whole.at[device, side])


def halves_scratch(arrays):
    return [DMA((3, arrays))]


class Halves:
    def __init__(self, place, halves, wholes, scratch):
        self.place = place
        self.pairs = list(zip(halves, wholes))
        (self.sem,) = scratch

    def keep(self, index):
        half, whole = self.pairs[index]
        return pltpu.make_async_copy(half, whole.at[:, self.place.side], self.sem.at[0, index])

    def copy(self, index, side):
        half, whole = self.pairs[index]
        return remote(
            half,
            whole.at[:, side],
            self.sem.at[1, index],
            self.sem.at[2, index],
            self.place.across(),
        )

    def start(self):
        for index in range(len(self.pairs)):
            self.copy(index, self.place.side).start()
            self.keep(index).start()

    def finish(self):
        for index in range(len(self.pairs)):
            self.keep(index).wait()
            self.copy(index, 1 - self.place.side).wait_recv()
            self.copy(index, self.place.side).wait_send()


REDUCE = 11
GATHER = 6
PIECES = 8


class Pack:
    def __init__(self, place, weights, outs, scratch):
        gate, up, down = weights
        pair, low = outs
        held_gate, held_up, held_down, in_sem, out_sem = scratch
        half, columns = held_gate.shape[0], pair.shape[2] // 2
        down_half = held_down.shape[1]
        rows = pl.ds(pl.multiple_of(place.side * half, half), half)
        self.ins = [
            pltpu.make_async_copy(gate.at[rows], held_gate, in_sem.at[0]),
            pltpu.make_async_copy(up.at[rows], held_up, in_sem.at[1]),
        ]
        self.outs = []
        for member in range(2 * LINE):
            start = (2 * member + place.side) * down_half
            down_rows = pl.ds(pl.multiple_of(start, down_half), down_half)
            self.ins.append(
                pltpu.make_async_copy(
                    down.at[down_rows], held_down.at[member], in_sem.at[2 + member]
                )
            )
            at = pl.ds(member * columns, columns)
            for index, (source, target) in enumerate(
                (
                    (held_gate.at[:, at], pair.at[member, :, pl.ds(0, columns)]),
                    (held_up.at[:, at], pair.at[member, :, pl.ds(columns, columns)]),
                    (held_down.at[member], low.at[member]),
                )
            ):
                sem = out_sem.at[index, member]
                self.outs.append(pltpu.make_async_copy(source, target, sem))

    def fetch(self):
        for copy in self.ins:
            copy.start()

    def put(self):
        for copy in self.ins:
            copy.wait()
        for copy in self.outs:
            copy.start()

    def finish(self):
        for copy in self.outs:
            copy.wait()


def first_kernel(
    own_ref,
    query,
    key,
    value,
    out,
    small,
    gate,
    up,
    down,
    gathered,
    qkv_all,
    out_all,
    small_all,
    pair,
    low,
    *scratch,
):
    place = Place()
    sender = Sender()
    own = scratch[0]
    own[...] = own_ref[...]
    greet_all(place)
    half, columns = qkv_all.shape[2], qkv_all.shape[3] // 3
    out_half = out_all.shape[2]
    rows = pl.ds(pl.multiple_of(place.side * half, half), half)

    def member(target):
        return lax.rem(target, 2 * LINE)

    def column_pair(weight, index):
        def source(target):
            start = pl.multiple_of(member(target) * columns, columns)
            return weight.at[rows, pl.ds(start, columns)]

        def spot(device, side):
            return qkv_all.at[device, side, :, pl.ds(index * columns, columns)]

        return (source, spot)

    def out_source(target):
        start = (2 * member(target) + place.side) * out_half
        return out.at[pl.ds(pl.multiple_of(start, out_half), out_half)]

    pairs = [
        (lambda target: small, lambda device, side: small_all.at[device, side]),
        column_pair(query, 0),
        column_pair(key, 1),
        column_pair(value, 2),
        (out_source, lambda device, side: out_all.at[device, side]),
    ]
    swap = Swap(place, pairs, scratch[GATHER : GATHER + 3])
    pack = Pack(place, (gate, up, down), (pair, low), scratch[GATHER + 3 :])

    def begin():
        swap.start()
        pack.fetch()

    def later():
        pack.put()
        swap.pass_on()

    gather_phase(place, sender, gathered, scratch[:GATHER], begin, later)
    swap.finish()
    pack.finish()
    sender.drain()


def hidden_kernel(
    partial, tokens, gain, pair, down, gathered, branch, hidden, pair_all, down_all, *scratch
):
    place = Place()
    sender = Sender()
    greet(place, True)
    halves = Halves(place, (pair, down), (pair_all, down_all), scratch[REDUCE + GATHER :])
    halves.start()
    reduce_phase(place, sender, partial, scratch[:REDUCE])
    total, own = scratch[4], scratch[REDUCE]
    rows, width = total.shape

    def body(at):
        value = total[at]
        scale = lax.rsqrt(jnp.sum(value * value, axis=1, keepdims=True) / width + EPS)
        result = tokens[at].astype(F32) + value * scale * gain[...]
        branch[at] = value
        hidden[at] = result
        own[at] = result.astype(BF)

    by_rows(rows, body)
    gather_phase(place, sender, gathered, scratch[REDUCE : REDUCE + GATHER])
    halves.finish()
    sender.drain()


def turn_kernel(partial, hidden, cotangent, gain, gathered, outputs, gain_grad, *scratch):
    place = Place()
    sender = Sender()
    greet(place)
    reduce_phase(place, sender, partial, scratch[:REDUCE])
    total, own = scratch[4], scratch[REDUCE]
    out_own = scratch[REDUCE + GATHER]
    rows, width = total.shape
    gain_grad[...] = jnp.zeros_like(gain_grad)

    def body(at):
        value = total[at]
        scale = lax.rsqrt(jnp.sum(value * value, axis=1, keepdims=True) / width + EPS)
        grads = cotangent[at].astype(F32)
        normed = value * scale
        out_own[at] = (hidden[at] + normed * gain[...]).astype(BF)
        gain_grad[...] += jnp.sum(grads * normed, axis=0, keepdims=True)
        gained = gain[...] * grads
        inner = jnp.sum(normed * gained, axis=1, keepdims=True)
        own[at] = (scale * (gained - normed * (inner / width))).astype(BF)

    by_rows(rows, body)
    finish = pair_phase(place, sender, out_own, outputs, scratch[REDUCE + GATHER + 1 :])
    gather_phase(place, sender, gathered, scratch[REDUCE : REDUCE + GATHER])
    finish()
    sender.drain()


class WeightGrads:
    def __init__(self, place, arrays, outs, scratch):
        self.place = place
        self.inner, self.grad_mlp, self.hidden, self.grad_pair = arrays
        self.outs = outs
        self.tall, self.turned, self.inner_turned = scratch[:3]
        self.fulls, self.others = scratch[3:5], scratch[5:7]
        self.fetch_sem, self.side_sem = scratch[7:]
        self.piece = self.tall.shape[3]

    def fetch(self, number, slot):
        columns = pl.ds(pl.multiple_of(number * self.piece, self.piece), self.piece)
        return [
            pltpu.make_async_copy(
                array.at[:, columns], self.tall.at[slot, index], self.fetch_sem.at[slot, index]
            )
            for index, array in enumerate((self.hidden, self.grad_mlp))
        ]

    def side_of(self, index, number, side):
        if index == 0:
            return self.fulls[0].at[number, :, side]
        return self.fulls[1].at[number, side]

    def crossing(self, number, index):
        return remote(
            self.side_of(index, number, 1 - self.place.side),
            self.others[index].at[number],
            self.side_sem.at[0, index, number],
            self.side_sem.at[1, index, number],
            self.place.across(),
        )

    def start(self):
        for copy in self.fetch(0, 0):
            copy.start()
        self.inner_turned[...] = self.inner[...].T

    def one(self, number, carry):
        slot = lax.rem(number, 2)
        for copy in self.fetch(number, slot):
            copy.wait()

        @pl.when(number < PIECES - 1)
        def _():
            for copy in self.fetch(number + 1, 1 - slot):
                copy.start()

        full, low = self.fulls
        self.turned[...] = self.tall[slot, 0].T
        columns = self.grad_pair.shape[1]
        step = columns // 4

        def columns_step(index, carry):
            at = pl.ds(pl.multiple_of(index * step, step), step)
            value = product(self.turned[...], self.grad_pair[:, at]).astype(BF)
            full[number, :, :, :, at] = value.reshape(full.shape[1:4] + (step,))
            return carry

        lax.fori_loop(0, 4, columns_step, 0)
        value = product(self.inner_turned[...], self.tall[slot, 1]).astype(BF)
        low[number] = value.reshape(low.shape[1:])
        for index in range(2):
            self.crossing(number, index).start()
        return carry

    def some(self, which):
        half = PIECES // 2
        lax.fori_loop(which * half, which * half + half, self.one, 0)

    def add(self):
        def step(number, carry):
            for index in range(2):
                self.crossing(number, index).wait_recv()
                own = self.side_of(index, number, self.place.side)[...].astype(F32)
                other = self.others[index][number].astype(F32)
                self.outs[index][number] = (own + other).astype(BF)
            return carry

        lax.fori_loop(0, PIECES, step, 0)

    def finish(self):
        def step(number, carry):
            for index in range(2):
                self.crossing(number, index).wait_send()
            return carry

        lax.fori_loop(0, PIECES, step, 0)


def branch_kernel(
    partial,
    branch,
    cotangent,
    gain,
    inner_low,
    grad_mlp,
    hidden_low,
    grad_pair,
    gathered,
    grad_hidden,
    gain_grad,
    pair_mine,
    down_mine,
    *scratch,
):
    place = Place()
    sender = Sender()
    greet(place, True)
    grads = WeightGrads(
        place,
        (inner_low, grad_mlp, hidden_low, grad_pair),
        (pair_mine, down_mine),
        scratch[REDUCE + GATHER :],
    )
    grads.start()
    reduce_phase(place, sender, partial, scratch[:REDUCE], idle=grads.some)
    total, own = scratch[4], scratch[REDUCE]
    rows, width = total.shape
    gain_grad[...] = jnp.zeros_like(gain_grad)

    def body(at):
        value = branch[at]
        scale = lax.rsqrt(jnp.sum(value * value, axis=1, keepdims=True) / width + EPS)
        grads = cotangent[at].astype(F32) + total[at]
        grad_hidden[at] = grads
        normed = value * scale
        gain_grad[...] += jnp.sum(grads * normed, axis=0, keepdims=True)
        gained = gain[...] * grads
        inner = jnp.sum(normed * gained, axis=1, keepdims=True)
        own[at] = (scale * (gained - normed * (inner / width))).astype(BF)

    by_rows(rows, body)
    gather_phase(
        place, sender, gathered, scratch[REDUCE : REDUCE + GATHER], last=grads.add
    )
    grads.finish()
    sender.drain()


def last_kernel(
    partial,
    grad_hidden,
    qkv,
    out,
    small,
    down,
    result,
    qkv_all,
    out_all,
    small_all,
    down_all,
    *scratch,
):
    place = Place()
    sender = Sender()
    parts = scratch[REDUCE + 1 :]
    swap_sems, halves_sems, parts = parts[:3], parts[3:4], parts[4:]
    qkv_own, qkv_other, out_own, out_other, small_own, small_other, fetch_sem, side_sem = parts
    greet_all(place)
    fetches, crossings = [], []
    for index, (grad, own, other) in enumerate(
        ((qkv, qkv_own, qkv_other), (out, out_own, out_other))
    ):
        fetches.append(
            pltpu.make_async_copy(grad.at[:, place.side], own, fetch_sem.at[index])
        )
        crossings.append(
            remote(
                grad.at[:, 1 - place.side],
                other,
                side_sem.at[0, index],
                side_sem.at[1, index],
                place.across(),
            )
        )
    crossings.append(
        remote(
            small,
            small_other,
            side_sem.at[0, 2],
            side_sem.at[1, 2],
            place.at(place.z, place.y, 1 - place.core),
        )
    )
    for copy in fetches + crossings:
        copy.start()
    pairs = ((small_own, small_all), (qkv_own, qkv_all), (out_own, out_all))
    swap = Swap(place, [whole_pair(*pair) for pair in pairs], swap_sems)
    halves = Halves(place, (down,), (down_all,), halves_sems)
    shared_rows = 2 * partial.shape[1] // place.count // 128

    def between():
        for fetch in fetches:
            fetch.wait()
        for crossing in crossings:
            crossing.wait()
        small_own[...] = small[...]
        small_own[:, :shared_rows] += small_other[:, :shared_rows]

        def one(index, carry):
            qkv_own[index] = (
                qkv_own[index].astype(F32) + qkv_other[index].astype(F32)
            ).astype(BF)
            out_own[index] = (
                out_own[index].astype(F32) + out_other[index].astype(F32)
            ).astype(BF)
            return carry

        lax.fori_loop(0, place.count, one, 0)
        swap.start()
        halves.start()

    reduce_phase(place, sender, partial, scratch[:REDUCE], between, late=swap.pass_on)
    total = scratch[4]

    def body(at):
        total[at] += grad_hidden[at]

    by_rows(total.shape[0], body)
    finish = pair_phase(place, sender, total, result, scratch[REDUCE : REDUCE + 1])
    finish()
    halves.finish()
    swap.finish()
    sender.drain()


def sum_kernel(value, moved, result, arrived, core_in, y_in, held, line_in, sem, side_sem):
    place = Place()
    z, y, core = place.z, place.y, place.core
    barrier = pltpu.get_barrier_semaphore()
    others = [place.at(z, y, 1 - core), place.at(z, 1 - y, core)]
    others += [place.at(lax.rem(z + k, LINE), y, core) for k in range(1, LINE)]
    for device in others + [place.across()]:
        signal(barrier, device)
    pl.semaphore_wait(barrier, len(others) + 1)
    source = moved
    if moved.shape != arrived.shape:
        source = moved.at[:, pl.ds(0, arrived.shape[1])]
    side = remote(source, arrived, side_sem.at[0], side_sem.at[1], place.across())
    side.start()
    first = remote(value, core_in, sem.at[0, 0], sem.at[1, 0], others[0])
    first.start()
    first.wait_recv()
    held[0] = value[...] + core_in[...]
    second = remote(held.at[0], y_in, sem.at[0, 1], sem.at[1, 1], others[1])
    second.start()
    second.wait_recv()
    held[1] = held[0] + y_in[...]
    sends = [
        remote(held.at[1], line_in.at[k - 1], sem.at[0, 1 + k], sem.at[1, 1 + k], others[1 + k])
        for k in range(1, LINE)
    ]
    for send in sends:
        send.start()
    line_in[LINE - 1] = held[1]
    for send in sends:
        send.wait_recv()
    added = jnp.zeros_like(value)
    for source in range(LINE):
        slot = lax.rem(z - source + 2 * LINE - 1, LINE)
        added = added + line_in[slot]
    result[...] = added
    first.wait_send()
    second.wait_send()
    for send in sends:
        send.wait_send()
    side.wait()


def widen_own_kernel(side, own, gate_out, up_out):
    columns = gate_out.shape[1]
    value = jnp.sum(own[:, 0].astype(F32), axis=0)
    gate_out[...] = value[:, :columns]
    up_out[...] = value[:, columns:]


def widen_other_kernel(side, gate, up, other, rest, down, gate_out, up_out, down_out):
    columns = gate_out.shape[1]
    first = other.shape[2]
    for part, start in ((other, 0), (rest, first)):
        value = jnp.sum(part[:, 0].astype(F32), axis=0)
        rows = pl.ds(start, part.shape[2])
        gate_out[rows] = value[:, :columns]
        up_out[rows] = value[:, columns:]
    down_out[...] = jnp.sum(down[:, 0].astype(F32), axis=0)


def talk(kernel, which, shapes, specs, scratch, microseconds, name=None):
    def call(*operands):
        return pl.pallas_call(
            kernel,
            out_shape=shapes,
            in_specs=specs[0],
            out_specs=specs[1],
            scratch_shapes=scratch,
            compiler_params=pltpu.CompilerParams(
                collective_id=which, has_side_effects=True, vmem_limit_bytes=48 << 20
            ),
            cost_estimate=pl.CostEstimate(
                flops=0, bytes_accessed=int(microseconds * 3.0e6), transcendentals=0
            ),
            name=name or kernel.__name__,
        )(*operands)

    return call


class Team:
    def __init__(self, local_heads, rows, width):
        self.fsdp = lax.axis_size("fsdp")
        self.tensor = lax.axis_size("tensor")
        self.size = 2 * LINE
        self.teams = self.fsdp // self.size
        assert self.fsdp % self.size == 0 and self.tensor == 2 and local_heads % self.size == 0
        self.member = lax.rem(lax.axis_index("fsdp"), self.size)
        self.core = lax.axis_index("tensor")
        self.context = lax.axis_index("context")
        self.groups = None
        if self.teams > 1:
            self.groups = [
                [team * self.size + one for one in range(self.size)] for team in range(self.teams)
            ]
        self.rows = rows
        self.width = width
        self.all_low = jax.ShapeDtypeStruct((2 * self.size * rows, width), BF)
        self.own_wide = jax.ShapeDtypeStruct((rows, width), F32)
        self.line_wide = jax.ShapeDtypeStruct((1, width), F32)
        self.reduces = reduce_scratch(rows, width)
        self.gathers = gather_scratch(rows, width)

    def whole(self, pieces):
        shape = (pieces.shape[0], 2) + pieces.shape[1:]
        return jax.ShapeDtypeStruct(shape, pieces.dtype)

    def first(self, own, weights, out, small, gate, up, down):
        rows, columns = weights[0].shape
        rows, columns = rows // 2, columns // self.size
        out_rows = out.shape[0] // self.size // 2
        wide = gate.shape[1]
        low = (self.size, down.shape[0] // self.size // 2, down.shape[1])
        *results, pair, low = talk(
            first_kernel,
            0,
            (
                self.all_low,
                jax.ShapeDtypeStruct((self.fsdp, 2, rows, 3 * columns), BF),
                jax.ShapeDtypeStruct((self.fsdp, 2, out_rows, out.shape[1]), BF),
                jax.ShapeDtypeStruct((self.fsdp, 2) + small.shape, F32),
                jax.ShapeDtypeStruct((self.size, rows, 2 * wide // self.size), BF),
                jax.ShapeDtypeStruct(low, BF),
            ),
            ([VMEM] * 6 + [HBM] * 3, (HBM,) * 6),
            self.gathers
            + swap_scratch(self.fsdp, 5)
            + [
                pltpu.VMEM((rows, wide), BF),
                pltpu.VMEM((rows, wide), BF),
                pltpu.VMEM(low, BF),
                DMA((2 + self.size,)),
                DMA((3, self.size)),
            ],
            80,
        )(own, *weights, out, small, gate, up, down)
        return *results, self.repeat(pair), self.repeat(low)

    def hidden(self, partial, tokens, gain, pair, down):
        return talk(
            hidden_kernel,
            1,
            (self.all_low, self.own_wide, self.own_wide, self.whole(pair), self.whole(down)),
            ([HBM, VMEM, VMEM, VMEM, VMEM], (HBM, VMEM, VMEM, HBM, HBM)),
            self.reduces + self.gathers + halves_scratch(2),
            100,
        )(partial, tokens, gain, pair, down)

    def turn(self, partial, hidden, cotangent, gain):
        pair = jax.ShapeDtypeStruct((2 * self.rows, self.width), BF)
        return talk(
            turn_kernel,
            2,
            (self.all_low, pair, self.line_wide),
            ([HBM, VMEM, VMEM, VMEM], (HBM, HBM, VMEM)),
            self.reduces + self.gathers + [pltpu.VMEM((self.rows, self.width), BF)] + pair_scratch(),
            100,
        )(partial, hidden, cotangent, gain)

    def branch(self, partial, branch, cotangent, gain, inner, grad_mlp, hidden, grad_pair):
        team_rows, units = inner.shape
        columns = grad_pair.shape[1]
        piece = self.width // PIECES
        count = self.fsdp // PIECES
        half = self.width // self.fsdp // 2
        pair_shape = (PIECES, count, half, columns)
        down_shape = (PIECES, units // 2, piece)

        def both(shape):
            return pltpu.VMEM((shape[0], 2) + shape[1:], BF)

        def sides_inside(shape):
            return pltpu.VMEM((shape[0], shape[1], 2) + shape[2:], BF)

        gathered, grad_hidden, gain_grad, pair_mine, down_mine = talk(
            branch_kernel,
            3,
            (
                self.all_low,
                self.own_wide,
                self.line_wide,
                jax.ShapeDtypeStruct(pair_shape, BF),
                jax.ShapeDtypeStruct(down_shape, BF),
            ),
            (
                [HBM, VMEM, VMEM, VMEM, VMEM, HBM, HBM, VMEM],
                (HBM, VMEM, VMEM, VMEM, VMEM),
            ),
            self.reduces
            + self.gathers
            + [
                pltpu.VMEM((2, 2, team_rows, piece), BF),
                pltpu.VMEM((piece, team_rows), BF),
                pltpu.VMEM((units, team_rows), BF),
                sides_inside(pair_shape),
                both(down_shape),
                pltpu.VMEM(pair_shape, BF),
                pltpu.VMEM(down_shape, BF),
                DMA((2, 2)),
                DMA((2, 2, PIECES)),
            ],
            100,
        )(partial, branch, cotangent, gain, inner, grad_mlp, hidden, grad_pair)
        down_mine = down_mine.reshape(PIECES, units // 2, count, piece // count)
        return (
            gathered,
            grad_hidden,
            gain_grad,
            pair_mine.reshape(self.fsdp, half, columns),
            down_mine.transpose(0, 2, 1, 3).reshape(self.fsdp, units // 2, piece // count),
        )

    def last(self, partial, grad_hidden, qkv, out, small, down):
        both = jax.ShapeDtypeStruct((2 * self.rows, self.width), F32)

        def same(array):
            return jax.ShapeDtypeStruct(array.shape, array.dtype)

        def half(array):
            return pltpu.VMEM((array.shape[0],) + array.shape[2:], array.dtype)

        held = pltpu.VMEM(small.shape, small.dtype)
        return talk(
            last_kernel,
            4,
            (both, same(qkv), same(out), self.whole(small), self.whole(down)),
            ([HBM, VMEM, HBM, HBM, VMEM, VMEM], (HBM,) * 5),
            self.reduces
            + pair_scratch()
            + swap_scratch(self.fsdp, 3)
            + halves_scratch(1)
            + [half(qkv), half(qkv), half(out), half(out), held, held, DMA((2,)), DMA((2, 3))],
            80,
        )(partial, grad_hidden, qkv, out, small, down)

    def total(self, values, moved, arrives):
        flat = values.reshape(-1, 128)
        shape = jax.ShapeDtypeStruct(flat.shape, F32)
        scratch = [pltpu.VMEM(flat.shape, F32)] * 2
        scratch += [pltpu.VMEM((2,) + flat.shape, F32), pltpu.VMEM((LINE,) + flat.shape, F32)]
        scratch += [DMA((2, LINE + 1)), DMA((2,))]
        which = 5 + self.sums
        self.sums += 1
        shapes = (shape, jax.ShapeDtypeStruct(arrives, moved.dtype))
        spaces = ([VMEM, HBM], (VMEM, HBM))
        call = talk(sum_kernel, which, shapes, spaces, scratch, 10, "sum_kernel")
        total, came = call(flat, moved)
        return total.reshape(values.shape), came

    sums = 0

    def half(self, array, axis):
        count = array.shape[axis] // 2
        return lax.dynamic_slice_in_dim(array, self.context * count, count, axis)

    def swap(self, pieces):
        return lax.all_to_all(pieces, "fsdp", split_axis=0, concat_axis=0, tiled=True)

    def repeat(self, pieces):
        return jnp.concatenate([pieces] * self.teams, axis=0) if self.teams > 1 else pieces

    def pieces(self, array):
        shape = (-1,) + array.shape[-2:] if array.ndim == 3 else (-1, 2 * array.shape[2], array.shape[3])
        array = array.reshape(shape)
        cut = array.reshape((self.teams, self.size) + array.shape[1:])
        spec = pl.BlockSpec((self.teams, 1) + array.shape[1:], lambda d, side: (0, d, 0, 0))
        return cut, spec

    def widen_own(self, own):
        half, columns = own.shape[1], own.shape[2] // 2
        cut, spec = self.pieces(own)
        wide = pl.BlockSpec((half, columns), lambda d, side: (side[0], d))
        return pl.pallas_call(
            widen_own_kernel,
            grid_spec=pltpu.PrefetchScalarGridSpec(
                num_scalar_prefetch=1, grid=(self.size,), in_specs=[spec], out_specs=[wide] * 2
            ),
            out_shape=[jax.ShapeDtypeStruct((2 * half, self.size * columns), F32)] * 2,
            name="widen_own_kernel",
        )(self.context.reshape(1).astype(jnp.int32), cut)

    def widen_other(self, gate, up, other, rest, down):
        half, columns = other.shape[1] + rest.shape[1], other.shape[2] // 2
        cuts, specs = zip(*[self.pieces(one) for one in (other, rest, down)])
        rows, down_columns = cuts[2].shape[2:]
        wide = pl.BlockSpec((half, columns), lambda d, side: (1 - side[0], d))
        return pl.pallas_call(
            widen_other_kernel,
            grid_spec=pltpu.PrefetchScalarGridSpec(
                num_scalar_prefetch=1,
                grid=(self.size,),
                in_specs=[HBM, HBM] + list(specs),
                out_specs=[wide, wide, pl.BlockSpec((rows, down_columns), lambda d, side: (d, 0))],
            ),
            out_shape=[
                jax.ShapeDtypeStruct(gate.shape, F32),
                jax.ShapeDtypeStruct(up.shape, F32),
                jax.ShapeDtypeStruct((self.size * rows, down_columns), F32),
            ],
            input_output_aliases={1: 0, 2: 1},
            name="widen_other_kernel",
        )(self.context.reshape(1).astype(jnp.int32), gate, up, *cuts)

    def columns_whole(self, came):
        return came.reshape(-1, came.shape[-1])

    def rows_whole(self, came):
        fsdp, two, rows, columns = came.shape
        return came.transpose(1, 2, 0, 3).reshape(two * rows, fsdp * columns)

    def of_columns(self, grad):
        rows, columns = grad.shape
        return grad.astype(BF).reshape(self.fsdp, 2, rows // self.fsdp // 2, columns)

    def of_rows(self, grad):
        rows, columns = grad.shape
        cut = grad.astype(BF).reshape(2, rows // 2, self.fsdp, columns // self.fsdp)
        return cut.transpose(2, 0, 1, 3)

    def added(self, came):
        if self.teams == 1:
            return came.astype(F32)
        came = came.reshape((self.teams, self.size) + came.shape[1:])
        return jnp.sum(came.astype(F32), axis=0)

    def columns_out(self, came, count):
        size, two, rows, columns = came.shape
        return [
            self.added(part.reshape(size, two * rows, -1))
            .transpose(1, 0, 2)
            .reshape(two * rows, -1)
            for part in jnp.split(came, count, axis=3)
        ]

    def rows_out(self, came):
        return self.added(came).reshape(-1, came.shape[-1])


def local(
    tokens,
    cont_lengths,
    w_query,
    w_key,
    w_value,
    w_output,
    query_gain,
    key_gain,
    attn_gain,
    w_gate,
    w_up,
    w_down,
    mlp_gain,
    cotangent,
):
    rows = tokens.shape[0]
    width = tokens.shape[1]
    fsdp = lax.axis_size("fsdp")
    tensor = lax.axis_size("tensor")
    local_heads = query_gain.shape[0]
    head_size = w_query.shape[1] // local_heads
    own_rows = rows // tensor
    team = Team(local_heads, own_rows, width)
    groups = team.size
    team_rows = groups * rows
    heads = local_heads // team.size
    later = lax.axis_index("context") == 1

    tokens_own = lax.dynamic_slice_in_dim(tokens, team.core * own_rows, own_rows, 0)
    grad_out = lax.dynamic_slice_in_dim(cotangent, team.core * own_rows, own_rows, 0)
    cut = query_gain.size
    share = attn_gain.size
    small = [query_gain.reshape(-1), key_gain.reshape(-1), attn_gain, mlp_gain]
    small = jnp.concatenate([one.astype(F32) for one in small + [cont_lengths.reshape(-1)]])
    small = jnp.pad(small, (0, 8 * 128 - small.size)).reshape(8, 128)
    tokens_all, qkv_came, output_came, small_came, pair_mine, down_mine = team.first(
        tokens_own, [w_query, w_key, w_value], w_output, small, w_gate, w_up, w_down
    )
    qkv_w = team.columns_whole(qkv_came)
    output_w = team.rows_whole(output_came)
    all_small = small_came[:, 0].reshape(fsdp, -1)
    query_gains = all_small[:, :cut].reshape(fsdp, local_heads, -1)
    key_gains = all_small[:, cut : 2 * cut].reshape(fsdp, local_heads, -1)
    query_gains = query_gains.transpose(1, 0, 2).reshape(local_heads, head_size)
    key_gains = key_gains.transpose(1, 0, 2).reshape(local_heads, head_size)
    flat_query = lax.dynamic_slice_in_dim(query_gains, team.member * heads, heads, 0).reshape(-1)
    flat_key = lax.dynamic_slice_in_dim(key_gains, team.member * heads, heads, 0).reshape(-1)
    gain_attn = all_small[:, 2 * cut : 2 * cut + share].reshape(1, -1)
    gain_mlp = all_small[:, 2 * cut + share : 2 * cut + 2 * share].reshape(1, -1)

    conts = cont_lengths.shape[1]
    lengths = all_small[:, 2 * cut + 2 * share : 2 * cut + 2 * share + conts].astype(jnp.int32)
    first_group = lax.axis_index("fsdp") - team.member
    lengths = lax.dynamic_slice_in_dim(lengths, first_group, groups, 0)
    segment, offset = jax.vmap(lambda one: layout(one, rows))(lengths)
    row_index = jnp.arange(rows, dtype=jnp.int32)
    positions = jnp.where(later, rows + offset, row_index[None, :])
    own_segment = jnp.where(later, segment, -1)
    cosine, sine = rotary_tables(positions, head_size)
    cosine = cosine[:, :, None, :]
    sine = sine[:, :, None, :]

    pair_came = team.swap(pair_mine)
    down_came = team.swap(down_mine)

    by_head = (groups, rows, heads, head_size)
    raw = product(tokens_all, qkv_w)
    query_raw, key_raw, value_raw = jnp.split(raw, 3, axis=1)
    value_low = value_raw.astype(BF)
    sums, sent_value = team.total(
        jnp.stack([jnp.sum(query_raw * query_raw, axis=1), jnp.sum(key_raw * key_raw, axis=1)]),
        value_low,
        value_low.shape,
    )
    value_low, sent_value = value_low.reshape(by_head), sent_value.reshape(by_head)
    scale_query = lax.rsqrt(sums[0] / width + EPS)[:, None]
    scale_key = lax.rsqrt(sums[1] / width + EPS)[:, None]
    query_norm = query_raw * scale_query * flat_query
    key_norm = key_raw * scale_key * flat_key
    query_low = rotate(query_norm.reshape(by_head), cosine, sine).astype(BF)
    key_low = rotate(key_norm.reshape(by_head), cosine, sine).astype(BF)
    sent_key = lax.ppermute(key_low, "context", [(0, 1)])
    keys_all = jnp.concatenate([sent_key, key_low], axis=1)
    values_all = jnp.concatenate([sent_value, value_low], axis=1)
    key_index = jnp.arange(2 * rows, dtype=jnp.int32)
    key_segment = jnp.concatenate([jnp.full((groups, rows), -2, jnp.int32), own_segment], axis=1)
    remote = (key_index < rows)[None, None, :] & later
    own_keys = (
        (key_index >= rows)[None, None, :]
        & (key_index[None, None, :] - rows <= row_index[None, :, None])
        & (key_segment[:, None, :] == own_segment[:, :, None])
    )
    allowed = (remote | own_keys)[:, None]
    scale = 1.0 / math.sqrt(head_size)
    scores = (
        jnp.einsum("gqhd,gkhd->ghqk", query_low, keys_all, preferred_element_type=F32) * scale
    )
    scores = jnp.where(allowed, scores, -1e30)
    highest = jnp.max(scores, axis=-1, keepdims=True)
    weights = jnp.exp(scores - highest)
    probs = weights / jnp.sum(weights, axis=-1, keepdims=True)
    probs_low = probs.astype(BF)
    mixed = jnp.einsum("ghqk,gkhd->gqhd", probs_low, values_all, preferred_element_type=F32)
    attended_low = mixed.reshape(team_rows, heads * head_size).astype(BF)
    hidden_all, attn_sum, hidden, pair_came, down_came = team.hidden(
        product(attended_low, output_w).astype(BF), tokens_own, gain_attn, pair_came, down_came
    )
    pair_w = team.columns_whole(pair_came)
    down_w = team.rows_whole(down_came)

    gate, upward = jnp.split(product(hidden_all, pair_w), 2, axis=1)
    sigma = jax.nn.sigmoid(gate)
    inner_low = (gate * sigma * upward).astype(BF)
    grad_mlp_all, outputs, grad_mlp_gain = team.turn(
        product(inner_low, down_w).astype(BF), hidden, grad_out, gain_mlp
    )
    grad_inner = product_right(grad_mlp_all, down_w)
    grad_gate_low = (grad_inner * upward * sigma * (1.0 + gate * (1.0 - sigma))).astype(BF)
    grad_up_low = (grad_inner * gate * sigma).astype(BF)
    grad_pair = jnp.concatenate([grad_gate_low, grad_up_low], axis=1)
    grad_branch_all, grad_hidden, grad_attn_gain, pair_mine, down_mine = team.branch(
        product_right(grad_pair, pair_w).astype(BF),
        attn_sum,
        grad_out,
        gain_attn,
        inner_low,
        grad_mlp_all,
        hidden_all,
        grad_pair,
    )
    pair_came = team.swap(pair_mine)
    grad_attended = product_right(grad_branch_all, output_w).astype(BF).reshape(by_head)

    grad_probs = jnp.einsum("gqhd,gkhd->ghqk", grad_attended, values_all, preferred_element_type=F32)
    centre = jnp.sum(probs * grad_probs, axis=-1, keepdims=True)
    grad_scores = (probs * (grad_probs - centre)).astype(BF)
    grad_query_rot = (
        jnp.einsum("ghqk,gkhd->gqhd", grad_scores, keys_all, preferred_element_type=F32) * scale
    )
    grad_keys = (
        jnp.einsum("ghqk,gqhd->gkhd", grad_scores, query_low, preferred_element_type=F32) * scale
    )
    grad_values = jnp.einsum("ghqk,gqhd->gkhd", probs_low, grad_attended, preferred_element_type=F32)
    back_value = lax.ppermute(grad_values[:, :rows].astype(BF), "context", [(1, 0)])
    back_key = lax.ppermute(grad_keys[:, :rows].astype(BF), "context", [(1, 0)])
    grad_key_rot = grad_keys[:, rows:] + back_key.astype(F32)
    grad_value_low = (
        (grad_values[:, rows:] + back_value.astype(F32)).reshape(team_rows, -1).astype(BF)
    )
    grad_query_norm = rotate_back(grad_query_rot, cosine, sine).reshape(team_rows, -1)
    grad_key_norm = rotate_back(grad_key_rot, cosine, sine).reshape(team_rows, -1)
    grad_query_gain = jnp.sum(grad_query_norm * query_raw * scale_query, axis=0)
    grad_key_gain = jnp.sum(grad_key_norm * key_raw * scale_key, axis=0)
    inner_sums = jnp.stack(
        [
            jnp.sum(query_raw * flat_query * grad_query_norm, axis=1),
            jnp.sum(key_raw * flat_key * grad_key_norm, axis=1),
        ]
    )
    inner_sums, pair_came = lax.optimization_barrier((inner_sums, pair_came))
    first = pair_came.shape[1] // 4
    pair_rest = lax.ppermute(pair_came[:, first:], "context", [(0, 1), (1, 0)])
    arrives = (pair_came.shape[0], first, pair_came.shape[2])
    totals, pair_other = team.total(inner_sums, pair_came, arrives)
    late_attended, late_grad, totals = lax.optimization_barrier(
        (attended_low, grad_branch_all, totals)
    )
    output_grad = team.of_rows(product_left(late_attended, late_grad))
    down_mine, totals = lax.optimization_barrier((down_mine, totals))
    down_came = team.swap(down_mine)
    grad_query_low = norm_back(
        query_raw, scale_query, flat_query, grad_query_norm, totals[0][:, None], width
    ).astype(BF)
    grad_key_low = norm_back(
        key_raw, scale_key, flat_key, grad_key_norm, totals[1][:, None], width
    ).astype(BF)
    grad_qkv = jnp.concatenate([grad_query_low, grad_key_low, grad_value_low], axis=1)
    qkv_grad = team.of_columns(product_left(tokens_all, grad_qkv))
    head_share = head_size // fsdp
    small = [
        grad_attn_gain.reshape(fsdp, share),
        grad_mlp_gain.reshape(fsdp, share),
        grad_query_gain.reshape(heads, fsdp, head_share).transpose(1, 0, 2).reshape(fsdp, -1),
        grad_key_gain.reshape(heads, fsdp, head_share).transpose(1, 0, 2).reshape(fsdp, -1),
    ]
    used = 2 * share + 2 * heads * head_share
    small = jnp.concatenate(small + [jnp.zeros((fsdp, 8 * 128 - used), F32)], axis=1)
    gate_own, up_own = team.widen_own(pair_came)
    partial, pair_rest, gate_own, up_own = lax.optimization_barrier(
        (product_right(grad_qkv, qkv_w).astype(BF), pair_rest, gate_own, up_own)
    )
    input_grad, qkv_came, output_came, small_came, down_came = team.last(
        partial,
        grad_hidden,
        qkv_grad,
        output_grad,
        small.reshape(fsdp, 8, 128),
        down_came,
    )
    grad_w_query, grad_w_key, grad_w_value = team.columns_out(qkv_came, 3)
    grad_w_gate, grad_w_up, grad_w_down = team.widen_other(
        gate_own, up_own, pair_other, pair_rest, down_came
    )
    grad_w_output = team.rows_out(output_came)
    came = jnp.sum(small_came, axis=1).reshape(fsdp, -1)
    row_gains = jnp.sum(came[:, : 2 * share], axis=0).reshape(2, share)
    head_gains = team.added(came[:, 2 * share : used]).reshape(team.size, 2, heads, head_share)
    head_gains = head_gains.transpose(1, 0, 2, 3).reshape(2, local_heads, head_share)
    return (
        outputs,
        input_grad,
        grad_w_query,
        grad_w_key,
        grad_w_value,
        grad_w_output,
        head_gains[0],
        head_gains[1],
        row_gains[0],
        grad_w_gate,
        grad_w_up,
        grad_w_down,
        row_gains[1],
    )


def solution(mesh):
    return jax.shard_map(
        local,
        mesh=mesh,
        in_specs=(
            P(("fsdp", "context"), None),
            P("fsdp", None),
            P("fsdp", "tensor"),
            P("fsdp", "tensor"),
            P("fsdp", "tensor"),
            P("tensor", "fsdp"),
            P("tensor", "fsdp"),
            P("tensor", "fsdp"),
            P("fsdp"),
            P("fsdp", "tensor"),
            P("fsdp", "tensor"),
            P("tensor", "fsdp"),
            P("fsdp"),
            P(("fsdp", "context"), None),
        ),
        out_specs=(
            P(("fsdp", "context"), None),
            P(("fsdp", "context"), None),
            P("fsdp", "tensor"),
            P("fsdp", "tensor"),
            P("fsdp", "tensor"),
            P("tensor", "fsdp"),
            P("tensor", "fsdp"),
            P("tensor", "fsdp"),
            P("fsdp"),
            P("fsdp", "tensor"),
            P("fsdp", "tensor"),
            P("tensor", "fsdp"),
            P("fsdp"),
        ),
        check_vma=False,
    )
```

```python
import functools
import math

import jax
import jax.numpy as jnp
from jax import lax
from jax.experimental import pallas as pl
from jax.experimental.pallas import tpu as pltpu
from jax.sharding import PartitionSpec as P

EPS = 1e-06
THETA = 500000.0
BF = jnp.bfloat16
F32 = jnp.float32


def product(left, right):
    return jnp.dot(left, right, preferred_element_type=F32)


def product_left(left, right):
    return jnp.einsum("rd,rf->df", left, right, preferred_element_type=F32)


def product_right(left, right):
    return jnp.einsum("rf,df->rd", left, right, preferred_element_type=F32)


def rotary_tables(positions, head_size):
    half = head_size // 2
    inverse = jnp.exp(-(2.0 * jnp.arange(half, dtype=F32) / head_size) * math.log(THETA))
    angles = positions.astype(F32)[..., None] * inverse
    angles = jnp.concatenate([angles, angles], axis=-1)
    return (jnp.cos(angles), jnp.sin(angles))


def rotate(values, cosine, sine):
    half = values.shape[-1] // 2
    turned = jnp.concatenate([-values[..., half:], values[..., :half]], axis=-1)
    return values * cosine + turned * sine


def rotate_back(grads, cosine, sine):
    half = grads.shape[-1] // 2
    scaled = grads * sine
    turned = jnp.concatenate([scaled[..., half:], -scaled[..., :half]], axis=-1)
    return grads * cosine + turned


def norm_back(values, scale, gain, grads, total, width):
    return scale * gain * grads - values * scale * scale * scale * (total / width)


def layout(lengths, rows):
    segment_ends = jnp.cumsum(lengths)
    segment_starts = segment_ends - lengths
    row_index = jnp.arange(rows, dtype=jnp.int32)
    segment = jnp.sum((row_index[:, None] >= segment_ends[None, :]).astype(jnp.int32), axis=1)
    chosen = segment[:, None] == jnp.arange(lengths.shape[0], dtype=jnp.int32)[None, :]
    offset = row_index - jnp.sum(jnp.where(chosen, segment_starts[None, :], 0), axis=1)
    return (segment, offset)


LINE = 4
CHUNK = 16
FEW = 8
MESH_ID = pl.DeviceIdType.MESH
HBM = pl.BlockSpec(memory_space=pl.ANY)
VMEM = pl.BlockSpec(memory_space=pltpu.VMEM)
DMA = pltpu.SemaphoreType.DMA


class Place:
    def __init__(self):
        device = lax.axis_index("fsdp")
        member = lax.rem(device, 2 * LINE)
        self.base = device - member
        self.z = member // 2
        self.y = lax.rem(member, 2)
        self.core = lax.axis_index("tensor")
        self.side = lax.axis_index("context")
        self.device = device
        self.count = lax.axis_size("fsdp")

    def across(self):
        return {"context": 1 - self.side}

    def at(self, z, y, core):
        return {"fsdp": self.base + 2 * z + y, "tensor": core}

    def near(self):
        yield None, self.at(self.z, self.y, 1 - self.core)
        yield None, self.at(self.z, 1 - self.y, self.core)
        yield self.z > 0, self.at(self.z - 1, self.y, self.core)
        yield self.z < LINE - 1, self.at(self.z + 1, self.y, self.core)

    def rows(self, z, y, core, count):
        start = ((2 * z + y) * 2 + core) * count
        return pl.ds(pl.multiple_of(start, count), count)


def guarded(condition, action):
    if condition is None:
        action()
    else:
        pl.when(condition)(action)


def signal(barrier, device):
    pl.semaphore_signal(barrier, inc=1, device_id=device, device_id_type=MESH_ID)


def greet(place, across=False):
    barrier = pltpu.get_barrier_semaphore()
    for condition, device in place.near():
        guarded(condition, functools.partial(signal, barrier, device))
    if across:
        signal(barrier, place.across())
    inside = (place.z > 0) & (place.z < LINE - 1)
    pl.semaphore_wait(barrier, jnp.where(inside, 4, 3) + int(across))


def greet_all(place):
    barrier = pltpu.get_barrier_semaphore()

    def one(step, carry):
        signal(barrier, {"fsdp": lax.rem(place.device + step, place.count)})
        return carry

    lax.fori_loop(1, place.count, one, 0)
    signal(barrier, place.across())
    signal(barrier, place.at(place.z, place.y, 1 - place.core))
    pl.semaphore_wait(barrier, place.count + 1)


class Sender:
    def __init__(self):
        self.sent = []

    def __call__(self, condition, make):
        def start():
            make().start()

        guarded(condition, start)
        self.sent.append((condition, make))

    def drain(self):
        for condition, make in self.sent:

            def wait(make=make):
                make().wait_send()

            guarded(condition, wait)


def remote(source, target, send, receive, device):
    return pltpu.make_async_remote_copy(
        src_ref=source,
        dst_ref=target,
        send_sem=send,
        recv_sem=receive,
        device_id=device,
        device_id_type=MESH_ID,
    )


def by_rows(rows, body, first=0):
    def step(index, carry):
        body(pl.ds(pl.multiple_of(index * CHUNK, CHUNK), CHUNK))
        return carry

    lax.fori_loop(first // CHUNK, rows // CHUNK, step, 0)


def reduce_scratch(rows, width):
    return [
        pltpu.VMEM((2 * LINE, rows, width), BF),
        pltpu.VMEM((2 * LINE, rows, width), BF),
        pltpu.VMEM((LINE, rows, width), BF),
        pltpu.VMEM((LINE + 1, rows, width), BF),
        pltpu.VMEM((rows, width), F32),
        DMA((2 * LINE,)),
        DMA((2, 2 * LINE)),
        DMA((2, LINE)),
        DMA((2, LINE + 1)),
        pltpu.VMEM((LINE + 1, rows // FEW, width), BF),
        DMA((2, LINE + 1)),
    ]


def reduce_phase(place, sender, partial, scratch, between=None, idle=None, late=None):
    mine, core_in, y_in, line_in, total, local_sem, core_sem, y_sem, line_sem = scratch[:9]
    few_in, few_sem = scratch[9:]
    rows = total.shape[0]
    few = rows // FEW
    z, y, core = place.z, place.y, place.core
    low = z < LINE // 2
    order = []
    for k in range(LINE - 1):
        down = LINE - 1 - k
        down = jnp.where(down <= z, down - 1, down)
        up = jnp.where(k >= z, k + 1, k)
        order.append(jnp.where(low, down, up))
    order.append(z)

    def fetch(slot):
        half = lax.rem(slot, 2)
        return pltpu.make_async_copy(
            partial.at[place.rows(slot // 2, half, core, rows)], mine.at[slot], local_sem.at[slot]
        )

    def to_core(slot):
        half = lax.rem(slot, 2)
        return remote(
            partial.at[place.rows(slot // 2, half, 1 - core, rows)],
            core_in.at[slot],
            core_sem.at[0, slot],
            core_sem.at[1, slot],
            place.at(z, y, 1 - core),
        )

    def to_y(block, first):
        at = pl.ds(first, rows - first)
        return remote(
            mine.at[2 * block + 1 - y, at],
            y_in.at[block, at],
            y_sem.at[0, block],
            y_sem.at[1, block],
            place.at(z, 1 - y, core),
        )

    def few_along(block):
        step = jnp.where(block > z, 1, -1)
        slot = jnp.where((step < 0) & (block == z - 1), LINE, block)
        return remote(
            mine.at[2 * block + 1 - y, pl.ds(0, few)],
            few_in.at[slot],
            few_sem.at[0, block],
            few_sem.at[1, slot],
            place.at(z + step, y, core),
        )

    def add_few(slot, source):
        remote(
            mine.at[0, pl.ds(0, few)],
            few_in.at[source],
            few_sem.at[0, 0],
            few_sem.at[1, source],
            place.at(z, y, 1 - core),
        ).wait_recv()

        def add(at):
            value = mine[slot, at].astype(F32) + few_in[source, at].astype(F32)
            mine[slot, at] = value.astype(BF)

        by_rows(few, add)

    def to_line(block):
        step = jnp.where(block > z, 1, -1)
        slot = jnp.where((step < 0) & (block == z - 1), LINE, block)
        return remote(
            mine.at[2 * block + y],
            line_in.at[slot],
            line_sem.at[0, block],
            line_sem.at[1, slot],
            place.at(z + step, y, core),
        )

    def from_line(slot):
        return remote(
            mine.at[0],
            line_in.at[slot],
            line_sem.at[0, 0],
            line_sem.at[1, slot],
            place.at(z, y, 1 - core),
        )

    for half in (1 - y, y):
        for block in order:
            sender(None, functools.partial(to_core, 2 * block + half))
            fetch(2 * block + half).start()

    for number, block in enumerate(order):
        slot = 2 * block + 1 - y
        fetch(slot).wait()
        to_core(slot).wait_recv()

        def add(at, slot=slot):
            value = mine[slot, at].astype(F32) + core_in[slot, at].astype(F32)
            mine[slot, at] = value.astype(BF)

        by_rows(rows, add)
        if number == LINE - 1:
            pl.when(z > 0)(functools.partial(add_few, slot, z))
            pl.when(z < LINE - 1)(functools.partial(add_few, slot, LINE))
            sender(None, functools.partial(to_y, block, 0))
        else:
            sender(None, functools.partial(to_y, block, few))
            inner = jnp.where(block > z, z > 0, z < LINE - 1)
            pl.when(inner)(functools.partial(add_few, slot, block))
            sender(None, functools.partial(few_along, block))

    for number, block in enumerate(order[:-1]):
        if number == LINE - 2 and between is not None:
            between()
        if idle is not None:
            idle(number)
        slot = 2 * block + y
        fetch(slot).wait()
        to_core(slot).wait_recv()
        to_y(block, few).wait_recv()
        inner = jnp.where(block > z, z > 0, z < LINE - 1)

        @pl.when(inner)
        def _(block=block, slot=slot):
            from_line(block).wait_recv()

            def add_first(at):
                value = mine[slot, at].astype(F32) + core_in[slot, at].astype(F32)
                mine[slot, at] = (value + line_in[block, at].astype(F32)).astype(BF)

            def add(at):
                value = mine[slot, at].astype(F32) + core_in[slot, at].astype(F32)
                value = value + y_in[block, at].astype(F32)
                mine[slot, at] = (value + line_in[block, at].astype(F32)).astype(BF)

            by_rows(few, add_first)
            by_rows(rows, add, few)

        @pl.when(jnp.logical_not(inner))
        def _(block=block, slot=slot):
            def add_first(at):
                value = mine[slot, at].astype(F32) + core_in[slot, at].astype(F32)
                mine[slot, at] = value.astype(BF)

            def add(at):
                value = mine[slot, at].astype(F32) + core_in[slot, at].astype(F32)
                mine[slot, at] = (value + y_in[block, at].astype(F32)).astype(BF)

            by_rows(few, add_first)
            by_rows(rows, add, few)

        sender(None, functools.partial(to_line, block))

    if late is not None:
        late()
    slot = 2 * z + y
    fetch(slot).wait()
    to_core(slot).wait_recv()
    to_y(z, 0).wait_recv()

    def start(at):
        value = mine[slot, at].astype(F32) + core_in[slot, at].astype(F32)
        total[at] = value + y_in[z, at].astype(F32)

    by_rows(rows, start)
    for condition, source in ((z > 0, z), (z < LINE - 1, LINE)):

        @pl.when(condition)
        def _(source=source):
            from_line(source).wait_recv()

            def add(at):
                total[at] += line_in[source, at].astype(F32)

            by_rows(rows, add)


def gather_scratch(rows, width):
    return [
        pltpu.VMEM((rows, width), BF),
        DMA((1,)),
        DMA((2, 2 * LINE)),
        DMA((2, LINE)),
        DMA((2, LINE + 2)),
        DMA((2, LINE + 2)),
    ]


def gather_phase(place, sender, gathered, scratch, between=None, later=None, last=None):
    own, local_sem, core_sem, y_sem, line_sem, few_sem = scratch
    rows = own.shape[0]
    few = rows // FEW
    z, y, core = place.z, place.y, place.core

    def spot(block, half):
        return gathered.at[place.rows(block, half, core, rows)]

    def to_core(source, block, half):
        return remote(
            source,
            spot(block, half),
            core_sem.at[0, 2 * block + half],
            core_sem.at[1, 2 * block + half],
            place.at(z, y, 1 - core),
        )

    def to_y(source, block):
        return remote(
            source,
            spot(block, y),
            y_sem.at[0, block],
            y_sem.at[1, block],
            place.at(z, 1 - y, core),
        )

    def to_line(source, block, step, index):
        return remote(
            source,
            spot(block, y),
            line_sem.at[0, index],
            line_sem.at[1, block],
            place.at(z + step, y, core),
        )

    def some(block, half, first, count):
        start = ((2 * block + half) * 2 + core) * rows + first
        return gathered.at[pl.ds(pl.multiple_of(start, few), count)]

    def rest_to_y(half, block):
        return remote(
            some(block, half, few, rows - few),
            some(block, half, few, rows - few),
            y_sem.at[0, block],
            y_sem.at[1, block],
            place.at(z, 1 - y, core),
        )

    def few_along(block, step, index):
        return remote(
            some(block, 1 - y, 0, few),
            some(block, 1 - y, 0, few),
            few_sem.at[0, index],
            few_sem.at[1, block],
            place.at(z + step, y, core),
        )

    keep = pltpu.make_async_copy(own, spot(z, y), local_sem.at[0])
    keep.start()
    sender(z < LINE - 1, functools.partial(to_line, own, z, 1, LINE))
    sender(z > 0, functools.partial(to_line, own, z, -1, LINE + 1))
    sender(None, functools.partial(to_y, own, z))
    sender(None, functools.partial(to_core, own, z, y))
    if between is not None:
        between()

    def took_y(block):
        remote(
            own,
            spot(block, 1 - y),
            y_sem.at[0, block],
            y_sem.at[1, block],
            place.at(z, 1 - y, core),
        ).wait_recv()

    def across_own():
        took_y(z)
        sender(z < LINE - 1, functools.partial(few_along, z, 1, LINE))
        sender(z > 0, functools.partial(few_along, z, -1, LINE + 1))
        sender(None, lambda: to_core(spot(z, 1 - y), z, 1 - y))

    def across(condition, block, step):
        guarded(condition, lambda: few_along(block, step, block).wait_recv())
        onward = condition & ((z < LINE - 1) if step > 0 else (z > 0))
        sender(onward, functools.partial(few_along, block, step, block))
        guarded(condition, lambda: rest_to_y(1 - y, block).wait_recv())
        sender(condition, lambda: to_core(spot(block, 1 - y), block, 1 - y))

    def along(condition, block, step):
        def took():
            to_line(own, block, step, block).wait_recv()

        guarded(condition, took)
        onward = condition & ((z < LINE - 1) if step > 0 else (z > 0))
        sender(onward, lambda: to_line(spot(block, y), block, step, block))
        sender(condition, lambda: rest_to_y(y, block))
        sender(condition, lambda: to_core(spot(block, y), block, y))

    for distance in range(1, LINE + 1):
        if distance < LINE:
            along(z >= distance, z - distance, 1)
            along(z + distance < LINE, z + distance, -1)
        if distance == 1:
            across_own()
        else:
            across(z >= distance - 1, z - distance + 1, 1)
            across(z + distance - 1 < LINE, z + distance - 1, -1)
        if distance == 1 and later is not None:
            later()
        if distance == LINE - 1 and last is not None:
            last()

    keep.wait()
    for block in range(LINE):
        for half in range(2):
            remote(
                own,
                gathered.at[place.rows(block, half, 1 - core, rows)],
                core_sem.at[0, 2 * block + half],
                core_sem.at[1, 2 * block + half],
                place.at(z, y, 1 - core),
            ).wait_recv()


def pair_scratch():
    return [DMA((3,))]


def pair_phase(place, sender, own, pair, scratch):
    (sem,) = scratch
    rows = own.shape[0]
    spot = pair.at[pl.ds(pl.multiple_of(place.core * rows, rows), rows)]
    keep = pltpu.make_async_copy(own, spot, sem.at[0])
    keep.start()

    def send():
        return remote(
            own, spot, sem.at[1], sem.at[2], place.at(place.z, place.y, 1 - place.core)
        )

    sender(None, send)

    def finish():
        keep.wait()
        other = pair.at[pl.ds(pl.multiple_of((1 - place.core) * rows, rows), rows)]
        remote(
            own, other, sem.at[1], sem.at[2], place.at(place.z, place.y, 1 - place.core)
        ).wait_recv()

    return finish


def swap_scratch(count, arrays):
    return [DMA((arrays,)), DMA((2, arrays, count)), DMA((2, arrays, count))]


class Swap:
    def __init__(self, place, pairs, scratch):
        self.place = place
        self.pairs = pairs
        self.local_sem, self.out_sem, self.side_sem = scratch

    def send(self, index, step):
        place = self.place
        source, spot = self.pairs[index]
        target = lax.rem(place.device + step, place.count)
        return remote(
            source(target),
            spot(place.device, place.side),
            self.out_sem.at[0, index, step],
            self.out_sem.at[1, index, step],
            {"fsdp": target},
        )

    def taken(self, index, step, side):
        device = lax.rem(self.place.device + self.place.count - step, self.place.count)
        return self.pairs[index][1](device, side)

    def come(self, index, step):
        place = self.place
        return remote(
            self.pairs[index][0](place.device),
            self.taken(index, step, place.side),
            self.out_sem.at[0, index, step],
            self.out_sem.at[1, index, step],
            place.across(),
        )

    def share(self, index, step, source=None):
        spot = self.taken(index, step, self.place.side)
        return remote(
            spot if source is None else source,
            spot,
            self.side_sem.at[0, index, step],
            self.side_sem.at[1, index, step],
            self.place.across(),
        )

    def shared(self, index, step):
        spot = self.taken(index, step, 1 - self.place.side)
        return remote(
            spot,
            spot,
            self.side_sem.at[0, index, step],
            self.side_sem.at[1, index, step],
            self.place.across(),
        )

    def keep(self, index):
        place = self.place
        source, spot = self.pairs[index]
        return pltpu.make_async_copy(
            source(place.device), spot(place.device, place.side), self.local_sem.at[index]
        )

    def each(self, first, body):
        def step(number, carry):
            for index in range(len(self.pairs)):
                body(index, number)
            return carry

        lax.fori_loop(first, self.place.count, step, 0)

    def start(self):
        self.each(1, lambda index, step: self.send(index, step).start())
        for index, (source, _) in enumerate(self.pairs):
            self.keep(index).start()
            self.share(index, 0, source(self.place.device)).start()

    def pass_on(self):
        def one(index, step):
            self.come(index, step).wait_recv()
            self.share(index, step).start()

        self.each(1, one)

    def finish(self):
        for index in range(len(self.pairs)):
            self.keep(index).wait()
        self.each(0, lambda index, step: self.shared(index, step).wait_recv())
        self.each(1, lambda index, step: self.send(index, step).wait_send())
        self.each(0, lambda index, step: self.share(index, step).wait_send())


def whole_pair(pieces, whole):
    return (lambda target: pieces.at[target], lambda device, side: whole.at[device, side])


def halves_scratch(arrays):
    return [DMA((3, arrays))]


class Halves:
    def __init__(self, place, halves, wholes, scratch):
        self.place = place
        self.pairs = list(zip(halves, wholes))
        (self.sem,) = scratch

    def keep(self, index):
        half, whole = self.pairs[index]
        return pltpu.make_async_copy(half, whole.at[:, self.place.side], self.sem.at[0, index])

    def copy(self, index, side):
        half, whole = self.pairs[index]
        return remote(
            half,
            whole.at[:, side],
            self.sem.at[1, index],
            self.sem.at[2, index],
            self.place.across(),
        )

    def start(self):
        for index in range(len(self.pairs)):
            self.copy(index, self.place.side).start()
            self.keep(index).start()

    def finish(self):
        for index in range(len(self.pairs)):
            self.keep(index).wait()
            self.copy(index, 1 - self.place.side).wait_recv()
            self.copy(index, self.place.side).wait_send()


REDUCE = 11
GATHER = 6
PIECES = 8


class Pack:
    def __init__(self, place, weights, outs, scratch):
        gate, up, down = weights
        pair, low = outs
        held_gate, held_up, held_down, in_sem, out_sem = scratch
        half, columns = held_gate.shape[0], pair.shape[2] // 2
        down_half = held_down.shape[1]
        rows = pl.ds(pl.multiple_of(place.side * half, half), half)
        self.ins = [
            pltpu.make_async_copy(gate.at[rows], held_gate, in_sem.at[0]),
            pltpu.make_async_copy(up.at[rows], held_up, in_sem.at[1]),
        ]
        self.outs = []
        for member in range(2 * LINE):
            start = (2 * member + place.side) * down_half
            down_rows = pl.ds(pl.multiple_of(start, down_half), down_half)
            self.ins.append(
                pltpu.make_async_copy(
                    down.at[down_rows], held_down.at[member], in_sem.at[2 + member]
                )
            )
            at = pl.ds(member * columns, columns)
            for index, (source, target) in enumerate(
                (
                    (held_gate.at[:, at], pair.at[member, :, pl.ds(0, columns)]),
                    (held_up.at[:, at], pair.at[member, :, pl.ds(columns, columns)]),
                    (held_down.at[member], low.at[member]),
                )
            ):
                sem = out_sem.at[index, member]
                self.outs.append(pltpu.make_async_copy(source, target, sem))

    def fetch(self):
        for copy in self.ins:
            copy.start()

    def put(self):
        for copy in self.ins:
            copy.wait()
        for copy in self.outs:
            copy.start()

    def finish(self):
        for copy in self.outs:
            copy.wait()


def first_kernel(
    own_ref,
    query,
    key,
    value,
    out,
    small,
    gate,
    up,
    down,
    gathered,
    qkv_all,
    out_all,
    small_all,
    pair,
    low,
    *scratch,
):
    place = Place()
    sender = Sender()
    own = scratch[0]
    own[...] = own_ref[...]
    greet_all(place)
    half, columns = qkv_all.shape[2], qkv_all.shape[3] // 3
    out_half = out_all.shape[2]
    rows = pl.ds(pl.multiple_of(place.side * half, half), half)

    def member(target):
        return lax.rem(target, 2 * LINE)

    def column_pair(weight, index):
        def source(target):
            start = pl.multiple_of(member(target) * columns, columns)
            return weight.at[rows, pl.ds(start, columns)]

        def spot(device, side):
            return qkv_all.at[device, side, :, pl.ds(index * columns, columns)]

        return (source, spot)

    def out_source(target):
        start = (2 * member(target) + place.side) * out_half
        return out.at[pl.ds(pl.multiple_of(start, out_half), out_half)]

    pairs = [
        (lambda target: small, lambda device, side: small_all.at[device, side]),
        column_pair(query, 0),
        column_pair(key, 1),
        column_pair(value, 2),
        (out_source, lambda device, side: out_all.at[device, side]),
    ]
    swap = Swap(place, pairs, scratch[GATHER : GATHER + 3])
    pack = Pack(place, (gate, up, down), (pair, low), scratch[GATHER + 3 :])

    def begin():
        swap.start()
        pack.fetch()

    def later():
        pack.put()
        swap.pass_on()

    gather_phase(place, sender, gathered, scratch[:GATHER], begin, later)
    swap.finish()
    pack.finish()
    sender.drain()


def hidden_kernel(
    partial, tokens, gain, pair, down, gathered, branch, hidden, pair_all, down_all, *scratch
):
    place = Place()
    sender = Sender()
    greet(place, True)
    halves = Halves(place, (pair, down), (pair_all, down_all), scratch[REDUCE + GATHER :])
    halves.start()
    reduce_phase(place, sender, partial, scratch[:REDUCE])
    total, own = scratch[4], scratch[REDUCE]
    rows, width = total.shape

    def body(at):
        value = total[at]
        scale = lax.rsqrt(jnp.sum(value * value, axis=1, keepdims=True) / width + EPS)
        result = tokens[at].astype(F32) + value * scale * gain[...]
        branch[at] = value
        hidden[at] = result
        own[at] = result.astype(BF)

    by_rows(rows, body)
    gather_phase(place, sender, gathered, scratch[REDUCE : REDUCE + GATHER])
    halves.finish()
    sender.drain()


def turn_kernel(partial, hidden, cotangent, gain, gathered, outputs, gain_grad, *scratch):
    place = Place()
    sender = Sender()
    greet(place)
    reduce_phase(place, sender, partial, scratch[:REDUCE])
    total, own = scratch[4], scratch[REDUCE]
    out_own = scratch[REDUCE + GATHER]
    rows, width = total.shape
    gain_grad[...] = jnp.zeros_like(gain_grad)

    def body(at):
        value = total[at]
        scale = lax.rsqrt(jnp.sum(value * value, axis=1, keepdims=True) / width + EPS)
        grads = cotangent[at].astype(F32)
        normed = value * scale
        out_own[at] = (hidden[at] + normed * gain[...]).astype(BF)
        gain_grad[...] += jnp.sum(grads * normed, axis=0, keepdims=True)
        gained = gain[...] * grads
        inner = jnp.sum(normed * gained, axis=1, keepdims=True)
        own[at] = (scale * (gained - normed * (inner / width))).astype(BF)

    by_rows(rows, body)
    finish = pair_phase(place, sender, out_own, outputs, scratch[REDUCE + GATHER + 1 :])
    gather_phase(place, sender, gathered, scratch[REDUCE : REDUCE + GATHER])
    finish()
    sender.drain()


class WeightGrads:
    def __init__(self, place, arrays, outs, scratch):
        self.place = place
        self.inner, self.grad_mlp, self.hidden, self.grad_pair = arrays
        self.outs = outs
        self.tall, self.turned, self.inner_turned = scratch[:3]
        self.fulls, self.others = scratch[3:5], scratch[5:7]
        self.fetch_sem, self.side_sem = scratch[7:]
        self.piece = self.tall.shape[3]

    def fetch(self, number, slot):
        columns = pl.ds(pl.multiple_of(number * self.piece, self.piece), self.piece)
        return [
            pltpu.make_async_copy(
                array.at[:, columns], self.tall.at[slot, index], self.fetch_sem.at[slot, index]
            )
            for index, array in enumerate((self.hidden, self.grad_mlp))
        ]

    def side_of(self, index, number, side):
        if index == 0:
            return self.fulls[0].at[number, :, side]
        return self.fulls[1].at[number, side]

    def crossing(self, number, index):
        return remote(
            self.side_of(index, number, 1 - self.place.side),
            self.others[index].at[number],
            self.side_sem.at[0, index, number],
            self.side_sem.at[1, index, number],
            self.place.across(),
        )

    def start(self):
        for copy in self.fetch(0, 0):
            copy.start()
        self.inner_turned[...] = self.inner[...].T

    def one(self, number, carry):
        slot = lax.rem(number, 2)
        for copy in self.fetch(number, slot):
            copy.wait()

        @pl.when(number < PIECES - 1)
        def _():
            for copy in self.fetch(number + 1, 1 - slot):
                copy.start()

        full, low = self.fulls
        self.turned[...] = self.tall[slot, 0].T
        columns = self.grad_pair.shape[1]
        step = columns // 4

        def columns_step(index, carry):
            at = pl.ds(pl.multiple_of(index * step, step), step)
            value = product(self.turned[...], self.grad_pair[:, at]).astype(BF)
            full[number, :, :, :, at] = value.reshape(full.shape[1:4] + (step,))
            return carry

        lax.fori_loop(0, 4, columns_step, 0)
        value = product(self.inner_turned[...], self.tall[slot, 1]).astype(BF)
        low[number] = value.reshape(low.shape[1:])
        for index in range(2):
            self.crossing(number, index).start()
        return carry

    def some(self, one):
        slots = LINE - 1
        first, end = (PIECES * one + slots - 1) // slots, (PIECES * (one + 1) + slots - 1) // slots
        lax.fori_loop(first, end, self.one, 0)

    def add(self):
        def step(number, carry):
            for index in range(2):
                self.crossing(number, index).wait_recv()
                own = self.side_of(index, number, self.place.side)[...].astype(F32)
                other = self.others[index][number].astype(F32)
                self.outs[index][number] = (own + other).astype(BF)
            return carry

        lax.fori_loop(0, PIECES, step, 0)

    def finish(self):
        def step(number, carry):
            for index in range(2):
                self.crossing(number, index).wait_send()
            return carry

        lax.fori_loop(0, PIECES, step, 0)


def branch_kernel(
    partial,
    branch,
    cotangent,
    gain,
    inner_low,
    grad_mlp,
    hidden_low,
    grad_pair,
    gathered,
    grad_hidden,
    gain_grad,
    pair_mine,
    down_mine,
    *scratch,
):
    place = Place()
    sender = Sender()
    greet(place, True)
    grads = WeightGrads(
        place,
        (inner_low, grad_mlp, hidden_low, grad_pair),
        (pair_mine, down_mine),
        scratch[REDUCE + GATHER :],
    )
    grads.start()
    reduce_phase(place, sender, partial, scratch[:REDUCE], idle=grads.some)
    total, own = scratch[4], scratch[REDUCE]
    rows, width = total.shape
    gain_grad[...] = jnp.zeros_like(gain_grad)

    def body(at):
        value = branch[at]
        scale = lax.rsqrt(jnp.sum(value * value, axis=1, keepdims=True) / width + EPS)
        grads = cotangent[at].astype(F32) + total[at]
        grad_hidden[at] = grads
        normed = value * scale
        gain_grad[...] += jnp.sum(grads * normed, axis=0, keepdims=True)
        gained = gain[...] * grads
        inner = jnp.sum(normed * gained, axis=1, keepdims=True)
        own[at] = (scale * (gained - normed * (inner / width))).astype(BF)

    by_rows(rows, body)
    gather_phase(
        place, sender, gathered, scratch[REDUCE : REDUCE + GATHER], last=grads.add
    )
    grads.finish()
    sender.drain()


def last_kernel(
    partial,
    grad_hidden,
    qkv,
    out,
    small,
    down,
    result,
    qkv_all,
    out_all,
    small_all,
    down_all,
    *scratch,
):
    place = Place()
    sender = Sender()
    parts = scratch[REDUCE + 1 :]
    swap_sems, halves_sems, parts = parts[:3], parts[3:4], parts[4:]
    qkv_own, qkv_other, out_own, out_other, small_own, small_other, fetch_sem, side_sem = parts
    greet_all(place)
    fetches, crossings = [], []
    for index, (grad, own, other) in enumerate(
        ((qkv, qkv_own, qkv_other), (out, out_own, out_other))
    ):
        fetches.append(
            pltpu.make_async_copy(grad.at[:, place.side], own, fetch_sem.at[index])
        )
        crossings.append(
            remote(
                grad.at[:, 1 - place.side],
                other,
                side_sem.at[0, index],
                side_sem.at[1, index],
                place.across(),
            )
        )
    crossings.append(
        remote(
            small,
            small_other,
            side_sem.at[0, 2],
            side_sem.at[1, 2],
            place.at(place.z, place.y, 1 - place.core),
        )
    )
    for copy in fetches + crossings:
        copy.start()
    pairs = ((small_own, small_all), (qkv_own, qkv_all), (out_own, out_all))
    swap = Swap(place, [whole_pair(*pair) for pair in pairs], swap_sems)
    halves = Halves(place, (down,), (down_all,), halves_sems)
    shared_rows = 2 * partial.shape[1] // place.count // 128

    def between():
        for fetch in fetches:
            fetch.wait()
        for crossing in crossings:
            crossing.wait()
        small_own[...] = small[...]
        small_own[:, :shared_rows] += small_other[:, :shared_rows]

        def one(index, carry):
            qkv_own[index] = (
                qkv_own[index].astype(F32) + qkv_other[index].astype(F32)
            ).astype(BF)
            out_own[index] = (
                out_own[index].astype(F32) + out_other[index].astype(F32)
            ).astype(BF)
            return carry

        lax.fori_loop(0, place.count, one, 0)
        swap.start()
        halves.start()

    reduce_phase(place, sender, partial, scratch[:REDUCE], between, late=swap.pass_on)
    total = scratch[4]

    def body(at):
        total[at] += grad_hidden[at]

    by_rows(total.shape[0], body)
    finish = pair_phase(place, sender, total, result, scratch[REDUCE : REDUCE + 1])
    finish()
    halves.finish()
    swap.finish()
    sender.drain()


def sum_kernel(value, moved, result, arrived, core_in, y_in, held, line_in, sem, side_sem):
    place = Place()
    z, y, core = place.z, place.y, place.core
    barrier = pltpu.get_barrier_semaphore()
    others = [place.at(z, y, 1 - core), place.at(z, 1 - y, core)]
    others += [place.at(lax.rem(z + k, LINE), y, core) for k in range(1, LINE)]
    for device in others + [place.across()]:
        signal(barrier, device)
    pl.semaphore_wait(barrier, len(others) + 1)
    source = moved
    if moved.shape != arrived.shape:
        source = moved.at[:, pl.ds(0, arrived.shape[1])]
    side = remote(source, arrived, side_sem.at[0], side_sem.at[1], place.across())
    side.start()
    first = remote(value, core_in, sem.at[0, 0], sem.at[1, 0], others[0])
    first.start()
    first.wait_recv()
    held[0] = value[...] + core_in[...]
    second = remote(held.at[0], y_in, sem.at[0, 1], sem.at[1, 1], others[1])
    second.start()
    second.wait_recv()
    held[1] = held[0] + y_in[...]
    sends = [
        remote(held.at[1], line_in.at[k - 1], sem.at[0, 1 + k], sem.at[1, 1 + k], others[1 + k])
        for k in range(1, LINE)
    ]
    for send in sends:
        send.start()
    line_in[LINE - 1] = held[1]
    for send in sends:
        send.wait_recv()
    added = jnp.zeros_like(value)
    for source in range(LINE):
        slot = lax.rem(z - source + 2 * LINE - 1, LINE)
        added = added + line_in[slot]
    result[...] = added
    first.wait_send()
    second.wait_send()
    for send in sends:
        send.wait_send()
    side.wait()


def widen_own_kernel(side, own, gate_out, up_out):
    columns = gate_out.shape[1]
    value = jnp.sum(own[:, 0].astype(F32), axis=0)
    gate_out[...] = value[:, :columns]
    up_out[...] = value[:, columns:]


def widen_other_kernel(side, gate, up, other, rest, down, gate_out, up_out, down_out):
    columns = gate_out.shape[1]
    first = other.shape[2]
    for part, start in ((other, 0), (rest, first)):
        value = jnp.sum(part[:, 0].astype(F32), axis=0)
        rows = pl.ds(start, part.shape[2])
        gate_out[rows] = value[:, :columns]
        up_out[rows] = value[:, columns:]
    down_out[...] = jnp.sum(down[:, 0].astype(F32), axis=0)


def talk(kernel, which, shapes, specs, scratch, microseconds, name=None):
    def call(*operands):
        return pl.pallas_call(
            kernel,
            out_shape=shapes,
            in_specs=specs[0],
            out_specs=specs[1],
            scratch_shapes=scratch,
            compiler_params=pltpu.CompilerParams(
                collective_id=which, has_side_effects=True, vmem_limit_bytes=48 << 20
            ),
            cost_estimate=pl.CostEstimate(
                flops=0, bytes_accessed=int(microseconds * 3.0e6), transcendentals=0
            ),
            name=name or kernel.__name__,
        )(*operands)

    return call


class Team:
    def __init__(self, local_heads, rows, width):
        self.fsdp = lax.axis_size("fsdp")
        self.tensor = lax.axis_size("tensor")
        self.size = 2 * LINE
        self.teams = self.fsdp // self.size
        assert self.fsdp % self.size == 0 and self.tensor == 2 and local_heads % self.size == 0
        self.member = lax.rem(lax.axis_index("fsdp"), self.size)
        self.core = lax.axis_index("tensor")
        self.context = lax.axis_index("context")
        self.groups = None
        if self.teams > 1:
            self.groups = [
                [team * self.size + one for one in range(self.size)] for team in range(self.teams)
            ]
        self.rows = rows
        self.width = width
        self.all_low = jax.ShapeDtypeStruct((2 * self.size * rows, width), BF)
        self.own_wide = jax.ShapeDtypeStruct((rows, width), F32)
        self.line_wide = jax.ShapeDtypeStruct((1, width), F32)
        self.reduces = reduce_scratch(rows, width)
        self.gathers = gather_scratch(rows, width)

    def whole(self, pieces):
        shape = (pieces.shape[0], 2) + pieces.shape[1:]
        return jax.ShapeDtypeStruct(shape, pieces.dtype)

    def first(self, own, weights, out, small, gate, up, down):
        rows, columns = weights[0].shape
        rows, columns = rows // 2, columns // self.size
        out_rows = out.shape[0] // self.size // 2
        wide = gate.shape[1]
        low = (self.size, down.shape[0] // self.size // 2, down.shape[1])
        *results, pair, low = talk(
            first_kernel,
            0,
            (
                self.all_low,
                jax.ShapeDtypeStruct((self.fsdp, 2, rows, 3 * columns), BF),
                jax.ShapeDtypeStruct((self.fsdp, 2, out_rows, out.shape[1]), BF),
                jax.ShapeDtypeStruct((self.fsdp, 2) + small.shape, F32),
                jax.ShapeDtypeStruct((self.size, rows, 2 * wide // self.size), BF),
                jax.ShapeDtypeStruct(low, BF),
            ),
            ([VMEM] * 6 + [HBM] * 3, (HBM,) * 6),
            self.gathers
            + swap_scratch(self.fsdp, 5)
            + [
                pltpu.VMEM((rows, wide), BF),
                pltpu.VMEM((rows, wide), BF),
                pltpu.VMEM(low, BF),
                DMA((2 + self.size,)),
                DMA((3, self.size)),
            ],
            80,
        )(own, *weights, out, small, gate, up, down)
        return *results, self.repeat(pair), self.repeat(low)

    def hidden(self, partial, tokens, gain, pair, down):
        return talk(
            hidden_kernel,
            1,
            (self.all_low, self.own_wide, self.own_wide, self.whole(pair), self.whole(down)),
            ([HBM, VMEM, VMEM, VMEM, VMEM], (HBM, VMEM, VMEM, HBM, HBM)),
            self.reduces + self.gathers + halves_scratch(2),
            100,
        )(partial, tokens, gain, pair, down)

    def turn(self, partial, hidden, cotangent, gain):
        pair = jax.ShapeDtypeStruct((2 * self.rows, self.width), BF)
        return talk(
            turn_kernel,
            2,
            (self.all_low, pair, self.line_wide),
            ([HBM, VMEM, VMEM, VMEM], (HBM, HBM, VMEM)),
            self.reduces + self.gathers + [pltpu.VMEM((self.rows, self.width), BF)] + pair_scratch(),
            100,
        )(partial, hidden, cotangent, gain)

    def branch(self, partial, branch, cotangent, gain, inner, grad_mlp, hidden, grad_pair):
        team_rows, units = inner.shape
        columns = grad_pair.shape[1]
        piece = self.width // PIECES
        count = self.fsdp // PIECES
        half = self.width // self.fsdp // 2
        pair_shape = (PIECES, count, half, columns)
        down_shape = (PIECES, units // 2, piece)

        def both(shape):
            return pltpu.VMEM((shape[0], 2) + shape[1:], BF)

        def sides_inside(shape):
            return pltpu.VMEM((shape[0], shape[1], 2) + shape[2:], BF)

        gathered, grad_hidden, gain_grad, pair_mine, down_mine = talk(
            branch_kernel,
            3,
            (
                self.all_low,
                self.own_wide,
                self.line_wide,
                jax.ShapeDtypeStruct(pair_shape, BF),
                jax.ShapeDtypeStruct(down_shape, BF),
            ),
            (
                [HBM, VMEM, VMEM, VMEM, VMEM, HBM, HBM, VMEM],
                (HBM, VMEM, VMEM, VMEM, VMEM),
            ),
            self.reduces
            + self.gathers
            + [
                pltpu.VMEM((2, 2, team_rows, piece), BF),
                pltpu.VMEM((piece, team_rows), BF),
                pltpu.VMEM((units, team_rows), BF),
                sides_inside(pair_shape),
                both(down_shape),
                pltpu.VMEM(pair_shape, BF),
                pltpu.VMEM(down_shape, BF),
                DMA((2, 2)),
                DMA((2, 2, PIECES)),
            ],
            100,
        )(partial, branch, cotangent, gain, inner, grad_mlp, hidden, grad_pair)
        down_mine = down_mine.reshape(PIECES, units // 2, count, piece // count)
        return (
            gathered,
            grad_hidden,
            gain_grad,
            pair_mine.reshape(self.fsdp, half, columns),
            down_mine.transpose(0, 2, 1, 3).reshape(self.fsdp, units // 2, piece // count),
        )

    def last(self, partial, grad_hidden, qkv, out, small, down):
        both = jax.ShapeDtypeStruct((2 * self.rows, self.width), F32)

        def same(array):
            return jax.ShapeDtypeStruct(array.shape, array.dtype)

        def half(array):
            return pltpu.VMEM((array.shape[0],) + array.shape[2:], array.dtype)

        held = pltpu.VMEM(small.shape, small.dtype)
        return talk(
            last_kernel,
            4,
            (both, same(qkv), same(out), self.whole(small), self.whole(down)),
            ([HBM, VMEM, HBM, HBM, VMEM, VMEM], (HBM,) * 5),
            self.reduces
            + pair_scratch()
            + swap_scratch(self.fsdp, 3)
            + halves_scratch(1)
            + [half(qkv), half(qkv), half(out), half(out), held, held, DMA((2,)), DMA((2, 3))],
            80,
        )(partial, grad_hidden, qkv, out, small, down)

    def total(self, values, moved, arrives):
        flat = values.reshape(-1, 128)
        shape = jax.ShapeDtypeStruct(flat.shape, F32)
        scratch = [pltpu.VMEM(flat.shape, F32)] * 2
        scratch += [pltpu.VMEM((2,) + flat.shape, F32), pltpu.VMEM((LINE,) + flat.shape, F32)]
        scratch += [DMA((2, LINE + 1)), DMA((2,))]
        which = 5 + self.sums
        self.sums += 1
        shapes = (shape, jax.ShapeDtypeStruct(arrives, moved.dtype))
        spaces = ([VMEM, HBM], (VMEM, HBM))
        call = talk(sum_kernel, which, shapes, spaces, scratch, 10, "sum_kernel")
        total, came = call(flat, moved)
        return total.reshape(values.shape), came

    sums = 0

    def half(self, array, axis):
        count = array.shape[axis] // 2
        return lax.dynamic_slice_in_dim(array, self.context * count, count, axis)

    def swap(self, pieces):
        return lax.all_to_all(pieces, "fsdp", split_axis=0, concat_axis=0, tiled=True)

    def repeat(self, pieces):
        return jnp.concatenate([pieces] * self.teams, axis=0) if self.teams > 1 else pieces

    def pieces(self, array):
        shape = (-1,) + array.shape[-2:] if array.ndim == 3 else (-1, 2 * array.shape[2], array.shape[3])
        array = array.reshape(shape)
        cut = array.reshape((self.teams, self.size) + array.shape[1:])
        spec = pl.BlockSpec((self.teams, 1) + array.shape[1:], lambda d, side: (0, d, 0, 0))
        return cut, spec

    def widen_own(self, own):
        half, columns = own.shape[1], own.shape[2] // 2
        cut, spec = self.pieces(own)
        wide = pl.BlockSpec((half, columns), lambda d, side: (side[0], d))
        return pl.pallas_call(
            widen_own_kernel,
            grid_spec=pltpu.PrefetchScalarGridSpec(
                num_scalar_prefetch=1, grid=(self.size,), in_specs=[spec], out_specs=[wide] * 2
            ),
            out_shape=[jax.ShapeDtypeStruct((2 * half, self.size * columns), F32)] * 2,
            name="widen_own_kernel",
        )(self.context.reshape(1).astype(jnp.int32), cut)

    def widen_other(self, gate, up, other, rest, down):
        half, columns = other.shape[1] + rest.shape[1], other.shape[2] // 2
        cuts, specs = zip(*[self.pieces(one) for one in (other, rest, down)])
        rows, down_columns = cuts[2].shape[2:]
        wide = pl.BlockSpec((half, columns), lambda d, side: (1 - side[0], d))
        return pl.pallas_call(
            widen_other_kernel,
            grid_spec=pltpu.PrefetchScalarGridSpec(
                num_scalar_prefetch=1,
                grid=(self.size,),
                in_specs=[HBM, HBM] + list(specs),
                out_specs=[wide, wide, pl.BlockSpec((rows, down_columns), lambda d, side: (d, 0))],
            ),
            out_shape=[
                jax.ShapeDtypeStruct(gate.shape, F32),
                jax.ShapeDtypeStruct(up.shape, F32),
                jax.ShapeDtypeStruct((self.size * rows, down_columns), F32),
            ],
            input_output_aliases={1: 0, 2: 1},
            name="widen_other_kernel",
        )(self.context.reshape(1).astype(jnp.int32), gate, up, *cuts)

    def columns_whole(self, came):
        return came.reshape(-1, came.shape[-1])

    def rows_whole(self, came):
        fsdp, two, rows, columns = came.shape
        return came.transpose(1, 2, 0, 3).reshape(two * rows, fsdp * columns)

    def of_columns(self, grad):
        rows, columns = grad.shape
        return grad.astype(BF).reshape(self.fsdp, 2, rows // self.fsdp // 2, columns)

    def of_rows(self, grad):
        rows, columns = grad.shape
        cut = grad.astype(BF).reshape(2, rows // 2, self.fsdp, columns // self.fsdp)
        return cut.transpose(2, 0, 1, 3)

    def added(self, came):
        if self.teams == 1:
            return came.astype(F32)
        came = came.reshape((self.teams, self.size) + came.shape[1:])
        return jnp.sum(came.astype(F32), axis=0)

    def columns_out(self, came, count):
        size, two, rows, columns = came.shape
        return [
            self.added(part.reshape(size, two * rows, -1))
            .transpose(1, 0, 2)
            .reshape(two * rows, -1)
            for part in jnp.split(came, count, axis=3)
        ]

    def rows_out(self, came):
        return self.added(came).reshape(-1, came.shape[-1])


def local(
    tokens,
    cont_lengths,
    w_query,
    w_key,
    w_value,
    w_output,
    query_gain,
    key_gain,
    attn_gain,
    w_gate,
    w_up,
    w_down,
    mlp_gain,
    cotangent,
):
    rows = tokens.shape[0]
    width = tokens.shape[1]
    fsdp = lax.axis_size("fsdp")
    tensor = lax.axis_size("tensor")
    local_heads = query_gain.shape[0]
    head_size = w_query.shape[1] // local_heads
    own_rows = rows // tensor
    team = Team(local_heads, own_rows, width)
    groups = team.size
    team_rows = groups * rows
    heads = local_heads // team.size
    later = lax.axis_index("context") == 1

    tokens_own = lax.dynamic_slice_in_dim(tokens, team.core * own_rows, own_rows, 0)
    grad_out = lax.dynamic_slice_in_dim(cotangent, team.core * own_rows, own_rows, 0)
    cut = query_gain.size
    share = attn_gain.size
    small = [query_gain.reshape(-1), key_gain.reshape(-1), attn_gain, mlp_gain]
    small = jnp.concatenate([one.astype(F32) for one in small + [cont_lengths.reshape(-1)]])
    small = jnp.pad(small, (0, 8 * 128 - small.size)).reshape(8, 128)
    tokens_all, qkv_came, output_came, small_came, pair_mine, down_mine = team.first(
        tokens_own, [w_query, w_key, w_value], w_output, small, w_gate, w_up, w_down
    )
    qkv_w = team.columns_whole(qkv_came)
    output_w = team.rows_whole(output_came)
    all_small = small_came[:, 0].reshape(fsdp, -1)
    query_gains = all_small[:, :cut].reshape(fsdp, local_heads, -1)
    key_gains = all_small[:, cut : 2 * cut].reshape(fsdp, local_heads, -1)
    query_gains = query_gains.transpose(1, 0, 2).reshape(local_heads, head_size)
    key_gains = key_gains.transpose(1, 0, 2).reshape(local_heads, head_size)
    flat_query = lax.dynamic_slice_in_dim(query_gains, team.member * heads, heads, 0).reshape(-1)
    flat_key = lax.dynamic_slice_in_dim(key_gains, team.member * heads, heads, 0).reshape(-1)
    gain_attn = all_small[:, 2 * cut : 2 * cut + share].reshape(1, -1)
    gain_mlp = all_small[:, 2 * cut + share : 2 * cut + 2 * share].reshape(1, -1)

    conts = cont_lengths.shape[1]
    lengths = all_small[:, 2 * cut + 2 * share : 2 * cut + 2 * share + conts].astype(jnp.int32)
    first_group = lax.axis_index("fsdp") - team.member
    lengths = lax.dynamic_slice_in_dim(lengths, first_group, groups, 0)
    segment, offset = jax.vmap(lambda one: layout(one, rows))(lengths)
    row_index = jnp.arange(rows, dtype=jnp.int32)
    positions = jnp.where(later, rows + offset, row_index[None, :])
    own_segment = jnp.where(later, segment, -1)
    cosine, sine = rotary_tables(positions, head_size)
    cosine = cosine[:, :, None, :]
    sine = sine[:, :, None, :]

    pair_came = team.swap(pair_mine)
    down_came = team.swap(down_mine)

    by_head = (groups, rows, heads, head_size)
    raw = product(tokens_all, qkv_w)
    query_raw, key_raw, value_raw = jnp.split(raw, 3, axis=1)
    value_low = value_raw.astype(BF)
    sums, sent_value = team.total(
        jnp.stack([jnp.sum(query_raw * query_raw, axis=1), jnp.sum(key_raw * key_raw, axis=1)]),
        value_low,
        value_low.shape,
    )
    value_low, sent_value = value_low.reshape(by_head), sent_value.reshape(by_head)
    scale_query = lax.rsqrt(sums[0] / width + EPS)[:, None]
    scale_key = lax.rsqrt(sums[1] / width + EPS)[:, None]
    query_norm = query_raw * scale_query * flat_query
    key_norm = key_raw * scale_key * flat_key
    query_low = rotate(query_norm.reshape(by_head), cosine, sine).astype(BF)
    key_low = rotate(key_norm.reshape(by_head), cosine, sine).astype(BF)
    sent_key = lax.ppermute(key_low, "context", [(0, 1)])
    keys_all = jnp.concatenate([sent_key, key_low], axis=1)
    values_all = jnp.concatenate([sent_value, value_low], axis=1)
    key_index = jnp.arange(2 * rows, dtype=jnp.int32)
    key_segment = jnp.concatenate([jnp.full((groups, rows), -2, jnp.int32), own_segment], axis=1)
    remote = (key_index < rows)[None, None, :] & later
    own_keys = (
        (key_index >= rows)[None, None, :]
        & (key_index[None, None, :] - rows <= row_index[None, :, None])
        & (key_segment[:, None, :] == own_segment[:, :, None])
    )
    allowed = (remote | own_keys)[:, None]
    scale = 1.0 / math.sqrt(head_size)
    scores = (
        jnp.einsum("gqhd,gkhd->ghqk", query_low, keys_all, preferred_element_type=F32) * scale
    )
    scores = jnp.where(allowed, scores, -1e30)
    highest = jnp.max(scores, axis=-1, keepdims=True)
    weights = jnp.exp(scores - highest)
    probs = weights / jnp.sum(weights, axis=-1, keepdims=True)
    probs_low = probs.astype(BF)
    mixed = jnp.einsum("ghqk,gkhd->gqhd", probs_low, values_all, preferred_element_type=F32)
    attended_low = mixed.reshape(team_rows, heads * head_size).astype(BF)
    hidden_all, attn_sum, hidden, pair_came, down_came = team.hidden(
        product(attended_low, output_w).astype(BF), tokens_own, gain_attn, pair_came, down_came
    )
    pair_w = team.columns_whole(pair_came)
    down_w = team.rows_whole(down_came)

    gate, upward = jnp.split(product(hidden_all, pair_w), 2, axis=1)
    sigma = jax.nn.sigmoid(gate)
    inner_low = (gate * sigma * upward).astype(BF)
    grad_mlp_all, outputs, grad_mlp_gain = team.turn(
        product(inner_low, down_w).astype(BF), hidden, grad_out, gain_mlp
    )
    grad_inner = product_right(grad_mlp_all, down_w)
    grad_gate_low = (grad_inner * upward * sigma * (1.0 + gate * (1.0 - sigma))).astype(BF)
    grad_up_low = (grad_inner * gate * sigma).astype(BF)
    grad_pair = jnp.concatenate([grad_gate_low, grad_up_low], axis=1)
    grad_branch_all, grad_hidden, grad_attn_gain, pair_mine, down_mine = team.branch(
        product_right(grad_pair, pair_w).astype(BF),
        attn_sum,
        grad_out,
        gain_attn,
        inner_low,
        grad_mlp_all,
        hidden_all,
        grad_pair,
    )
    pair_came = team.swap(pair_mine)
    grad_attended = product_right(grad_branch_all, output_w).astype(BF).reshape(by_head)

    grad_probs = jnp.einsum("gqhd,gkhd->ghqk", grad_attended, values_all, preferred_element_type=F32)
    centre = jnp.sum(probs * grad_probs, axis=-1, keepdims=True)
    grad_scores = (probs * (grad_probs - centre)).astype(BF)
    grad_query_rot = (
        jnp.einsum("ghqk,gkhd->gqhd", grad_scores, keys_all, preferred_element_type=F32) * scale
    )
    grad_keys = (
        jnp.einsum("ghqk,gqhd->gkhd", grad_scores, query_low, preferred_element_type=F32) * scale
    )
    grad_values = jnp.einsum("ghqk,gqhd->gkhd", probs_low, grad_attended, preferred_element_type=F32)
    back_value = lax.ppermute(grad_values[:, :rows].astype(BF), "context", [(1, 0)])
    back_key = lax.ppermute(grad_keys[:, :rows].astype(BF), "context", [(1, 0)])
    grad_key_rot = grad_keys[:, rows:] + back_key.astype(F32)
    grad_value_low = (
        (grad_values[:, rows:] + back_value.astype(F32)).reshape(team_rows, -1).astype(BF)
    )
    grad_query_norm = rotate_back(grad_query_rot, cosine, sine).reshape(team_rows, -1)
    grad_key_norm = rotate_back(grad_key_rot, cosine, sine).reshape(team_rows, -1)
    grad_query_gain = jnp.sum(grad_query_norm * query_raw * scale_query, axis=0)
    grad_key_gain = jnp.sum(grad_key_norm * key_raw * scale_key, axis=0)
    inner_sums = jnp.stack(
        [
            jnp.sum(query_raw * flat_query * grad_query_norm, axis=1),
            jnp.sum(key_raw * flat_key * grad_key_norm, axis=1),
        ]
    )
    inner_sums, pair_came = lax.optimization_barrier((inner_sums, pair_came))
    first = pair_came.shape[1] // 4
    pair_rest = lax.ppermute(pair_came[:, first:], "context", [(0, 1), (1, 0)])
    arrives = (pair_came.shape[0], first, pair_came.shape[2])
    totals, pair_other = team.total(inner_sums, pair_came, arrives)
    late_attended, late_grad, totals = lax.optimization_barrier(
        (attended_low, grad_branch_all, totals)
    )
    output_grad = team.of_rows(product_left(late_attended, late_grad))
    down_mine, totals = lax.optimization_barrier((down_mine, totals))
    down_came = team.swap(down_mine)
    grad_query_low = norm_back(
        query_raw, scale_query, flat_query, grad_query_norm, totals[0][:, None], width
    ).astype(BF)
    grad_key_low = norm_back(
        key_raw, scale_key, flat_key, grad_key_norm, totals[1][:, None], width
    ).astype(BF)
    grad_qkv = jnp.concatenate([grad_query_low, grad_key_low, grad_value_low], axis=1)
    qkv_grad = team.of_columns(product_left(tokens_all, grad_qkv))
    head_share = head_size // fsdp
    small = [
        grad_attn_gain.reshape(fsdp, share),
        grad_mlp_gain.reshape(fsdp, share),
        grad_query_gain.reshape(heads, fsdp, head_share).transpose(1, 0, 2).reshape(fsdp, -1),
        grad_key_gain.reshape(heads, fsdp, head_share).transpose(1, 0, 2).reshape(fsdp, -1),
    ]
    used = 2 * share + 2 * heads * head_share
    small = jnp.concatenate(small + [jnp.zeros((fsdp, 8 * 128 - used), F32)], axis=1)
    gate_own, up_own = team.widen_own(pair_came)
    partial, pair_rest, gate_own, up_own = lax.optimization_barrier(
        (product_right(grad_qkv, qkv_w).astype(BF), pair_rest, gate_own, up_own)
    )
    input_grad, qkv_came, output_came, small_came, down_came = team.last(
        partial,
        grad_hidden,
        qkv_grad,
        output_grad,
        small.reshape(fsdp, 8, 128),
        down_came,
    )
    grad_w_query, grad_w_key, grad_w_value = team.columns_out(qkv_came, 3)
    grad_w_gate, grad_w_up, grad_w_down = team.widen_other(
        gate_own, up_own, pair_other, pair_rest, down_came
    )
    grad_w_output = team.rows_out(output_came)
    came = jnp.sum(small_came, axis=1).reshape(fsdp, -1)
    row_gains = jnp.sum(came[:, : 2 * share], axis=0).reshape(2, share)
    head_gains = team.added(came[:, 2 * share : used]).reshape(team.size, 2, heads, head_share)
    head_gains = head_gains.transpose(1, 0, 2, 3).reshape(2, local_heads, head_share)
    return (
        outputs,
        input_grad,
        grad_w_query,
        grad_w_key,
        grad_w_value,
        grad_w_output,
        head_gains[0],
        head_gains[1],
        row_gains[0],
        grad_w_gate,
        grad_w_up,
        grad_w_down,
        row_gains[1],
    )


def solution(mesh):
    return jax.shard_map(
        local,
        mesh=mesh,
        in_specs=(
            P(("fsdp", "context"), None),
            P("fsdp", None),
            P("fsdp", "tensor"),
            P("fsdp", "tensor"),
            P("fsdp", "tensor"),
            P("tensor", "fsdp"),
            P("tensor", "fsdp"),
            P("tensor", "fsdp"),
            P("fsdp"),
            P("fsdp", "tensor"),
            P("fsdp", "tensor"),
            P("tensor", "fsdp"),
            P("fsdp"),
            P(("fsdp", "context"), None),
        ),
        out_specs=(
            P(("fsdp", "context"), None),
            P(("fsdp", "context"), None),
            P("fsdp", "tensor"),
            P("fsdp", "tensor"),
            P("fsdp", "tensor"),
            P("tensor", "fsdp"),
            P("tensor", "fsdp"),
            P("tensor", "fsdp"),
            P("fsdp"),
            P("fsdp", "tensor"),
            P("fsdp", "tensor"),
            P("tensor", "fsdp"),
            P("fsdp"),
        ),
        check_vma=False,
    )
```
